32 devices in a mesh: dp: 2 (over x), tp: 4 (over z), pp: 4 (over y, core).
Axes of the slice: x: 2, y: 2, z: 4, core: 2. Of those that a mesh axis runs over, the one named last changes fastest.
Arguments:
- hidden_in: bfloat16 [16, 512, 2048], P('dp', 'tp'), parts along dimension 0
- seg_ids: int32 [16, 512], P('dp'), parts along dimension 0
- positions: int32 [16, 512], P('dp'), parts along dimension 0
- attn_norm: bfloat16 [4, 2048], P('pp')
- w_query: bfloat16 [4, 2048, 2048], P('pp', None, 'tp')
- w_key: bfloat16 [4, 2048, 2048], P('pp', None, 'tp')
- w_value: bfloat16 [4, 2048, 2048], P('pp', None, 'tp')
- w_out: bfloat16 [4, 2048, 2048], P('pp', 'tp')
- mlp_norm: bfloat16 [4, 2048], P('pp')
- w_gate: bfloat16 [4, 2048, 8192], P('pp', None, 'tp')
- w_up: bfloat16 [4, 2048, 8192], P('pp', None, 'tp')
- w_down: bfloat16 [4, 8192, 2048], P('pp', 'tp')
Outputs:
- output: bfloat16 [16, 512, 2048], P('dp', 'tp'), parts along dimension 0
There are 2 independent parts. The reference program is written for one: setup_inputs(seed, part) draws one part's arguments, and reference() takes and returns one part's arrays. A program takes and returns all parts, laid end to end along the dimension named above; an argument that names none is the same for every part.
All inputs are finite; a program needn't handle non-finite values.
Results may differ from the reference program's by a relative error of at most 0.02.
Values are sent between devices in bfloat16 or wider.
A program may use at most 1 GiB of HBM per device.

```python
import jax
import jax.numpy as jnp
import numpy as np
from jax import lax

MICRO_BATCHES = 8
SEQ_LEN = 512
MODEL_DIM = 2048
Q_HEADS = 16
KV_HEADS = 16
HEAD_DIM = 128
FFN_DIM = 8192
STAGES = 4
SEG_CUTS = 3

NORM_EPS = 1e-5
ROPE_THETA = 500000.0
ROPE_FACTOR = 8.0
LOW_FREQ = 1.0
HIGH_FREQ = 4.0
ORIG_CTX = 8192.0
QUERY_BLOCK = min(SEQ_LEN, 256)


def rope_freqs():
    base_freq = 1.0 / (ROPE_THETA ** (np.arange(0, HEAD_DIM, 2) / HEAD_DIM))
    wavelen = 2.0 * np.pi / base_freq
    smooth = (ORIG_CTX / wavelen - LOW_FREQ) / (HIGH_FREQ - LOW_FREQ)
    blended = (1.0 - smooth) * base_freq / ROPE_FACTOR + smooth * base_freq
    scaled = np.where(wavelen > ORIG_CTX / LOW_FREQ, base_freq / ROPE_FACTOR, blended)
    return np.where(wavelen < ORIG_CTX / HIGH_FREQ, base_freq, scaled)


def rms_norm(hidden, gain):
    hidden_f = hidden.astype(jnp.float32)
    inv_rms = lax.rsqrt(jnp.mean(hidden_f * hidden_f, axis=-1, keepdims=True) + NORM_EPS)
    return (hidden_f * inv_rms * gain.astype(jnp.float32)).astype(jnp.bfloat16)


def apply_rope(proj, cos_tab, sin_tab):
    half_dim = proj.shape[-1] // 2
    lead_part = proj[..., :half_dim]
    tail_part = proj[..., half_dim:]
    cos_wide = cos_tab[..., None, :]
    sin_wide = sin_tab[..., None, :]
    return jnp.concatenate([lead_part * cos_wide - tail_part * sin_wide, tail_part * cos_wide + lead_part * sin_wide], axis=-1)


def attention(q_rot, k_rot, v_proj, seg_row):
    groups = Q_HEADS // KV_HEADS
    n_blocks = SEQ_LEN // QUERY_BLOCK
    q_blocks = q_rot.reshape(n_blocks, QUERY_BLOCK, KV_HEADS, groups, HEAD_DIM)
    seg_blocks = seg_row.reshape(n_blocks, QUERY_BLOCK)
    col_ids = jnp.arange(SEQ_LEN)
    row_blocks = col_ids.reshape(n_blocks, QUERY_BLOCK)
    key_f = k_rot.astype(jnp.float32)
    value_f = v_proj.astype(jnp.float32)

    def one_block(blk_args):
        q_blk, seg_blk, row_blk = blk_args
        scores = jnp.einsum('qngd,knd->ngqk', q_blk.astype(jnp.float32), key_f) * HEAD_DIM ** -0.5
        allowed = (seg_blk[:, None] == seg_row[None, :]) & (row_blk[:, None] >= col_ids[None, :])
        scores = jnp.where(allowed, scores, -1e30)
        attn_probs = jax.nn.softmax(scores, axis=-1).astype(jnp.bfloat16).astype(jnp.float32)
        context = jnp.einsum('ngqk,knd->qngd', attn_probs, value_f)
        return context.astype(jnp.bfloat16).reshape(QUERY_BLOCK, Q_HEADS * HEAD_DIM)

    return lax.map(one_block, (q_blocks, seg_blocks, row_blocks)).reshape(SEQ_LEN, Q_HEADS * HEAD_DIM)


def layer(hidden, weights, cos_tab, sin_tab, seg_row):
    gain_attn, w_query, w_key, w_value, w_out, gain_mlp, w_gate, w_up, w_down = weights
    normed = rms_norm(hidden, gain_attn)
    q_proj = jnp.dot(normed, w_query, preferred_element_type=jnp.float32).reshape(SEQ_LEN, Q_HEADS, HEAD_DIM)
    k_proj = jnp.dot(normed, w_key, preferred_element_type=jnp.float32).reshape(SEQ_LEN, KV_HEADS, HEAD_DIM)
    v_proj = jnp.dot(normed, w_value, preferred_element_type=jnp.float32).astype(jnp.bfloat16).reshape(SEQ_LEN, KV_HEADS, HEAD_DIM)
    q_rot = apply_rope(q_proj, cos_tab, sin_tab).astype(jnp.bfloat16)
    k_rot = apply_rope(k_proj, cos_tab, sin_tab).astype(jnp.bfloat16)
    context = attention(q_rot, k_rot, v_proj, seg_row)
    attn_out = jnp.dot(context, w_out, preferred_element_type=jnp.float32).astype(jnp.bfloat16)
    mid_state = (hidden.astype(jnp.float32) + attn_out.astype(jnp.float32)).astype(jnp.bfloat16)
    normed_mlp = rms_norm(mid_state, gain_mlp)
    gate_proj = jnp.dot(normed_mlp, w_gate, preferred_element_type=jnp.float32)
    up_proj = jnp.dot(normed_mlp, w_up, preferred_element_type=jnp.float32)
    hidden_act = (jax.nn.silu(gate_proj) * up_proj).astype(jnp.bfloat16)
    down_out = jnp.dot(hidden_act, w_down, preferred_element_type=jnp.float32).astype(jnp.bfloat16)
    return (mid_state.astype(jnp.float32) + down_out.astype(jnp.float32)).astype(jnp.bfloat16)


def draw_layout(layout_key):
    cut_key, step_key = jax.random.split(layout_key)
    cuts = jax.random.randint(cut_key, (MICRO_BATCHES, SEG_CUTS), 1, SEQ_LEN)
    token_idx = jnp.arange(SEQ_LEN)
    seg_ids = jnp.sum(token_idx[None, :, None] >= cuts[:, None, :], axis=-1).astype(jnp.int32)
    step_sizes = jax.random.randint(step_key, (MICRO_BATCHES, SEQ_LEN), 1, 4)
    run_after = jnp.cumsum(step_sizes, axis=1)
    run_before = run_after - step_sizes
    starts = jnp.concatenate([jnp.ones((MICRO_BATCHES, 1), dtype=jnp.bool_), seg_ids[:, 1:] != seg_ids[:, :-1]], axis=1)
    start_idx = lax.cummax(jnp.where(starts, token_idx[None, :], 0), axis=1)
    positions = (run_before - jnp.take_along_axis(run_before, start_idx, axis=1)).astype(jnp.int32)
    return seg_ids, positions


def normal_draw(draw_key, shape, fan_in):
    return (jax.random.normal(draw_key, shape, jnp.float32) * fan_in ** -0.5).astype(jnp.bfloat16)


def gain_draw(draw_key):
    return jax.random.uniform(draw_key, (STAGES, MODEL_DIM), jnp.float32, 0.5, 1.5).astype(jnp.bfloat16)


def setup_inputs(seed: int = 0, part: int = 0) -> dict:
    base_key = jax.random.key(seed)
    part_key = jax.random.fold_in(base_key, part)
    hidden_key, layout_key = jax.random.split(part_key)
    hidden_in = jax.random.normal(hidden_key, (MICRO_BATCHES, SEQ_LEN, MODEL_DIM), jnp.float32).astype(jnp.bfloat16)
    seg_ids, positions = draw_layout(layout_key)
    w_keys = jax.random.split(base_key, 9)
    q_dim = Q_HEADS * HEAD_DIM
    kv_dim = KV_HEADS * HEAD_DIM
    return dict(
        hidden_in=hidden_in,
        seg_ids=seg_ids,
        positions=positions,
        attn_norm=gain_draw(w_keys[0]),
        w_query=normal_draw(w_keys[1], (STAGES, MODEL_DIM, q_dim), MODEL_DIM),
        w_key=normal_draw(w_keys[2], (STAGES, MODEL_DIM, kv_dim), MODEL_DIM),
        w_value=normal_draw(w_keys[3], (STAGES, MODEL_DIM, kv_dim), MODEL_DIM),
        w_out=normal_draw(w_keys[4], (STAGES, q_dim, MODEL_DIM), q_dim),
        mlp_norm=gain_draw(w_keys[5]),
        w_gate=normal_draw(w_keys[6], (STAGES, MODEL_DIM, FFN_DIM), MODEL_DIM),
        w_up=normal_draw(w_keys[7], (STAGES, MODEL_DIM, FFN_DIM), MODEL_DIM),
        w_down=normal_draw(w_keys[8], (STAGES, FFN_DIM, MODEL_DIM), FFN_DIM),
    )


def reference(hidden_in, seg_ids, positions, attn_norm, w_query, w_key, w_value, w_out, mlp_norm, w_gate, w_up, w_down):
    inv_freq = jnp.asarray(rope_freqs(), dtype=jnp.float32)
    stacked = (attn_norm, w_query, w_key, w_value, w_out, mlp_norm, w_gate, w_up, w_down)

    def one_micro(micro_args):
        hidden, seg_row, pos_row = micro_args
        angles = pos_row.astype(jnp.float32)[:, None] * inv_freq[None, :]
        cos_tab = jnp.cos(angles)
        sin_tab = jnp.sin(angles)

        def layer_step(carry, weights):
            return layer(carry, weights, cos_tab, sin_tab, seg_row), None

        final_state, _ = lax.scan(layer_step, hidden, stacked)
        return final_state

    return lax.map(one_micro, (hidden_in, seg_ids, positions))
```

```python
import functools
import math

import jax
import jax.numpy as jnp
import numpy as np
from jax import lax
from jax.experimental import pallas as pl
from jax.experimental.pallas import tpu as pltpu
from jax.sharding import PartitionSpec as P

HEAD_DIM = 128
NORM_EPS = 1e-5
ROPE_THETA = 500000.0
ROPE_FACTOR = 8.0
LOW_FREQ = 1.0
HIGH_FREQ = 4.0
ORIG_CTX = 8192.0
NEG = -1e30
MESH = pl.DeviceIdType.MESH
F32 = jnp.float32
BF16 = jnp.bfloat16


def rope_freqs():
    base_freq = 1.0 / (ROPE_THETA ** (np.arange(0, HEAD_DIM, 2) / HEAD_DIM))
    wavelen = 2.0 * np.pi / base_freq
    smooth = (ORIG_CTX / wavelen - LOW_FREQ) / (HIGH_FREQ - LOW_FREQ)
    blended = (1.0 - smooth) * base_freq / ROPE_FACTOR + smooth * base_freq
    scaled = np.where(wavelen > ORIG_CTX / LOW_FREQ, base_freq / ROPE_FACTOR, blended)
    return np.where(wavelen < ORIG_CTX / HIGH_FREQ, base_freq, scaled)


def kernel(n_stages, x_ref, seg_ref, cols_ref, invf_ref, ga_ref, gm_ref,
           wq_ref, wk_ref, wv_ref, wo_ref, wg_ref, wu_ref, wd_ref,
           out_ref,
           wqkv_hbm, wo_hbm, hin_hbm,
           wg_s, wu_s, wd_s, wst, wost, gb, px, ps, kc, vc, hv, h1b, pacc, oacc, sendb, h2b, act, acc, abuf, qb, ob,
           table, cols, mask,
           wr, wx, wsnd, wfwd, wxs, hin_sem, xs, ag, s1s, s2s, pxr, pxs, psr, s4s, s5s, outr, outf, ofs,
           wst_sem, wost_sem, mlp_sem, hv_sem, cols_sem, gate):
    n_mb, T, D = x_ref.shape
    QL = wq_ref.shape[2]
    FL = wg_ref.shape[2]
    NB = wg_s.shape[0]
    FB = FL // NB
    S = seg_ref.shape[1]
    NJ = S // T
    NH = QL // HEAD_DIM
    N = (n_mb // 2) * NJ
    DB = D // NB
    scale = HEAD_DIM ** -0.5
    RB = 16

    hx = lax.axis_index("dp")
    z = lax.axis_index("tp")
    s = lax.axis_index("pp")
    is_home = (z == 1) | (z == 2)
    is_outer = (z == 0) | (z == 3)
    hb = lax.rem(z + 1, 2) * 0 + (z - 1)
    peer = 3 - z
    outer = 3 * (z - 1)
    inner = 1 + z // 2
    odd = lax.rem(s, 2)

    def rcopy(src, dst, ssem, rsem, **dev):
        return pltpu.make_async_remote_copy(src_ref=src, dst_ref=dst, send_sem=ssem, recv_sem=rsem,
                                            device_id=dev, device_id_type=MESH)

    def local(src, dst, sem):
        return pltpu.make_async_copy(src, dst, sem)

    wqkv_own = (wq_ref, wk_ref, wv_ref, wo_ref)

    def mlp_copies():
        cps = []
        for n in range(NB):
            cps.append(local(wg_ref.at[0, :, pl.ds(n * FB, FB)], wg_s.at[n], mlp_sem.at[0, n]))
            cps.append(local(wu_ref.at[0, :, pl.ds(n * FB, FB)], wu_s.at[n], mlp_sem.at[1, n]))
            cps.append(local(wd_ref.at[0, :, pl.ds(n * DB, DB)], wd_s.at[n], mlp_sem.at[2, n]))
        return cps

    for c in mlp_copies():
        c.start()

    def x_copy(w, home):
        return rcopy(x_ref.at[2 * w + (home - 1)], hin_hbm.at[w * NJ + z], xs.at[w, home - 1],
                     hin_sem.at[w * NJ + z], tp=home)

    def x_start(w):
        for home in (1, 2):
            @pl.when((s == 0) & (z != home))
            def _():
                x_copy(w, home).start()

    def x_wait(w):
        for home in (1, 2):
            @pl.when((s == 0) & (z != home))
            def _():
                x_copy(w, home).wait_send()

    x_start(0)

    def half(ref, m, h):
        rows = (D if m < 3 else QL) // 2
        return ref.at[pl.ds(h * rows, rows), :]

    def wslot(r, m):
        return wqkv_hbm.at[r, m] if m < 3 else wo_hbm.at[r]

    def own_w(m):
        return wqkv_own[m].at[0]

    def o_send(m):
        return rcopy(own_w(m), wslot(0, m), wsnd.at[m], wr.at[0, m], tp=inner)

    def p_send(m):
        return rcopy(half(own_w(m), m, hx), half(wslot(1, m), m, hx), wsnd.at[m], wr.at[1, m], tp=peer)

    def f_send(m):
        return rcopy(half(wslot(0, m), m, hx), half(wslot(2, m), m, hx), wfwd.at[m], wr.at[2, m], tp=peer)

    def x_send(r, m):
        return rcopy(half(wslot(r, m), m, hx), half(wslot(r, m), m, hx), wxs.at[r - 1, m], wx.at[r - 1, m], dp=1 - hx)

    @pl.when(odd == 1)
    def _():
        pl.semaphore_wait(gate, 1)

    @pl.when(is_outer)
    def _():
        for m in range(4):
            o_send(m).start()
        for m in range(4):
            o_send(m).wait_send()

    @pl.when(is_home)
    def _():
        for m in range(4):
            p_send(m).start()
        cps = [local(cols_ref.at[2 * w + hb], cols.at[w], cols_sem.at[w]) for w in range(n_mb // 2)]
        for c in cps:
            c.start()
        for c in cps:
            c.wait()
        lane = lax.broadcasted_iota(jnp.int32, (RB, HEAD_DIM), 1)

        def zero_rows(b, carry):
            for i in range(4):
                kc[i, pl.ds(b * RB, RB), :] = jnp.zeros((RB, QL), BF16)
                vc[i, pl.ds(b * RB, RB), :] = jnp.zeros((RB, QL), BF16)
            return carry
        lax.fori_loop(0, S // RB, zero_rows, 0)

        for w in range(n_mb // 2):
            def table_rows(b, carry, w=w):
                pos = cols[w, pl.ds(b * RB, RB), 0:1].astype(F32)
                ang = pos * invf_ref[0:1, :]
                table[w, pl.ds(b * RB, RB), :] = jnp.where(lane < HEAD_DIM // 2, jnp.cos(ang), jnp.sin(ang))
                return carry
            lax.fori_loop(0, S // RB, table_rows, 0)

        steps = [("p", 0), ("o", 0), ("p", 1), ("p", 2), ("o", 1), ("p", 3), ("f", 0), ("o", 2), ("f", 1), ("f", 2), ("o", 3), ("f", 3)]
        for kind, m in steps:
            if kind == "o":
                o_send(m).wait_recv()
                f_send(m).start()
            elif kind == "p":
                p_send(m).wait_recv()
                x_send(1, m).start()
            else:
                f_send(m).wait_recv()
                x_send(2, m).start()
        for m in range(4):
            x_send(1, m).wait_recv()
            x_send(2, m).wait_recv()
        for m in range(4):
            p_send(m).wait_send()
            f_send(m).wait_send()
            x_send(1, m).wait_send()
            x_send(2, m).wait_send()

    @pl.when(odd == 0)
    def _():
        pl.semaphore_signal(gate, inc=1, device_id={"pp": s + 1}, device_id_type=MESH)

    def pf_qkv(i, m, start):
        sl = lax.rem(3 * i + m, 4)

        @pl.when(i == 0)
        def _():
            c = local(own_w(m), wst.at[sl], wst_sem.at[sl])
            c.start() if start else c.wait()

        @pl.when(i != 0)
        def _():
            c = local(wqkv_hbm.at[lax.rem(i + 3, 4), m], wst.at[sl], wst_sem.at[sl])
            c.start() if start else c.wait()

    def pf_wo(i, start):
        sl = lax.rem(i, 2)

        @pl.when(i == 0)
        def _():
            c = local(own_w(3), wost.at[sl], wost_sem.at[sl])
            c.start() if start else c.wait()

        @pl.when(i != 0)
        def _():
            c = local(wo_hbm.at[lax.rem(i + 3, 4)], wost.at[sl], wost_sem.at[sl])
            c.start() if start else c.wait()

    @pl.when(is_home)
    def _():
        for m in range(3):
            pf_qkv(0, m, True)
        pf_wo(0, True)

    for c in mlp_copies():
        c.wait()

    def hin_copy(u):
        return rcopy(h2b, hin_hbm.at[u], s5s, hin_sem.at[u], pp=lax.rem(s + 1, n_stages))

    def s1_outer(u):
        blk = gb.at[lax.rem(u, 3), pl.ds(pl.multiple_of(hb * T, T), T), :]
        return rcopy(blk, blk, s1s.at[0], ag.at[hb, lax.rem(u, 3)], tp=outer)

    def s1_peer(u):
        blk = gb.at[lax.rem(u, 3), pl.ds(pl.multiple_of(hb * T, T), T), :]
        return rcopy(blk, blk, s1s.at[1], ag.at[hb, lax.rem(u, 3)], tp=peer)

    def s2_copy(u):
        blk = gb.at[lax.rem(u, 3), pl.ds(pl.multiple_of((1 - hb) * T, T), T), :]
        return rcopy(blk, blk, s2s, ag.at[1 - hb, lax.rem(u, 3)], tp=outer)

    def ag_wait(b, u):
        blk = gb.at[lax.rem(u, 3), pl.ds(pl.multiple_of(b * T, T), T), :]
        local(blk, blk, ag.at[b, lax.rem(u, 3)]).wait()

    def s3_copy(u):
        sl = lax.rem(u, 2)
        return rcopy(px.at[sl], px.at[sl], pxs.at[sl], pxr.at[sl], tp=inner)

    def s4_copy(u):
        return rcopy(sendb, ps.at[lax.rem(u, 2)], s4s, psr.at[lax.rem(u, 2)], tp=peer)

    def out_copy(u, mb, j):
        return rcopy(h2b, out_ref.at[mb], s5s, outr.at[mb], tp=j)

    def norm_rows(src, gain, dst):
        hf = src.astype(F32)
        inv = lax.rsqrt(jnp.mean(hf * hf, axis=-1, keepdims=True) + NORM_EPS)
        return (hf * inv * gain.astype(F32)).astype(BF16)

    def attention(u):
        w = u // NJ
        j = lax.rem(u, NJ)
        mb = 2 * w + hb
        row0 = pl.multiple_of(j * T, T)
        from_x = (s == 0) & (j == z)

        @pl.when(from_x)
        def _():
            c = local(x_ref.at[mb], hv, hv_sem)
            c.start()
            c.wait()

        @pl.when(jnp.logical_not(from_x))
        def _():
            hin_copy(u).wait_recv()
            c = local(hin_hbm.at[u], hv, hv_sem)
            c.start()
            c.wait()

        def norm_a(b, carry):
            rows = pl.ds(b * RB, RB)
            abuf[rows, :] = norm_rows(hv[rows, :], ga_ref[0:1, :], None)
            return carry
        lax.fori_loop(0, T // RB, norm_a, 0)

        def mask_rows(b, carry):
            r = pl.ds(b * RB, RB)
            segc = cols[w, pl.ds(row0 + b * RB, RB), 1:2]
            segr = seg_ref[pl.ds(mb, 1), :]
            ti = lax.broadcasted_iota(jnp.int32, (RB, S), 0) + (row0 + b * RB)
            ui = lax.broadcasted_iota(jnp.int32, (RB, S), 1)
            mask[r, :] = jnp.where((segc == segr) & (ui <= ti), 1.0, 0.0)
            return carry
        lax.fori_loop(0, T // RB, mask_rows, 0)

        def rope(val, dst_rows):
            pk = table[w, pl.ds(row0, T), :]
            lane = lax.broadcasted_iota(jnp.int32, (T, HEAD_DIM), 1)
            swapped = pltpu.roll(pk, HEAD_DIM // 2, 1)
            cosw = jnp.where(lane < HEAD_DIM // 2, pk, swapped)
            sinw = jnp.where(lane < HEAD_DIM // 2, -swapped, pk)
            outs = []
            for h in range(NH):
                v = val[:, h * HEAD_DIM:(h + 1) * HEAD_DIM]
                outs.append((v * cosw + pltpu.roll(v, HEAD_DIM // 2, 1) * sinw).astype(BF16))
            return outs

        def shard(i, carry):
            @pl.when((i < 3))
            def _():
                pf_wo(i + 1, True)

            def piece(m):
                pf_qkv(i, m, False)
                val = jnp.dot(abuf[...], wst[lax.rem(3 * i + m, 4)], preferred_element_type=F32)

                @pl.when(i < 3)
                def _():
                    pf_qkv(i + 1, m, True)

                @pl.when((i == 3) & (u < N - 1))
                def _():
                    pf_qkv(0, m, True)
                return val

            for h, val in enumerate(rope(piece(0), None)):
                qb[:, h * HEAD_DIM:(h + 1) * HEAD_DIM] = val
            for h, val in enumerate(rope(piece(1), None)):
                kc[i, pl.ds(row0, T), h * HEAD_DIM:(h + 1) * HEAD_DIM] = val
            vc[i, pl.ds(row0, T), :] = piece(2).astype(BF16)
            for h in range(NH):
                cs = slice(h * HEAD_DIM, (h + 1) * HEAD_DIM)
                sc = lax.dot_general(qb[:, cs], kc[i, :, cs], (((1,), (1,)), ((), ())), preferred_element_type=F32) * scale
                sc = jnp.where(mask[...] > 0.5, sc, NEG)
                e = jnp.exp(sc - jnp.max(sc, axis=-1, keepdims=True))
                p = (e * (1.0 / jnp.sum(e, axis=-1, keepdims=True))).astype(BF16)
                ob[:, cs] = jnp.dot(p, vc[i, :, cs], preferred_element_type=F32).astype(BF16)
            pf_wo(i, False)
            y = jnp.dot(ob[...], wost[lax.rem(i, 2)], preferred_element_type=F32)

            @pl.when(i == 0)
            def _():
                acc[...] = y

            @pl.when(i != 0)
            def _():
                acc[...] = acc[...] + y
            return carry
        lax.fori_loop(0, 4, shard, 0)

        @pl.when(u < N - 1)
        def _():
            pf_wo(0, True)

        def norm_b(b, carry):
            rows = pl.ds(b * RB, RB)
            h1 = (hv[rows, :].astype(F32) + acc[rows, :].astype(BF16).astype(F32)).astype(BF16)
            h1b[lax.rem(u, 3), rows, :] = h1
            gb[lax.rem(u, 3), pl.ds(pl.multiple_of(hb * T + b * RB, RB), RB), :] = norm_rows(h1, gm_ref[0:1, :], None)
            return carry
        lax.fori_loop(0, T // RB, norm_b, 0)

    def mlp(sl):
        def up(n, carry):
            xin = gb[sl]
            g = jnp.dot(xin, wg_s[n], preferred_element_type=F32)
            u_ = jnp.dot(xin, wu_s[n], preferred_element_type=F32)
            act[:, pl.ds(pl.multiple_of(n * FB, FB), FB)] = (jax.nn.silu(g) * u_).astype(BF16)
            return carry
        lax.fori_loop(0, NB, up, 0)

        def down(n, carry):
            pacc[:, pl.ds(pl.multiple_of(n * DB, DB), DB)] = jnp.dot(act[...], wd_s[n], preferred_element_type=F32)
            return carry
        lax.fori_loop(0, NB, down, 0)

    def body(u, carry):
        slot = lax.rem(u, 3)

        @pl.when(is_home)
        def _():
            @pl.when((s == 0) & (lax.rem(u, NJ) == 0) & (u + NJ < N))
            def _():
                for home in (1, 2):
                    @pl.when(z != home)
                    def _():
                        x_copy(u // NJ + 1, home).start()

            @pl.when(u < N)
            def _():
                attention(u)

            @pl.when((u >= 1) & (u <= N))
            def _():
                s1_outer(u - 1).wait_send()
                s1_peer(u - 1).wait_send()

            @pl.when(u < N)
            def _():
                s1_outer(u).start()
                s1_peer(u).start()

            @pl.when((u >= 2) & (u < N + 2))
            def _():
                v = u - 2
                sl = lax.rem(v, 2)
                s3_copy(v).wait_recv()

                @pl.when(v >= 1)
                def _():
                    s4_copy(v - 1).wait_send()

                def comb(b, carry):
                    rows = pl.ds(b * RB, RB)
                    mine = pl.ds(pl.multiple_of(hb * T + b * RB, RB), RB)
                    theirs = pl.ds(pl.multiple_of((1 - hb) * T + b * RB, RB), RB)
                    oacc[rows, :] = pacc[mine, :] + px[sl, mine, :].astype(F32)
                    sendb[rows, :] = (pacc[theirs, :] + px[sl, theirs, :].astype(F32)).astype(BF16)
                    return carry
                lax.fori_loop(0, T // RB, comb, 0)
                s4_copy(v).start()

        @pl.when(is_outer & (u < N))
        def _():
            @pl.when((s == 0) & (lax.rem(u, NJ) == 0) & (u + NJ < N))
            def _():
                for home in (1, 2):
                    x_copy(u // NJ + 1, home).start()
            ag_wait(0, u)
            ag_wait(1, u)

        @pl.when((is_home & (u >= 1) & (u <= N)) | (is_outer & (u < N)))
        def _():
            mlp(lax.rem(u + 2 * (is_home.astype(jnp.int32)), 3))

        @pl.when(is_outer & (u < N))
        def _():
            sl = lax.rem(u, 2)

            @pl.when(u >= 2)
            def _():
                s3_copy(u - 2).wait_send()

            def conv(b, carry):
                rows = pl.ds(b * RB, RB)
                px[sl, rows, :] = pacc[rows, :].astype(BF16)
                return carry
            lax.fori_loop(0, 2 * T // RB, conv, 0)
            s3_copy(u).start()

        @pl.when(is_home)
        def _():
            @pl.when((u >= 1) & (u <= N))
            def _():
                s2_copy(u - 1).wait_send()

            @pl.when(u < N)
            def _():
                ag_wait(1 - hb, u)
                s2_copy(u).start()

            @pl.when((u >= 2) & (u < N + 2))
            def _():
                v = u - 2
                s4_wait = s4_copy(v)
                s4_wait.wait_recv()
                vw = v // NJ
                vj = lax.rem(v, NJ)

                @pl.when(v >= 1)
                def _():
                    hin_copy(v).wait_send()

                def fin(b, carry):
                    rows = pl.ds(b * RB, RB)
                    d = (oacc[rows, :] + ps[lax.rem(v, 2), rows, :].astype(F32)).astype(BF16)
                    h2b[rows, :] = (h1b[lax.rem(v, 3), rows, :].astype(F32) + d.astype(F32)).astype(BF16)
                    return carry
                lax.fori_loop(0, T // RB, fin, 0)

                @pl.when(s < n_stages - 1)
                def _():
                    hin_copy(v).start()

                @pl.when((s == n_stages - 1) & (vj != z))
                def _():
                    out_copy(v, 2 * vw + hb, vj).start()

                @pl.when((s == n_stages - 1) & (vj == z))
                def _():
                    local(h2b, out_ref.at[2 * vw + hb], s5s).start()

        v = u - 4

        @pl.when((s == n_stages - 1) & (v >= 0) & (v < N))
        def _():
            @pl.when(lax.rem(v, NJ) == z)
            def _():
                for b in (0, 1):
                    mb = 2 * (v // NJ) + b

                    @pl.when(z - 1 != b)
                    def _(mb=mb):
                        local(out_ref.at[mb], out_ref.at[mb], outr.at[mb]).wait()
                    for p in range(n_stages - 1):
                        rcopy(out_ref.at[mb], out_ref.at[mb], ofs.at[mb, p], outf, pp=p).start()
        return carry

    lax.fori_loop(0, N + 4, body, 0)

    @pl.when(is_home)
    def _():
        s4_copy(N - 1).wait_send()
        hin_copy(N - 1).wait_send()

    @pl.when(is_outer)
    def _():
        s3_copy(N - 2).wait_send()
        s3_copy(N - 1).wait_send()

    for w in range(n_mb // 2):
        x_wait(w)

    @pl.when(s == n_stages - 1)
    def _():
        for mb in range(n_mb):
            for p in range(n_stages - 1):
                rcopy(out_ref.at[mb], out_ref.at[mb], ofs.at[mb, p], outf, pp=p).wait_send()

    @pl.when(s < n_stages - 1)
    def _():
        rcopy(out_ref, out_ref, ofs.at[0, 0], outf, pp=s).wait_recv()


def solution(mesh):
    n_stages = mesh.shape['pp']

    def stage_program(hidden_in, seg_ids, positions, attn_norm, w_query, w_key, w_value, w_out, mlp_norm, w_gate, w_up, w_down):
        n_mb, T, D = hidden_in.shape
        S = seg_ids.shape[1]
        QL = w_query.shape[2]
        FL = w_gate.shape[2]
        NJ = S // T
        N = (n_mb // 2) * NJ
        NB = max(1, FL // 512)
        cols = jnp.stack([positions, seg_ids], axis=-1)
        invf = jnp.asarray(np.tile(rope_freqs(), 2)[None, :], F32)
        any_spec = pl.BlockSpec(memory_space=pl.ANY)
        vmem = pl.BlockSpec(memory_space=pltpu.VMEM)
        dma = pltpu.SemaphoreType.DMA
        scratch = [
            pltpu.VMEM((NB, D, FL // NB), BF16), pltpu.VMEM((NB, D, FL // NB), BF16), pltpu.VMEM((NB, FL, D // NB), BF16),
            pltpu.VMEM((4, D, QL), BF16), pltpu.VMEM((2, QL, D), BF16),
            pltpu.VMEM((3, 2 * T, D), BF16),
            pltpu.VMEM((2, 2 * T, D), BF16),
            pltpu.VMEM((2, T, D), BF16),
            pltpu.VMEM((4, S, QL), BF16), pltpu.VMEM((4, S, QL), BF16),
            pltpu.VMEM((T, D), BF16),
            pltpu.VMEM((3, T, D), BF16),
            pltpu.VMEM((2 * T, D), F32),
            pltpu.VMEM((T, D), F32),
            pltpu.VMEM((T, D), BF16),
            pltpu.VMEM((T, D), BF16),
            pltpu.VMEM((2 * T, FL), BF16),
            pltpu.VMEM((T, D), F32),
            pltpu.VMEM((T, D), BF16),
            pltpu.VMEM((T, QL), BF16), pltpu.VMEM((T, QL), BF16),
            pltpu.VMEM((n_mb // 2, S, HEAD_DIM), F32),
            pltpu.VMEM((n_mb // 2, S, 2), jnp.int32),
            pltpu.VMEM((T, S), F32),
            dma((3, 4)), dma((2, 4)), dma((4,)), dma((4,)), dma((2, 4)),
            dma((N,)), dma((n_mb // 2, 2)), dma((2, 3)), dma((2,)), dma, dma((2,)), dma((2,)), dma((2,)), dma, dma,
            dma((n_mb,)), dma, dma((n_mb, n_stages - 1)),
            dma((4,)), dma((2,)), dma((3, NB)), dma, dma((n_mb // 2,)),
            pltpu.SemaphoreType.REGULAR,
        ]
        return pl.pallas_call(
            functools.partial(kernel, n_stages),
            out_shape=[jax.ShapeDtypeStruct(hidden_in.shape, BF16), jax.ShapeDtypeStruct((3, 3, D, QL), BF16),
                       jax.ShapeDtypeStruct((3, QL, D), BF16), jax.ShapeDtypeStruct((N, T, D), BF16)],
            in_specs=[any_spec, vmem, any_spec, vmem, vmem, vmem] + [any_spec] * 7,
            out_specs=[any_spec] * 4,
            scratch_shapes=scratch,
            compiler_params=pltpu.CompilerParams(has_side_effects=True, vmem_limit_bytes=67_043_328),
        )(hidden_in, seg_ids, cols, invf, attn_norm, mlp_norm, w_query, w_key, w_value, w_out, w_gate, w_up, w_down)[0]

    act_spec = P('dp', 'tp', None)
    row_spec = P('dp', None)
    gain_spec = P('pp', None)
    col_spec = P('pp', None, 'tp')
    rows_spec = P('pp', 'tp', None)
    return jax.shard_map(stage_program, mesh=mesh,
                         in_specs=(act_spec, row_spec, row_spec, gain_spec, col_spec, col_spec, col_spec, rows_spec, gain_spec, col_spec, col_spec, rows_spec),
                         out_specs=act_spec, check_vma=False)
```

```python
import functools
import math

import jax
import jax.numpy as jnp
import numpy as np
from jax import lax
from jax.experimental import pallas as pl
from jax.experimental.pallas import tpu as pltpu
from jax.sharding import PartitionSpec as P

HEAD_DIM = 128
NORM_EPS = 1e-5
ROPE_THETA = 500000.0
ROPE_FACTOR = 8.0
LOW_FREQ = 1.0
HIGH_FREQ = 4.0
ORIG_CTX = 8192.0
NEG = -1e30
MESH = pl.DeviceIdType.MESH
F32 = jnp.float32
BF16 = jnp.bfloat16


def rope_freqs():
    base_freq = 1.0 / (ROPE_THETA ** (np.arange(0, HEAD_DIM, 2) / HEAD_DIM))
    wavelen = 2.0 * np.pi / base_freq
    smooth = (ORIG_CTX / wavelen - LOW_FREQ) / (HIGH_FREQ - LOW_FREQ)
    blended = (1.0 - smooth) * base_freq / ROPE_FACTOR + smooth * base_freq
    scaled = np.where(wavelen > ORIG_CTX / LOW_FREQ, base_freq / ROPE_FACTOR, blended)
    return np.where(wavelen < ORIG_CTX / HIGH_FREQ, base_freq, scaled)


def kernel(n_stages, x_ref, seg_ref, cols_ref, invf_ref, ga_ref, gm_ref,
           wq_ref, wk_ref, wv_ref, wo_ref, wg_ref, wu_ref, wd_ref,
           out_ref,
           wqkv_hbm, wo_hbm, hin_hbm,
           wg_s, wu_s, wd_s, wst, gb, px, ps, kc, vc, hv, h1b, pacc, oacc, sendb, h2b, act, yb, abuf, qb, ob,
           table, cols, mask, sbuf, pbuf,
           wr, wx, wsnd, wfwd, wxs, hin_sem, xs, ag, s1s, s2s, pxr, pxs, psr, s4s, s5s, outr, outf, ofs,
           wst_sem, wo_sem, mlp_sem, hv_sem, cols_sem, gate):
    n_mb, T, D = x_ref.shape
    QL = wq_ref.shape[2]
    FL = wg_ref.shape[2]
    NB = wg_s.shape[0]
    FB = FL // NB
    S = seg_ref.shape[1]
    NJ = S // T
    NH = QL // HEAD_DIM
    N = (n_mb // 2) * NJ
    DB = D // NB
    scale = HEAD_DIM ** -0.5
    RB = 16
    NR = 32
    OB = wst.shape[3]
    NO = D // OB

    hx = lax.axis_index("dp")
    z = lax.axis_index("tp")
    s = lax.axis_index("pp")
    is_home = (z == 1) | (z == 2)
    is_outer = (z == 0) | (z == 3)
    hb = lax.rem(z + 1, 2) * 0 + (z - 1)
    peer = 3 - z
    outer = 3 * (z - 1)
    inner = 1 + z // 2
    odd = lax.rem(s, 2)

    def rcopy(src, dst, ssem, rsem, **dev):
        return pltpu.make_async_remote_copy(src_ref=src, dst_ref=dst, send_sem=ssem, recv_sem=rsem,
                                            device_id=dev, device_id_type=MESH)

    def local(src, dst, sem):
        return pltpu.make_async_copy(src, dst, sem)

    wqkv_own = (wq_ref, wk_ref, wv_ref, wo_ref)

    def mlp_copies():
        cps = []
        for n in range(NB):
            cps.append(local(wg_ref.at[0, :, pl.ds(n * FB, FB)], wg_s.at[n], mlp_sem.at[0, n]))
            cps.append(local(wu_ref.at[0, :, pl.ds(n * FB, FB)], wu_s.at[n], mlp_sem.at[1, n]))
            cps.append(local(wd_ref.at[0, :, pl.ds(n * DB, DB)], wd_s.at[n], mlp_sem.at[2, n]))
        return cps

    def x_copy(w, home):
        return rcopy(x_ref.at[2 * w + (home - 1)], hin_hbm.at[w * NJ + z], xs.at[w, home - 1],
                     hin_sem.at[w * NJ + z], tp=home)

    def x_start(w):
        for home in (1, 2):
            @pl.when((s == 0) & (z != home))
            def _():
                x_copy(w, home).start()

    def x_wait(w):
        for home in (1, 2):
            @pl.when((s == 0) & (z != home))
            def _():
                x_copy(w, home).wait_send()

    def half(ref, m, h):
        rows = (D if m < 3 else QL) // 2
        return ref.at[pl.ds(h * rows, rows), :]

    def wslot(r, m):
        return wqkv_hbm.at[r, m] if m < 3 else wo_hbm.at[r]

    def own_w(m):
        return wqkv_own[m].at[0]

    def o_send(m):
        return rcopy(own_w(m), wslot(0, m), wsnd.at[m], wr.at[0, m], tp=inner)

    def p_send(m):
        return rcopy(half(own_w(m), m, hx), half(wslot(1, m), m, hx), wsnd.at[m], wr.at[1, m], tp=peer)

    def f_send(m):
        return rcopy(half(wslot(0, m), m, hx), half(wslot(2, m), m, hx), wfwd.at[m], wr.at[2, m], tp=peer)

    def x_send(r, m):
        return rcopy(half(wslot(r, m), m, hx), half(wslot(r, m), m, hx), wxs.at[r - 1, m], wx.at[r - 1, m], dp=1 - hx)

    @pl.when(odd == 1)
    def _():
        with jax.named_scope('w_gate'):
            pl.semaphore_wait(gate, 1)

    @pl.when(is_outer)
    def _():
        for m in range(4):
            o_send(m).start()
        x_start(0)
        for c in mlp_copies():
            c.start()
        for m in range(4):
            o_send(m).wait_send()

    @pl.when(is_home)
    def _():
        for m in range(4):
            p_send(m).start()
        x_start(0)
        for c in mlp_copies():
            c.start()
        cps = [local(cols_ref.at[2 * w + hb], cols.at[w], cols_sem.at[w]) for w in range(n_mb // 2)]
        for c in cps:
            c.start()
        for c in cps:
            c.wait()
        lane = lax.broadcasted_iota(jnp.int32, (RB, HEAD_DIM), 1)

        def zero_rows(b, carry):
            for i in range(4):
                kc[i, pl.ds(b * RB, RB), :] = jnp.zeros((RB, QL), BF16)
                vc[i, pl.ds(b * RB, RB), :] = jnp.zeros((RB, QL), BF16)
            return carry
        lax.fori_loop(0, S // RB, zero_rows, 0)

        for w in range(n_mb // 2):
            def table_rows(b, carry, w=w):
                pos = cols[w, pl.ds(b * RB, RB), 0:1].astype(F32)
                ang = pos * invf_ref[0:1, :]
                table[w, pl.ds(b * RB, RB), :] = jnp.where(lane < HEAD_DIM // 2, jnp.cos(ang), jnp.sin(ang))
                return carry
            with jax.named_scope('table'):
                lax.fori_loop(0, S // RB, table_rows, 0)

        steps = [("p", 0), ("o", 0), ("p", 1), ("p", 2), ("o", 1), ("p", 3), ("f", 0), ("o", 2), ("f", 1), ("f", 2), ("o", 3), ("f", 3)]
        for kind, m in steps:
          with jax.named_scope('w_' + kind + str(m)):
            if kind == "o":
                o_send(m).wait_recv()
                f_send(m).start()
            elif kind == "p":
                p_send(m).wait_recv()
                x_send(1, m).start()
            else:
                f_send(m).wait_recv()
                x_send(2, m).start()
        for m in range(4):
            x_send(1, m).wait_recv()
            x_send(2, m).wait_recv()
        for m in range(4):
            p_send(m).wait_send()
            f_send(m).wait_send()
            x_send(1, m).wait_send()
            x_send(2, m).wait_send()

    @pl.when(odd == 0)
    def _():
        pl.semaphore_signal(gate, inc=1, device_id={"pp": s + 1}, device_id_type=MESH)

    def group_copies(g):
        p = g % 2
        if g < 4:
            return [local(own_w(m) if g == 0 else wqkv_hbm.at[g - 1, m], wst.at[p, m], wst_sem.at[p, m]) for m in range(3)]
        cps = []
        for m in range(3 if g == 4 else 1):
            n = (g - 4) * 3 + m
            for i in range(4):
                src = own_w(3) if i == 0 else wo_hbm.at[i - 1]
                cps.append(local(src.at[:, pl.ds(n * OB, OB)], wst.at[p, m, pl.ds(i * QL, QL), pl.ds(0, OB)], wo_sem.at[p, m, i]))
        return cps

    def group_start(g):
        for c in group_copies(g):
            c.start()

    def group_wait(g):
        for c in group_copies(g):
            c.wait()

    @pl.when(is_home)
    def _():
        group_start(0)
        group_start(1)

    for c in mlp_copies():
        c.wait()

    def hin_copy(u):
        return rcopy(h2b, hin_hbm.at[u], s5s, hin_sem.at[u], pp=lax.rem(s + 1, n_stages))

    def s1_outer(u):
        blk = gb.at[lax.rem(u, 3), pl.ds(pl.multiple_of(hb * T, T), T), :]
        return rcopy(blk, blk, s1s.at[0], ag.at[hb, lax.rem(u, 3)], tp=outer)

    def s1_peer(u):
        blk = gb.at[lax.rem(u, 3), pl.ds(pl.multiple_of(hb * T, T), T), :]
        return rcopy(blk, blk, s1s.at[1], ag.at[hb, lax.rem(u, 3)], tp=peer)

    def s2_copy(u):
        blk = gb.at[lax.rem(u, 3), pl.ds(pl.multiple_of((1 - hb) * T, T), T), :]
        return rcopy(blk, blk, s2s, ag.at[1 - hb, lax.rem(u, 3)], tp=outer)

    def ag_wait(b, u):
        blk = gb.at[lax.rem(u, 3), pl.ds(pl.multiple_of(b * T, T), T), :]
        local(blk, blk, ag.at[b, lax.rem(u, 3)]).wait()

    def s3_copy(u):
        sl = lax.rem(u, 2)
        return rcopy(px.at[sl], px.at[sl], pxs.at[sl], pxr.at[sl], tp=inner)

    def s4_copy(u):
        return rcopy(sendb, ps.at[lax.rem(u, 2)], s4s, psr.at[lax.rem(u, 2)], tp=peer)

    def out_copy(u, mb, j):
        return rcopy(h2b, out_ref.at[mb], s5s, outr.at[mb], tp=j)

    def norm_rows(src, gain, dst):
        hf = src.astype(F32)
        inv = lax.rsqrt(jnp.mean(hf * hf, axis=-1, keepdims=True) + NORM_EPS)
        return (hf * inv * gain.astype(F32)).astype(BF16)

    def attention(u):
      with jax.named_scope('attn'):
        attention_(u)

    def attention_(u):
        w = u // NJ
        j = lax.rem(u, NJ)
        mb = 2 * w + hb
        row0 = pl.multiple_of(j * T, T)
        from_x = (s == 0) & (j == z)

        @pl.when(from_x)
        def _():
            c = local(x_ref.at[mb], hv, hv_sem)
            c.start()
            c.wait()

        @pl.when(jnp.logical_not(from_x))
        def _():
            with jax.named_scope('w_hin'):
                hin_copy(u).wait_recv()
            c = local(hin_hbm.at[u], hv, hv_sem)
            c.start()
            c.wait()

        def norm_a(b, carry):
            rows = pl.ds(b * NR, NR)
            abuf[rows, :] = norm_rows(hv[rows, :], ga_ref[0:1, :], None)
            return carry
        lax.fori_loop(0, T // NR, norm_a, 0)

        segc = cols[w, pl.ds(row0, T), 1:2]
        segr = seg_ref[pl.ds(mb, 1), :]
        ti = lax.broadcasted_iota(jnp.int32, (T, S), 0) + row0
        ui = lax.broadcasted_iota(jnp.int32, (T, S), 1)
        mask[...] = jnp.where((segc == segr) & (ui <= ti), 1.0, 0.0)

        def rope(val):
            pk = table[w, pl.ds(row0, T), :]
            lane = lax.broadcasted_iota(jnp.int32, (T, HEAD_DIM), 1)
            swapped = pltpu.roll(pk, HEAD_DIM // 2, 1)
            cosw = jnp.where(lane < HEAD_DIM // 2, pk, swapped)
            sinw = jnp.where(lane < HEAD_DIM // 2, -swapped, pk)
            outs = []
            for h in range(NH):
                v = val[:, h * HEAD_DIM:(h + 1) * HEAD_DIM]
                outs.append((v * cosw + pltpu.roll(v, HEAD_DIM // 2, 1) * sinw).astype(BF16))
            return outs

        def hcols(h):
            return slice(h * HEAD_DIM, (h + 1) * HEAD_DIM)

        def proj(i):
            p = i % 2
            for h, val in enumerate(rope(jnp.dot(abuf[...], wst[p, 0], preferred_element_type=F32))):
                qb[p, :, hcols(h)] = val
            for h, val in enumerate(rope(jnp.dot(abuf[...], wst[p, 1], preferred_element_type=F32))):
                kc[i, pl.ds(row0, T), hcols(h)] = val
            vc[i, pl.ds(row0, T), :] = jnp.dot(abuf[...], wst[p, 2], preferred_element_type=F32).astype(BF16)

        def heads(i):
            for h in range(NH):
                sc = lax.dot_general(qb[i % 2, :, hcols(h)], kc[i, :, hcols(h)], (((1,), (1,)), ((), ())),
                                     preferred_element_type=F32) * scale
                sbuf[h] = jnp.where(mask[...] > 0.5, sc, NEG)
            for h in range(NH):
                for r in range(0, T, 32):
                    sc = sbuf[h, r:r + 32, :]
                    e = jnp.exp(sc - jnp.max(sc, axis=-1, keepdims=True))
                    pbuf[h, r:r + 32, :] = (e * (1.0 / jnp.sum(e, axis=-1, keepdims=True))).astype(BF16)
            for h in range(NH):
                ob[:, i * QL + h * HEAD_DIM:i * QL + (h + 1) * HEAD_DIM] = jnp.dot(
                    pbuf[h], vc[i, :, hcols(h)], preferred_element_type=F32).astype(BF16)

        with jax.named_scope('shards'):
            group_wait(0)
            proj(0)
            group_start(2)
            for i in range(3):
                group_wait(i + 1)
                proj(i + 1)
                group_start(i + 3)
                heads(i)
                if i == 1:
                    combine(u)
            group_wait(4)
            heads(3)
        with jax.named_scope('wo'):
            for n in range(NO):
                if n == 3:
                    group_wait(5)
                yb[:, n * OB:(n + 1) * OB] = jnp.dot(ob[...], wst[n // 3, n % 3, :4 * QL, :OB], preferred_element_type=F32).astype(BF16)

        @pl.when(u < N - 1)
        def _():
            group_start(0)
            group_start(1)

        def norm_b(b, carry):
            rows = pl.ds(b * NR, NR)
            h1 = (hv[rows, :].astype(F32) + yb[rows, :].astype(F32)).astype(BF16)
            h1b[lax.rem(u, 3), rows, :] = h1
            gb[lax.rem(u, 3), pl.ds(pl.multiple_of(hb * T + b * NR, NR), NR), :] = norm_rows(h1, gm_ref[0:1, :], None)
            return carry
        lax.fori_loop(0, T // NR, norm_b, 0)

    def mlp(sl):
      with jax.named_scope('mlp'):
        mlp_(sl)

    def mlp_(sl):
        def up(n, carry):
            xin = gb[sl]
            g = jnp.dot(xin, wg_s[n], preferred_element_type=F32)
            u_ = jnp.dot(xin, wu_s[n], preferred_element_type=F32)
            act[:, pl.ds(pl.multiple_of(n * FB, FB), FB)] = (jax.nn.silu(g) * u_).astype(BF16)
            return carry
        lax.fori_loop(0, NB, up, 0)

        def down(n, carry):
            pacc[:, pl.ds(pl.multiple_of(n * DB, DB), DB)] = jnp.dot(act[...], wd_s[n], preferred_element_type=F32)
            return carry
        lax.fori_loop(0, NB, down, 0)

    def forward(u):
        @pl.when((u >= 2) & (u <= N + 1))
        def _():
            s2_copy(u - 2).wait_send()

        @pl.when((u >= 1) & (u <= N))
        def _():
            with jax.named_scope('w_ag'):
                ag_wait(1 - hb, u - 1)
            s2_copy(u - 1).start()

    def combine(u):
        @pl.when((u >= 2) & (u < N + 2))
        def _():
            v = u - 2
            sl = lax.rem(v, 2)
            with jax.named_scope('w_s3'):
                s3_copy(v).wait_recv()

            @pl.when(v >= 1)
            def _():
                s4_copy(v - 1).wait_send()

            def comb(b, carry):
                rows = pl.ds(b * RB, RB)
                mine = pl.ds(pl.multiple_of(hb * T + b * RB, RB), RB)
                theirs = pl.ds(pl.multiple_of((1 - hb) * T + b * RB, RB), RB)
                oacc[rows, :] = pacc[mine, :] + px[sl, mine, :].astype(F32)
                sendb[rows, :] = (pacc[theirs, :] + px[sl, theirs, :].astype(F32)).astype(BF16)
                return carry
            lax.fori_loop(0, T // RB, comb, 0)
            s4_copy(v).start()

    def finish(u):
        @pl.when((u >= 2) & (u < N + 2))
        def _():
            v = u - 2
            with jax.named_scope('w_s4'):
                s4_copy(v).wait_recv()
            vw = v // NJ
            vj = lax.rem(v, NJ)

            @pl.when(v >= 1)
            def _():
                hin_copy(v).wait_send()

            def fin(b, carry):
                rows = pl.ds(b * RB, RB)
                d = (oacc[rows, :] + ps[lax.rem(v, 2), rows, :].astype(F32)).astype(BF16)
                h2b[rows, :] = (h1b[lax.rem(v, 3), rows, :].astype(F32) + d.astype(F32)).astype(BF16)
                return carry
            lax.fori_loop(0, T // RB, fin, 0)

            @pl.when(s < n_stages - 1)
            def _():
                hin_copy(v).start()

            @pl.when((s == n_stages - 1) & (vj != z))
            def _():
                out_copy(v, 2 * vw + hb, vj).start()

            @pl.when((s == n_stages - 1) & (vj == z))
            def _():
                local(h2b, out_ref.at[2 * vw + hb], s5s).start()

    def body(u, carry):
        @pl.when(is_home)
        def _():
            @pl.when((s == 0) & (lax.rem(u, NJ) == 0) & (u + NJ < N))
            def _():
                for home in (1, 2):
                    @pl.when(z != home)
                    def _():
                        x_copy(u // NJ + 1, home).start()

            forward(u)

            @pl.when(u < N)
            def _():
                attention(u)

            @pl.when(u >= N)
            def _():
                combine(u)

            @pl.when((u >= 1) & (u <= N))
            def _():
                s1_outer(u - 1).wait_send()
                s1_peer(u - 1).wait_send()

            @pl.when(u < N)
            def _():
                s1_outer(u).start()
                s1_peer(u).start()

            finish(u)

        @pl.when(is_outer & (u < N))
        def _():
            @pl.when((s == 0) & (lax.rem(u, NJ) == 0) & (u + NJ < N))
            def _():
                for home in (1, 2):
                    x_copy(u // NJ + 1, home).start()
            with jax.named_scope('w_ag_outer'):
                ag_wait(0, u)
                ag_wait(1, u)

        @pl.when((is_home & (u >= 1) & (u <= N)) | (is_outer & (u < N)))
        def _():
            mlp(lax.rem(u + 2 * (is_home.astype(jnp.int32)), 3))

        @pl.when(is_outer & (u < N))
        def _():
            sl = lax.rem(u, 2)

            @pl.when(u >= 2)
            def _():
                s3_copy(u - 2).wait_send()

            def conv(b, carry):
                rows = pl.ds(b * RB, RB)
                px[sl, rows, :] = pacc[rows, :].astype(BF16)
                return carry
            with jax.named_scope('conv'):
                lax.fori_loop(0, 2 * T // RB, conv, 0)
            s3_copy(u).start()

        v = u - 4

        @pl.when((s == n_stages - 1) & (v >= 0) & (v < N))
        def _():
            @pl.when(lax.rem(v, NJ) == z)
            def _():
                for b in (0, 1):
                    mb = 2 * (v // NJ) + b

                    @pl.when(z - 1 != b)
                    def _(mb=mb):
                        local(out_ref.at[mb], out_ref.at[mb], outr.at[mb]).wait()
                    for p in range(n_stages - 1):
                        rcopy(out_ref.at[mb], out_ref.at[mb], ofs.at[mb, p], outf, pp=p).start()
        return carry

    lax.fori_loop(0, N + 4, body, 0)

    @pl.when(is_home)
    def _():
        s4_copy(N - 1).wait_send()
        hin_copy(N - 1).wait_send()

    @pl.when(is_outer)
    def _():
        s3_copy(N - 2).wait_send()
        s3_copy(N - 1).wait_send()

    for w in range(n_mb // 2):
        x_wait(w)

    @pl.when(s == n_stages - 1)
    def _():
        for mb in range(n_mb):
            for p in range(n_stages - 1):
                rcopy(out_ref.at[mb], out_ref.at[mb], ofs.at[mb, p], outf, pp=p).wait_send()

    @pl.when(s < n_stages - 1)
    def _():
        rcopy(out_ref, out_ref, ofs.at[0, 0], outf, pp=s).wait_recv()


def solution(mesh):
    n_stages = mesh.shape['pp']

    def stage_program(hidden_in, seg_ids, positions, attn_norm, w_query, w_key, w_value, w_out, mlp_norm, w_gate, w_up, w_down):
        n_mb, T, D = hidden_in.shape
        S = seg_ids.shape[1]
        QL = w_query.shape[2]
        FL = w_gate.shape[2]
        NJ = S // T
        N = (n_mb // 2) * NJ
        NB = max(1, FL // 512)
        cols = jnp.stack([positions, seg_ids], axis=-1)
        invf = jnp.asarray(np.tile(rope_freqs(), 2)[None, :], F32)
        any_spec = pl.BlockSpec(memory_space=pl.ANY)
        vmem = pl.BlockSpec(memory_space=pltpu.VMEM)
        dma = pltpu.SemaphoreType.DMA
        scratch = [
            pltpu.VMEM((NB, D, FL // NB), BF16), pltpu.VMEM((NB, D, FL // NB), BF16), pltpu.VMEM((NB, FL, D // NB), BF16),
            pltpu.VMEM((2, 3, max(D, 4 * QL), QL), BF16),
            pltpu.VMEM((3, 2 * T, D), BF16),
            pltpu.VMEM((2, 2 * T, D), BF16),
            pltpu.VMEM((2, T, D), BF16),
            pltpu.VMEM((4, S, QL), BF16), pltpu.VMEM((4, S, QL), BF16),
            pltpu.VMEM((T, D), BF16),
            pltpu.VMEM((3, T, D), BF16),
            pltpu.VMEM((2 * T, D), F32),
            pltpu.VMEM((T, D), F32),
            pltpu.VMEM((T, D), BF16),
            pltpu.VMEM((T, D), BF16),
            pltpu.VMEM((2 * T, FL), BF16),
            pltpu.VMEM((T, D), BF16),
            pltpu.VMEM((T, D), BF16),
            pltpu.VMEM((2, T, QL), BF16), pltpu.VMEM((T, 4 * QL), BF16),
            pltpu.VMEM((n_mb // 2, S, HEAD_DIM), F32),
            pltpu.VMEM((n_mb // 2, S, 2), jnp.int32),
            pltpu.VMEM((T, S), F32), pltpu.VMEM((QL // HEAD_DIM, T, S), F32), pltpu.VMEM((QL // HEAD_DIM, T, S), BF16),
            dma((3, 4)), dma((2, 4)), dma((4,)), dma((4,)), dma((2, 4)),
            dma((N,)), dma((n_mb // 2, 2)), dma((2, 3)), dma((2,)), dma, dma((2,)), dma((2,)), dma((2,)), dma, dma,
            dma((n_mb,)), dma, dma((n_mb, n_stages - 1)),
            dma((2, 3)), dma((2, 3, 4)), dma((3, NB)), dma, dma((n_mb // 2,)),
            pltpu.SemaphoreType.REGULAR,
        ]
        return pl.pallas_call(
            functools.partial(kernel, n_stages),
            out_shape=[jax.ShapeDtypeStruct(hidden_in.shape, BF16), jax.ShapeDtypeStruct((3, 3, D, QL), BF16),
                       jax.ShapeDtypeStruct((3, QL, D), BF16), jax.ShapeDtypeStruct((N, T, D), BF16)],
            in_specs=[any_spec, vmem, any_spec, vmem, vmem, vmem] + [any_spec] * 7,
            out_specs=[any_spec] * 4,
            scratch_shapes=scratch,
            compiler_params=pltpu.CompilerParams(has_side_effects=True, vmem_limit_bytes=67_043_328),
        )(hidden_in, seg_ids, cols, invf, attn_norm, mlp_norm, w_query, w_key, w_value, w_out, w_gate, w_up, w_down)[0]

    act_spec = P('dp', 'tp', None)
    row_spec = P('dp', None)
    gain_spec = P('pp', None)
    col_spec = P('pp', None, 'tp')
    rows_spec = P('pp', 'tp', None)
    return jax.shard_map(stage_program, mesh=mesh,
                         in_specs=(act_spec, row_spec, row_spec, gain_spec, col_spec, col_spec, col_spec, rows_spec, gain_spec, col_spec, col_spec, rows_spec),
                         out_specs=act_spec, check_vma=False)
```

```python
import functools
import math

import jax
import jax.numpy as jnp
import numpy as np
from jax import lax
from jax.experimental import pallas as pl
from jax.experimental.pallas import tpu as pltpu
from jax.sharding import PartitionSpec as P

HEAD_DIM = 128
NORM_EPS = 1e-5
ROPE_THETA = 500000.0
ROPE_FACTOR = 8.0
LOW_FREQ = 1.0
HIGH_FREQ = 4.0
ORIG_CTX = 8192.0
NEG = -1e30
MESH = pl.DeviceIdType.MESH
F32 = jnp.float32
BF16 = jnp.bfloat16


def rope_freqs():
    base_freq = 1.0 / (ROPE_THETA ** (np.arange(0, HEAD_DIM, 2) / HEAD_DIM))
    wavelen = 2.0 * np.pi / base_freq
    smooth = (ORIG_CTX / wavelen - LOW_FREQ) / (HIGH_FREQ - LOW_FREQ)
    blended = (1.0 - smooth) * base_freq / ROPE_FACTOR + smooth * base_freq
    scaled = np.where(wavelen > ORIG_CTX / LOW_FREQ, base_freq / ROPE_FACTOR, blended)
    return np.where(wavelen < ORIG_CTX / HIGH_FREQ, base_freq, scaled)


def kernel(n_stages, x_ref, seg_ref, cols_ref, invf_ref, ga_ref, gm_ref,
           wq_ref, wk_ref, wv_ref, wo_ref, wg_ref, wu_ref, wd_ref,
           out_ref,
           wqkv_hbm, wo_hbm, hin_hbm,
           wg_s, wu_s, wd_s, wst, gb, px, ps, kc, vc, hin, h1b, pacc, oacc, sendb, h2b, act, yb, abuf, qb, ob,
           table, cols, mask, sbuf, pbuf,
           wr, wx, wsnd, wfwd, wxs, hin_sem, xs, ag, s1s, s2s, pxr, pxs, psr, s4s, s5s, outr, outf, ofs,
           wst_sem, wo_sem, mlp_sem, hv_sem, cols_sem, gate, cred):
    n_mb, T, D = x_ref.shape
    QL = wq_ref.shape[2]
    FL = wg_ref.shape[2]
    NB = wg_s.shape[0]
    FB = FL // NB
    S = seg_ref.shape[1]
    NJ = S // T
    NH = QL // HEAD_DIM
    N = (n_mb // 2) * NJ
    DB = D // NB
    scale = HEAD_DIM ** -0.5
    RB = 16
    NR = 32
    HS = hin.shape[0]
    OB = wst.shape[3]
    NO = D // OB

    hx = lax.axis_index("dp")
    z = lax.axis_index("tp")
    s = lax.axis_index("pp")
    is_home = (z == 1) | (z == 2)
    is_outer = (z == 0) | (z == 3)
    hb = lax.rem(z + 1, 2) * 0 + (z - 1)
    peer = 3 - z
    outer = 3 * (z - 1)
    inner = 1 + z // 2
    odd = lax.rem(s, 2)

    def rcopy(src, dst, ssem, rsem, **dev):
        return pltpu.make_async_remote_copy(src_ref=src, dst_ref=dst, send_sem=ssem, recv_sem=rsem,
                                            device_id=dev, device_id_type=MESH)

    def local(src, dst, sem):
        return pltpu.make_async_copy(src, dst, sem)

    wqkv_own = (wq_ref, wk_ref, wv_ref, wo_ref)

    def mlp_copies():
        cps = []
        for n in range(NB):
            cps.append(local(wg_ref.at[0, :, pl.ds(n * FB, FB)], wg_s.at[n], mlp_sem.at[0, n]))
            cps.append(local(wu_ref.at[0, :, pl.ds(n * FB, FB)], wu_s.at[n], mlp_sem.at[1, n]))
            cps.append(local(wd_ref.at[0, :, pl.ds(n * DB, DB)], wd_s.at[n], mlp_sem.at[2, n]))
        return cps

    def x_copy(w, home):
        return rcopy(x_ref.at[2 * w + (home - 1)], hin_hbm.at[w * NJ + z], xs.at[w, home - 1],
                     hin_sem.at[w * NJ + z], tp=home)

    def x_start(w):
        for home in (1, 2):
            @pl.when((s == 0) & (z != home))
            def _():
                x_copy(w, home).start()

    def x_wait(w):
        for home in (1, 2):
            @pl.when((s == 0) & (z != home))
            def _():
                x_copy(w, home).wait_send()

    def half(ref, m, h):
        rows = (D if m < 3 else QL) // 2
        return ref.at[pl.ds(h * rows, rows), :]

    def wslot(r, m):
        return wqkv_hbm.at[r, m] if m < 3 else wo_hbm.at[r]

    def own_w(m):
        return wqkv_own[m].at[0]

    def o_send(k):
        h = hx if k < 4 else 1 - hx
        return rcopy(half(own_w(k % 4), k % 4, h), half(wslot(0, k % 4), k % 4, h), wsnd.at[k], wr.at[0, k], tp=inner)

    def p_send(m):
        return rcopy(half(own_w(m), m, hx), half(wslot(1, m), m, hx), wsnd.at[m], wr.at[1, m], tp=peer)

    def f_send(m):
        return rcopy(half(wslot(0, m), m, hx), half(wslot(2, m), m, hx), wfwd.at[m], wr.at[2, m], tp=peer)

    def x_send(r, m):
        return rcopy(half(wslot(r, m), m, hx), half(wslot(r, m), m, hx), wxs.at[r - 1, m], wx.at[r - 1, m], dp=1 - hx)

    def release():
        @pl.when(odd == 0)
        def _():
            pl.semaphore_signal(gate, inc=1, device_id={"pp": s + 1}, device_id_type=MESH)

    @pl.when(odd == 1)
    def _():
        for c in mlp_copies():
            c.start()
        with jax.named_scope('w_gate'):
            pl.semaphore_wait(gate, 1)

    @pl.when(is_outer)
    def _():
        for k in range(8):
            o_send(k).start()

        @pl.when(odd == 0)
        def _():
            x_start(0)
            for c in mlp_copies():
                c.start()
        for k in range(4):
            o_send(k).wait_send()
        release()
        for k in range(4, 8):
            o_send(k).wait_send()

    @pl.when(is_home)
    def _():
        for m in range(4):
            p_send(m).start()

        @pl.when(odd == 0)
        def _():
            for c in mlp_copies():
                c.start()
        cps = [local(cols_ref.at[2 * w + hb], cols.at[w], cols_sem.at[w]) for w in range(n_mb // 2)]
        for c in cps:
            c.start()
        for c in cps:
            c.wait()
        lane = lax.broadcasted_iota(jnp.int32, (RB, HEAD_DIM), 1)

        def zero_rows(b, carry):
            for i in range(4):
                kc[i, pl.ds(b * RB, RB), :] = jnp.zeros((RB, QL), BF16)
                vc[i, pl.ds(b * RB, RB), :] = jnp.zeros((RB, QL), BF16)
            return carry
        lax.fori_loop(0, S // RB, zero_rows, 0)

        def tables(w):
            def table_rows(b, carry):
                pos = cols[w, pl.ds(b * RB, RB), 0:1].astype(F32)
                ang = pos * invf_ref[0:1, :]
                table[w, pl.ds(b * RB, RB), :] = jnp.where(lane < HEAD_DIM // 2, jnp.cos(ang), jnp.sin(ang))
                return carry
            with jax.named_scope('table'):
                lax.fori_loop(0, S // RB, table_rows, 0)

        steps = [("o", 0), ("p", 0), ("t", 0), ("o", 1), ("p", 1), ("t", 1), ("o", 2), ("p", 2), ("t", 2), ("o", 3), ("p", 3), ("g", 0), ("t", 3),
                 ("f", 0), ("f", 1), ("f", 2), ("f", 3)]
        for kind, m in steps:
          with jax.named_scope('w_' + kind + str(m)):
            if kind == "o":
                o_send(m).wait_recv()
                f_send(m).start()
            elif kind == "p":
                p_send(m).wait_recv()
                x_send(1, m).start()
            elif kind == "f":
                f_send(m).wait_recv()
                x_send(2, m).start()
            elif kind == "g":
                release()
            elif m < n_mb // 2:
                tables(m)
        x_start(0)
        for k in range(4, 8):
            o_send(k).wait_recv()
        for m in range(4):
            x_send(1, m).wait_recv()
            x_send(2, m).wait_recv()
        for m in range(4):
            p_send(m).wait_send()
            f_send(m).wait_send()
            x_send(1, m).wait_send()
            x_send(2, m).wait_send()

    def group_copies(g):
        p = g % 2
        if g < 4:
            return [local(own_w(m) if g == 0 else wqkv_hbm.at[g - 1, m], wst.at[p, m], wst_sem.at[p, m]) for m in range(3)]
        cps = []
        for m in range(3 if g == 4 else 1):
            n = (g - 4) * 3 + m
            for i in range(4):
                src = own_w(3) if i == 0 else wo_hbm.at[i - 1]
                cps.append(local(src.at[:, pl.ds(n * OB, OB)], wst.at[p, m, pl.ds(i * QL, QL), pl.ds(0, OB)], wo_sem.at[p, m, i]))
        return cps

    def group_start(g):
        for c in group_copies(g):
            c.start()

    def group_wait(g):
        for c in group_copies(g):
            c.wait()

    def h_fetch(u):
        mb = 2 * (u // NJ) + hb
        here = lax.rem(u, NJ) == z
        dst = hin.at[lax.rem(u, HS)]

        @pl.when((s == 0) & here)
        def _():
            local(x_ref.at[mb], dst, hv_sem).start()

        @pl.when((s == 0) & jnp.logical_not(here))
        def _():
            local(hin_hbm.at[u], hin_hbm.at[u], hin_sem.at[u]).wait()
            local(hin_hbm.at[u], dst, hv_sem).start()

    @pl.when(is_home)
    def _():
        group_start(0)
        group_start(1)
        h_fetch(0)

    for c in mlp_copies():
        c.wait()

    def hin_copy(u):
        return rcopy(h2b, hin.at[lax.rem(u, HS)], s5s, hin_sem.at[u], pp=lax.rem(s + 1, n_stages))

    def s1_outer(u):
        blk = gb.at[lax.rem(u, 3), pl.ds(pl.multiple_of(hb * T, T), T), :]
        return rcopy(blk, blk, s1s.at[0], ag.at[hb, lax.rem(u, 3)], tp=outer)

    def s1_peer(u):
        blk = gb.at[lax.rem(u, 3), pl.ds(pl.multiple_of(hb * T, T), T), :]
        return rcopy(blk, blk, s1s.at[1], ag.at[hb, lax.rem(u, 3)], tp=peer)

    def s2_copy(u):
        blk = gb.at[lax.rem(u, 3), pl.ds(pl.multiple_of((1 - hb) * T, T), T), :]
        return rcopy(blk, blk, s2s, ag.at[1 - hb, lax.rem(u, 3)], tp=outer)

    def ag_wait(b, u):
        blk = gb.at[lax.rem(u, 3), pl.ds(pl.multiple_of(b * T, T), T), :]
        local(blk, blk, ag.at[b, lax.rem(u, 3)]).wait()

    def s3_copy(u, b):
        sl = lax.rem(u, 2)
        blk = px.at[sl, pl.ds(pl.multiple_of(b * T, T), T), :]
        return rcopy(blk, blk, pxs.at[sl, b], pxr.at[sl, b], tp=inner)

    def s4_copy(u):
        return rcopy(sendb, ps.at[lax.rem(u, 2)], s4s, psr.at[lax.rem(u, 2)], tp=peer)

    def out_copy(u, mb, j):
        return rcopy(h2b, out_ref.at[mb], s5s, outr.at[mb], tp=j)

    def norm_rows(src, gain, dst):
        hf = src.astype(F32)
        inv = lax.rsqrt(jnp.mean(hf * hf, axis=-1, keepdims=True) + NORM_EPS)
        return (hf * inv * gain.astype(F32)).astype(BF16)

    def attention(u):
      with jax.named_scope('attn'):
        attention_(u)

    def attention_(u):
        w = u // NJ
        j = lax.rem(u, NJ)
        mb = 2 * w + hb
        row0 = pl.multiple_of(j * T, T)
        hs = lax.rem(u, HS)

        with jax.named_scope('w_hin'):
            @pl.when(s == 0)
            def _():
                local(x_ref.at[mb], hin.at[hs], hv_sem).wait()

            @pl.when(s > 0)
            def _():
                hin_copy(u).wait_recv()

        def norm_a(b, carry):
            rows = pl.ds(b * NR, NR)
            abuf[rows, :] = norm_rows(hin[hs, rows, :], ga_ref[0:1, :], None)
            return carry
        lax.fori_loop(0, T // NR, norm_a, 0)

        segc = cols[w, pl.ds(row0, T), 1:2]
        segr = seg_ref[pl.ds(mb, 1), :]
        ti = lax.broadcasted_iota(jnp.int32, (T, S), 0) + row0
        ui = lax.broadcasted_iota(jnp.int32, (T, S), 1)
        mask[...] = jnp.where((segc == segr) & (ui <= ti), 1.0, 0.0)

        def rope(val):
            pk = table[w, pl.ds(row0, T), :]
            lane = lax.broadcasted_iota(jnp.int32, (T, HEAD_DIM), 1)
            swapped = pltpu.roll(pk, HEAD_DIM // 2, 1)
            cosw = jnp.where(lane < HEAD_DIM // 2, pk, swapped)
            sinw = jnp.where(lane < HEAD_DIM // 2, -swapped, pk)
            outs = []
            for h in range(NH):
                v = val[:, h * HEAD_DIM:(h + 1) * HEAD_DIM]
                outs.append((v * cosw + pltpu.roll(v, HEAD_DIM // 2, 1) * sinw).astype(BF16))
            return outs

        def hcols(h):
            return slice(h * HEAD_DIM, (h + 1) * HEAD_DIM)

        def proj(i):
            p = i % 2
            for h, val in enumerate(rope(jnp.dot(abuf[...], wst[p, 0], preferred_element_type=F32))):
                qb[p, :, hcols(h)] = val
            for h, val in enumerate(rope(jnp.dot(abuf[...], wst[p, 1], preferred_element_type=F32))):
                kc[i, pl.ds(row0, T), hcols(h)] = val
            vc[i, pl.ds(row0, T), :] = jnp.dot(abuf[...], wst[p, 2], preferred_element_type=F32).astype(BF16)

        def heads(i):
            for h in range(NH):
                sc = lax.dot_general(qb[i % 2, :, hcols(h)], kc[i, :, hcols(h)], (((1,), (1,)), ((), ())),
                                     preferred_element_type=F32) * scale
                sbuf[h] = jnp.where(mask[...] > 0.5, sc, NEG)
            for h in range(NH):
                for r in range(0, T, 32):
                    sc = sbuf[h, r:r + 32, :]
                    e = jnp.exp(sc - jnp.max(sc, axis=-1, keepdims=True))
                    pbuf[h, r:r + 32, :] = (e * (1.0 / jnp.sum(e, axis=-1, keepdims=True))).astype(BF16)
            for h in range(NH):
                ob[:, i * QL + h * HEAD_DIM:i * QL + (h + 1) * HEAD_DIM] = jnp.dot(
                    pbuf[h], vc[i, :, hcols(h)], preferred_element_type=F32).astype(BF16)

        with jax.named_scope('shards'):
            group_wait(0)
            proj(0)
            group_start(2)
            for i in range(3):
                group_wait(i + 1)
                proj(i + 1)
                group_start(i + 3)
                heads(i)
                if i == 0:
                    finish(u)

                    @pl.when(u < N - 1)
                    def _():
                        h_fetch(u + 1)
            group_wait(4)
            heads(3)
        with jax.named_scope('wo'):
            for n in range(NO):
                if n == 3:
                    group_wait(5)
                yb[:, n * OB:(n + 1) * OB] = jnp.dot(ob[...], wst[n // 3, n % 3, :4 * QL, :OB], preferred_element_type=F32).astype(BF16)

        @pl.when(u < N - 1)
        def _():
            group_start(0)
            group_start(1)

        def norm_b(b, carry):
            rows = pl.ds(b * NR, NR)
            h1 = (hin[hs, rows, :].astype(F32) + yb[rows, :].astype(F32)).astype(BF16)
            h1b[lax.rem(u, 3), rows, :] = h1
            gb[lax.rem(u, 3), pl.ds(pl.multiple_of(hb * T + b * NR, NR), NR), :] = norm_rows(h1, gm_ref[0:1, :], None)
            return carry
        lax.fori_loop(0, T // NR, norm_b, 0)

        @pl.when((s > 0) & (u < N - HS))
        def _():
            pl.semaphore_signal(cred, inc=1, device_id={"pp": s - 1}, device_id_type=MESH)

    def mlp(sl, row0, rows, store):
        UN = 2 if NB % 2 == 0 else 1

        def up(q, carry):
            for n in [q * UN + k for k in range(UN)]:
                xin = gb[sl, pl.ds(row0, rows), :]
                g = jnp.dot(xin, wg_s[n], preferred_element_type=F32)
                u_ = jnp.dot(xin, wu_s[n], preferred_element_type=F32)
                act[0:rows, pl.ds(pl.multiple_of(n * FB, FB), FB)] = (jax.nn.silu(g) * u_).astype(BF16)
            return carry
        lax.fori_loop(0, NB // UN, up, 0)

        def down(q, carry):
            for n in [q * UN + k for k in range(UN)]:
                store(pl.ds(pl.multiple_of(n * DB, DB), DB), jnp.dot(act[0:rows, :], wd_s[n], preferred_element_type=F32))
            return carry
        lax.fori_loop(0, NB // UN, down, 0)

    def mlp_home(u):
        def store(c, val):
            pacc[:, c] = val
        with jax.named_scope('mlp'):
            mlp(lax.rem(u, 3), 0, 2 * T, store)

    def mlp_outer(u, b):
        def store(c, val):
            px[lax.rem(u, 2), pl.ds(pl.multiple_of(b * T, T), T), c] = val.astype(BF16)
        with jax.named_scope('mlp_o'):
            mlp(lax.rem(u, 3), pl.multiple_of(b * T, T), T, store)

    def forward(u):
        @pl.when((u >= 1) & (u <= N))
        def _():
            s2_copy(u - 1).wait_send()

        @pl.when(u < N)
        def _():
            with jax.named_scope('w_ag'):
                ag_wait(1 - hb, u)
            s2_copy(u).start()

    def combine(v):
        sl = lax.rem(v, 2)
        with jax.named_scope('w_s3'):
            s3_copy(v, 0).wait_recv()
            s3_copy(v, 1).wait_recv()

        @pl.when(v >= 1)
        def _():
            s4_copy(v - 1).wait_send()

        def comb(b, carry):
            rows = pl.ds(b * RB, RB)
            mine = pl.ds(pl.multiple_of(hb * T + b * RB, RB), RB)
            theirs = pl.ds(pl.multiple_of((1 - hb) * T + b * RB, RB), RB)
            oacc[rows, :] = pacc[mine, :] + px[sl, mine, :].astype(F32)
            sendb[rows, :] = (pacc[theirs, :] + px[sl, theirs, :].astype(F32)).astype(BF16)
            return carry
        lax.fori_loop(0, T // RB, comb, 0)
        s4_copy(v).start()

    def finish(u):
        @pl.when((u >= 2) & (u < N + 2))
        def _():
            v = u - 2
            with jax.named_scope('w_s4'):
                s4_copy(v).wait_recv()
            vw = v // NJ
            vj = lax.rem(v, NJ)

            @pl.when(v >= 1)
            def _():
                hin_copy(v).wait_send()

            def fin(b, carry):
                rows = pl.ds(b * RB, RB)
                d = (oacc[rows, :] + ps[lax.rem(v, 2), rows, :].astype(F32)).astype(BF16)
                h2b[rows, :] = (h1b[lax.rem(v, 3), rows, :].astype(F32) + d.astype(F32)).astype(BF16)
                return carry
            lax.fori_loop(0, T // RB, fin, 0)

            @pl.when((s < n_stages - 1) & (v >= HS))
            def _():
                with jax.named_scope('w_cred'):
                    pl.semaphore_wait(cred, 1)

            @pl.when(s < n_stages - 1)
            def _():
                hin_copy(v).start()

            @pl.when((s == n_stages - 1) & (vj != z))
            def _():
                out_copy(v, 2 * vw + hb, vj).start()

            @pl.when((s == n_stages - 1) & (vj == z))
            def _():
                local(h2b, out_ref.at[2 * vw + hb], s5s).start()

    def body(u, carry):
        @pl.when((s == 0) & (lax.rem(u, NJ) == 0) & (u + NJ < N))
        def _():
            x_start(u // NJ + 1)

        @pl.when(is_home)
        def _():
            @pl.when(u < N)
            def _():
                attention(u)

            @pl.when(u >= N)
            def _():
                finish(u)

            @pl.when((u >= 1) & (u <= N))
            def _():
                s1_outer(u - 1).wait_send()
                s1_peer(u - 1).wait_send()

            @pl.when(u < N)
            def _():
                s1_peer(u).start()
                s1_outer(u).start()

            @pl.when((u >= 1) & (u <= N))
            def _():
                mlp_home(u - 1)
                combine(u - 1)

            forward(u)

        @pl.when(is_outer & (u < N))
        def _():
            for k in (0, 1):
                b = inner - 1 if k == 0 else 2 - inner
                with jax.named_scope('w_ag_outer'):
                    ag_wait(b, u)

                @pl.when(u >= 2)
                def _():
                    s3_copy(u - 2, b).wait_send()
                mlp_outer(u, b)
                s3_copy(u, b).start()

        v = u - 4

        @pl.when((s == n_stages - 1) & (v >= 0) & (v < N))
        def _():
            @pl.when(lax.rem(v, NJ) == z)
            def _():
                for b in (0, 1):
                    mb = 2 * (v // NJ) + b

                    @pl.when(z - 1 != b)
                    def _(mb=mb):
                        local(out_ref.at[mb], out_ref.at[mb], outr.at[mb]).wait()
                    for p in range(n_stages - 1):
                        rcopy(out_ref.at[mb], out_ref.at[mb], ofs.at[mb, p], outf, pp=p).start()
        return carry

    lax.fori_loop(0, N + 4, body, 0)

    @pl.when(is_home)
    def _():
        s4_copy(N - 1).wait_send()
        hin_copy(N - 1).wait_send()

    @pl.when(is_outer)
    def _():
        for b in (0, 1):
            s3_copy(N - 2, b).wait_send()
            s3_copy(N - 1, b).wait_send()

    for w in range(n_mb // 2):
        x_wait(w)

    @pl.when(s == n_stages - 1)
    def _():
        for mb in range(n_mb):
            for p in range(n_stages - 1):
                rcopy(out_ref.at[mb], out_ref.at[mb], ofs.at[mb, p], outf, pp=p).wait_send()

    @pl.when(s < n_stages - 1)
    def _():
        rcopy(out_ref, out_ref, ofs.at[0, 0], outf, pp=s).wait_recv()


def solution(mesh):
    n_stages = mesh.shape['pp']

    def stage_program(hidden_in, seg_ids, positions, attn_norm, w_query, w_key, w_value, w_out, mlp_norm, w_gate, w_up, w_down):
        n_mb, T, D = hidden_in.shape
        S = seg_ids.shape[1]
        QL = w_query.shape[2]
        FL = w_gate.shape[2]
        NJ = S // T
        N = (n_mb // 2) * NJ
        NB = max(1, FL // 512)
        cols = jnp.stack([positions, seg_ids], axis=-1)
        invf = jnp.asarray(np.tile(rope_freqs(), 2)[None, :], F32)
        any_spec = pl.BlockSpec(memory_space=pl.ANY)
        vmem = pl.BlockSpec(memory_space=pltpu.VMEM)
        dma = pltpu.SemaphoreType.DMA
        scratch = [
            pltpu.VMEM((NB, D, FL // NB), BF16), pltpu.VMEM((NB, D, FL // NB), BF16), pltpu.VMEM((NB, FL, D // NB), BF16),
            pltpu.VMEM((2, 3, max(D, 4 * QL), QL), BF16),
            pltpu.VMEM((3, 2 * T, D), BF16),
            pltpu.VMEM((2, 2 * T, D), BF16),
            pltpu.VMEM((2, T, D), BF16),
            pltpu.VMEM((4, S, QL), BF16), pltpu.VMEM((4, S, QL), BF16),
            pltpu.VMEM((4, T, D), BF16),
            pltpu.VMEM((3, T, D), BF16),
            pltpu.VMEM((2 * T, D), F32),
            pltpu.VMEM((T, D), F32),
            pltpu.VMEM((T, D), BF16),
            pltpu.VMEM((T, D), BF16),
            pltpu.VMEM((2 * T, FL), BF16),
            pltpu.VMEM((T, D), BF16),
            pltpu.VMEM((T, D), BF16),
            pltpu.VMEM((2, T, QL), BF16), pltpu.VMEM((T, 4 * QL), BF16),
            pltpu.VMEM((n_mb // 2, S, HEAD_DIM), F32),
            pltpu.VMEM((n_mb // 2, S, 2), jnp.int32),
            pltpu.VMEM((T, S), F32), pltpu.VMEM((QL // HEAD_DIM, T, S), F32), pltpu.VMEM((QL // HEAD_DIM, T, S), BF16),
            dma((3, 8)), dma((2, 4)), dma((8,)), dma((4,)), dma((2, 4)),
            dma((N,)), dma((n_mb // 2, 2)), dma((2, 3)), dma((2,)), dma, dma((2, 2)), dma((2, 2)), dma((2,)), dma, dma,
            dma((n_mb,)), dma, dma((n_mb, n_stages - 1)),
            dma((2, 3)), dma((2, 3, 4)), dma((3, NB)), dma, dma((n_mb // 2,)),
            pltpu.SemaphoreType.REGULAR, pltpu.SemaphoreType.REGULAR,
        ]
        return pl.pallas_call(
            functools.partial(kernel, n_stages),
            out_shape=[jax.ShapeDtypeStruct(hidden_in.shape, BF16), jax.ShapeDtypeStruct((3, 3, D, QL), BF16),
                       jax.ShapeDtypeStruct((3, QL, D), BF16), jax.ShapeDtypeStruct((N, T, D), BF16)],
            in_specs=[any_spec, vmem, any_spec, vmem, vmem, vmem] + [any_spec] * 7,
            out_specs=[any_spec] * 4,
            scratch_shapes=scratch,
            compiler_params=pltpu.CompilerParams(has_side_effects=True, vmem_limit_bytes=67_043_328),
        )(hidden_in, seg_ids, cols, invf, attn_norm, mlp_norm, w_query, w_key, w_value, w_out, w_gate, w_up, w_down)[0]

    act_spec = P('dp', 'tp', None)
    row_spec = P('dp', None)
    gain_spec = P('pp', None)
    col_spec = P('pp', None, 'tp')
    rows_spec = P('pp', 'tp', None)
    return jax.shard_map(stage_program, mesh=mesh,
                         in_specs=(act_spec, row_spec, row_spec, gain_spec, col_spec, col_spec, col_spec, rows_spec, gain_spec, col_spec, col_spec, rows_spec),
                         out_specs=act_spec, check_vma=False)
```

```python
import functools
import math

import jax
import jax.numpy as jnp
import numpy as np
from jax import lax
from jax.experimental import pallas as pl
from jax.experimental.pallas import tpu as pltpu
from jax.sharding import PartitionSpec as P

HEAD_DIM = 128
NORM_EPS = 1e-5
ROPE_THETA = 500000.0
ROPE_FACTOR = 8.0
LOW_FREQ = 1.0
HIGH_FREQ = 4.0
ORIG_CTX = 8192.0
NEG = -1e30
MESH = pl.DeviceIdType.MESH
F32 = jnp.float32
BF16 = jnp.bfloat16


def rope_freqs():
    base_freq = 1.0 / (ROPE_THETA ** (np.arange(0, HEAD_DIM, 2) / HEAD_DIM))
    wavelen = 2.0 * np.pi / base_freq
    smooth = (ORIG_CTX / wavelen - LOW_FREQ) / (HIGH_FREQ - LOW_FREQ)
    blended = (1.0 - smooth) * base_freq / ROPE_FACTOR + smooth * base_freq
    scaled = np.where(wavelen > ORIG_CTX / LOW_FREQ, base_freq / ROPE_FACTOR, blended)
    return np.where(wavelen < ORIG_CTX / HIGH_FREQ, base_freq, scaled)


def kernel(n_stages, x_ref, seg_ref, cols_ref, invf_ref, ga_ref, gm_ref,
           wq_ref, wk_ref, wv_ref, wo_ref, wg_ref, wu_ref, wd_ref,
           out_ref,
           wqkv_hbm, wo_hbm, hin_hbm,
           wg_s, wu_s, wd_s, wst, gb, px, ps, kc, vc, hin, h1b, pacc, oacc, sendb, h2b, act, yb, abuf, qb, ob,
           table, cols, mask, sbuf, pbuf,
           wr, wx, wsnd, wfwd, wxs, hin_sem, xs, ag, s1s, s2s, pxr, pxs, psr, s4s, s5s, outr, outf, ofs,
           wst_sem, wo_sem, mlp_sem, hv_sem, cols_sem, xp, xq, op, od, gate, cred):
    n_mb, T, D = x_ref.shape
    QL = wq_ref.shape[2]
    FL = wg_ref.shape[2]
    NB = wg_s.shape[0]
    FB = FL // NB
    S = seg_ref.shape[1]
    NJ = S // T
    NH = QL // HEAD_DIM
    N = (n_mb // 2) * NJ
    DB = D // NB
    scale = HEAD_DIM ** -0.5
    RB = 16
    NR = 32
    HS = hin.shape[0]
    OB = wst.shape[3]
    NO = D // OB

    hx = lax.axis_index("dp")
    z = lax.axis_index("tp")
    s = lax.axis_index("pp")
    is_home = (z == 1) | (z == 2)
    is_outer = (z == 0) | (z == 3)
    hb = lax.rem(z + 1, 2) * 0 + (z - 1)
    peer = 3 - z
    outer = 3 * (z - 1)
    inner = 1 + z // 2
    odd = lax.rem(s, 2)

    def rcopy(src, dst, ssem, rsem, **dev):
        return pltpu.make_async_remote_copy(src_ref=src, dst_ref=dst, send_sem=ssem, recv_sem=rsem,
                                            device_id=dev, device_id_type=MESH)

    def local(src, dst, sem):
        return pltpu.make_async_copy(src, dst, sem)

    wqkv_own = (wq_ref, wk_ref, wv_ref, wo_ref)

    def mlp_copies():
        cps = []
        for n in range(NB):
            cps.append(local(wg_ref.at[0, :, pl.ds(n * FB, FB)], wg_s.at[n], mlp_sem.at[0, n]))
            cps.append(local(wu_ref.at[0, :, pl.ds(n * FB, FB)], wu_s.at[n], mlp_sem.at[1, n]))
            cps.append(local(wd_ref.at[0, :, pl.ds(n * DB, DB)], wd_s.at[n], mlp_sem.at[2, n]))
        return cps

    NW = n_mb // 2

    def x_copy(w, home):
        u = w * NJ + z
        return rcopy(x_ref.at[2 * w + (home - 1)], hin_hbm.at[u], xs.at[w, home - 1], (hin_sem if w == 0 else xp).at[u], tp=home)

    def x_each(w, act):
        for home in (1, 2):
            @pl.when((s == (0 if w == 0 else 2)) & (z != home))
            def _():
                act(x_copy(w, home))

    def x_pass(w, j):
        u = w * NJ + j
        return rcopy(hin_hbm.at[u], hin_hbm.at[u], xq.at[w, j], hin_sem.at[u], pp=0)

    def half(ref, m, h):
        rows = (D if m < 3 else QL) // 2
        return ref.at[pl.ds(h * rows, rows), :]

    def wslot(r, m):
        return wqkv_hbm.at[r, m] if m < 3 else wo_hbm.at[r]

    def own_w(m):
        return wqkv_own[m].at[0]

    def o_send(k):
        h = hx if k < 4 else 1 - hx
        return rcopy(half(own_w(k % 4), k % 4, h), half(wslot(0, k % 4), k % 4, h), wsnd.at[k], wr.at[0, k], tp=inner)

    def p_send(m):
        return rcopy(half(own_w(m), m, hx), half(wslot(1, m), m, hx), wsnd.at[m], wr.at[1, m], tp=peer)

    def f_send(m):
        return rcopy(half(wslot(0, m), m, hx), half(wslot(2, m), m, hx), wfwd.at[m], wr.at[2, m], tp=peer)

    def x_send(r, m):
        return rcopy(half(wslot(r, m), m, hx), half(wslot(r, m), m, hx), wxs.at[r - 1, m], wx.at[r - 1, m], dp=1 - hx)

    def w_ready(ms):
        for m in ms:
            o_send(4 + m).wait_recv()
            x_send(1, m).wait_recv()
            x_send(2, m).wait_recv()

    def release():
        @pl.when(odd == 0)
        def _():
            pl.semaphore_signal(gate, inc=1, device_id={"pp": s + 1}, device_id_type=MESH)

    @pl.when(odd == 1)
    def _():
        for c in mlp_copies():
            c.start()
        with jax.named_scope('w_gate'):
            pl.semaphore_wait(gate, 1)

    @pl.when(is_outer)
    def _():
        for k in range(8):
            o_send(k).start()

        @pl.when(odd == 0)
        def _():
            x_each(0, lambda c: c.start())
            for c in mlp_copies():
                c.start()
        for k in range(4):
            o_send(k).wait_send()
        release()
        for w in range(1, NW):
            x_each(w, lambda c: c.start())

    @pl.when(is_home)
    def _():
        for m in range(4):
            p_send(m).start()

        @pl.when(odd == 0)
        def _():
            for c in mlp_copies():
                c.start()
        cps = [local(cols_ref.at[2 * w + hb], cols.at[w], cols_sem.at[w]) for w in range(n_mb // 2)]
        for c in cps:
            c.start()
        for c in cps:
            c.wait()
        lane = lax.broadcasted_iota(jnp.int32, (RB, HEAD_DIM), 1)

        def zero_rows(b, carry):
            for i in range(4):
                kc[i, pl.ds(b * RB, RB), :] = jnp.zeros((RB, QL), BF16)
                vc[i, pl.ds(b * RB, RB), :] = jnp.zeros((RB, QL), BF16)
            return carry
        lax.fori_loop(0, S // RB, zero_rows, 0)

        def tables(w):
            def table_rows(b, carry):
                pos = cols[w, pl.ds(b * RB, RB), 0:1].astype(F32)
                ang = pos * invf_ref[0:1, :]
                table[w, pl.ds(b * RB, RB), :] = jnp.where(lane < HEAD_DIM // 2, jnp.cos(ang), jnp.sin(ang))
                return carry
            with jax.named_scope('table'):
                lax.fori_loop(0, S // RB, table_rows, 0)

        steps = [("o", 0), ("p", 0), ("t", 0), ("o", 1), ("p", 1), ("t", 1), ("o", 2), ("p", 2), ("t", 2), ("o", 3), ("p", 3), ("g", 0), ("t", 3),
                 ("f", 0), ("f", 1), ("f", 2), ("f", 3)]
        for kind, m in steps:
          with jax.named_scope('w_' + kind + str(m)):
            if kind == "o":
                o_send(m).wait_recv()
                f_send(m).start()
            elif kind == "p":
                p_send(m).wait_recv()
                x_send(1, m).start()
            elif kind == "f":
                f_send(m).wait_recv()
                x_send(2, m).start()
            elif kind == "g":
                release()
            elif m < n_mb // 2:
                tables(m)
        for w in range(NW):
            x_each(w, lambda c: c.start())
        w_ready(range(3))

        @pl.when(s == 2)
        def _():
            for w in range(1, NW):
                for j in range(NJ):
                    @pl.when(z != j)
                    def _():
                        local(hin_hbm.at[w * NJ + j], hin_hbm.at[w * NJ + j], xp.at[w * NJ + j]).wait()
                        x_pass(w, j).start()

    def group_copies(g):
        p = g % 2
        if g < 4:
            return [local(own_w(m) if g == 0 else wqkv_hbm.at[g - 1, m], wst.at[p, m], wst_sem.at[p, m]) for m in range(3)]
        cps = []
        for m in range(3 if g == 4 else 1):
            n = (g - 4) * 3 + m
            for i in range(4):
                src = own_w(3) if i == 0 else wo_hbm.at[i - 1]
                cps.append(local(src.at[:, pl.ds(n * OB, OB)], wst.at[p, m, pl.ds(i * QL, QL), pl.ds(0, OB)], wo_sem.at[p, m, i]))
        return cps

    def group_start(g):
        for c in group_copies(g):
            c.start()

    def group_wait(g):
        for c in group_copies(g):
            c.wait()

    def h_fetch(u):
        mb = 2 * (u // NJ) + hb
        here = lax.rem(u, NJ) == z
        dst = hin.at[lax.rem(u, HS)]

        @pl.when((s == 0) & here)
        def _():
            local(x_ref.at[mb], dst, hv_sem).start()

        @pl.when((s == 0) & jnp.logical_not(here))
        def _():
            local(hin_hbm.at[u], hin_hbm.at[u], hin_sem.at[u]).wait()
            local(hin_hbm.at[u], dst, hv_sem).start()

    @pl.when(is_home)
    def _():
        group_start(0)
        group_start(1)
        h_fetch(0)

    for c in mlp_copies():
        c.wait()

    def hin_copy(u):
        return rcopy(h2b, hin.at[lax.rem(u, HS)], s5s, hin_sem.at[u], pp=lax.rem(s + 1, n_stages))

    def s1_outer(u):
        blk = gb.at[lax.rem(u, 3), pl.ds(pl.multiple_of(hb * T, T), T), :]
        return rcopy(blk, blk, s1s.at[0], ag.at[hb, lax.rem(u, 3)], tp=outer)

    def s1_peer(u):
        blk = gb.at[lax.rem(u, 3), pl.ds(pl.multiple_of(hb * T, T), T), :]
        return rcopy(blk, blk, s1s.at[1], ag.at[hb, lax.rem(u, 3)], tp=peer)

    def s2_copy(u):
        blk = gb.at[lax.rem(u, 3), pl.ds(pl.multiple_of((1 - hb) * T, T), T), :]
        return rcopy(blk, blk, s2s, ag.at[1 - hb, lax.rem(u, 3)], tp=outer)

    def ag_wait(b, u):
        blk = gb.at[lax.rem(u, 3), pl.ds(pl.multiple_of(b * T, T), T), :]
        local(blk, blk, ag.at[b, lax.rem(u, 3)]).wait()

    def s3_copy(u, b):
        sl = lax.rem(u, 2)
        blk = px.at[sl, pl.ds(pl.multiple_of(b * T, T), T), :]
        return rcopy(blk, blk, pxs.at[sl, b], pxr.at[sl, b], tp=inner)

    def s4_copy(u):
        return rcopy(sendb, ps.at[lax.rem(u, 2)], s4s, psr.at[lax.rem(u, 2)], tp=peer)

    def park_copy(u):
        return rcopy(h2b, hin_hbm.at[u], s5s, op.at[u], pp=1)

    def out_copy(u, mb, j):
        return rcopy(h2b, out_ref.at[mb], s5s, outr.at[mb], tp=j)

    def norm_rows(src, gain, dst):
        hf = src.astype(F32)
        inv = lax.rsqrt(jnp.mean(hf * hf, axis=-1, keepdims=True) + NORM_EPS)
        return (hf * inv * gain.astype(F32)).astype(BF16)

    def attention(u):
      with jax.named_scope('attn'):
        attention_(u)

    def attention_(u):
        w = u // NJ
        j = lax.rem(u, NJ)
        mb = 2 * w + hb
        row0 = pl.multiple_of(j * T, T)
        hs = lax.rem(u, HS)

        with jax.named_scope('w_hin'):
            @pl.when(s == 0)
            def _():
                local(x_ref.at[mb], hin.at[hs], hv_sem).wait()

            @pl.when(s > 0)
            def _():
                hin_copy(u).wait_recv()

        def norm_a(b, carry):
            rows = pl.ds(b * NR, NR)
            abuf[rows, :] = norm_rows(hin[hs, rows, :], ga_ref[0:1, :], None)
            return carry
        lax.fori_loop(0, T // NR, norm_a, 0)

        segc = cols[w, pl.ds(row0, T), 1:2]
        segr = seg_ref[pl.ds(mb, 1), :]
        ti = lax.broadcasted_iota(jnp.int32, (T, S), 0) + row0
        ui = lax.broadcasted_iota(jnp.int32, (T, S), 1)
        mask[...] = jnp.where((segc == segr) & (ui <= ti), 1.0, 0.0)

        def rope(val):
            pk = table[w, pl.ds(row0, T), :]
            lane = lax.broadcasted_iota(jnp.int32, (T, HEAD_DIM), 1)
            swapped = pltpu.roll(pk, HEAD_DIM // 2, 1)
            cosw = jnp.where(lane < HEAD_DIM // 2, pk, swapped)
            sinw = jnp.where(lane < HEAD_DIM // 2, -swapped, pk)
            outs = []
            for h in range(NH):
                v = val[:, h * HEAD_DIM:(h + 1) * HEAD_DIM]
                outs.append((v * cosw + pltpu.roll(v, HEAD_DIM // 2, 1) * sinw).astype(BF16))
            return outs

        def hcols(h):
            return slice(h * HEAD_DIM, (h + 1) * HEAD_DIM)

        def proj(i):
            p = i % 2
            for h, val in enumerate(rope(jnp.dot(abuf[...], wst[p, 0], preferred_element_type=F32))):
                qb[p, :, hcols(h)] = val
            for h, val in enumerate(rope(jnp.dot(abuf[...], wst[p, 1], preferred_element_type=F32))):
                kc[i, pl.ds(row0, T), hcols(h)] = val
            vc[i, pl.ds(row0, T), :] = jnp.dot(abuf[...], wst[p, 2], preferred_element_type=F32).astype(BF16)

        def heads(i):
            for h in range(NH):
                sc = lax.dot_general(qb[i % 2, :, hcols(h)], kc[i, :, hcols(h)], (((1,), (1,)), ((), ())),
                                     preferred_element_type=F32) * scale
                sbuf[h] = jnp.where(mask[...] > 0.5, sc, NEG)
            for h in range(NH):
                for r in range(0, T, 32):
                    sc = sbuf[h, r:r + 32, :]
                    e = jnp.exp(sc - jnp.max(sc, axis=-1, keepdims=True))
                    pbuf[h, r:r + 32, :] = (e * (1.0 / jnp.sum(e, axis=-1, keepdims=True))).astype(BF16)
            for h in range(NH):
                ob[:, i * QL + h * HEAD_DIM:i * QL + (h + 1) * HEAD_DIM] = jnp.dot(
                    pbuf[h], vc[i, :, hcols(h)], preferred_element_type=F32).astype(BF16)

        with jax.named_scope('shards'):
            group_wait(0)
            proj(0)
            group_start(2)
            for i in range(3):
                group_wait(i + 1)
                proj(i + 1)
                if i == 1:
                    @pl.when(u == 0)
                    def _():
                        w_ready([3])
                group_start(i + 3)
                heads(i)
                if i == 0:
                    finish(u)

                    @pl.when(u < N - 1)
                    def _():
                        h_fetch(u + 1)
            group_wait(4)
            heads(3)
        with jax.named_scope('wo'):
            for n in range(NO):
                if n == 3:
                    group_wait(5)
                yb[:, n * OB:(n + 1) * OB] = jnp.dot(ob[...], wst[n // 3, n % 3, :4 * QL, :OB], preferred_element_type=F32).astype(BF16)

        @pl.when(u < N - 1)
        def _():
            group_start(0)
            group_start(1)

        def norm_b(b, carry):
            rows = pl.ds(b * NR, NR)
            h1 = (hin[hs, rows, :].astype(F32) + yb[rows, :].astype(F32)).astype(BF16)
            h1b[lax.rem(u, 3), rows, :] = h1
            gb[lax.rem(u, 3), pl.ds(pl.multiple_of(hb * T + b * NR, NR), NR), :] = norm_rows(h1, gm_ref[0:1, :], None)
            return carry
        lax.fori_loop(0, T // NR, norm_b, 0)

        @pl.when((s > 0) & (u < N - HS))
        def _():
            pl.semaphore_signal(cred, inc=1, device_id={"pp": s - 1}, device_id_type=MESH)

    def mlp(sl, row0, rows, store):
        UN = 2 if NB % 2 == 0 else 1

        def up(q, carry):
            for n in [q * UN + k for k in range(UN)]:
                xin = gb[sl, pl.ds(row0, rows), :]
                g = jnp.dot(xin, wg_s[n], preferred_element_type=F32)
                u_ = jnp.dot(xin, wu_s[n], preferred_element_type=F32)
                act[0:rows, pl.ds(pl.multiple_of(n * FB, FB), FB)] = (jax.nn.silu(g) * u_).astype(BF16)
            return carry
        lax.fori_loop(0, NB // UN, up, 0)

        def down(q, carry):
            for n in [q * UN + k for k in range(UN)]:
                store(pl.ds(pl.multiple_of(n * DB, DB), DB), jnp.dot(act[0:rows, :], wd_s[n], preferred_element_type=F32))
            return carry
        lax.fori_loop(0, NB // UN, down, 0)

    def mlp_home(u):
        def store(c, val):
            pacc[:, c] = val
        with jax.named_scope('mlp'):
            mlp(lax.rem(u, 3), 0, 2 * T, store)

    def mlp_outer(u, b):
        def store(c, val):
            px[lax.rem(u, 2), pl.ds(pl.multiple_of(b * T, T), T), c] = val.astype(BF16)
        with jax.named_scope('mlp_o'):
            mlp(lax.rem(u, 3), pl.multiple_of(b * T, T), T, store)

    def forward(u):
        @pl.when((u >= 1) & (u <= N))
        def _():
            s2_copy(u - 1).wait_send()

        @pl.when(u < N)
        def _():
            with jax.named_scope('w_ag'):
                ag_wait(1 - hb, u)
            s2_copy(u).start()

    def combine(v):
        sl = lax.rem(v, 2)
        with jax.named_scope('w_s3'):
            s3_copy(v, 0).wait_recv()
            s3_copy(v, 1).wait_recv()

        @pl.when(v >= 1)
        def _():
            s4_copy(v - 1).wait_send()

        def comb(b, carry):
            rows = pl.ds(b * RB, RB)
            mine = pl.ds(pl.multiple_of(hb * T + b * RB, RB), RB)
            theirs = pl.ds(pl.multiple_of((1 - hb) * T + b * RB, RB), RB)
            oacc[rows, :] = pacc[mine, :] + px[sl, mine, :].astype(F32)
            sendb[rows, :] = (pacc[theirs, :] + px[sl, theirs, :].astype(F32)).astype(BF16)
            return carry
        lax.fori_loop(0, T // RB, comb, 0)
        s4_copy(v).start()

    def finish(u):
        @pl.when((u >= 2) & (u < N + 2))
        def _():
            v = u - 2
            with jax.named_scope('w_s4'):
                s4_copy(v).wait_recv()
            vw = v // NJ
            vj = lax.rem(v, NJ)

            @pl.when(v >= 1)
            def _():
                hin_copy(v).wait_send()

            def fin(b, carry):
                rows = pl.ds(b * RB, RB)
                d = (oacc[rows, :] + ps[lax.rem(v, 2), rows, :].astype(F32)).astype(BF16)
                h2b[rows, :] = (h1b[lax.rem(v, 3), rows, :].astype(F32) + d.astype(F32)).astype(BF16)
                return carry
            lax.fori_loop(0, T // RB, fin, 0)

            @pl.when((s < n_stages - 1) & (v >= HS))
            def _():
                with jax.named_scope('w_cred'):
                    pl.semaphore_wait(cred, 1)

            @pl.when(s < n_stages - 1)
            def _():
                hin_copy(v).start()

            @pl.when((s == n_stages - 1) & (v < N - NJ))
            def _():
                park_copy(v).start()

            @pl.when((s == n_stages - 1) & (v >= N - NJ) & (vj != z))
            def _():
                out_copy(v, 2 * vw + hb, vj).start()

            @pl.when((s == n_stages - 1) & (v >= N - NJ) & (vj == z))
            def _():
                local(h2b, out_ref.at[2 * vw + hb], s5s).start()

    def body(u, carry):
        @pl.when(is_home)
        def _():
            @pl.when(u < N)
            def _():
                attention(u)

            @pl.when(u >= N)
            def _():
                finish(u)

            @pl.when((u >= 1) & (u <= N))
            def _():
                s1_outer(u - 1).wait_send()
                s1_peer(u - 1).wait_send()

            @pl.when(u < N)
            def _():
                s1_peer(u).start()
                s1_outer(u).start()

            @pl.when((u >= 1) & (u <= N))
            def _():
                mlp_home(u - 1)
                combine(u - 1)

            forward(u)

        @pl.when(is_outer & (u < N))
        def _():
            for k in (0, 1):
                b = inner - 1 if k == 0 else 2 - inner
                with jax.named_scope('w_ag_outer'):
                    ag_wait(b, u)

                @pl.when(u >= 2)
                def _():
                    s3_copy(u - 2, b).wait_send()
                mlp_outer(u, b)
                s3_copy(u, b).start()

        v = u - 4

        @pl.when((s == n_stages - 1) & (v >= N - NJ) & (v < N) & (lax.rem(v, NJ) == z))
        def _():
            for b in (0, 1):
                mb = 2 * NW - 2 + b

                @pl.when(z - 1 != b)
                def _(mb=mb):
                    local(out_ref.at[mb], out_ref.at[mb], outr.at[mb]).wait()
                out_fwd(mb, 1, outr.at[mb]).start()
                out_fwd(mb, 2, outf).start()
        return carry

    def out_fwd(mb, p, sem):
        return rcopy(out_ref.at[mb], out_ref.at[mb], ofs.at[mb, p], sem, pp=p)

    lax.fori_loop(0, N + 4, body, 0)

    def od_copy(v):
        return rcopy(hin_hbm.at[v], out_ref.at[2 * (v // NJ) + hb], od.at[v], outr.at[2 * (v // NJ) + hb], tp=lax.rem(v, NJ))

    @pl.when(s == 1)
    def _():
        def spread(v, carry):
            vj = lax.rem(v, NJ)
            mine = 2 * (v // NJ) + hb

            @pl.when(is_home)
            def _():
                local(hin_hbm.at[v], hin_hbm.at[v], op.at[v]).wait()

            @pl.when(is_home & (vj != z))
            def _():
                od_copy(v).start()

            @pl.when(is_home & (vj == z))
            def _():
                c = local(hin_hbm.at[v], hin.at[0], hv_sem)
                c.start()
                c.wait()
                c = local(hin.at[0], out_ref.at[mine], hv_sem)
                c.start()
                c.wait()

            @pl.when(vj == z)
            def _():
                for b in (0, 1):
                    mb = 2 * (v // NJ) + b

                    @pl.when(z - 1 != b)
                    def _(mb=mb):
                        local(out_ref.at[mb], out_ref.at[mb], outr.at[mb]).wait()
                    for p in (3, 0, 2):
                        out_fwd(mb, p, outf).start()
            return carry
        lax.fori_loop(0, N - NJ, spread, 0)

        for b in (0, 1):
            mb = 2 * NW - 2 + b
            local(out_ref.at[mb], out_ref.at[mb], outr.at[mb]).wait()
            out_fwd(mb, 0, outf).start()

    @pl.when(is_home)
    def _():
        s4_copy(N - 1).wait_send()
        hin_copy(N - 1).wait_send()

    @pl.when(is_outer)
    def _():
        for b in (0, 1):
            s3_copy(N - 2, b).wait_send()
            s3_copy(N - 1, b).wait_send()

    @pl.when(is_outer)
    def _():
        for k in range(4, 8):
            o_send(k).wait_send()

    @pl.when(is_home)
    def _():
        for m in range(4):
            p_send(m).wait_send()
            f_send(m).wait_send()
            x_send(1, m).wait_send()
            x_send(2, m).wait_send()

        @pl.when(s == 2)
        def _():
            for w in range(1, NW):
                for j in range(NJ):
                    @pl.when(z != j)
                    def _():
                        x_pass(w, j).wait_send()

        @pl.when(s == 1)
        def _():
            def spread_done(v, carry):
                @pl.when(lax.rem(v, NJ) != z)
                def _():
                    od_copy(v).wait_send()
                return carry
            lax.fori_loop(0, N - NJ, spread_done, 0)

    for w in range(NW):
        x_each(w, lambda c: c.wait_send())

    @pl.when(s == 1)
    def _():
        for mb in range(n_mb - 2):
            for p in (3, 0, 2):
                out_fwd(mb, p, outf).wait_send()
        for mb in (n_mb - 2, n_mb - 1):
            out_fwd(mb, 0, outf).wait_send()

    @pl.when(s == n_stages - 1)
    def _():
        for mb in (n_mb - 2, n_mb - 1):
            for p in (1, 2):
                out_fwd(mb, p, outf).wait_send()
        early = out_ref.at[pl.ds(0, n_mb - 2)]
        local(early, early, outf).wait()

    @pl.when((s == 0) | (s == 2))
    def _():
        local(out_ref, out_ref, outf).wait()


def solution(mesh):
    n_stages = mesh.shape['pp']

    def stage_program(hidden_in, seg_ids, positions, attn_norm, w_query, w_key, w_value, w_out, mlp_norm, w_gate, w_up, w_down):
        n_mb, T, D = hidden_in.shape
        S = seg_ids.shape[1]
        QL = w_query.shape[2]
        FL = w_gate.shape[2]
        NJ = S // T
        N = (n_mb // 2) * NJ
        NB = max(1, FL // 512)
        cols = jnp.stack([positions, seg_ids], axis=-1)
        invf = jnp.asarray(np.tile(rope_freqs(), 2)[None, :], F32)
        any_spec = pl.BlockSpec(memory_space=pl.ANY)
        vmem = pl.BlockSpec(memory_space=pltpu.VMEM)
        dma = pltpu.SemaphoreType.DMA
        scratch = [
            pltpu.VMEM((NB, D, FL // NB), BF16), pltpu.VMEM((NB, D, FL // NB), BF16), pltpu.VMEM((NB, FL, D // NB), BF16),
            pltpu.VMEM((2, 3, max(D, 4 * QL), QL), BF16),
            pltpu.VMEM((3, 2 * T, D), BF16),
            pltpu.VMEM((2, 2 * T, D), BF16),
            pltpu.VMEM((2, T, D), BF16),
            pltpu.VMEM((4, S, QL), BF16), pltpu.VMEM((4, S, QL), BF16),
            pltpu.VMEM((4, T, D), BF16),
            pltpu.VMEM((3, T, D), BF16),
            pltpu.VMEM((2 * T, D), F32),
            pltpu.VMEM((T, D), F32),
            pltpu.VMEM((T, D), BF16),
            pltpu.VMEM((T, D), BF16),
            pltpu.VMEM((2 * T, FL), BF16),
            pltpu.VMEM((T, D), BF16),
            pltpu.VMEM((T, D), BF16),
            pltpu.VMEM((2, T, QL), BF16), pltpu.VMEM((T, 4 * QL), BF16),
            pltpu.VMEM((n_mb // 2, S, HEAD_DIM), F32),
            pltpu.VMEM((n_mb // 2, S, 2), jnp.int32),
            pltpu.VMEM((T, S), F32), pltpu.VMEM((QL // HEAD_DIM, T, S), F32), pltpu.VMEM((QL // HEAD_DIM, T, S), BF16),
            dma((3, 8)), dma((2, 4)), dma((8,)), dma((4,)), dma((2, 4)),
            dma((N,)), dma((n_mb // 2, 2)), dma((2, 3)), dma((2,)), dma, dma((2, 2)), dma((2, 2)), dma((2,)), dma, dma,
            dma((n_mb,)), dma, dma((n_mb, n_stages)),
            dma((2, 3)), dma((2, 3, 4)), dma((3, NB)), dma, dma((n_mb // 2,)), dma((N,)), dma((n_mb // 2, NJ)), dma((N,)), dma((N,)),
            pltpu.SemaphoreType.REGULAR, pltpu.SemaphoreType.REGULAR,
        ]
        return pl.pallas_call(
            functools.partial(kernel, n_stages),
            out_shape=[jax.ShapeDtypeStruct(hidden_in.shape, BF16), jax.ShapeDtypeStruct((3, 3, D, QL), BF16),
                       jax.ShapeDtypeStruct((3, QL, D), BF16), jax.ShapeDtypeStruct((N, T, D), BF16)],
            in_specs=[any_spec, vmem, any_spec, vmem, vmem, vmem] + [any_spec] * 7,
            out_specs=[any_spec] * 4,
            scratch_shapes=scratch,
            compiler_params=pltpu.CompilerParams(has_side_effects=True, vmem_limit_bytes=67_043_328),
        )(hidden_in, seg_ids, cols, invf, attn_norm, mlp_norm, w_query, w_key, w_value, w_out, w_gate, w_up, w_down)[0]

    act_spec = P('dp', 'tp', None)
    row_spec = P('dp', None)
    gain_spec = P('pp', None)
    col_spec = P('pp', None, 'tp')
    rows_spec = P('pp', 'tp', None)
    return jax.shard_map(stage_program, mesh=mesh,
                         in_specs=(act_spec, row_spec, row_spec, gain_spec, col_spec, col_spec, col_spec, rows_spec, gain_spec, col_spec, col_spec, rows_spec),
                         out_specs=act_spec, check_vma=False)
```

```python
import functools
import math

import jax
import jax.numpy as jnp
import numpy as np
from jax import lax
from jax.experimental import pallas as pl
from jax.experimental.pallas import tpu as pltpu
from jax.sharding import PartitionSpec as P

HEAD_DIM = 128
NORM_EPS = 1e-5
ROPE_THETA = 500000.0
ROPE_FACTOR = 8.0
LOW_FREQ = 1.0
HIGH_FREQ = 4.0
ORIG_CTX = 8192.0
NEG = -1e30
MESH = pl.DeviceIdType.MESH
F32 = jnp.float32
BF16 = jnp.bfloat16


def rope_freqs():
    base_freq = 1.0 / (ROPE_THETA ** (np.arange(0, HEAD_DIM, 2) / HEAD_DIM))
    wavelen = 2.0 * np.pi / base_freq
    smooth = (ORIG_CTX / wavelen - LOW_FREQ) / (HIGH_FREQ - LOW_FREQ)
    blended = (1.0 - smooth) * base_freq / ROPE_FACTOR + smooth * base_freq
    scaled = np.where(wavelen > ORIG_CTX / LOW_FREQ, base_freq / ROPE_FACTOR, blended)
    return np.where(wavelen < ORIG_CTX / HIGH_FREQ, base_freq, scaled)


def kernel(n_stages, x_ref, seg_ref, cols_ref, invf_ref, ga_ref, gm_ref,
           wq_ref, wk_ref, wv_ref, wo_ref, wg_ref, wu_ref, wd_ref,
           out_ref,
           wqkv_hbm, wo_hbm, hin_hbm,
           wg_s, wu_s, wd_s, wst, gb, px, ps, kc, vc, hin, h1b, pacc, oacc, sendb, h2b, act, yb, abuf, qb, ob,
           table, cols, mask, sbuf, pbuf,
           wr, wx, wsnd, wfwd, wxs, hin_sem, xs, ag, s1s, s2s, pxr, pxs, psr, s4s, s5s, outr, outf, ofs,
           wst_sem, wo_sem, mlp_sem, hv_sem, cols_sem, xp, xq, op, od, gate, cred):
    n_mb, T, D = x_ref.shape
    QL = wq_ref.shape[2]
    FL = wg_ref.shape[2]
    NB = wg_s.shape[0]
    FB = FL // NB
    S = seg_ref.shape[1]
    NJ = S // T
    NH = QL // HEAD_DIM
    N = (n_mb // 2) * NJ
    DB = D // NB
    scale = HEAD_DIM ** -0.5
    RB = 16
    NR = 32
    HS = hin.shape[0]
    OB = wst.shape[3]
    NO = D // OB

    hx = lax.axis_index("dp")
    z = lax.axis_index("tp")
    s = lax.axis_index("pp")
    is_home = (z == 1) | (z == 2)
    is_outer = (z == 0) | (z == 3)
    hb = lax.rem(z + 1, 2) * 0 + (z - 1)
    peer = 3 - z
    outer = 3 * (z - 1)
    inner = 1 + z // 2
    odd = lax.rem(s, 2)

    def rcopy(src, dst, ssem, rsem, **dev):
        return pltpu.make_async_remote_copy(src_ref=src, dst_ref=dst, send_sem=ssem, recv_sem=rsem,
                                            device_id=dev, device_id_type=MESH)

    def local(src, dst, sem):
        return pltpu.make_async_copy(src, dst, sem)

    wqkv_own = (wq_ref, wk_ref, wv_ref, wo_ref)

    def mlp_copies():
        cps = []
        for n in range(NB):
            cps.append(local(wg_ref.at[0, :, pl.ds(n * FB, FB)], wg_s.at[n], mlp_sem.at[0, n]))
            cps.append(local(wu_ref.at[0, :, pl.ds(n * FB, FB)], wu_s.at[n], mlp_sem.at[1, n]))
            cps.append(local(wd_ref.at[0, :, pl.ds(n * DB, DB)], wd_s.at[n], mlp_sem.at[2, n]))
        return cps

    NW = n_mb // 2

    def x_copy(w, home):
        u = w * NJ + z
        return rcopy(x_ref.at[2 * w + (home - 1)], hin_hbm.at[u], xs.at[w, home - 1], (hin_sem if w == 0 else xp).at[u], tp=home)

    def x_each(w, act):
        for home in (1, 2):
            @pl.when((s == (0 if w == 0 else 2)) & (z != home))
            def _():
                act(x_copy(w, home))

    def x_pass(w, j):
        u = w * NJ + j
        return rcopy(hin_hbm.at[u], hin_hbm.at[u], xq.at[w, j], hin_sem.at[u], pp=0)

    def half(ref, m, h):
        rows = (D if m < 3 else QL) // 2
        return ref.at[pl.ds(h * rows, rows), :]

    def wslot(r, m):
        return wqkv_hbm.at[r, m] if m < 3 else wo_hbm.at[r]

    def own_w(m):
        return wqkv_own[m].at[0]

    def o_send(k):
        h = hx if k < 4 else 1 - hx
        return rcopy(half(own_w(k % 4), k % 4, h), half(wslot(0, k % 4), k % 4, h), wsnd.at[k], wr.at[0, k], tp=inner)

    def p_send(m):
        return rcopy(half(own_w(m), m, hx), half(wslot(1, m), m, hx), wsnd.at[m], wr.at[1, m], tp=peer)

    def f_send(m):
        return rcopy(half(wslot(0, m), m, hx), half(wslot(2, m), m, hx), wfwd.at[m], wr.at[2, m], tp=peer)

    def x_send(r, m):
        return rcopy(half(wslot(r, m), m, hx), half(wslot(r, m), m, hx), wxs.at[r - 1, m], wx.at[r - 1, m], dp=1 - hx)

    def w_ready(rs, ms):
        for m in ms:
            if 0 in rs:
                o_send(4 + m).wait_recv()
            for r in (1, 2):
                if r in rs:
                    x_send(r, m).wait_recv()

    def release():
        @pl.when(odd == 0)
        def _():
            pl.semaphore_signal(gate, inc=1, device_id={"pp": s + 1}, device_id_type=MESH)

    @pl.when(odd == 1)
    def _():
        for c in mlp_copies():
            c.start()
        with jax.named_scope('w_gate'):
            pl.semaphore_wait(gate, 1)

    @pl.when(is_outer)
    def _():
        for k in range(8):
            o_send(k).start()

        @pl.when(odd == 0)
        def _():
            x_each(0, lambda c: c.start())
            for c in mlp_copies():
                c.start()
        for k in range(6):
            o_send(k).wait_send()
        release()
        for w in range(1, NW):
            x_each(w, lambda c: c.start())

    @pl.when(is_home)
    def _():
        for m in range(4):
            p_send(m).start()

        @pl.when(odd == 0)
        def _():
            for c in mlp_copies():
                c.start()
        cps = [local(cols_ref.at[2 * w + hb], cols.at[w], cols_sem.at[w]) for w in range(n_mb // 2)]
        for c in cps:
            c.start()
        for c in cps:
            c.wait()
        lane = lax.broadcasted_iota(jnp.int32, (RB, HEAD_DIM), 1)

        def zero_rows(b, carry):
            for i in range(4):
                kc[i, pl.ds(b * RB, RB), :] = jnp.zeros((RB, QL), BF16)
                vc[i, pl.ds(b * RB, RB), :] = jnp.zeros((RB, QL), BF16)
            return carry
        lax.fori_loop(0, S // RB, zero_rows, 0)

        def tables(w):
            def table_rows(b, carry):
                pos = cols[w, pl.ds(b * RB, RB), 0:1].astype(F32)
                ang = pos * invf_ref[0:1, :]
                table[w, pl.ds(b * RB, RB), :] = jnp.where(lane < HEAD_DIM // 2, jnp.cos(ang), jnp.sin(ang))
                return carry
            with jax.named_scope('table'):
                lax.fori_loop(0, S // RB, table_rows, 0)

        steps = [("o", 0), ("p", 0), ("t", 0), ("o", 1), ("p", 1), ("t", 1), ("o", 2), ("p", 2), ("t", 2), ("o", 3), ("p", 3), ("t", 3),
                 ("f", 0), ("f", 1), ("g", 0), ("f", 2), ("f", 3)]
        for kind, m in steps:
          with jax.named_scope('w_' + kind + str(m)):
            if kind == "o":
                o_send(m).wait_recv()
                f_send(m).start()
            elif kind == "p":
                p_send(m).wait_recv()
                x_send(1, m).start()
            elif kind == "f":
                f_send(m).wait_recv()
                x_send(2, m).start()
            elif kind == "g":
                release()
            elif m < n_mb // 2:
                tables(m)
        for w in range(NW):
            x_each(w, lambda c: c.start())
        w_ready([0, 1], range(3))

        @pl.when(s == 2)
        def _():
            for w in range(1, NW):
                for j in range(NJ):
                    @pl.when(z != j)
                    def _():
                        local(hin_hbm.at[w * NJ + j], hin_hbm.at[w * NJ + j], xp.at[w * NJ + j]).wait()
                        x_pass(w, j).start()

    def group_copies(g):
        p = g % 2
        if g < 4:
            return [local(own_w(m) if g == 0 else wqkv_hbm.at[g - 1, m], wst.at[p, m], wst_sem.at[p, m]) for m in range(3)]
        cps = []
        for m in range(3 if g == 4 else 1):
            n = (g - 4) * 3 + m
            for i in range(4):
                src = own_w(3) if i == 0 else wo_hbm.at[i - 1]
                cps.append(local(src.at[:, pl.ds(n * OB, OB)], wst.at[p, m, pl.ds(i * QL, QL), pl.ds(0, OB)], wo_sem.at[p, m, i]))
        return cps

    def group_start(g):
        for c in group_copies(g):
            c.start()

    def group_wait(g):
        for c in group_copies(g):
            c.wait()

    def h_fetch(u):
        mb = 2 * (u // NJ) + hb
        here = lax.rem(u, NJ) == z
        dst = hin.at[lax.rem(u, HS)]

        @pl.when((s == 0) & here)
        def _():
            local(x_ref.at[mb], dst, hv_sem).start()

        @pl.when((s == 0) & jnp.logical_not(here))
        def _():
            local(hin_hbm.at[u], hin_hbm.at[u], hin_sem.at[u]).wait()
            local(hin_hbm.at[u], dst, hv_sem).start()

    @pl.when(is_home)
    def _():
        group_start(0)
        group_start(1)
        h_fetch(0)

    for c in mlp_copies():
        c.wait()

    def hin_copy(u):
        return rcopy(h2b, hin.at[lax.rem(u, HS)], s5s, hin_sem.at[u], pp=lax.rem(s + 1, n_stages))

    def s1_outer(u):
        blk = gb.at[lax.rem(u, 3), pl.ds(pl.multiple_of(hb * T, T), T), :]
        return rcopy(blk, blk, s1s.at[0], ag.at[hb, lax.rem(u, 3)], tp=outer)

    def s1_peer(u):
        blk = gb.at[lax.rem(u, 3), pl.ds(pl.multiple_of(hb * T, T), T), :]
        return rcopy(blk, blk, s1s.at[1], ag.at[hb, lax.rem(u, 3)], tp=peer)

    def s2_copy(u):
        blk = gb.at[lax.rem(u, 3), pl.ds(pl.multiple_of((1 - hb) * T, T), T), :]
        return rcopy(blk, blk, s2s, ag.at[1 - hb, lax.rem(u, 3)], tp=outer)

    def ag_wait(b, u):
        blk = gb.at[lax.rem(u, 3), pl.ds(pl.multiple_of(b * T, T), T), :]
        local(blk, blk, ag.at[b, lax.rem(u, 3)]).wait()

    def s3_copy(u, b):
        sl = lax.rem(u, 2)
        blk = px.at[sl, pl.ds(pl.multiple_of(b * T, T), T), :]
        return rcopy(blk, blk, pxs.at[sl, b], pxr.at[sl, b], tp=inner)

    def s4_copy(u):
        return rcopy(sendb, ps.at[lax.rem(u, 2)], s4s, psr.at[lax.rem(u, 2)], tp=peer)

    def park_copy(u):
        return rcopy(h2b, hin_hbm.at[u], s5s, op.at[u], pp=1)

    def out_copy(u, mb, j):
        return rcopy(h2b, out_ref.at[mb], s5s, outr.at[mb], tp=j)

    def norm_rows(src, gain, dst):
        hf = src.astype(F32)
        inv = lax.rsqrt(jnp.mean(hf * hf, axis=-1, keepdims=True) + NORM_EPS)
        return (hf * inv * gain.astype(F32)).astype(BF16)

    def attention(u):
      with jax.named_scope('attn'):
        attention_(u)

    def attention_(u):
        w = u // NJ
        j = lax.rem(u, NJ)
        mb = 2 * w + hb
        row0 = pl.multiple_of(j * T, T)
        hs = lax.rem(u, HS)

        with jax.named_scope('w_hin'):
            @pl.when(s == 0)
            def _():
                local(x_ref.at[mb], hin.at[hs], hv_sem).wait()

            @pl.when(s > 0)
            def _():
                hin_copy(u).wait_recv()

        def norm_a(b, carry):
            rows = pl.ds(b * NR, NR)
            abuf[rows, :] = norm_rows(hin[hs, rows, :], ga_ref[0:1, :], None)
            return carry
        lax.fori_loop(0, T // NR, norm_a, 0)

        segc = cols[w, pl.ds(row0, T), 1:2]
        segr = seg_ref[pl.ds(mb, 1), :]
        ti = lax.broadcasted_iota(jnp.int32, (T, S), 0) + row0
        ui = lax.broadcasted_iota(jnp.int32, (T, S), 1)
        mask[...] = jnp.where((segc == segr) & (ui <= ti), 1.0, 0.0)

        def rope(val):
            pk = table[w, pl.ds(row0, T), :]
            lane = lax.broadcasted_iota(jnp.int32, (T, HEAD_DIM), 1)
            swapped = pltpu.roll(pk, HEAD_DIM // 2, 1)
            cosw = jnp.where(lane < HEAD_DIM // 2, pk, swapped)
            sinw = jnp.where(lane < HEAD_DIM // 2, -swapped, pk)
            outs = []
            for h in range(NH):
                v = val[:, h * HEAD_DIM:(h + 1) * HEAD_DIM]
                outs.append((v * cosw + pltpu.roll(v, HEAD_DIM // 2, 1) * sinw).astype(BF16))
            return outs

        def hcols(h):
            return slice(h * HEAD_DIM, (h + 1) * HEAD_DIM)

        def proj(i):
            p = i % 2
            for h, val in enumerate(rope(jnp.dot(abuf[...], wst[p, 0], preferred_element_type=F32))):
                qb[p, :, hcols(h)] = val
            for h, val in enumerate(rope(jnp.dot(abuf[...], wst[p, 1], preferred_element_type=F32))):
                kc[i, pl.ds(row0, T), hcols(h)] = val
            vc[i, pl.ds(row0, T), :] = jnp.dot(abuf[...], wst[p, 2], preferred_element_type=F32).astype(BF16)

        def heads(i):
            for h in range(NH):
                sc = lax.dot_general(qb[i % 2, :, hcols(h)], kc[i, :, hcols(h)], (((1,), (1,)), ((), ())),
                                     preferred_element_type=F32) * scale
                sbuf[h] = jnp.where(mask[...] > 0.5, sc, NEG)
            for h in range(NH):
                for r in range(0, T, 32):
                    sc = sbuf[h, r:r + 32, :]
                    e = jnp.exp(sc - jnp.max(sc, axis=-1, keepdims=True))
                    pbuf[h, r:r + 32, :] = (e * (1.0 / jnp.sum(e, axis=-1, keepdims=True))).astype(BF16)
            for h in range(NH):
                ob[:, i * QL + h * HEAD_DIM:i * QL + (h + 1) * HEAD_DIM] = jnp.dot(
                    pbuf[h], vc[i, :, hcols(h)], preferred_element_type=F32).astype(BF16)

        with jax.named_scope('shards'):
            group_wait(0)
            proj(0)
            group_start(2)
            for i in range(3):
                group_wait(i + 1)
                proj(i + 1)
                if i < 2:
                    @pl.when(u == 0)
                    def _():
                        if i == 0:
                            w_ready([2], range(3))
                        else:
                            w_ready([0, 1, 2], [3])
                group_start(i + 3)
                heads(i)
                if i == 0:
                    @pl.when(u < N - 1)
                    def _():
                        h_fetch(u + 1)
            group_wait(4)
            heads(3)
            finish(u)
        with jax.named_scope('wo'):
            for n in range(NO):
                if n == 3:
                    group_wait(5)
                yb[:, n * OB:(n + 1) * OB] = jnp.dot(ob[...], wst[n // 3, n % 3, :4 * QL, :OB], preferred_element_type=F32).astype(BF16)

        @pl.when(u < N - 1)
        def _():
            group_start(0)
            group_start(1)

        def norm_b(b, carry):
            rows = pl.ds(b * NR, NR)
            h1 = (hin[hs, rows, :].astype(F32) + yb[rows, :].astype(F32)).astype(BF16)
            h1b[lax.rem(u, 3), rows, :] = h1
            gb[lax.rem(u, 3), pl.ds(pl.multiple_of(hb * T + b * NR, NR), NR), :] = norm_rows(h1, gm_ref[0:1, :], None)
            return carry
        lax.fori_loop(0, T // NR, norm_b, 0)

        @pl.when((s > 0) & (u < N - HS))
        def _():
            pl.semaphore_signal(cred, inc=1, device_id={"pp": s - 1}, device_id_type=MESH)

    def mlp(sl, row0, rows, store):
        UN = 2 if NB % 2 == 0 else 1

        def up(q, carry):
            for n in [q * UN + k for k in range(UN)]:
                xin = gb[sl, pl.ds(row0, rows), :]
                g = jnp.dot(xin, wg_s[n], preferred_element_type=F32)
                u_ = jnp.dot(xin, wu_s[n], preferred_element_type=F32)
                act[0:rows, pl.ds(pl.multiple_of(n * FB, FB), FB)] = (jax.nn.silu(g) * u_).astype(BF16)
            return carry
        lax.fori_loop(0, NB // UN, up, 0)

        def down(q, carry):
            for n in [q * UN + k for k in range(UN)]:
                store(pl.ds(pl.multiple_of(n * DB, DB), DB), jnp.dot(act[0:rows, :], wd_s[n], preferred_element_type=F32))
            return carry
        lax.fori_loop(0, NB // UN, down, 0)

    def mlp_home(u):
        def store(c, val):
            pacc[:, c] = val
        with jax.named_scope('mlp'):
            mlp(lax.rem(u, 3), 0, 2 * T, store)

    def mlp_outer(u, b):
        def store(c, val):
            px[lax.rem(u, 2), pl.ds(pl.multiple_of(b * T, T), T), c] = val.astype(BF16)
        with jax.named_scope('mlp_o'):
            mlp(lax.rem(u, 3), pl.multiple_of(b * T, T), T, store)

    def forward(u):
        @pl.when((u >= 1) & (u <= N))
        def _():
            s2_copy(u - 1).wait_send()

        @pl.when(u < N)
        def _():
            with jax.named_scope('w_ag'):
                ag_wait(1 - hb, u)
            s2_copy(u).start()

    def combine(v):
        sl = lax.rem(v, 2)
        with jax.named_scope('w_s3'):
            s3_copy(v, 0).wait_recv()
            s3_copy(v, 1).wait_recv()

        @pl.when(v >= 1)
        def _():
            s4_copy(v - 1).wait_send()

        def comb(b, carry):
            rows = pl.ds(b * RB, RB)
            mine = pl.ds(pl.multiple_of(hb * T + b * RB, RB), RB)
            theirs = pl.ds(pl.multiple_of((1 - hb) * T + b * RB, RB), RB)
            oacc[rows, :] = pacc[mine, :] + px[sl, mine, :].astype(F32)
            sendb[rows, :] = (pacc[theirs, :] + px[sl, theirs, :].astype(F32)).astype(BF16)
            return carry
        lax.fori_loop(0, T // RB, comb, 0)
        s4_copy(v).start()

    def finish(u):
        @pl.when((u >= 2) & (u < N + 2))
        def _():
            v = u - 2
            with jax.named_scope('w_s4'):
                s4_copy(v).wait_recv()
            vw = v // NJ
            vj = lax.rem(v, NJ)

            @pl.when(v >= 1)
            def _():
                hin_copy(v).wait_send()

            def fin(b, carry):
                rows = pl.ds(b * RB, RB)
                d = (oacc[rows, :] + ps[lax.rem(v, 2), rows, :].astype(F32)).astype(BF16)
                h2b[rows, :] = (h1b[lax.rem(v, 3), rows, :].astype(F32) + d.astype(F32)).astype(BF16)
                return carry
            lax.fori_loop(0, T // RB, fin, 0)

            @pl.when((s < n_stages - 1) & (v >= HS))
            def _():
                with jax.named_scope('w_cred'):
                    pl.semaphore_wait(cred, 1)

            @pl.when(s < n_stages - 1)
            def _():
                hin_copy(v).start()

            @pl.when((s == n_stages - 1) & (v < N - NJ))
            def _():
                park_copy(v).start()

            @pl.when((s == n_stages - 1) & (v >= N - NJ) & (vj != z))
            def _():
                out_copy(v, 2 * vw + hb, vj).start()

            @pl.when((s == n_stages - 1) & (v >= N - NJ) & (vj == z))
            def _():
                local(h2b, out_ref.at[2 * vw + hb], s5s).start()

    def body(u, carry):
        @pl.when(is_home)
        def _():
            @pl.when(u < N)
            def _():
                attention(u)

            @pl.when(u >= N)
            def _():
                finish(u)

            @pl.when((u >= 1) & (u <= N))
            def _():
                s1_outer(u - 1).wait_send()
                s1_peer(u - 1).wait_send()

            @pl.when(u < N)
            def _():
                s1_peer(u).start()
                s1_outer(u).start()

            @pl.when((u >= 1) & (u <= N))
            def _():
                mlp_home(u - 1)

            forward(u)

            @pl.when((u >= 1) & (u <= N))
            def _():
                combine(u - 1)

        @pl.when(is_outer & (u < N))
        def _():
            for k in (0, 1):
                b = inner - 1 if k == 0 else 2 - inner
                with jax.named_scope('w_ag_outer'):
                    ag_wait(b, u)

                @pl.when(u >= 2)
                def _():
                    s3_copy(u - 2, b).wait_send()
                mlp_outer(u, b)
                s3_copy(u, b).start()

        v = u - 4

        @pl.when((s == n_stages - 1) & (v >= N - NJ) & (v < N) & (lax.rem(v, NJ) == z))
        def _():
            for b in (0, 1):
                mb = 2 * NW - 2 + b

                @pl.when(z - 1 != b)
                def _(mb=mb):
                    local(out_ref.at[mb], out_ref.at[mb], outr.at[mb]).wait()
                out_fwd(mb, 1, outr.at[mb]).start()
                out_fwd(mb, 2, outf).start()
        return carry

    def out_fwd(mb, p, sem):
        return rcopy(out_ref.at[mb], out_ref.at[mb], ofs.at[mb, p], sem, pp=p)

    lax.fori_loop(0, N + 4, body, 0)

    def od_copy(v):
        return rcopy(hin_hbm.at[v], out_ref.at[2 * (v // NJ) + hb], od.at[v], outr.at[2 * (v // NJ) + hb], tp=lax.rem(v, NJ))

    @pl.when(s == 1)
    def _():
        def spread(v, carry):
            vj = lax.rem(v, NJ)
            mine = 2 * (v // NJ) + hb

            @pl.when(is_home)
            def _():
                local(hin_hbm.at[v], hin_hbm.at[v], op.at[v]).wait()

            @pl.when(is_home & (vj != z))
            def _():
                od_copy(v).start()

            @pl.when(is_home & (vj == z))
            def _():
                c = local(hin_hbm.at[v], hin.at[0], hv_sem)
                c.start()
                c.wait()
                c = local(hin.at[0], out_ref.at[mine], hv_sem)
                c.start()
                c.wait()

            @pl.when(vj == z)
            def _():
                for b in (0, 1):
                    mb = 2 * (v // NJ) + b

                    @pl.when(z - 1 != b)
                    def _(mb=mb):
                        local(out_ref.at[mb], out_ref.at[mb], outr.at[mb]).wait()
                    for p in (3, 0, 2):
                        out_fwd(mb, p, outf).start()
            return carry
        lax.fori_loop(0, N - NJ, spread, 0)

        for b in (0, 1):
            mb = 2 * NW - 2 + b
            local(out_ref.at[mb], out_ref.at[mb], outr.at[mb]).wait()
            out_fwd(mb, 0, outf).start()

    @pl.when(is_home)
    def _():
        s4_copy(N - 1).wait_send()
        hin_copy(N - 1).wait_send()

    @pl.when(is_outer)
    def _():
        for b in (0, 1):
            s3_copy(N - 2, b).wait_send()
            s3_copy(N - 1, b).wait_send()

    @pl.when(is_outer)
    def _():
        for k in range(6, 8):
            o_send(k).wait_send()

    @pl.when(is_home)
    def _():
        for m in range(4):
            p_send(m).wait_send()
            f_send(m).wait_send()
            x_send(1, m).wait_send()
            x_send(2, m).wait_send()

        @pl.when(s == 2)
        def _():
            for w in range(1, NW):
                for j in range(NJ):
                    @pl.when(z != j)
                    def _():
                        x_pass(w, j).wait_send()

        @pl.when(s == 1)
        def _():
            def spread_done(v, carry):
                @pl.when(lax.rem(v, NJ) != z)
                def _():
                    od_copy(v).wait_send()
                return carry
            lax.fori_loop(0, N - NJ, spread_done, 0)

    for w in range(NW):
        x_each(w, lambda c: c.wait_send())

    @pl.when(s == 1)
    def _():
        for mb in range(n_mb - 2):
            for p in (3, 0, 2):
                out_fwd(mb, p, outf).wait_send()
        for mb in (n_mb - 2, n_mb - 1):
            out_fwd(mb, 0, outf).wait_send()

    @pl.when(s == n_stages - 1)
    def _():
        for mb in (n_mb - 2, n_mb - 1):
            for p in (1, 2):
                out_fwd(mb, p, outf).wait_send()
        early = out_ref.at[pl.ds(0, n_mb - 2)]
        local(early, early, outf).wait()

    @pl.when((s == 0) | (s == 2))
    def _():
        local(out_ref, out_ref, outf).wait()


def solution(mesh):
    n_stages = mesh.shape['pp']

    def stage_program(hidden_in, seg_ids, positions, attn_norm, w_query, w_key, w_value, w_out, mlp_norm, w_gate, w_up, w_down):
        n_mb, T, D = hidden_in.shape
        S = seg_ids.shape[1]
        QL = w_query.shape[2]
        FL = w_gate.shape[2]
        NJ = S // T
        N = (n_mb // 2) * NJ
        NB = max(1, FL // 512)
        cols = jnp.stack([positions, seg_ids], axis=-1)
        invf = jnp.asarray(np.tile(rope_freqs(), 2)[None, :], F32)
        any_spec = pl.BlockSpec(memory_space=pl.ANY)
        vmem = pl.BlockSpec(memory_space=pltpu.VMEM)
        dma = pltpu.SemaphoreType.DMA
        scratch = [
            pltpu.VMEM((NB, D, FL // NB), BF16), pltpu.VMEM((NB, D, FL // NB), BF16), pltpu.VMEM((NB, FL, D // NB), BF16),
            pltpu.VMEM((2, 3, max(D, 4 * QL), QL), BF16),
            pltpu.VMEM((3, 2 * T, D), BF16),
            pltpu.VMEM((2, 2 * T, D), BF16),
            pltpu.VMEM((2, T, D), BF16),
            pltpu.VMEM((4, S, QL), BF16), pltpu.VMEM((4, S, QL), BF16),
            pltpu.VMEM((4, T, D), BF16),
            pltpu.VMEM((3, T, D), BF16),
            pltpu.VMEM((2 * T, D), F32),
            pltpu.VMEM((T, D), F32),
            pltpu.VMEM((T, D), BF16),
            pltpu.VMEM((T, D), BF16),
            pltpu.VMEM((2 * T, FL), BF16),
            pltpu.VMEM((T, D), BF16),
            pltpu.VMEM((T, D), BF16),
            pltpu.VMEM((2, T, QL), BF16), pltpu.VMEM((T, 4 * QL), BF16),
            pltpu.VMEM((n_mb // 2, S, HEAD_DIM), F32),
            pltpu.VMEM((n_mb // 2, S, 2), jnp.int32),
            pltpu.VMEM((T, S), F32), pltpu.VMEM((QL // HEAD_DIM, T, S), F32), pltpu.VMEM((QL // HEAD_DIM, T, S), BF16),
            dma((3, 8)), dma((2, 4)), dma((8,)), dma((4,)), dma((2, 4)),
            dma((N,)), dma((n_mb // 2, 2)), dma((2, 3)), dma((2,)), dma, dma((2, 2)), dma((2, 2)), dma((2,)), dma, dma,
            dma((n_mb,)), dma, dma((n_mb, n_stages)),
            dma((2, 3)), dma((2, 3, 4)), dma((3, NB)), dma, dma((n_mb // 2,)), dma((N,)), dma((n_mb // 2, NJ)), dma((N,)), dma((N,)),
            pltpu.SemaphoreType.REGULAR, pltpu.SemaphoreType.REGULAR,
        ]
        return pl.pallas_call(
            functools.partial(kernel, n_stages),
            out_shape=[jax.ShapeDtypeStruct(hidden_in.shape, BF16), jax.ShapeDtypeStruct((3, 3, D, QL), BF16),
                       jax.ShapeDtypeStruct((3, QL, D), BF16), jax.ShapeDtypeStruct((N, T, D), BF16)],
            in_specs=[any_spec, vmem, any_spec, vmem, vmem, vmem] + [any_spec] * 7,
            out_specs=[any_spec] * 4,
            scratch_shapes=scratch,
            compiler_params=pltpu.CompilerParams(has_side_effects=True, vmem_limit_bytes=67_043_328),
        )(hidden_in, seg_ids, cols, invf, attn_norm, mlp_norm, w_query, w_key, w_value, w_out, w_gate, w_up, w_down)[0]

    act_spec = P('dp', 'tp', None)
    row_spec = P('dp', None)
    gain_spec = P('pp', None)
    col_spec = P('pp', None, 'tp')
    rows_spec = P('pp', 'tp', None)
    return jax.shard_map(stage_program, mesh=mesh,
                         in_specs=(act_spec, row_spec, row_spec, gain_spec, col_spec, col_spec, col_spec, rows_spec, gain_spec, col_spec, col_spec, rows_spec),
                         out_specs=act_spec, check_vma=False)
```

```python
import functools
import math

import jax
import jax.numpy as jnp
import numpy as np
from jax import lax
from jax.experimental import pallas as pl
from jax.experimental.pallas import tpu as pltpu
from jax.sharding import PartitionSpec as P

HEAD_DIM = 128
NORM_EPS = 1e-5
ROPE_THETA = 500000.0
ROPE_FACTOR = 8.0
LOW_FREQ = 1.0
HIGH_FREQ = 4.0
ORIG_CTX = 8192.0
NEG = -1e30
MESH = pl.DeviceIdType.MESH
F32 = jnp.float32
BF16 = jnp.bfloat16


def rope_freqs():
    base_freq = 1.0 / (ROPE_THETA ** (np.arange(0, HEAD_DIM, 2) / HEAD_DIM))
    wavelen = 2.0 * np.pi / base_freq
    smooth = (ORIG_CTX / wavelen - LOW_FREQ) / (HIGH_FREQ - LOW_FREQ)
    blended = (1.0 - smooth) * base_freq / ROPE_FACTOR + smooth * base_freq
    scaled = np.where(wavelen > ORIG_CTX / LOW_FREQ, base_freq / ROPE_FACTOR, blended)
    return np.where(wavelen < ORIG_CTX / HIGH_FREQ, base_freq, scaled)


def kernel(n_stages, x_ref, seg_ref, cols_ref, invf_ref, ga_ref, gm_ref,
           wq_ref, wk_ref, wv_ref, wo_ref, wg_ref, wu_ref, wd_ref,
           out_ref,
           wqkv_hbm, wo_hbm, hin_hbm,
           wg_s, wu_s, wd_s, wst, gb, px, ps, kc, vc, hin, h1b, pacc, oacc, sendb, h2b, act, yb, abuf, qb, ob,
           table, cols, mask, sbuf, pbuf,
           wr, wx, wsnd, wfwd, wxs, hin_sem, xs, ag, s1s, s2s, pxr, pxs, psr, s4s, s5s, outr, outf, ofs,
           wst_sem, wo_sem, mlp_sem, hv_sem, cols_sem, xp, xq, op, od, gate, cred):
    n_mb, T, D = x_ref.shape
    QL = wq_ref.shape[2]
    FL = wg_ref.shape[2]
    NB = wg_s.shape[0]
    FB = FL // NB
    S = seg_ref.shape[1]
    NJ = S // T
    NH = QL // HEAD_DIM
    N = (n_mb // 2) * NJ
    DB = D // NB
    scale = HEAD_DIM ** -0.5
    RB = 16
    NR = 32
    HS = hin.shape[0]
    OB = wst.shape[3]
    NO = D // OB

    hx = lax.axis_index("dp")
    z = lax.axis_index("tp")
    s = lax.axis_index("pp")
    is_home = (z == 1) | (z == 2)
    is_outer = (z == 0) | (z == 3)
    hb = lax.rem(z + 1, 2) * 0 + (z - 1)
    peer = 3 - z
    outer = 3 * (z - 1)
    inner = 1 + z // 2
    odd = lax.rem(s, 2)

    def rcopy(src, dst, ssem, rsem, **dev):
        return pltpu.make_async_remote_copy(src_ref=src, dst_ref=dst, send_sem=ssem, recv_sem=rsem,
                                            device_id=dev, device_id_type=MESH)

    def local(src, dst, sem):
        return pltpu.make_async_copy(src, dst, sem)

    wqkv_own = (wq_ref, wk_ref, wv_ref, wo_ref)

    def mlp_copies():
        cps = []
        for n in range(NB):
            cps.append(local(wg_ref.at[0, :, pl.ds(n * FB, FB)], wg_s.at[n], mlp_sem.at[0, n]))
            cps.append(local(wu_ref.at[0, :, pl.ds(n * FB, FB)], wu_s.at[n], mlp_sem.at[1, n]))
            cps.append(local(wd_ref.at[0, :, pl.ds(n * DB, DB)], wd_s.at[n], mlp_sem.at[2, n]))
        return cps

    NW = n_mb // 2

    def x_copy(w, home):
        u = w * NJ + z
        return rcopy(x_ref.at[2 * w + (home - 1)], hin_hbm.at[u], xs.at[w, home - 1], (hin_sem if w == 0 else xp).at[u], tp=home)

    def x_each(w, act):
        for home in (1, 2):
            @pl.when((s == (0 if w == 0 else 2)) & (z != home))
            def _():
                act(x_copy(w, home))

    def x_pass(w, j):
        u = w * NJ + j
        return rcopy(hin_hbm.at[u], hin_hbm.at[u], xq.at[w, j], hin_sem.at[u], pp=0)

    def half(ref, m, h):
        rows = (D if m < 3 else QL) // 2
        return ref.at[pl.ds(h * rows, rows), :]

    def wslot(r, m):
        return wqkv_hbm.at[r, m] if m < 3 else wo_hbm.at[r]

    def own_w(m):
        return wqkv_own[m].at[0]

    def o_send(k):
        h = hx if k < 4 else 1 - hx
        return rcopy(half(own_w(k % 4), k % 4, h), half(wslot(0, k % 4), k % 4, h), wsnd.at[k], wr.at[0, k], tp=inner)

    def p_send(m):
        return rcopy(half(own_w(m), m, hx), half(wslot(1, m), m, hx), wsnd.at[m], wr.at[1, m], tp=peer)

    def f_send(m):
        return rcopy(half(wslot(0, m), m, hx), half(wslot(2, m), m, hx), wfwd.at[m], wr.at[2, m], tp=peer)

    def x_send(r, m):
        return rcopy(half(wslot(r, m), m, hx), half(wslot(r, m), m, hx), wxs.at[r - 1, m], wx.at[r - 1, m], dp=1 - hx)

    def w_ready(rs, ms):
        for m in ms:
            if 0 in rs:
                o_send(4 + m).wait_recv()
            for r in (1, 2):
                if r in rs:
                    x_send(r, m).wait_recv()

    def release():
        @pl.when(odd == 0)
        def _():
            pl.semaphore_signal(gate, inc=1, device_id={"pp": s + 1}, device_id_type=MESH)

    @pl.when(odd == 1)
    def _():
        for c in mlp_copies():
            c.start()
        with jax.named_scope('w_gate'):
            pl.semaphore_wait(gate, 1)

    @pl.when(is_outer)
    def _():
        for k in range(8):
            o_send(k).start()

        @pl.when(odd == 0)
        def _():
            x_each(0, lambda c: c.start())
            for c in mlp_copies():
                c.start()
        for k in range(5):
            o_send(k).wait_send()
        release()
        for w in range(1, NW):
            x_each(w, lambda c: c.start())

    @pl.when(is_home)
    def _():
        for m in range(4):
            p_send(m).start()

        @pl.when(odd == 0)
        def _():
            for c in mlp_copies():
                c.start()
        cps = [local(cols_ref.at[2 * w + hb], cols.at[w], cols_sem.at[w]) for w in range(n_mb // 2)]
        for c in cps:
            c.start()
        for c in cps:
            c.wait()
        lane = lax.broadcasted_iota(jnp.int32, (RB, HEAD_DIM), 1)

        def zero_rows(b, carry):
            for i in range(4):
                kc[i, pl.ds(b * RB, RB), :] = jnp.zeros((RB, QL), BF16)
                vc[i, pl.ds(b * RB, RB), :] = jnp.zeros((RB, QL), BF16)
            return carry
        lax.fori_loop(0, S // RB, zero_rows, 0)

        def tables(w):
            def table_rows(b, carry):
                pos = cols[w, pl.ds(b * RB, RB), 0:1].astype(F32)
                ang = pos * invf_ref[0:1, :]
                table[w, pl.ds(b * RB, RB), :] = jnp.where(lane < HEAD_DIM // 2, jnp.cos(ang), jnp.sin(ang))
                return carry
            with jax.named_scope('table'):
                lax.fori_loop(0, S // RB, table_rows, 0)

        steps = [("o", 0), ("p", 0), ("t", 0), ("o", 1), ("p", 1), ("t", 1), ("o", 2), ("p", 2), ("t", 2), ("o", 3), ("p", 3), ("t", 3),
                 ("f", 0), ("g", 0), ("f", 1), ("f", 2), ("f", 3)]
        for kind, m in steps:
          with jax.named_scope('w_' + kind + str(m)):
            if kind == "o":
                o_send(m).wait_recv()
                f_send(m).start()
            elif kind == "p":
                p_send(m).wait_recv()
                x_send(1, m).start()
            elif kind == "f":
                f_send(m).wait_recv()
                x_send(2, m).start()
            elif kind == "g":
                release()
            elif m < n_mb // 2:
                tables(m)
        for w in range(NW):
            x_each(w, lambda c: c.start())
        w_ready([0, 1], range(3))

        @pl.when(s == 2)
        def _():
            for w in range(1, NW):
                for j in range(NJ):
                    @pl.when(z != j)
                    def _():
                        local(hin_hbm.at[w * NJ + j], hin_hbm.at[w * NJ + j], xp.at[w * NJ + j]).wait()
                        x_pass(w, j).start()

    def group_copies(g):
        p = g % 2
        if g < 4:
            return [local(own_w(m) if g == 0 else wqkv_hbm.at[g - 1, m], wst.at[p, m], wst_sem.at[p, m]) for m in range(3)]
        cps = []
        for m in range(3 if g == 4 else 1):
            n = (g - 4) * 3 + m
            for i in range(4):
                src = own_w(3) if i == 0 else wo_hbm.at[i - 1]
                cps.append(local(src.at[:, pl.ds(n * OB, OB)], wst.at[p, m, pl.ds(i * QL, QL), pl.ds(0, OB)], wo_sem.at[p, m, i]))
        return cps

    def group_start(g):
        for c in group_copies(g):
            c.start()

    def group_wait(g):
        for c in group_copies(g):
            c.wait()

    def h_fetch(u):
        mb = 2 * (u // NJ) + hb
        here = lax.rem(u, NJ) == z
        dst = hin.at[lax.rem(u, HS)]

        @pl.when((s == 0) & here)
        def _():
            local(x_ref.at[mb], dst, hv_sem).start()

        @pl.when((s == 0) & jnp.logical_not(here))
        def _():
            local(hin_hbm.at[u], hin_hbm.at[u], hin_sem.at[u]).wait()
            local(hin_hbm.at[u], dst, hv_sem).start()

    @pl.when(is_home)
    def _():
        group_start(0)
        group_start(1)
        h_fetch(0)

    for c in mlp_copies():
        c.wait()

    def hin_copy(u):
        return rcopy(h2b, hin.at[lax.rem(u, HS)], s5s, hin_sem.at[u], pp=lax.rem(s + 1, n_stages))

    def s1_outer(u):
        blk = gb.at[lax.rem(u, 3), pl.ds(pl.multiple_of(hb * T, T), T), :]
        return rcopy(blk, blk, s1s.at[0], ag.at[hb, lax.rem(u, 3)], tp=outer)

    def s1_peer(u):
        blk = gb.at[lax.rem(u, 3), pl.ds(pl.multiple_of(hb * T, T), T), :]
        return rcopy(blk, blk, s1s.at[1], ag.at[hb, lax.rem(u, 3)], tp=peer)

    def s2_copy(u):
        blk = gb.at[lax.rem(u, 3), pl.ds(pl.multiple_of((1 - hb) * T, T), T), :]
        return rcopy(blk, blk, s2s, ag.at[1 - hb, lax.rem(u, 3)], tp=outer)

    def ag_wait(b, u):
        blk = gb.at[lax.rem(u, 3), pl.ds(pl.multiple_of(b * T, T), T), :]
        local(blk, blk, ag.at[b, lax.rem(u, 3)]).wait()

    def s3_copy(u, b):
        sl = lax.rem(u, 2)
        blk = px.at[sl, pl.ds(pl.multiple_of(b * T, T), T), :]
        return rcopy(blk, blk, pxs.at[sl, b], pxr.at[sl, b], tp=inner)

    def s4_copy(u):
        return rcopy(sendb, ps.at[lax.rem(u, 2)], s4s, psr.at[lax.rem(u, 2)], tp=peer)

    def park_copy(u):
        return rcopy(h2b, hin_hbm.at[u], s5s, op.at[u], pp=1)

    def out_copy(u, mb, j):
        return rcopy(h2b, out_ref.at[mb], s5s, outr.at[mb], tp=j)

    def norm_rows(src, gain, dst):
        hf = src.astype(F32)
        inv = lax.rsqrt(jnp.mean(hf * hf, axis=-1, keepdims=True) + NORM_EPS)
        return (hf * inv * gain.astype(F32)).astype(BF16)

    def attention(u):
      with jax.named_scope('attn'):
        attention_(u)

    def attention_(u):
        w = u // NJ
        j = lax.rem(u, NJ)
        mb = 2 * w + hb
        row0 = pl.multiple_of(j * T, T)
        hs = lax.rem(u, HS)

        with jax.named_scope('w_hin'):
            @pl.when(s == 0)
            def _():
                local(x_ref.at[mb], hin.at[hs], hv_sem).wait()

            @pl.when(s > 0)
            def _():
                hin_copy(u).wait_recv()

        def norm_a(b, carry):
            rows = pl.ds(b * NR, NR)
            abuf[rows, :] = norm_rows(hin[hs, rows, :], ga_ref[0:1, :], None)
            return carry
        lax.fori_loop(0, T // NR, norm_a, 0)

        segc = cols[w, pl.ds(row0, T), 1:2]
        segr = seg_ref[pl.ds(mb, 1), :]
        ti = lax.broadcasted_iota(jnp.int32, (T, S), 0) + row0
        ui = lax.broadcasted_iota(jnp.int32, (T, S), 1)
        mask[...] = jnp.where((segc == segr) & (ui <= ti), 1.0, 0.0)

        def rope(val):
            pk = table[w, pl.ds(row0, T), :]
            lane = lax.broadcasted_iota(jnp.int32, (T, HEAD_DIM), 1)
            swapped = pltpu.roll(pk, HEAD_DIM // 2, 1)
            cosw = jnp.where(lane < HEAD_DIM // 2, pk, swapped)
            sinw = jnp.where(lane < HEAD_DIM // 2, -swapped, pk)
            outs = []
            for h in range(NH):
                v = val[:, h * HEAD_DIM:(h + 1) * HEAD_DIM]
                outs.append((v * cosw + pltpu.roll(v, HEAD_DIM // 2, 1) * sinw).astype(BF16))
            return outs

        def hcols(h):
            return slice(h * HEAD_DIM, (h + 1) * HEAD_DIM)

        def proj(i):
            p = i % 2
            for h, val in enumerate(rope(jnp.dot(abuf[...], wst[p, 0], preferred_element_type=F32))):
                qb[p, :, hcols(h)] = val
            for h, val in enumerate(rope(jnp.dot(abuf[...], wst[p, 1], preferred_element_type=F32))):
                kc[i, pl.ds(row0, T), hcols(h)] = val
            vc[i, pl.ds(row0, T), :] = jnp.dot(abuf[...], wst[p, 2], preferred_element_type=F32).astype(BF16)

        def heads(i):
            for h in range(NH):
                sc = lax.dot_general(qb[i % 2, :, hcols(h)], kc[i, :, hcols(h)], (((1,), (1,)), ((), ())),
                                     preferred_element_type=F32) * scale
                sbuf[h] = jnp.where(mask[...] > 0.5, sc, NEG)
            for h in range(NH):
                for r in range(0, T, 32):
                    sc = sbuf[h, r:r + 32, :]
                    e = jnp.exp(sc - jnp.max(sc, axis=-1, keepdims=True))
                    pbuf[h, r:r + 32, :] = (e * (1.0 / jnp.sum(e, axis=-1, keepdims=True))).astype(BF16)
            for h in range(NH):
                ob[:, i * QL + h * HEAD_DIM:i * QL + (h + 1) * HEAD_DIM] = jnp.dot(
                    pbuf[h], vc[i, :, hcols(h)], preferred_element_type=F32).astype(BF16)

        with jax.named_scope('shards'):
            group_wait(0)
            proj(0)
            group_start(2)
            for i in range(3):
                group_wait(i + 1)
                proj(i + 1)
                if i < 2:
                    @pl.when(u == 0)
                    def _():
                        if i == 0:
                            w_ready([2], range(3))
                        else:
                            w_ready([0, 1, 2], [3])
                group_start(i + 3)
                heads(i)
                if i == 1:
                    @pl.when(u >= 2)
                    def _():
                        combine(u - 2)
                if i == 0:
                    @pl.when(u < N - 1)
                    def _():
                        h_fetch(u + 1)
            group_wait(4)
            heads(3)
        with jax.named_scope('wo'):
            for n in range(NO):
                if n == 3:
                    group_wait(5)
                yb[:, n * OB:(n + 1) * OB] = jnp.dot(ob[...], wst[n // 3, n % 3, :4 * QL, :OB], preferred_element_type=F32).astype(BF16)

        @pl.when(u < N - 1)
        def _():
            group_start(0)
            group_start(1)

        def norm_b(b, carry):
            rows = pl.ds(b * NR, NR)
            h1 = (hin[hs, rows, :].astype(F32) + yb[rows, :].astype(F32)).astype(BF16)
            h1b[lax.rem(u, 3), rows, :] = h1
            gb[lax.rem(u, 3), pl.ds(pl.multiple_of(hb * T + b * NR, NR), NR), :] = norm_rows(h1, gm_ref[0:1, :], None)
            return carry
        lax.fori_loop(0, T // NR, norm_b, 0)

        @pl.when((s > 0) & (u < N - HS))
        def _():
            pl.semaphore_signal(cred, inc=1, device_id={"pp": s - 1}, device_id_type=MESH)

    def mlp(sl, row0, rows, store):
        UN = 2 if NB % 2 == 0 else 1

        def up(q, carry):
            for n in [q * UN + k for k in range(UN)]:
                xin = gb[sl, pl.ds(row0, rows), :]
                g = jnp.dot(xin, wg_s[n], preferred_element_type=F32)
                u_ = jnp.dot(xin, wu_s[n], preferred_element_type=F32)
                act[0:rows, pl.ds(pl.multiple_of(n * FB, FB), FB)] = (jax.nn.silu(g) * u_).astype(BF16)
            return carry
        lax.fori_loop(0, NB // UN, up, 0)

        def down(q, carry):
            for n in [q * UN + k for k in range(UN)]:
                store(pl.ds(pl.multiple_of(n * DB, DB), DB), jnp.dot(act[0:rows, :], wd_s[n], preferred_element_type=F32))
            return carry
        lax.fori_loop(0, NB // UN, down, 0)

    def mlp_home(u):
        def store(c, val):
            pacc[:, c] = val
        with jax.named_scope('mlp'):
            mlp(lax.rem(u, 3), 0, 2 * T, store)

    def mlp_outer(u, b):
        def store(c, val):
            px[lax.rem(u, 2), pl.ds(pl.multiple_of(b * T, T), T), c] = val.astype(BF16)
        with jax.named_scope('mlp_o'):
            mlp(lax.rem(u, 3), pl.multiple_of(b * T, T), T, store)

    def forward(u):
        @pl.when((u >= 1) & (u <= N))
        def _():
            s2_copy(u - 1).wait_send()

        @pl.when(u < N)
        def _():
            with jax.named_scope('w_ag'):
                ag_wait(1 - hb, u)
            s2_copy(u).start()

    def combine(v):
        sl = lax.rem(v, 2)
        with jax.named_scope('w_s3'):
            s3_copy(v, 0).wait_recv()
            s3_copy(v, 1).wait_recv()

        @pl.when(v >= 1)
        def _():
            s4_copy(v - 1).wait_send()

        def comb(b, carry):
            rows = pl.ds(b * RB, RB)
            mine = pl.ds(pl.multiple_of(hb * T + b * RB, RB), RB)
            theirs = pl.ds(pl.multiple_of((1 - hb) * T + b * RB, RB), RB)
            oacc[rows, :] = pacc[mine, :] + px[sl, mine, :].astype(F32)
            sendb[rows, :] = (pacc[theirs, :] + px[sl, theirs, :].astype(F32)).astype(BF16)
            return carry
        lax.fori_loop(0, T // RB, comb, 0)
        s4_copy(v).start()

    def finish(u):
        @pl.when((u >= 2) & (u < N + 2))
        def _():
            v = u - 2
            with jax.named_scope('w_s4'):
                s4_copy(v).wait_recv()
            vw = v // NJ
            vj = lax.rem(v, NJ)

            @pl.when(v >= 1)
            def _():
                hin_copy(v).wait_send()

            def fin(b, carry):
                rows = pl.ds(b * RB, RB)
                d = (oacc[rows, :] + ps[lax.rem(v, 2), rows, :].astype(F32)).astype(BF16)
                h2b[rows, :] = (h1b[lax.rem(v, 3), rows, :].astype(F32) + d.astype(F32)).astype(BF16)
                return carry
            lax.fori_loop(0, T // RB, fin, 0)

            @pl.when((s < n_stages - 1) & (v >= HS))
            def _():
                with jax.named_scope('w_cred'):
                    pl.semaphore_wait(cred, 1)

            @pl.when(s < n_stages - 1)
            def _():
                hin_copy(v).start()

            @pl.when((s == n_stages - 1) & (v < N - NJ))
            def _():
                park_copy(v).start()

            @pl.when((s == n_stages - 1) & (v >= N - NJ) & (vj != z))
            def _():
                out_copy(v, 2 * vw + hb, vj).start()

            @pl.when((s == n_stages - 1) & (v >= N - NJ) & (vj == z))
            def _():
                local(h2b, out_ref.at[2 * vw + hb], s5s).start()

    def body(u, carry):
        @pl.when(is_home)
        def _():
            @pl.when(u < N)
            def _():
                attention(u)

            @pl.when((u >= N) & (u < N + 2))
            def _():
                combine(u - 2)

            @pl.when((u >= 1) & (u <= N))
            def _():
                s1_outer(u - 1).wait_send()
                s1_peer(u - 1).wait_send()

            @pl.when(u < N)
            def _():
                s1_peer(u).start()
                s1_outer(u).start()

            @pl.when((u >= 1) & (u <= N))
            def _():
                mlp_home(u - 1)

            finish(u)
            forward(u)

        @pl.when(is_outer & (u < N))
        def _():
            for k in (0, 1):
                b = inner - 1 if k == 0 else 2 - inner
                with jax.named_scope('w_ag_outer'):
                    ag_wait(b, u)

                @pl.when(u >= 2)
                def _():
                    s3_copy(u - 2, b).wait_send()
                mlp_outer(u, b)
                s3_copy(u, b).start()

        v = u - 4

        @pl.when((s == n_stages - 1) & (v >= N - NJ) & (v < N) & (lax.rem(v, NJ) == z))
        def _():
            for b in (0, 1):
                mb = 2 * NW - 2 + b

                @pl.when(z - 1 != b)
                def _(mb=mb):
                    local(out_ref.at[mb], out_ref.at[mb], outr.at[mb]).wait()
                out_fwd(mb, 1, outr.at[mb]).start()
                out_fwd(mb, 2, outf).start()
        return carry

    def out_fwd(mb, p, sem):
        return rcopy(out_ref.at[mb], out_ref.at[mb], ofs.at[mb, p], sem, pp=p)

    lax.fori_loop(0, N + 4, body, 0)

    def od_copy(v):
        return rcopy(hin_hbm.at[v], out_ref.at[2 * (v // NJ) + hb], od.at[v], outr.at[2 * (v // NJ) + hb], tp=lax.rem(v, NJ))

    @pl.when(s == 1)
    def _():
        def spread(v, carry):
            vj = lax.rem(v, NJ)
            mine = 2 * (v // NJ) + hb

            @pl.when(is_home)
            def _():
                local(hin_hbm.at[v], hin_hbm.at[v], op.at[v]).wait()

            @pl.when(is_home & (vj != z))
            def _():
                od_copy(v).start()

            @pl.when(is_home & (vj == z))
            def _():
                c = local(hin_hbm.at[v], hin.at[0], hv_sem)
                c.start()
                c.wait()
                c = local(hin.at[0], out_ref.at[mine], hv_sem)
                c.start()
                c.wait()

            @pl.when(vj == z)
            def _():
                for b in (0, 1):
                    mb = 2 * (v // NJ) + b

                    @pl.when(z - 1 != b)
                    def _(mb=mb):
                        local(out_ref.at[mb], out_ref.at[mb], outr.at[mb]).wait()
                    for p in (3, 0, 2):
                        out_fwd(mb, p, outf).start()
            return carry
        lax.fori_loop(0, N - NJ, spread, 0)

        for b in (0, 1):
            mb = 2 * NW - 2 + b
            local(out_ref.at[mb], out_ref.at[mb], outr.at[mb]).wait()
            out_fwd(mb, 0, outf).start()

    @pl.when(is_home)
    def _():
        s4_copy(N - 1).wait_send()
        hin_copy(N - 1).wait_send()

    @pl.when(is_outer)
    def _():
        for b in (0, 1):
            s3_copy(N - 2, b).wait_send()
            s3_copy(N - 1, b).wait_send()

    @pl.when(is_outer)
    def _():
        for k in range(5, 8):
            o_send(k).wait_send()

    @pl.when(is_home)
    def _():
        for m in range(4):
            p_send(m).wait_send()
            f_send(m).wait_send()
            x_send(1, m).wait_send()
            x_send(2, m).wait_send()

        @pl.when(s == 2)
        def _():
            for w in range(1, NW):
                for j in range(NJ):
                    @pl.when(z != j)
                    def _():
                        x_pass(w, j).wait_send()

        @pl.when(s == 1)
        def _():
            def spread_done(v, carry):
                @pl.when(lax.rem(v, NJ) != z)
                def _():
                    od_copy(v).wait_send()
                return carry
            lax.fori_loop(0, N - NJ, spread_done, 0)

    for w in range(NW):
        x_each(w, lambda c: c.wait_send())

    @pl.when(s == 1)
    def _():
        for mb in range(n_mb - 2):
            for p in (3, 0, 2):
                out_fwd(mb, p, outf).wait_send()
        for mb in (n_mb - 2, n_mb - 1):
            out_fwd(mb, 0, outf).wait_send()

    @pl.when(s == n_stages - 1)
    def _():
        for mb in (n_mb - 2, n_mb - 1):
            for p in (1, 2):
                out_fwd(mb, p, outf).wait_send()
        early = out_ref.at[pl.ds(0, n_mb - 2)]
        local(early, early, outf).wait()

    @pl.when((s == 0) | (s == 2))
    def _():
        local(out_ref, out_ref, outf).wait()


def solution(mesh):
    n_stages = mesh.shape['pp']

    def stage_program(hidden_in, seg_ids, positions, attn_norm, w_query, w_key, w_value, w_out, mlp_norm, w_gate, w_up, w_down):
        n_mb, T, D = hidden_in.shape
        S = seg_ids.shape[1]
        QL = w_query.shape[2]
        FL = w_gate.shape[2]
        NJ = S // T
        N = (n_mb // 2) * NJ
        NB = max(1, FL // 512)
        cols = jnp.stack([positions, seg_ids], axis=-1)
        invf = jnp.asarray(np.tile(rope_freqs(), 2)[None, :], F32)
        any_spec = pl.BlockSpec(memory_space=pl.ANY)
        vmem = pl.BlockSpec(memory_space=pltpu.VMEM)
        dma = pltpu.SemaphoreType.DMA
        scratch = [
            pltpu.VMEM((NB, D, FL // NB), BF16), pltpu.VMEM((NB, D, FL // NB), BF16), pltpu.VMEM((NB, FL, D // NB), BF16),
            pltpu.VMEM((2, 3, max(D, 4 * QL), QL), BF16),
            pltpu.VMEM((3, 2 * T, D), BF16),
            pltpu.VMEM((2, 2 * T, D), BF16),
            pltpu.VMEM((2, T, D), BF16),
            pltpu.VMEM((4, S, QL), BF16), pltpu.VMEM((4, S, QL), BF16),
            pltpu.VMEM((4, T, D), BF16),
            pltpu.VMEM((3, T, D), BF16),
            pltpu.VMEM((2 * T, D), F32),
            pltpu.VMEM((T, D), F32),
            pltpu.VMEM((T, D), BF16),
            pltpu.VMEM((T, D), BF16),
            pltpu.VMEM((2 * T, FL), BF16),
            pltpu.VMEM((T, D), BF16),
            pltpu.VMEM((T, D), BF16),
            pltpu.VMEM((2, T, QL), BF16), pltpu.VMEM((T, 4 * QL), BF16),
            pltpu.VMEM((n_mb // 2, S, HEAD_DIM), F32),
            pltpu.VMEM((n_mb // 2, S, 2), jnp.int32),
            pltpu.VMEM((T, S), F32), pltpu.VMEM((QL // HEAD_DIM, T, S), F32), pltpu.VMEM((QL // HEAD_DIM, T, S), BF16),
            dma((3, 8)), dma((2, 4)), dma((8,)), dma((4,)), dma((2, 4)),
            dma((N,)), dma((n_mb // 2, 2)), dma((2, 3)), dma((2,)), dma, dma((2, 2)), dma((2, 2)), dma((2,)), dma, dma,
            dma((n_mb,)), dma, dma((n_mb, n_stages)),
            dma((2, 3)), dma((2, 3, 4)), dma((3, NB)), dma, dma((n_mb // 2,)), dma((N,)), dma((n_mb // 2, NJ)), dma((N,)), dma((N,)),
            pltpu.SemaphoreType.REGULAR, pltpu.SemaphoreType.REGULAR,
        ]
        return pl.pallas_call(
            functools.partial(kernel, n_stages),
            out_shape=[jax.ShapeDtypeStruct(hidden_in.shape, BF16), jax.ShapeDtypeStruct((3, 3, D, QL), BF16),
                       jax.ShapeDtypeStruct((3, QL, D), BF16), jax.ShapeDtypeStruct((N, T, D), BF16)],
            in_specs=[any_spec, vmem, any_spec, vmem, vmem, vmem] + [any_spec] * 7,
            out_specs=[any_spec] * 4,
            scratch_shapes=scratch,
            compiler_params=pltpu.CompilerParams(has_side_effects=True, vmem_limit_bytes=67_043_328),
        )(hidden_in, seg_ids, cols, invf, attn_norm, mlp_norm, w_query, w_key, w_value, w_out, w_gate, w_up, w_down)[0]

    act_spec = P('dp', 'tp', None)
    row_spec = P('dp', None)
    gain_spec = P('pp', None)
    col_spec = P('pp', None, 'tp')
    rows_spec = P('pp', 'tp', None)
    return jax.shard_map(stage_program, mesh=mesh,
                         in_specs=(act_spec, row_spec, row_spec, gain_spec, col_spec, col_spec, col_spec, rows_spec, gain_spec, col_spec, col_spec, rows_spec),
                         out_specs=act_spec, check_vma=False)
```

```python
import functools
import math

import jax
import jax.numpy as jnp
import numpy as np
from jax import lax
from jax.experimental import pallas as pl
from jax.experimental.pallas import tpu as pltpu
from jax.sharding import PartitionSpec as P

HEAD_DIM = 128
NORM_EPS = 1e-5
ROPE_THETA = 500000.0
ROPE_FACTOR = 8.0
LOW_FREQ = 1.0
HIGH_FREQ = 4.0
ORIG_CTX = 8192.0
NEG = -1e30
MESH = pl.DeviceIdType.MESH
F32 = jnp.float32
BF16 = jnp.bfloat16


def rope_freqs():
    base_freq = 1.0 / (ROPE_THETA ** (np.arange(0, HEAD_DIM, 2) / HEAD_DIM))
    wavelen = 2.0 * np.pi / base_freq
    smooth = (ORIG_CTX / wavelen - LOW_FREQ) / (HIGH_FREQ - LOW_FREQ)
    blended = (1.0 - smooth) * base_freq / ROPE_FACTOR + smooth * base_freq
    scaled = np.where(wavelen > ORIG_CTX / LOW_FREQ, base_freq / ROPE_FACTOR, blended)
    return np.where(wavelen < ORIG_CTX / HIGH_FREQ, base_freq, scaled)


def kernel(n_stages, x_ref, seg_ref, cols_ref, invf_ref, ga_ref, gm_ref,
           wq_ref, wk_ref, wv_ref, wo_ref, wg_ref, wu_ref, wd_ref,
           out_ref,
           wqkv_hbm, wo_hbm, hin_hbm,
           wg_s, wu_s, wd_s, wst, gb, px, ps, kc, vc, hin, h1b, pacc, oacc, sendb, h2b, act, yb, abuf, qb, ob,
           table, cols, mask, sbuf, pbuf,
           wr, wx, wsnd, wfwd, wxs, hin_sem, xs, ag, s1s, s2s, pxr, pxs, psr, s4s, s5s, outr, outf, ofs,
           wst_sem, wo_sem, mlp_sem, hv_sem, cols_sem, xp, xq, op, od, gate, cred):
    n_mb, T, D = x_ref.shape
    QL = wq_ref.shape[2]
    FL = wg_ref.shape[2]
    NB = wg_s.shape[0]
    FB = FL // NB
    S = seg_ref.shape[1]
    NJ = S // T
    NH = QL // HEAD_DIM
    N = (n_mb // 2) * NJ
    DB = D // NB
    scale = HEAD_DIM ** -0.5
    RB = 16
    NR = 32
    HS = hin.shape[0]
    OB = wst.shape[3]
    NO = D // OB

    hx = lax.axis_index("dp")
    z = lax.axis_index("tp")
    s = lax.axis_index("pp")
    is_home = (z == 1) | (z == 2)
    is_outer = (z == 0) | (z == 3)
    hb = lax.rem(z + 1, 2) * 0 + (z - 1)
    peer = 3 - z
    outer = 3 * (z - 1)
    inner = 1 + z // 2
    odd = lax.rem(s, 2)

    def rcopy(src, dst, ssem, rsem, **dev):
        return pltpu.make_async_remote_copy(src_ref=src, dst_ref=dst, send_sem=ssem, recv_sem=rsem,
                                            device_id=dev, device_id_type=MESH)

    def local(src, dst, sem):
        return pltpu.make_async_copy(src, dst, sem)

    wqkv_own = (wq_ref, wk_ref, wv_ref, wo_ref)

    def mlp_copies():
        cps = []
        for n in range(NB):
            cps.append(local(wg_ref.at[0, :, pl.ds(n * FB, FB)], wg_s.at[n], mlp_sem.at[0, n]))
            cps.append(local(wu_ref.at[0, :, pl.ds(n * FB, FB)], wu_s.at[n], mlp_sem.at[1, n]))
            cps.append(local(wd_ref.at[0, :, pl.ds(n * DB, DB)], wd_s.at[n], mlp_sem.at[2, n]))
        return cps

    NW = n_mb // 2

    def x_copy(w, home):
        u = w * NJ + z
        return rcopy(x_ref.at[2 * w + (home - 1)], hin_hbm.at[u], xs.at[w, home - 1], (hin_sem if w == 0 else xp).at[u], tp=home)

    def x_each(w, act):
        for home in (1, 2):
            @pl.when((s == (0 if w == 0 else 2)) & (z != home))
            def _():
                act(x_copy(w, home))

    def x_pass(w, j):
        u = w * NJ + j
        return rcopy(hin_hbm.at[u], hin_hbm.at[u], xq.at[w, j], hin_sem.at[u], pp=0)

    def half(ref, m, h):
        rows = (D if m < 3 else QL) // 2
        return ref.at[pl.ds(h * rows, rows), :]

    def wslot(r, m):
        return wqkv_hbm.at[r, m] if m < 3 else wo_hbm.at[r]

    def own_w(m):
        return wqkv_own[m].at[0]

    def o_send(k):
        h = hx if k < 4 else 1 - hx
        return rcopy(half(own_w(k % 4), k % 4, h), half(wslot(0, k % 4), k % 4, h), wsnd.at[k], wr.at[0, k], tp=inner)

    def p_send(m):
        return rcopy(half(own_w(m), m, hx), half(wslot(1, m), m, hx), wsnd.at[m], wr.at[1, m], tp=peer)

    def f_send(m):
        return rcopy(half(wslot(0, m), m, hx), half(wslot(2, m), m, hx), wfwd.at[m], wr.at[2, m], tp=peer)

    def x_send(r, m):
        return rcopy(half(wslot(r, m), m, hx), half(wslot(r, m), m, hx), wxs.at[r - 1, m], wx.at[r - 1, m], dp=1 - hx)

    def w_ready(rs, ms):
        for m in ms:
            if 0 in rs:
                o_send(4 + m).wait_recv()
            for r in (1, 2):
                if r in rs:
                    x_send(r, m).wait_recv()

    def release():
        @pl.when(odd == 0)
        def _():
            pl.semaphore_signal(gate, inc=1, device_id={"pp": s + 1}, device_id_type=MESH)

    @pl.when(odd == 1)
    def _():
        for c in mlp_copies():
            c.start()
        with jax.named_scope('w_gate'):
            pl.semaphore_wait(gate, 1)

    @pl.when(is_outer)
    def _():
        for k in range(8):
            o_send(k).start()

        @pl.when(odd == 0)
        def _():
            x_each(0, lambda c: c.start())
            for c in mlp_copies():
                c.start()
        for k in range(5):
            o_send(k).wait_send()
        release()
        for w in range(1, NW):
            x_each(w, lambda c: c.start())

    @pl.when(is_home)
    def _():
        for m in range(4):
            p_send(m).start()

        @pl.when(odd == 0)
        def _():
            for c in mlp_copies():
                c.start()
        cps = [local(cols_ref.at[2 * w + hb], cols.at[w], cols_sem.at[w]) for w in range(n_mb // 2)]
        for c in cps:
            c.start()
        for c in cps:
            c.wait()
        lane = lax.broadcasted_iota(jnp.int32, (RB, HEAD_DIM), 1)

        def zero_rows(b, carry):
            for i in range(4):
                kc[i, pl.ds(b * RB, RB), :] = jnp.zeros((RB, QL), BF16)
                vc[i, pl.ds(b * RB, RB), :] = jnp.zeros((RB, QL), BF16)
            return carry
        lax.fori_loop(0, S // RB, zero_rows, 0)

        def tables(w):
            def table_rows(b, carry):
                pos = cols[w, pl.ds(b * RB, RB), 0:1].astype(F32)
                ang = pos * invf_ref[0:1, :]
                table[w, pl.ds(b * RB, RB), :] = jnp.where(lane < HEAD_DIM // 2, jnp.cos(ang), jnp.sin(ang))
                return carry
            with jax.named_scope('table'):
                lax.fori_loop(0, S // RB, table_rows, 0)

        steps = [("o", 0), ("p", 0), ("t", 0), ("o", 1), ("p", 1), ("t", 1), ("o", 2), ("p", 2), ("t", 2), ("o", 3), ("p", 3), ("t", 3),
                 ("f", 0), ("g", 0), ("f", 1), ("f", 2), ("f", 3)]
        for kind, m in steps:
          with jax.named_scope('w_' + kind + str(m)):
            if kind == "o":
                o_send(m).wait_recv()
                f_send(m).start()
            elif kind == "p":
                p_send(m).wait_recv()
                x_send(1, m).start()
            elif kind == "f":
                f_send(m).wait_recv()
                x_send(2, m).start()
            elif kind == "g":
                release()
            elif m < n_mb // 2:
                tables(m)
        for w in range(NW):
            x_each(w, lambda c: c.start())
        w_ready([0, 1], range(3))

        @pl.when(s == 2)
        def _():
            for w in range(1, NW):
                for j in range(NJ):
                    @pl.when(z != j)
                    def _():
                        local(hin_hbm.at[w * NJ + j], hin_hbm.at[w * NJ + j], xp.at[w * NJ + j]).wait()
                        x_pass(w, j).start()

    def group_copies(g):
        p = g % 2
        if g < 4:
            return [local(own_w(m) if g == 0 else wqkv_hbm.at[g - 1, m], wst.at[p, m], wst_sem.at[p, m]) for m in range(3)]
        cps = []
        for m in range(3 if g == 4 else 1):
            n = (g - 4) * 3 + m
            for i in range(4):
                src = own_w(3) if i == 0 else wo_hbm.at[i - 1]
                cps.append(local(src.at[:, pl.ds(n * OB, OB)], wst.at[p, m, pl.ds(i * QL, QL), pl.ds(0, OB)], wo_sem.at[p, m, i]))
        return cps

    def group_start(g):
        for c in group_copies(g):
            c.start()

    def group_wait(g):
        for c in group_copies(g):
            c.wait()

    def h_fetch(u):
        mb = 2 * (u // NJ) + hb
        here = lax.rem(u, NJ) == z
        dst = hin.at[lax.rem(u, HS)]

        @pl.when((s == 0) & here)
        def _():
            local(x_ref.at[mb], dst, hv_sem).start()

        @pl.when((s == 0) & jnp.logical_not(here))
        def _():
            local(hin_hbm.at[u], hin_hbm.at[u], hin_sem.at[u]).wait()
            local(hin_hbm.at[u], dst, hv_sem).start()

    @pl.when(is_home)
    def _():
        group_start(0)
        group_start(1)
        h_fetch(0)

    for c in mlp_copies():
        c.wait()

    def hin_copy(u):
        return rcopy(h2b, hin.at[lax.rem(u, HS)], s5s, hin_sem.at[u], pp=lax.rem(s + 1, n_stages))

    def s1_outer(u):
        blk = gb.at[lax.rem(u, 3), pl.ds(pl.multiple_of(hb * T, T), T), :]
        return rcopy(blk, blk, s1s.at[0], ag.at[hb, lax.rem(u, 3)], tp=outer)

    def s1_peer(u):
        blk = gb.at[lax.rem(u, 3), pl.ds(pl.multiple_of(hb * T, T), T), :]
        return rcopy(blk, blk, s1s.at[1], ag.at[hb, lax.rem(u, 3)], tp=peer)

    def s2_copy(u):
        blk = gb.at[lax.rem(u, 3), pl.ds(pl.multiple_of((1 - hb) * T, T), T), :]
        return rcopy(blk, blk, s2s, ag.at[1 - hb, lax.rem(u, 3)], tp=outer)

    def ag_wait(b, u):
        blk = gb.at[lax.rem(u, 3), pl.ds(pl.multiple_of(b * T, T), T), :]
        local(blk, blk, ag.at[b, lax.rem(u, 3)]).wait()

    def s3_copy(u, b):
        sl = lax.rem(u, 2)
        blk = px.at[sl, pl.ds(pl.multiple_of(b * T, T), T), :]
        return rcopy(blk, blk, pxs.at[sl, b], pxr.at[sl, b], tp=inner)

    def s4_copy(u):
        return rcopy(sendb, ps.at[lax.rem(u, 2)], s4s, psr.at[lax.rem(u, 2)], tp=peer)

    def park_copy(u):
        return rcopy(h2b, hin_hbm.at[u], s5s, op.at[u], pp=1)

    def out_copy(u, mb, j):
        return rcopy(h2b, out_ref.at[mb], s5s, outr.at[mb], tp=j)

    def norm_rows(src, gain, dst):
        hf = src.astype(F32)
        inv = lax.rsqrt(jnp.mean(hf * hf, axis=-1, keepdims=True) + NORM_EPS)
        return (hf * inv * gain.astype(F32)).astype(BF16)

    def attention(u):
      with jax.named_scope('attn'):
        attention_(u)

    def attention_(u):
        w = u // NJ
        j = lax.rem(u, NJ)
        mb = 2 * w + hb
        row0 = pl.multiple_of(j * T, T)
        hs = lax.rem(u, HS)

        with jax.named_scope('w_hin'):
            @pl.when(s == 0)
            def _():
                local(x_ref.at[mb], hin.at[hs], hv_sem).wait()

            @pl.when(s > 0)
            def _():
                hin_copy(u).wait_recv()

        def norm_a(b, carry):
            rows = pl.ds(b * NR, NR)
            abuf[rows, :] = norm_rows(hin[hs, rows, :], ga_ref[0:1, :], None)
            return carry
        lax.fori_loop(0, T // NR, norm_a, 0)

        segc = cols[w, pl.ds(row0, T), 1:2]
        segr = seg_ref[pl.ds(mb, 1), :]
        ti = lax.broadcasted_iota(jnp.int32, (T, S), 0) + row0
        ui = lax.broadcasted_iota(jnp.int32, (T, S), 1)
        mask[...] = jnp.where((segc == segr) & (ui <= ti), 1.0, 0.0)

        def rope(val):
            pk = table[w, pl.ds(row0, T), :]
            lane = lax.broadcasted_iota(jnp.int32, (T, HEAD_DIM), 1)
            swapped = pltpu.roll(pk, HEAD_DIM // 2, 1)
            cosw = jnp.where(lane < HEAD_DIM // 2, pk, swapped)
            sinw = jnp.where(lane < HEAD_DIM // 2, -swapped, pk)
            outs = []
            for h in range(NH):
                v = val[:, h * HEAD_DIM:(h + 1) * HEAD_DIM]
                outs.append((v * cosw + pltpu.roll(v, HEAD_DIM // 2, 1) * sinw).astype(BF16))
            return outs

        def hcols(h):
            return slice(h * HEAD_DIM, (h + 1) * HEAD_DIM)

        def proj(i):
            p = i % 2
            for h, val in enumerate(rope(jnp.dot(abuf[...], wst[p, 0], preferred_element_type=F32))):
                qb[p, :, hcols(h)] = val
            for h, val in enumerate(rope(jnp.dot(abuf[...], wst[p, 1], preferred_element_type=F32))):
                kc[i, pl.ds(row0, T), hcols(h)] = val
            vc[i, pl.ds(row0, T), :] = jnp.dot(abuf[...], wst[p, 2], preferred_element_type=F32).astype(BF16)

        def heads(i):
            for h in range(NH):
                sc = lax.dot_general(qb[i % 2, :, hcols(h)], kc[i, :, hcols(h)], (((1,), (1,)), ((), ())),
                                     preferred_element_type=F32) * scale
                sbuf[h] = jnp.where(mask[...] > 0.5, sc, NEG)
            for h in range(NH):
                for r in range(0, T, 32):
                    sc = sbuf[h, r:r + 32, :]
                    e = jnp.exp(sc - jnp.max(sc, axis=-1, keepdims=True))
                    pbuf[h, r:r + 32, :] = (e * (1.0 / jnp.sum(e, axis=-1, keepdims=True))).astype(BF16)
            for h in range(NH):
                ob[:, i * QL + h * HEAD_DIM:i * QL + (h + 1) * HEAD_DIM] = jnp.dot(
                    pbuf[h], vc[i, :, hcols(h)], preferred_element_type=F32).astype(BF16)

        with jax.named_scope('shards'):
            group_wait(0)
            proj(0)
            group_start(2)
            for i in range(3):
                group_wait(i + 1)
                proj(i + 1)
                if i < 2:
                    @pl.when(u == 0)
                    def _():
                        if i == 0:
                            w_ready([2], range(3))
                        else:
                            w_ready([0, 1, 2], [3])
                group_start(i + 3)
                heads(i)
                if i == 0:
                    @pl.when(u < N - 1)
                    def _():
                        h_fetch(u + 1)
            group_wait(4)
            heads(3)
        with jax.named_scope('wo'):
            for n in range(NO):
                if n == 3:
                    group_wait(5)
                yb[:, n * OB:(n + 1) * OB] = jnp.dot(ob[...], wst[n // 3, n % 3, :4 * QL, :OB], preferred_element_type=F32).astype(BF16)

        @pl.when(u < N - 1)
        def _():
            group_start(0)
            group_start(1)

        def norm_b(b, carry):
            rows = pl.ds(b * NR, NR)
            h1 = (hin[hs, rows, :].astype(F32) + yb[rows, :].astype(F32)).astype(BF16)
            h1b[lax.rem(u, 3), rows, :] = h1
            gb[lax.rem(u, 3), pl.ds(pl.multiple_of(hb * T + b * NR, NR), NR), :] = norm_rows(h1, gm_ref[0:1, :], None)
            return carry
        lax.fori_loop(0, T // NR, norm_b, 0)

        @pl.when((s > 0) & (u < N - HS))
        def _():
            pl.semaphore_signal(cred, inc=1, device_id={"pp": s - 1}, device_id_type=MESH)

    def mlp(sl, row0, rows, store):
        UN = 2 if NB % 2 == 0 else 1

        def up(q, carry):
            for n in [q * UN + k for k in range(UN)]:
                xin = gb[sl, pl.ds(row0, rows), :]
                g = jnp.dot(xin, wg_s[n], preferred_element_type=F32)
                u_ = jnp.dot(xin, wu_s[n], preferred_element_type=F32)
                act[0:rows, pl.ds(pl.multiple_of(n * FB, FB), FB)] = (jax.nn.silu(g) * u_).astype(BF16)
            return carry
        lax.fori_loop(0, NB // UN, up, 0)

        def down(q, carry):
            for n in [q * UN + k for k in range(UN)]:
                store(pl.ds(pl.multiple_of(n * DB, DB), DB), jnp.dot(act[0:rows, :], wd_s[n], preferred_element_type=F32))
            return carry
        lax.fori_loop(0, NB // UN, down, 0)

    def mlp_home(u):
        def store(c, val):
            pacc[:, c] = val
        with jax.named_scope('mlp'):
            mlp(lax.rem(u, 3), 0, 2 * T, store)

    def mlp_outer(u, b):
        def store(c, val):
            px[lax.rem(u, 2), pl.ds(pl.multiple_of(b * T, T), T), c] = val.astype(BF16)
        with jax.named_scope('mlp_o'):
            mlp(lax.rem(u, 3), pl.multiple_of(b * T, T), T, store)

    def forward(u):
        @pl.when((u >= 1) & (u <= N))
        def _():
            s2_copy(u - 1).wait_send()

        @pl.when(u < N)
        def _():
            with jax.named_scope('w_ag'):
                ag_wait(1 - hb, u)
            s2_copy(u).start()

    def combine(v):
        sl = lax.rem(v, 2)
        with jax.named_scope('w_s3'):
            s3_copy(v, 0).wait_recv()
            s3_copy(v, 1).wait_recv()

        @pl.when(v >= 1)
        def _():
            s4_copy(v - 1).wait_send()

        def comb(b, carry):
            rows = pl.ds(b * RB, RB)
            mine = pl.ds(pl.multiple_of(hb * T + b * RB, RB), RB)
            theirs = pl.ds(pl.multiple_of((1 - hb) * T + b * RB, RB), RB)
            oacc[rows, :] = pacc[mine, :] + px[sl, mine, :].astype(F32)
            sendb[rows, :] = (pacc[theirs, :] + px[sl, theirs, :].astype(F32)).astype(BF16)
            return carry
        lax.fori_loop(0, T // RB, comb, 0)
        s4_copy(v).start()

    def finish(u):
        @pl.when((u >= 2) & (u < N + 2))
        def _():
            v = u - 2
            with jax.named_scope('w_s4'):
                s4_copy(v).wait_recv()
            vw = v // NJ
            vj = lax.rem(v, NJ)

            @pl.when(v >= 1)
            def _():
                hin_copy(v).wait_send()

            def fin(b, carry):
                rows = pl.ds(b * RB, RB)
                d = (oacc[rows, :] + ps[lax.rem(v, 2), rows, :].astype(F32)).astype(BF16)
                h2b[rows, :] = (h1b[lax.rem(v, 3), rows, :].astype(F32) + d.astype(F32)).astype(BF16)
                return carry
            lax.fori_loop(0, T // RB, fin, 0)

            @pl.when((s < n_stages - 1) & (v >= HS))
            def _():
                with jax.named_scope('w_cred'):
                    pl.semaphore_wait(cred, 1)

            @pl.when(s < n_stages - 1)
            def _():
                hin_copy(v).start()

            @pl.when((s == n_stages - 1) & (v < N - NJ))
            def _():
                park_copy(v).start()

            @pl.when((s == n_stages - 1) & (v >= N - NJ) & (vj != z))
            def _():
                out_copy(v, 2 * vw + hb, vj).start()

            @pl.when((s == n_stages - 1) & (v >= N - NJ) & (vj == z))
            def _():
                local(h2b, out_ref.at[2 * vw + hb], s5s).start()

    def body(u, carry):
        @pl.when(is_home)
        def _():
            @pl.when(u < N)
            def _():
                attention(u)

            @pl.when((u >= 1) & (u <= N))
            def _():
                s1_outer(u - 1).wait_send()
                s1_peer(u - 1).wait_send()

            @pl.when(u < N)
            def _():
                s1_peer(u).start()
                s1_outer(u).start()

            @pl.when((u >= 1) & (u <= N))
            def _():
                mlp_home(u - 1)

            finish(u)
            forward(u)

            @pl.when((u >= 1) & (u <= N))
            def _():
                combine(u - 1)

        @pl.when(is_outer & (u < N))
        def _():
            for k in (0, 1):
                b = inner - 1 if k == 0 else 2 - inner
                with jax.named_scope('w_ag_outer'):
                    ag_wait(b, u)

                @pl.when(u >= 2)
                def _():
                    s3_copy(u - 2, b).wait_send()
                mlp_outer(u, b)
                s3_copy(u, b).start()

        v = u - 4

        @pl.when((s == n_stages - 1) & (v >= N - NJ) & (v < N) & (lax.rem(v, NJ) == z))
        def _():
            for b in (0, 1):
                mb = 2 * NW - 2 + b

                @pl.when(z - 1 != b)
                def _(mb=mb):
                    local(out_ref.at[mb], out_ref.at[mb], outr.at[mb]).wait()
                out_fwd(mb, 1, outr.at[mb]).start()
                out_fwd(mb, 2, outf).start()
        return carry

    def out_fwd(mb, p, sem):
        return rcopy(out_ref.at[mb], out_ref.at[mb], ofs.at[mb, p], sem, pp=p)

    lax.fori_loop(0, N + 4, body, 0)

    def od_copy(v):
        return rcopy(hin_hbm.at[v], out_ref.at[2 * (v // NJ) + hb], od.at[v], outr.at[2 * (v // NJ) + hb], tp=lax.rem(v, NJ))

    @pl.when(s == 1)
    def _():
        def spread(v, carry):
            vj = lax.rem(v, NJ)
            mine = 2 * (v // NJ) + hb

            @pl.when(is_home)
            def _():
                local(hin_hbm.at[v], hin_hbm.at[v], op.at[v]).wait()

            @pl.when(is_home & (vj != z))
            def _():
                od_copy(v).start()

            @pl.when(is_home & (vj == z))
            def _():
                c = local(hin_hbm.at[v], hin.at[0], hv_sem)
                c.start()
                c.wait()
                c = local(hin.at[0], out_ref.at[mine], hv_sem)
                c.start()
                c.wait()

            @pl.when(vj == z)
            def _():
                for b in (0, 1):
                    mb = 2 * (v // NJ) + b

                    @pl.when(z - 1 != b)
                    def _(mb=mb):
                        local(out_ref.at[mb], out_ref.at[mb], outr.at[mb]).wait()
                    for p in (3, 0, 2):
                        out_fwd(mb, p, outf).start()
            return carry
        lax.fori_loop(0, N - NJ, spread, 0)

        for b in (0, 1):
            mb = 2 * NW - 2 + b
            local(out_ref.at[mb], out_ref.at[mb], outr.at[mb]).wait()
            out_fwd(mb, 0, outf).start()

    @pl.when(is_home)
    def _():
        s4_copy(N - 1).wait_send()
        hin_copy(N - 1).wait_send()

    @pl.when(is_outer)
    def _():
        for b in (0, 1):
            s3_copy(N - 2, b).wait_send()
            s3_copy(N - 1, b).wait_send()

    @pl.when(is_outer)
    def _():
        for k in range(5, 8):
            o_send(k).wait_send()

    @pl.when(is_home)
    def _():
        for m in range(4):
            p_send(m).wait_send()
            f_send(m).wait_send()
            x_send(1, m).wait_send()
            x_send(2, m).wait_send()

        @pl.when(s == 2)
        def _():
            for w in range(1, NW):
                for j in range(NJ):
                    @pl.when(z != j)
                    def _():
                        x_pass(w, j).wait_send()

        @pl.when(s == 1)
        def _():
            def spread_done(v, carry):
                @pl.when(lax.rem(v, NJ) != z)
                def _():
                    od_copy(v).wait_send()
                return carry
            lax.fori_loop(0, N - NJ, spread_done, 0)

    for w in range(NW):
        x_each(w, lambda c: c.wait_send())

    @pl.when(s == 1)
    def _():
        for mb in range(n_mb - 2):
            for p in (3, 0, 2):
                out_fwd(mb, p, outf).wait_send()
        for mb in (n_mb - 2, n_mb - 1):
            out_fwd(mb, 0, outf).wait_send()

    @pl.when(s == n_stages - 1)
    def _():
        for mb in (n_mb - 2, n_mb - 1):
            for p in (1, 2):
                out_fwd(mb, p, outf).wait_send()
        early = out_ref.at[pl.ds(0, n_mb - 2)]
        local(early, early, outf).wait()

    @pl.when((s == 0) | (s == 2))
    def _():
        local(out_ref, out_ref, outf).wait()


def solution(mesh):
    n_stages = mesh.shape['pp']

    def stage_program(hidden_in, seg_ids, positions, attn_norm, w_query, w_key, w_value, w_out, mlp_norm, w_gate, w_up, w_down):
        n_mb, T, D = hidden_in.shape
        S = seg_ids.shape[1]
        QL = w_query.shape[2]
        FL = w_gate.shape[2]
        NJ = S // T
        N = (n_mb // 2) * NJ
        NB = max(1, FL // 512)
        cols = jnp.stack([positions, seg_ids], axis=-1)
        invf = jnp.asarray(np.tile(rope_freqs(), 2)[None, :], F32)
        any_spec = pl.BlockSpec(memory_space=pl.ANY)
        vmem = pl.BlockSpec(memory_space=pltpu.VMEM)
        dma = pltpu.SemaphoreType.DMA
        scratch = [
            pltpu.VMEM((NB, D, FL // NB), BF16), pltpu.VMEM((NB, D, FL // NB), BF16), pltpu.VMEM((NB, FL, D // NB), BF16),
            pltpu.VMEM((2, 3, max(D, 4 * QL), QL), BF16),
            pltpu.VMEM((3, 2 * T, D), BF16),
            pltpu.VMEM((2, 2 * T, D), BF16),
            pltpu.VMEM((2, T, D), BF16),
            pltpu.VMEM((4, S, QL), BF16), pltpu.VMEM((4, S, QL), BF16),
            pltpu.VMEM((4, T, D), BF16),
            pltpu.VMEM((3, T, D), BF16),
            pltpu.VMEM((2 * T, D), F32),
            pltpu.VMEM((T, D), F32),
            pltpu.VMEM((T, D), BF16),
            pltpu.VMEM((T, D), BF16),
            pltpu.VMEM((2 * T, FL), BF16),
            pltpu.VMEM((T, D), BF16),
            pltpu.VMEM((T, D), BF16),
            pltpu.VMEM((2, T, QL), BF16), pltpu.VMEM((T, 4 * QL), BF16),
            pltpu.VMEM((n_mb // 2, S, HEAD_DIM), F32),
            pltpu.VMEM((n_mb // 2, S, 2), jnp.int32),
            pltpu.VMEM((T, S), F32), pltpu.VMEM((QL // HEAD_DIM, T, S), F32), pltpu.VMEM((QL // HEAD_DIM, T, S), BF16),
            dma((3, 8)), dma((2, 4)), dma((8,)), dma((4,)), dma((2, 4)),
            dma((N,)), dma((n_mb // 2, 2)), dma((2, 3)), dma((2,)), dma, dma((2, 2)), dma((2, 2)), dma((2,)), dma, dma,
            dma((n_mb,)), dma, dma((n_mb, n_stages)),
            dma((2, 3)), dma((2, 3, 4)), dma((3, NB)), dma, dma((n_mb // 2,)), dma((N,)), dma((n_mb // 2, NJ)), dma((N,)), dma((N,)),
            pltpu.SemaphoreType.REGULAR, pltpu.SemaphoreType.REGULAR,
        ]
        return pl.pallas_call(
            functools.partial(kernel, n_stages),
            out_shape=[jax.ShapeDtypeStruct(hidden_in.shape, BF16), jax.ShapeDtypeStruct((3, 3, D, QL), BF16),
                       jax.ShapeDtypeStruct((3, QL, D), BF16), jax.ShapeDtypeStruct((N, T, D), BF16)],
            in_specs=[any_spec, vmem, any_spec, vmem, vmem, vmem] + [any_spec] * 7,
            out_specs=[any_spec] * 4,
            scratch_shapes=scratch,
            compiler_params=pltpu.CompilerParams(has_side_effects=True, vmem_limit_bytes=67_043_328),
        )(hidden_in, seg_ids, cols, invf, attn_norm, mlp_norm, w_query, w_key, w_value, w_out, w_gate, w_up, w_down)[0]

    act_spec = P('dp', 'tp', None)
    row_spec = P('dp', None)
    gain_spec = P('pp', None)
    col_spec = P('pp', None, 'tp')
    rows_spec = P('pp', 'tp', None)
    return jax.shard_map(stage_program, mesh=mesh,
                         in_specs=(act_spec, row_spec, row_spec, gain_spec, col_spec, col_spec, col_spec, rows_spec, gain_spec, col_spec, col_spec, rows_spec),
                         out_specs=act_spec, check_vma=False)
```

```python
import functools
import math

import jax
import jax.numpy as jnp
import numpy as np
from jax import lax
from jax.experimental import pallas as pl
from jax.experimental.pallas import tpu as pltpu
from jax.sharding import PartitionSpec as P

HEAD_DIM = 128
NORM_EPS = 1e-5
ROPE_THETA = 500000.0
ROPE_FACTOR = 8.0
LOW_FREQ = 1.0
HIGH_FREQ = 4.0
ORIG_CTX = 8192.0
NEG = -1e30
MESH = pl.DeviceIdType.MESH
F32 = jnp.float32
BF16 = jnp.bfloat16


def rope_freqs():
    base_freq = 1.0 / (ROPE_THETA ** (np.arange(0, HEAD_DIM, 2) / HEAD_DIM))
    wavelen = 2.0 * np.pi / base_freq
    smooth = (ORIG_CTX / wavelen - LOW_FREQ) / (HIGH_FREQ - LOW_FREQ)
    blended = (1.0 - smooth) * base_freq / ROPE_FACTOR + smooth * base_freq
    scaled = np.where(wavelen > ORIG_CTX / LOW_FREQ, base_freq / ROPE_FACTOR, blended)
    return np.where(wavelen < ORIG_CTX / HIGH_FREQ, base_freq, scaled)


def kernel(n_stages, x_ref, seg_ref, pos_ref, invf_ref, ga_ref, gm_ref,
           wq_ref, wk_ref, wv_ref, wo_ref, wg_ref, wu_ref, wd_ref,
           out_ref,
           wqkv_hbm, wo_hbm, hin_hbm,
           wg_s, wu_s, wd_s, wres, wst, gb, px, ps, kc, vc, hin, h1b, pacc, oacc, sendb, h2b, act, abuf, qb,
           table, mask, pbuf,
           wr, wx, wsnd, wfwd, wxs, hin_sem, xs, ag, s1s, s2s, pxr, pxs, psr, s4s, s5s, outr, outf, ofs,
           wres_sem, wst_sem, wo_sem, mlp_sem, hv_sem, s6s, xp, xq, op, od, gate, cred):
    n_mb, T, D = x_ref.shape
    QL = wq_ref.shape[2]
    FL = wg_ref.shape[2]
    NB = wg_s.shape[0]
    FB = FL // NB
    S = seg_ref.shape[1]
    NJ = S // T
    NH = QL // HEAD_DIM
    N = (n_mb // 2) * NJ
    DB = D // NB
    scale = HEAD_DIM ** -0.5
    RB = 16
    NR = 32
    HS = hin.shape[0]
    OB = wst.shape[3]
    NO = D // OB

    hx = lax.axis_index("dp")
    z = lax.axis_index("tp")
    s = lax.axis_index("pp")
    is_home = (z == 1) | (z == 2)
    is_outer = (z == 0) | (z == 3)
    hb = lax.rem(z + 1, 2) * 0 + (z - 1)
    peer = 3 - z
    outer = 3 * (z - 1)
    inner = 1 + z // 2
    odd = lax.rem(s, 2)

    def rcopy(src, dst, ssem, rsem, **dev):
        return pltpu.make_async_remote_copy(src_ref=src, dst_ref=dst, send_sem=ssem, recv_sem=rsem,
                                            device_id=dev, device_id_type=MESH)

    def local(src, dst, sem):
        return pltpu.make_async_copy(src, dst, sem)

    def column(ref, mb, j):
        row = ref[pl.ds(mb, 1), :]
        part = row[:, 0:T]
        for c in range(1, NJ):
            part = jnp.where(j == c, row[:, c * T:(c + 1) * T], part)
        return jnp.broadcast_to(part, (HEAD_DIM, T)).T

    wqkv_own = (wq_ref, wk_ref, wv_ref, wo_ref)

    def mlp_copies():
        cps = []
        for n in range(NB):
            cps.append(local(wg_ref.at[0, :, pl.ds(n * FB, FB)], wg_s.at[n], mlp_sem.at[0, n]))
            cps.append(local(wu_ref.at[0, :, pl.ds(n * FB, FB)], wu_s.at[n], mlp_sem.at[1, n]))
            cps.append(local(wd_ref.at[0, :, pl.ds(n * DB, DB)], wd_s.at[n], mlp_sem.at[2, n]))
        return cps

    NW = n_mb // 2

    def x_copy(w, home):
        u = w * NJ + z
        return rcopy(x_ref.at[2 * w + (home - 1)], hin_hbm.at[u], xs.at[w, home - 1], (hin_sem if w == 0 else xp).at[u], tp=home)

    def x_each(w, act):
        for home in (1, 2):
            @pl.when((s == (0 if w == 0 else 2)) & (z != home))
            def _():
                act(x_copy(w, home))

    def x_pass(w, j):
        u = w * NJ + j
        return rcopy(hin_hbm.at[u], hin_hbm.at[u], xq.at[w, j], hin_sem.at[u], pp=0)

    def half(ref, m, h):
        rows = (D if m < 3 else QL) // 2
        return ref.at[pl.ds(h * rows, rows), :]

    def wslot(r, m):
        return wqkv_hbm.at[r, m] if m < 3 else wo_hbm.at[pl.ds((r + 1) * QL, QL)]

    def own_w(m):
        return wqkv_own[m].at[0]

    def wo_own():
        return local(own_w(3), wo_hbm.at[pl.ds(0, QL)], wo_sem)

    def o_send(k):
        h = hx if k < 4 else 1 - hx
        return rcopy(half(own_w(k % 4), k % 4, h), half(wslot(0, k % 4), k % 4, h), wsnd.at[k], wr.at[0, k], tp=inner)

    def p_send(m):
        return rcopy(half(own_w(m), m, hx), half(wslot(1, m), m, hx), wsnd.at[m], wr.at[1, m], tp=peer)

    def f_send(m):
        return rcopy(half(wslot(0, m), m, hx), half(wslot(2, m), m, hx), wfwd.at[m], wr.at[2, m], tp=peer)

    def x_send(r, m):
        return rcopy(half(wslot(r, m), m, hx), half(wslot(r, m), m, hx), wxs.at[r - 1, m], wx.at[r - 1, m], dp=1 - hx)

    def w_ready(rs, ms):
        for m in ms:
            if 0 in rs:
                o_send(4 + m).wait_recv()
            for r in (1, 2):
                if r in rs:
                    x_send(r, m).wait_recv()

    def release():
        @pl.when(odd == 0)
        def _():
            pl.semaphore_signal(gate, inc=1, device_id={"pp": s + 1}, device_id_type=MESH)

    @pl.when(odd == 1)
    def _():
        for c in mlp_copies():
            c.start()
        with jax.named_scope('w_gate'):
            pl.semaphore_wait(gate, 1)

    @pl.when(is_outer)
    def _():
        for k in range(8):
            o_send(k).start()

        @pl.when(odd == 0)
        def _():
            x_each(0, lambda c: c.start())
            for c in mlp_copies():
                c.start()
        for k in range(5):
            o_send(k).wait_send()
        release()
        for w in range(1, NW):
            x_each(w, lambda c: c.start())

    @pl.when(is_home)
    def _():
        for m in range(4):
            p_send(m).start()
        wo_own().start()

        @pl.when(odd == 0)
        def _():
            for c in mlp_copies():
                c.start()
        def zero_rows(b, carry):
            for i in range(4):
                kc[i, pl.ds(b * RB, RB), :] = jnp.zeros((RB, QL), BF16)
                vc[i, pl.ds(b * RB, RB), :] = jnp.zeros((RB, QL), BF16)
            return carry
        lax.fori_loop(0, S // RB, zero_rows, 0)

        def tables(w):
            lane = lax.broadcasted_iota(jnp.int32, (T, HEAD_DIM), 1)

            def table_rows(b, carry):
                rows = pl.ds(pl.multiple_of(b * T, T), T)
                ang = column(pos_ref, 2 * w + hb, b).astype(F32) * invf_ref[0:1, :]
                table[w, rows, :] = jnp.where(lane < HEAD_DIM // 2, jnp.cos(ang), jnp.sin(ang))
                return carry
            with jax.named_scope('table'):
                lax.fori_loop(0, NJ, table_rows, 0)

        steps = [("o", 0), ("p", 0), ("t", 0), ("o", 1), ("p", 1), ("t", 1), ("o", 2), ("p", 2), ("t", 2), ("o", 3), ("p", 3), ("t", 3),
                 ("f", 0), ("g", 0), ("f", 1), ("f", 2), ("f", 3)]
        for kind, m in steps:
          with jax.named_scope('w_' + kind + str(m)):
            if kind == "o":
                o_send(m).wait_recv()
                f_send(m).start()
            elif kind == "p":
                p_send(m).wait_recv()
                x_send(1, m).start()
            elif kind == "f":
                f_send(m).wait_recv()
                x_send(2, m).start()
            elif kind == "g":
                release()
            elif m < n_mb // 2:
                tables(m)
        for w in range(NW):
            x_each(w, lambda c: c.start())
        w_ready([0, 1], range(3))

        @pl.when(s == 2)
        def _():
            for w in range(1, NW):
                for j in range(NJ):
                    @pl.when(z != j)
                    def _():
                        local(hin_hbm.at[w * NJ + j], hin_hbm.at[w * NJ + j], xp.at[w * NJ + j]).wait()
                        x_pass(w, j).start()

    def gslot(g, u):
        return lax.rem(g - 1 + u, 2)

    def group_copies(g, u):
        if g == 0:
            return [local(own_w(m), wres.at[m], wres_sem.at[m]) for m in range(3)]
        p = gslot(g, u)
        if g < 4:
            return [local(wqkv_hbm.at[g - 1], wst.at[p], wst_sem.at[p, 0])]
        return [local(wo_hbm.at[:, pl.ds(((g - 4) * 3 + m) * OB, OB)], wst.at[p, m], wst_sem.at[p, m]) for m in range(3 if g == 4 else 1)]

    def group_start(g, u):
        for c in group_copies(g, u):
            c.start()

    def group_wait(g, u):
        for c in group_copies(g, u):
            c.wait()

    def h_fetch(u):
        mb = 2 * (u // NJ) + hb
        here = lax.rem(u, NJ) == z
        dst = hin.at[lax.rem(u, HS)]

        @pl.when((s == 0) & here)
        def _():
            local(x_ref.at[mb], dst, hv_sem).start()

        @pl.when((s == 0) & jnp.logical_not(here))
        def _():
            local(hin_hbm.at[u], hin_hbm.at[u], hin_sem.at[u]).wait()
            local(hin_hbm.at[u], dst, hv_sem).start()

    @pl.when(is_home)
    def _():
        group_start(0, 0)
        group_start(1, 0)
        group_start(2, 0)
        h_fetch(0)

    for c in mlp_copies():
        c.wait()

    def hin_copy(u):
        return rcopy(h2b, hin.at[lax.rem(u, HS)], s5s, hin_sem.at[u], pp=lax.rem(s + 1, n_stages))

    def s1_outer(u):
        blk = gb.at[lax.rem(u, 3), pl.ds(pl.multiple_of(hb * T, T), T), :]
        return rcopy(blk, blk, s1s.at[0], ag.at[hb, lax.rem(u, 3)], tp=outer)

    def s1_peer(u):
        blk = gb.at[lax.rem(u, 3), pl.ds(pl.multiple_of(hb * T, T), T), :]
        return rcopy(blk, blk, s1s.at[1], ag.at[hb, lax.rem(u, 3)], tp=peer)

    def s2_copy(u):
        blk = gb.at[lax.rem(u, 3), pl.ds(pl.multiple_of((1 - hb) * T, T), T), :]
        return rcopy(blk, blk, s2s, ag.at[1 - hb, lax.rem(u, 3)], tp=outer)

    def ag_wait(b, u):
        blk = gb.at[lax.rem(u, 3), pl.ds(pl.multiple_of(b * T, T), T), :]
        local(blk, blk, ag.at[b, lax.rem(u, 3)]).wait()

    def s3_copy(u, b):
        sl = lax.rem(u, 2)
        blk = px.at[sl, pl.ds(pl.multiple_of(b * T, T), T), :]
        return rcopy(blk, blk, pxs.at[sl, b], pxr.at[sl, b], tp=inner)

    def s4_copy(u):
        return rcopy(sendb, ps.at[lax.rem(u, 2)], s4s, psr.at[lax.rem(u, 2)], tp=peer)

    def park_copy(u):
        return rcopy(h2b, hin_hbm.at[u], s5s, op.at[u], pp=1)

    def out_copy(u, mb, j):
        return rcopy(h2b, out_ref.at[mb], s5s, outr.at[mb], tp=j)

    def out_copy1(u, mb, j):
        return rcopy(h2b, out_ref.at[mb], s6s, outr.at[mb], tp=j, pp=1)

    def norm_rows(src, gain, dst):
        hf = src.astype(F32)
        inv = lax.rsqrt(jnp.mean(hf * hf, axis=-1, keepdims=True) + NORM_EPS)
        return (hf * inv * gain.astype(F32)).astype(BF16)

    def attention(u):
      with jax.named_scope('attn'):
        attention_(u)

    def attention_(u):
        w = u // NJ
        j = lax.rem(u, NJ)
        mb = 2 * w + hb
        row0 = pl.multiple_of(j * T, T)
        hs = lax.rem(u, HS)

        with jax.named_scope('w_hin'):
            @pl.when(s == 0)
            def _():
                local(x_ref.at[mb], hin.at[hs], hv_sem).wait()

            @pl.when(s > 0)
            def _():
                hin_copy(u).wait_recv()

        def norm_a(b, carry):
            rows = pl.ds(b * NR, NR)
            abuf[rows, :] = norm_rows(hin[hs, rows, :], ga_ref[0:1, :], None)
            return carry
        lax.fori_loop(0, T // NR, norm_a, 0)

        segrow = seg_ref[pl.ds(mb, 1), :]
        segc = column(seg_ref, mb, j)
        ti = lax.broadcasted_iota(jnp.int32, (T, HEAD_DIM), 0) + row0
        for c in range(0, S, HEAD_DIM):
            segr = segrow[:, c:c + HEAD_DIM]
            ui = lax.broadcasted_iota(jnp.int32, (T, HEAD_DIM), 1) + c
            mask[:, c:c + HEAD_DIM] = jnp.where((segc == segr) & (ui <= ti), 1.0, 0.0)

        def rope(val):
            pk = table[w, pl.ds(row0, T), :]
            lane = lax.broadcasted_iota(jnp.int32, (T, HEAD_DIM), 1)
            swapped = pltpu.roll(pk, HEAD_DIM // 2, 1)
            cosw = jnp.where(lane < HEAD_DIM // 2, pk, swapped)
            sinw = jnp.where(lane < HEAD_DIM // 2, -swapped, pk)
            outs = []
            for h in range(NH):
                v = val[:, h * HEAD_DIM:(h + 1) * HEAD_DIM]
                outs.append((v * cosw + pltpu.roll(v, HEAD_DIM // 2, 1) * sinw).astype(BF16))
            return outs

        def hcols(h):
            return slice(h * HEAD_DIM, (h + 1) * HEAD_DIM)

        def proj(i):
            p = i % 2

            def w(m):
                return wres[m] if i == 0 else wst[gslot(i, u), m]
            for h, val in enumerate(rope(jnp.dot(abuf[...], w(0), preferred_element_type=F32))):
                qb[p, :, hcols(h)] = val
            for h, val in enumerate(rope(jnp.dot(abuf[...], w(1), preferred_element_type=F32))):
                kc[i, pl.ds(row0, T), hcols(h)] = val
            vc[i, pl.ds(row0, T), :] = jnp.dot(abuf[...], w(2), preferred_element_type=F32).astype(BF16)

        def heads(i):
            for h in range(NH):
                sc = lax.dot_general(qb[i % 2, :, hcols(h)], kc[i, :, hcols(h)], (((1,), (1,)), ((), ())),
                                     preferred_element_type=F32) * scale
                pacc[0:T, h * S:(h + 1) * S] = jnp.where(mask[...] > 0.5, sc, NEG)
            for h in range(NH):
                for r in range(0, T, 32):
                    sc = pacc[r:r + 32, h * S:(h + 1) * S]
                    e = jnp.exp(sc - jnp.max(sc, axis=-1, keepdims=True))
                    pbuf[h, r:r + 32, :] = (e * (1.0 / jnp.sum(e, axis=-1, keepdims=True))).astype(BF16)
            for h in range(NH):
                act[0:T, i * QL + h * HEAD_DIM:i * QL + (h + 1) * HEAD_DIM] = jnp.dot(
                    pbuf[h], vc[i, :, hcols(h)], preferred_element_type=F32).astype(BF16)

        with jax.named_scope('shards'):
            @pl.when(u == 0)
            def _():
                group_wait(0, u)
            proj(0)
            for i in range(3):
                group_wait(i + 1, u)
                proj(i + 1)
                if i < 2:
                    @pl.when(u == 0)
                    def _():
                        if i == 0:
                            w_ready([2], range(3))
                        else:
                            w_ready([0, 1, 2], [3])
                            wo_own().wait()
                group_start(i + 3, u)
                heads(i)
                if i == 0:
                    @pl.when(u < N - 1)
                    def _():
                        h_fetch(u + 1)
            heads(3)

        @pl.when(odd == 1)
        def _():
            finish(u)
        with jax.named_scope('wo'):
            def wo_block(n, w):
                act[T:2 * T, n * OB:(n + 1) * OB] = jnp.dot(act[0:T, 0:4 * QL], w, preferred_element_type=F32).astype(BF16)

            group_wait(4, u)
            group_wait(5, u)
            for n in range(3):
                wo_block(n, wst[gslot(4, u), n])

            wo_block(3, wst[gslot(5, u), 0])

            @pl.when(u < N - 1)
            def _():
                group_start(1, u + 1)
                group_start(2, u + 1)

        def norm_b(b, carry):
            rows = pl.ds(b * NR, NR)
            h1 = (hin[hs, rows, :].astype(F32) + act[pl.ds(pl.multiple_of(T + b * NR, NR), NR), 0:D].astype(F32)).astype(BF16)
            h1b[lax.rem(u, 3), rows, :] = h1
            gb[lax.rem(u, 3), pl.ds(pl.multiple_of(hb * T + b * NR, NR), NR), :] = norm_rows(h1, gm_ref[0:1, :], None)
            return carry
        lax.fori_loop(0, T // NR, norm_b, 0)

        @pl.when((s > 0) & (u < N - HS))
        def _():
            pl.semaphore_signal(cred, inc=1, device_id={"pp": s - 1}, device_id_type=MESH)

    def mlp(sl, row0, rows, store):
        UN = 2 if NB % 2 == 0 else 1

        def up(q, carry):
            for n in [q * UN + k for k in range(UN)]:
                xin = gb[sl, pl.ds(row0, rows), :]
                g = jnp.dot(xin, wg_s[n], preferred_element_type=F32)
                u_ = jnp.dot(xin, wu_s[n], preferred_element_type=F32)
                act[0:rows, pl.ds(pl.multiple_of(n * FB, FB), FB)] = (jax.nn.silu(g) * u_).astype(BF16)
            return carry
        lax.fori_loop(0, NB // UN, up, 0)

        def down(q, carry):
            for n in [q * UN + k for k in range(UN)]:
                store(pl.ds(pl.multiple_of(n * DB, DB), DB), jnp.dot(act[0:rows, 0:FL], wd_s[n], preferred_element_type=F32))
            return carry
        lax.fori_loop(0, NB // UN, down, 0)

    def mlp_home(u):
        def store(c, val):
            pacc[:, c] = val
        with jax.named_scope('mlp'):
            mlp(lax.rem(u, 3), 0, 2 * T, store)

    def mlp_outer(u, b):
        def store(c, val):
            px[lax.rem(u, 2), pl.ds(pl.multiple_of(b * T, T), T), c] = val.astype(BF16)
        with jax.named_scope('mlp_o'):
            mlp(lax.rem(u, 3), pl.multiple_of(b * T, T), T, store)

    def forward(u):
        @pl.when((u >= 1) & (u <= N))
        def _():
            s2_copy(u - 1).wait_send()

        @pl.when(u < N)
        def _():
            with jax.named_scope('w_ag'):
                ag_wait(1 - hb, u)
            s2_copy(u).start()

    def combine(v):
        sl = lax.rem(v, 2)
        with jax.named_scope('w_s3'):
            s3_copy(v, 0).wait_recv()
            s3_copy(v, 1).wait_recv()

        @pl.when(v >= 1)
        def _():
            s4_copy(v - 1).wait_send()

        def comb(b, carry):
            rows = pl.ds(b * RB, RB)
            mine = pl.ds(pl.multiple_of(hb * T + b * RB, RB), RB)
            theirs = pl.ds(pl.multiple_of((1 - hb) * T + b * RB, RB), RB)
            oacc[rows, :] = pacc[mine, :] + px[sl, mine, :].astype(F32)
            sendb[rows, :] = (pacc[theirs, :] + px[sl, theirs, :].astype(F32)).astype(BF16)
            return carry
        lax.fori_loop(0, T // RB, comb, 0)
        s4_copy(v).start()

    def finish(u):
        @pl.when((u >= 2) & (u < N + 2))
        def _():
            v = u - 2
            with jax.named_scope('w_s4'):
                s4_copy(v).wait_recv()
            vw = v // NJ
            vj = lax.rem(v, NJ)

            @pl.when(v >= 1)
            def _():
                hin_copy(v).wait_send()

            @pl.when((s == n_stages - 1) & (v > N - NJ))
            def _():
                out_copy1(v, 2 * vw + hb, vj).wait_send()

            def fin(b, carry):
                rows = pl.ds(b * RB, RB)
                d = (oacc[rows, :] + ps[lax.rem(v, 2), rows, :].astype(F32)).astype(BF16)
                h2b[rows, :] = (h1b[lax.rem(v, 3), rows, :].astype(F32) + d.astype(F32)).astype(BF16)
                return carry
            lax.fori_loop(0, T // RB, fin, 0)

            @pl.when((s < n_stages - 1) & (v >= HS))
            def _():
                with jax.named_scope('w_cred'):
                    pl.semaphore_wait(cred, 1)

            @pl.when(s < n_stages - 1)
            def _():
                hin_copy(v).start()

            @pl.when((s == n_stages - 1) & (v < N - NJ))
            def _():
                park_copy(v).start()

            @pl.when((s == n_stages - 1) & (v >= N - NJ))
            def _():
                out_copy1(v, 2 * vw + hb, vj).start()

            @pl.when((s == n_stages - 1) & (v >= N - NJ) & (vj != z))
            def _():
                out_copy(v, 2 * vw + hb, vj).start()

            @pl.when((s == n_stages - 1) & (v >= N - NJ) & (vj == z))
            def _():
                local(h2b, out_ref.at[2 * vw + hb], s5s).start()

    def body(u, carry):
        @pl.when(is_home)
        def _():
            @pl.when(u < N)
            def _():
                attention(u)

            @pl.when((u >= 1) & (u <= N))
            def _():
                s1_outer(u - 1).wait_send()
                s1_peer(u - 1).wait_send()

            @pl.when(u < N)
            def _():
                s1_peer(u).start()
                s1_outer(u).start()

            @pl.when((u >= 1) & (u <= N))
            def _():
                mlp_home(u - 1)

            @pl.when((odd == 0) | (u >= N))
            def _():
                finish(u)

            forward(u)

            @pl.when((u >= 1) & (u <= N))
            def _():
                combine(u - 1)

        @pl.when(is_outer & (u < N))
        def _():
            for k in (0, 1):
                b = inner - 1 if k == 0 else 2 - inner
                with jax.named_scope('w_ag_outer'):
                    ag_wait(b, u)

                @pl.when(u >= 2)
                def _():
                    s3_copy(u - 2, b).wait_send()
                mlp_outer(u, b)
                s3_copy(u, b).start()

        v = u - 4

        @pl.when((s == n_stages - 1) & (v >= N - NJ) & (v < N) & (lax.rem(v, NJ) == z))
        def _():
            for b in (0, 1):
                mb = 2 * NW - 2 + b

                @pl.when(z - 1 != b)
                def _(mb=mb):
                    local(out_ref.at[mb], out_ref.at[mb], outr.at[mb]).wait()
                out_fwd(mb, 2, outf).start()
        return carry

    def out_fwd(mb, p, sem):
        return rcopy(out_ref.at[mb], out_ref.at[mb], ofs.at[mb, p], sem, pp=p)

    lax.fori_loop(0, N + 4, body, 0)

    def od_copy(v):
        return rcopy(hin_hbm.at[v], out_ref.at[2 * (v // NJ) + hb], od.at[v], outr.at[2 * (v // NJ) + hb], tp=lax.rem(v, NJ))

    @pl.when(s == 1)
    def _():
        def spread(v, carry):
            vj = lax.rem(v, NJ)
            mine = 2 * (v // NJ) + hb

            @pl.when(is_home)
            def _():
                local(hin_hbm.at[v], hin_hbm.at[v], op.at[v]).wait()

            @pl.when(is_home & (vj != z))
            def _():
                od_copy(v).start()

            @pl.when(is_home & (vj == z))
            def _():
                c = local(hin_hbm.at[v], hin.at[0], hv_sem)
                c.start()
                c.wait()
                c = local(hin.at[0], out_ref.at[mine], hv_sem)
                c.start()
                c.wait()

            @pl.when(vj == z)
            def _():
                for b in (0, 1):
                    mb = 2 * (v // NJ) + b

                    @pl.when(z - 1 != b)
                    def _(mb=mb):
                        local(out_ref.at[mb], out_ref.at[mb], outr.at[mb]).wait()
                    for p in (3, 0, 2):
                        out_fwd(mb, p, outf).start()
            return carry
        lax.fori_loop(0, N - NJ, spread, 0)

        for b in (0, 1):
            mb = 2 * NW - 2 + b
            local(out_ref.at[mb], out_ref.at[mb], outr.at[mb]).wait()
            out_fwd(mb, 0, outf).start()

    @pl.when(is_home)
    def _():
        s4_copy(N - 1).wait_send()
        hin_copy(N - 1).wait_send()

        @pl.when(s == n_stages - 1)
        def _():
            out_copy1(N - 1, n_mb - 2 + hb, NJ - 1).wait_send()

    @pl.when(is_outer)
    def _():
        for b in (0, 1):
            s3_copy(N - 2, b).wait_send()
            s3_copy(N - 1, b).wait_send()

    @pl.when(is_outer)
    def _():
        for k in range(5, 8):
            o_send(k).wait_send()

    @pl.when(is_home)
    def _():
        for m in range(4):
            p_send(m).wait_send()
            f_send(m).wait_send()
            x_send(1, m).wait_send()
            x_send(2, m).wait_send()

        @pl.when(s == 2)
        def _():
            for w in range(1, NW):
                for j in range(NJ):
                    @pl.when(z != j)
                    def _():
                        x_pass(w, j).wait_send()

        @pl.when(s == 1)
        def _():
            def spread_done(v, carry):
                @pl.when(lax.rem(v, NJ) != z)
                def _():
                    od_copy(v).wait_send()
                return carry
            lax.fori_loop(0, N - NJ, spread_done, 0)

    for w in range(NW):
        x_each(w, lambda c: c.wait_send())

    @pl.when(s == 1)
    def _():
        for mb in range(n_mb - 2):
            for p in (3, 0, 2):
                out_fwd(mb, p, outf).wait_send()
        for mb in (n_mb - 2, n_mb - 1):
            out_fwd(mb, 0, outf).wait_send()

    @pl.when(s == n_stages - 1)
    def _():
        for mb in (n_mb - 2, n_mb - 1):
            out_fwd(mb, 2, outf).wait_send()
        early = out_ref.at[pl.ds(0, n_mb - 2)]
        local(early, early, outf).wait()

    @pl.when((s == 0) | (s == 2))
    def _():
        local(out_ref, out_ref, outf).wait()


def solution(mesh):
    n_stages = mesh.shape['pp']

    def stage_program(hidden_in, seg_ids, positions, attn_norm, w_query, w_key, w_value, w_out, mlp_norm, w_gate, w_up, w_down):
        n_mb, T, D = hidden_in.shape
        S = seg_ids.shape[1]
        QL = w_query.shape[2]
        FL = w_gate.shape[2]
        NJ = S // T
        N = (n_mb // 2) * NJ
        NB = max(1, FL // 512)
        invf = jnp.asarray(np.tile(rope_freqs(), 2)[None, :], F32)
        any_spec = pl.BlockSpec(memory_space=pl.ANY)
        vmem = pl.BlockSpec(memory_space=pltpu.VMEM)
        dma = pltpu.SemaphoreType.DMA
        scratch = [
            pltpu.VMEM((NB, D, FL // NB), BF16), pltpu.VMEM((NB, D, FL // NB), BF16), pltpu.VMEM((NB, FL, D // NB), BF16),
            pltpu.VMEM((3, D, QL), BF16), pltpu.VMEM((2, 3, D, QL), BF16),
            pltpu.VMEM((3, 2 * T, D), BF16),
            pltpu.VMEM((2, 2 * T, D), BF16),
            pltpu.VMEM((2, T, D), BF16),
            pltpu.VMEM((4, S, QL), BF16), pltpu.VMEM((4, S, QL), BF16),
            pltpu.VMEM((4, T, D), BF16),
            pltpu.VMEM((3, T, D), BF16),
            pltpu.VMEM((2 * T, D), F32),
            pltpu.VMEM((T, D), F32),
            pltpu.VMEM((T, D), BF16),
            pltpu.VMEM((T, D), BF16),
            pltpu.VMEM((2 * T, max(D, FL, 4 * QL)), BF16),
            pltpu.VMEM((T, D), BF16),
            pltpu.VMEM((2, T, QL), BF16),
            pltpu.VMEM((n_mb // 2, S, HEAD_DIM), F32),
            pltpu.VMEM((T, S), F32), pltpu.VMEM((QL // HEAD_DIM, T, S), BF16),
            dma((3, 8)), dma((2, 4)), dma((8,)), dma((4,)), dma((2, 4)),
            dma((N,)), dma((n_mb // 2, 2)), dma((2, 3)), dma((2,)), dma, dma((2, 2)), dma((2, 2)), dma((2,)), dma, dma,
            dma((n_mb,)), dma, dma((n_mb, n_stages)),
            dma((3,)), dma((2, 3)), dma, dma((3, NB)), dma, dma, dma((N,)), dma((n_mb // 2, NJ)), dma((N,)), dma((N,)),
            pltpu.SemaphoreType.REGULAR, pltpu.SemaphoreType.REGULAR,
        ]
        return pl.pallas_call(
            functools.partial(kernel, n_stages),
            out_shape=[jax.ShapeDtypeStruct(hidden_in.shape, BF16), jax.ShapeDtypeStruct((3, 3, D, QL), BF16),
                       jax.ShapeDtypeStruct((4 * QL, D), BF16), jax.ShapeDtypeStruct((N, T, D), BF16)],
            in_specs=[any_spec, vmem, vmem, vmem, vmem, vmem] + [any_spec] * 7,
            out_specs=[any_spec] * 4,
            scratch_shapes=scratch,
            compiler_params=pltpu.CompilerParams(has_side_effects=True, vmem_limit_bytes=67_043_328),
        )(hidden_in, seg_ids, positions, invf, attn_norm, mlp_norm, w_query, w_key, w_value, w_out, w_gate, w_up, w_down)[0]

    act_spec = P('dp', 'tp', None)
    row_spec = P('dp', None)
    gain_spec = P('pp', None)
    col_spec = P('pp', None, 'tp')
    rows_spec = P('pp', 'tp', None)
    return jax.shard_map(stage_program, mesh=mesh,
                         in_specs=(act_spec, row_spec, row_spec, gain_spec, col_spec, col_spec, col_spec, rows_spec, gain_spec, col_spec, col_spec, rows_spec),
                         out_specs=act_spec, check_vma=False)
```

```python
import functools
import math

import jax
import jax.numpy as jnp
import numpy as np
from jax import lax
from jax.experimental import pallas as pl
from jax.experimental.pallas import tpu as pltpu
from jax.sharding import PartitionSpec as P

HEAD_DIM = 128
NORM_EPS = 1e-5
ROPE_THETA = 500000.0
ROPE_FACTOR = 8.0
LOW_FREQ = 1.0
HIGH_FREQ = 4.0
ORIG_CTX = 8192.0
NEG = -1e30
MESH = pl.DeviceIdType.MESH
F32 = jnp.float32
BF16 = jnp.bfloat16


def rope_freqs():
    base_freq = 1.0 / (ROPE_THETA ** (np.arange(0, HEAD_DIM, 2) / HEAD_DIM))
    wavelen = 2.0 * np.pi / base_freq
    smooth = (ORIG_CTX / wavelen - LOW_FREQ) / (HIGH_FREQ - LOW_FREQ)
    blended = (1.0 - smooth) * base_freq / ROPE_FACTOR + smooth * base_freq
    scaled = np.where(wavelen > ORIG_CTX / LOW_FREQ, base_freq / ROPE_FACTOR, blended)
    return np.where(wavelen < ORIG_CTX / HIGH_FREQ, base_freq, scaled)


def kernel(n_stages, x_ref, seg_ref, pos_ref, invf_ref, ga_ref, gm_ref,
           wq_ref, wk_ref, wv_ref, wo_ref, wg_ref, wu_ref, wd_ref,
           out_ref,
           wqkv_hbm, wo_hbm, hin_hbm,
           wg_s, wu_s, wd_s, wres, wst, gb, px, ps, kc, vc, hin, h1b, pacc, oacc, sendb, h2b, act, abuf, qb,
           table, mask, pbuf,
           wr, wx, wsnd, wfwd, wxs, hin_sem, xs, ag, s1s, s2s, pxr, pxs, psr, s4s, s5s, outr, outf, ofs,
           wres_sem, wst_sem, wo_sem, mlp_sem, hv_sem, s6s, xp, xq, op, od, gate, cred):
    n_mb, T, D = x_ref.shape
    QL = wq_ref.shape[2]
    FL = wg_ref.shape[2]
    NB = wg_s.shape[0]
    FB = FL // NB
    S = seg_ref.shape[1]
    NJ = S // T
    NH = QL // HEAD_DIM
    N = (n_mb // 2) * NJ
    DB = D // NB
    scale = HEAD_DIM ** -0.5
    RB = 16
    NR = 32
    HS = hin.shape[0]
    OB = wst.shape[3]
    NO = D // OB

    hx = lax.axis_index("dp")
    z = lax.axis_index("tp")
    s = lax.axis_index("pp")
    is_home = (z == 1) | (z == 2)
    is_outer = (z == 0) | (z == 3)
    hb = lax.rem(z + 1, 2) * 0 + (z - 1)
    peer = 3 - z
    outer = 3 * (z - 1)
    inner = 1 + z // 2
    odd = lax.rem(s, 2)

    def rcopy(src, dst, ssem, rsem, **dev):
        return pltpu.make_async_remote_copy(src_ref=src, dst_ref=dst, send_sem=ssem, recv_sem=rsem,
                                            device_id=dev, device_id_type=MESH)

    def local(src, dst, sem):
        return pltpu.make_async_copy(src, dst, sem)

    def column(ref, mb, j):
        row = ref[pl.ds(mb, 1), :]
        part = row[:, 0:T]
        for c in range(1, NJ):
            part = jnp.where(j == c, row[:, c * T:(c + 1) * T], part)
        return jnp.broadcast_to(part, (HEAD_DIM, T)).T

    wqkv_own = (wq_ref, wk_ref, wv_ref, wo_ref)

    def mlp_copies():
        cps = []
        for n in range(NB):
            cps.append(local(wg_ref.at[0, :, pl.ds(n * FB, FB)], wg_s.at[n], mlp_sem.at[0, n]))
            cps.append(local(wu_ref.at[0, :, pl.ds(n * FB, FB)], wu_s.at[n], mlp_sem.at[1, n]))
            cps.append(local(wd_ref.at[0, :, pl.ds(n * DB, DB)], wd_s.at[n], mlp_sem.at[2, n]))
        return cps

    NW = n_mb // 2

    def x_copy(w, home):
        u = w * NJ + z
        return rcopy(x_ref.at[2 * w + (home - 1)], hin_hbm.at[u], xs.at[w, home - 1], (hin_sem if w == 0 else xp).at[u], tp=home)

    def x_each(w, act):
        for home in (1, 2):
            @pl.when((s == (0 if w == 0 else 2)) & (z != home))
            def _():
                act(x_copy(w, home))

    def x_pass(w, j):
        u = w * NJ + j
        return rcopy(hin_hbm.at[u], hin_hbm.at[u], xq.at[w, j], hin_sem.at[u], pp=0)

    def half(ref, m, h):
        rows = (D if m < 3 else QL) // 2
        return ref.at[pl.ds(h * rows, rows), :]

    def wslot(r, m):
        return wqkv_hbm.at[r, m] if m < 3 else wo_hbm.at[pl.ds((r + 1) * QL, QL)]

    def own_w(m):
        return wqkv_own[m].at[0]

    def wo_own():
        return local(own_w(3), wo_hbm.at[pl.ds(0, QL)], wo_sem)

    def o_send(k):
        h = hx if k < 4 else 1 - hx
        return rcopy(half(own_w(k % 4), k % 4, h), half(wslot(0, k % 4), k % 4, h), wsnd.at[k], wr.at[0, k], tp=inner)

    def p_send(m):
        return rcopy(half(own_w(m), m, hx), half(wslot(1, m), m, hx), wsnd.at[m], wr.at[1, m], tp=peer)

    def f_send(m):
        return rcopy(half(wslot(0, m), m, hx), half(wslot(2, m), m, hx), wfwd.at[m], wr.at[2, m], tp=peer)

    def x_send(r, m):
        return rcopy(half(wslot(r, m), m, hx), half(wslot(r, m), m, hx), wxs.at[r - 1, m], wx.at[r - 1, m], dp=1 - hx)

    def w_ready(rs, ms):
        for m in ms:
            if 0 in rs:
                o_send(4 + m).wait_recv()
            for r in (1, 2):
                if r in rs:
                    x_send(r, m).wait_recv()

    def release():
        @pl.when(odd == 0)
        def _():
            pl.semaphore_signal(gate, inc=1, device_id={"pp": s + 1}, device_id_type=MESH)

    @pl.when(odd == 1)
    def _():
        for c in mlp_copies():
            c.start()
        with jax.named_scope('w_gate'):
            pl.semaphore_wait(gate, 1)

    @pl.when(is_outer)
    def _():
        for k in range(8):
            o_send(k).start()

        @pl.when(odd == 0)
        def _():
            x_each(0, lambda c: c.start())
            for c in mlp_copies():
                c.start()
        for k in range(5):
            o_send(k).wait_send()
        release()
        for w in range(1, NW):
            x_each(w, lambda c: c.start())

    @pl.when(is_home)
    def _():
        for m in range(4):
            p_send(m).start()
        wo_own().start()

        @pl.when(odd == 0)
        def _():
            for c in mlp_copies():
                c.start()
        def zero_rows(b, carry):
            for i in range(4):
                kc[i, pl.ds(b * RB, RB), :] = jnp.zeros((RB, QL), BF16)
                vc[i, pl.ds(b * RB, RB), :] = jnp.zeros((RB, QL), BF16)
            return carry
        lax.fori_loop(0, S // RB, zero_rows, 0)

        def tables(w):
            lane = lax.broadcasted_iota(jnp.int32, (T, HEAD_DIM), 1)

            def table_rows(b, carry):
                rows = pl.ds(pl.multiple_of(b * T, T), T)
                ang = column(pos_ref, 2 * w + hb, b).astype(F32) * invf_ref[0:1, :]
                table[w, rows, :] = jnp.where(lane < HEAD_DIM // 2, jnp.cos(ang), jnp.sin(ang))
                return carry
            with jax.named_scope('table'):
                lax.fori_loop(0, NJ, table_rows, 0)

        steps = [("o", 0), ("p", 0), ("t", 0), ("o", 1), ("p", 1), ("t", 1), ("o", 2), ("p", 2), ("t", 2), ("o", 3), ("p", 3), ("t", 3),
                 ("f", 0), ("g", 0), ("f", 1), ("f", 2), ("f", 3)]
        for kind, m in steps:
          with jax.named_scope('w_' + kind + str(m)):
            if kind == "o":
                o_send(m).wait_recv()
                f_send(m).start()
            elif kind == "p":
                p_send(m).wait_recv()
                x_send(1, m).start()
            elif kind == "f":
                f_send(m).wait_recv()
                x_send(2, m).start()
            elif kind == "g":
                release()
            elif m < n_mb // 2:
                tables(m)
        for w in range(NW):
            x_each(w, lambda c: c.start())
        w_ready([0, 1], range(3))

        @pl.when(s == 2)
        def _():
            for w in range(1, NW):
                for j in range(NJ):
                    @pl.when(z != j)
                    def _():
                        local(hin_hbm.at[w * NJ + j], hin_hbm.at[w * NJ + j], xp.at[w * NJ + j]).wait()
                        x_pass(w, j).start()

    def gslot(g, u):
        return lax.rem(g - 1 + u, 2)

    def group_copies(g, u):
        if g == 0:
            return [local(own_w(m), wres.at[m], wres_sem.at[m]) for m in range(3)]
        p = gslot(g, u)
        if g < 4:
            return [local(wqkv_hbm.at[g - 1], wst.at[p], wst_sem.at[p, 0])]
        return [local(wo_hbm.at[:, pl.ds(((g - 4) * 3 + m) * OB, OB)], wst.at[p, m], wst_sem.at[p, m]) for m in range(3 if g == 4 else 1)]

    def group_start(g, u):
        for c in group_copies(g, u):
            c.start()

    def group_wait(g, u):
        for c in group_copies(g, u):
            c.wait()

    def h_fetch(u):
        mb = 2 * (u // NJ) + hb
        here = lax.rem(u, NJ) == z
        dst = hin.at[lax.rem(u, HS)]

        @pl.when((s == 0) & here)
        def _():
            local(x_ref.at[mb], dst, hv_sem).start()

        @pl.when((s == 0) & jnp.logical_not(here))
        def _():
            local(hin_hbm.at[u], hin_hbm.at[u], hin_sem.at[u]).wait()
            local(hin_hbm.at[u], dst, hv_sem).start()

    @pl.when(is_home)
    def _():
        group_start(0, 0)
        group_start(1, 0)
        group_start(2, 0)
        h_fetch(0)

    for c in mlp_copies():
        c.wait()

    def hin_copy(u):
        return rcopy(h2b, hin.at[lax.rem(u, HS)], s5s, hin_sem.at[u], pp=lax.rem(s + 1, n_stages))

    def s1_outer(u):
        blk = gb.at[lax.rem(u, 3), pl.ds(pl.multiple_of(hb * T, T), T), :]
        return rcopy(blk, blk, s1s.at[0], ag.at[hb, lax.rem(u, 3)], tp=outer)

    def s1_peer(u):
        blk = gb.at[lax.rem(u, 3), pl.ds(pl.multiple_of(hb * T, T), T), :]
        return rcopy(blk, blk, s1s.at[1], ag.at[hb, lax.rem(u, 3)], tp=peer)

    def s2_copy(u):
        blk = gb.at[lax.rem(u, 3), pl.ds(pl.multiple_of((1 - hb) * T, T), T), :]
        return rcopy(blk, blk, s2s, ag.at[1 - hb, lax.rem(u, 3)], tp=outer)

    def ag_wait(b, u):
        blk = gb.at[lax.rem(u, 3), pl.ds(pl.multiple_of(b * T, T), T), :]
        local(blk, blk, ag.at[b, lax.rem(u, 3)]).wait()

    def s3_copy(u, b):
        sl = lax.rem(u, 2)
        blk = px.at[sl, pl.ds(pl.multiple_of(b * T, T), T), :]
        return rcopy(blk, blk, pxs.at[sl, b], pxr.at[sl, b], tp=inner)

    def s4_copy(u):
        return rcopy(sendb, ps.at[lax.rem(u, 2)], s4s, psr.at[lax.rem(u, 2)], tp=peer)

    def park_copy(u):
        return rcopy(h2b, hin_hbm.at[u], s5s, op.at[u], pp=1)

    def last_copy():
        mb = n_mb - 2 + hb
        return rcopy(h2b, out_ref.at[mb], s6s, outr.at[mb], tp=NJ - 1)

    def norm_rows(src, gain, dst):
        hf = src.astype(F32)
        inv = lax.rsqrt(jnp.mean(hf * hf, axis=-1, keepdims=True) + NORM_EPS)
        return (hf * inv * gain.astype(F32)).astype(BF16)

    def attention(u):
      with jax.named_scope('attn'):
        attention_(u)

    def attention_(u):
        w = u // NJ
        j = lax.rem(u, NJ)
        mb = 2 * w + hb
        row0 = pl.multiple_of(j * T, T)
        hs = lax.rem(u, HS)

        with jax.named_scope('w_hin'):
            @pl.when(s == 0)
            def _():
                local(x_ref.at[mb], hin.at[hs], hv_sem).wait()

            @pl.when(s > 0)
            def _():
                hin_copy(u).wait_recv()

        def norm_a(b, carry):
            rows = pl.ds(b * NR, NR)
            abuf[rows, :] = norm_rows(hin[hs, rows, :], ga_ref[0:1, :], None)
            return carry
        lax.fori_loop(0, T // NR, norm_a, 0)

        segrow = seg_ref[pl.ds(mb, 1), :]
        segc = column(seg_ref, mb, j)
        ti = lax.broadcasted_iota(jnp.int32, (T, HEAD_DIM), 0) + row0
        for c in range(0, S, HEAD_DIM):
            segr = segrow[:, c:c + HEAD_DIM]
            ui = lax.broadcasted_iota(jnp.int32, (T, HEAD_DIM), 1) + c
            mask[:, c:c + HEAD_DIM] = jnp.where((segc == segr) & (ui <= ti), 1.0, 0.0)

        def rope(val):
            pk = table[w, pl.ds(row0, T), :]
            lane = lax.broadcasted_iota(jnp.int32, (T, HEAD_DIM), 1)
            swapped = pltpu.roll(pk, HEAD_DIM // 2, 1)
            cosw = jnp.where(lane < HEAD_DIM // 2, pk, swapped)
            sinw = jnp.where(lane < HEAD_DIM // 2, -swapped, pk)
            outs = []
            for h in range(NH):
                v = val[:, h * HEAD_DIM:(h + 1) * HEAD_DIM]
                outs.append((v * cosw + pltpu.roll(v, HEAD_DIM // 2, 1) * sinw).astype(BF16))
            return outs

        def hcols(h):
            return slice(h * HEAD_DIM, (h + 1) * HEAD_DIM)

        def proj(i):
            p = i % 2

            def w(m):
                return wres[m] if i == 0 else wst[gslot(i, u), m]
            for h, val in enumerate(rope(jnp.dot(abuf[...], w(0), preferred_element_type=F32))):
                qb[p, :, hcols(h)] = val
            for h, val in enumerate(rope(jnp.dot(abuf[...], w(1), preferred_element_type=F32))):
                kc[i, pl.ds(row0, T), hcols(h)] = val
            vc[i, pl.ds(row0, T), :] = jnp.dot(abuf[...], w(2), preferred_element_type=F32).astype(BF16)

        def heads(i):
            for h in range(NH):
                sc = lax.dot_general(qb[i % 2, :, hcols(h)], kc[i, :, hcols(h)], (((1,), (1,)), ((), ())),
                                     preferred_element_type=F32) * scale
                pacc[0:T, h * S:(h + 1) * S] = jnp.where(mask[...] > 0.5, sc, NEG)
            for h in range(NH):
                for r in range(0, T, 32):
                    sc = pacc[r:r + 32, h * S:(h + 1) * S]
                    e = jnp.exp(sc - jnp.max(sc, axis=-1, keepdims=True))
                    pbuf[h, r:r + 32, :] = (e * (1.0 / jnp.sum(e, axis=-1, keepdims=True))).astype(BF16)
            for h in range(NH):
                act[0:T, i * QL + h * HEAD_DIM:i * QL + (h + 1) * HEAD_DIM] = jnp.dot(
                    pbuf[h], vc[i, :, hcols(h)], preferred_element_type=F32).astype(BF16)

        with jax.named_scope('shards'):
            @pl.when(u == 0)
            def _():
                group_wait(0, u)
            proj(0)
            for i in range(3):
                group_wait(i + 1, u)
                proj(i + 1)
                if i < 2:
                    @pl.when(u == 0)
                    def _():
                        if i == 0:
                            w_ready([2], range(3))
                        else:
                            w_ready([0, 1, 2], [3])
                            wo_own().wait()
                group_start(i + 3, u)
                heads(i)
                if i == 0:
                    @pl.when(u < N - 1)
                    def _():
                        h_fetch(u + 1)
            heads(3)

        finish(u)
        with jax.named_scope('wo'):
            def wo_block(n, w):
                act[T:2 * T, n * OB:(n + 1) * OB] = jnp.dot(act[0:T, 0:4 * QL], w, preferred_element_type=F32).astype(BF16)

            group_wait(4, u)
            group_wait(5, u)
            for n in range(3):
                wo_block(n, wst[gslot(4, u), n])

            wo_block(3, wst[gslot(5, u), 0])

            @pl.when(u < N - 1)
            def _():
                group_start(1, u + 1)
                group_start(2, u + 1)

        def norm_b(b, carry):
            rows = pl.ds(b * NR, NR)
            h1 = (hin[hs, rows, :].astype(F32) + act[pl.ds(pl.multiple_of(T + b * NR, NR), NR), 0:D].astype(F32)).astype(BF16)
            h1b[lax.rem(u, 3), rows, :] = h1
            gb[lax.rem(u, 3), pl.ds(pl.multiple_of(hb * T + b * NR, NR), NR), :] = norm_rows(h1, gm_ref[0:1, :], None)
            return carry
        lax.fori_loop(0, T // NR, norm_b, 0)

        @pl.when((s > 0) & (u < N - HS))
        def _():
            pl.semaphore_signal(cred, inc=1, device_id={"pp": s - 1}, device_id_type=MESH)

    def mlp(sl, row0, rows, store):
        UN = 2 if NB % 2 == 0 else 1

        def up(q, carry):
            for n in [q * UN + k for k in range(UN)]:
                xin = gb[sl, pl.ds(row0, rows), :]
                g = jnp.dot(xin, wg_s[n], preferred_element_type=F32)
                u_ = jnp.dot(xin, wu_s[n], preferred_element_type=F32)
                act[0:rows, pl.ds(pl.multiple_of(n * FB, FB), FB)] = (jax.nn.silu(g) * u_).astype(BF16)
            return carry
        lax.fori_loop(0, NB // UN, up, 0)

        def down(q, carry):
            for n in [q * UN + k for k in range(UN)]:
                store(pl.ds(pl.multiple_of(n * DB, DB), DB), jnp.dot(act[0:rows, 0:FL], wd_s[n], preferred_element_type=F32))
            return carry
        lax.fori_loop(0, NB // UN, down, 0)

    def mlp_home(u):
        def store(c, val):
            pacc[:, c] = val
        with jax.named_scope('mlp'):
            mlp(lax.rem(u, 3), 0, 2 * T, store)

    def mlp_outer(u, b):
        def store(c, val):
            px[lax.rem(u, 2), pl.ds(pl.multiple_of(b * T, T), T), c] = val.astype(BF16)
        with jax.named_scope('mlp_o'):
            mlp(lax.rem(u, 3), pl.multiple_of(b * T, T), T, store)

    def forward(u):
        @pl.when((u >= 1) & (u <= N))
        def _():
            s2_copy(u - 1).wait_send()

        @pl.when(u < N)
        def _():
            with jax.named_scope('w_ag'):
                ag_wait(1 - hb, u)
            s2_copy(u).start()

    def combine(v):
        sl = lax.rem(v, 2)
        with jax.named_scope('w_s3'):
            s3_copy(v, 0).wait_recv()
            s3_copy(v, 1).wait_recv()

        @pl.when(v >= 1)
        def _():
            s4_copy(v - 1).wait_send()

        def comb(b, carry):
            rows = pl.ds(b * RB, RB)
            mine = pl.ds(pl.multiple_of(hb * T + b * RB, RB), RB)
            theirs = pl.ds(pl.multiple_of((1 - hb) * T + b * RB, RB), RB)
            oacc[rows, :] = pacc[mine, :] + px[sl, mine, :].astype(F32)
            sendb[rows, :] = (pacc[theirs, :] + px[sl, theirs, :].astype(F32)).astype(BF16)
            return carry
        lax.fori_loop(0, T // RB, comb, 0)
        s4_copy(v).start()

    def finish(u):
        @pl.when((u >= 2) & (u < N + 2))
        def _():
            v = u - 2
            with jax.named_scope('w_s4'):
                s4_copy(v).wait_recv()
            vw = v // NJ
            vj = lax.rem(v, NJ)

            @pl.when(v >= 1)
            def _():
                hin_copy(v).wait_send()

            def fin(b, carry):
                rows = pl.ds(b * RB, RB)
                d = (oacc[rows, :] + ps[lax.rem(v, 2), rows, :].astype(F32)).astype(BF16)
                h2b[rows, :] = (h1b[lax.rem(v, 3), rows, :].astype(F32) + d.astype(F32)).astype(BF16)
                return carry
            lax.fori_loop(0, T // RB, fin, 0)

            @pl.when((s < n_stages - 1) & (v >= HS))
            def _():
                with jax.named_scope('w_cred'):
                    pl.semaphore_wait(cred, 1)

            @pl.when(s < n_stages - 1)
            def _():
                hin_copy(v).start()

            @pl.when(s == n_stages - 1)
            def _():
                park_copy(v).start()

            @pl.when((s == n_stages - 1) & (v == N - 1))
            def _():
                last_copy().start()

    def body(u, carry):
        @pl.when(is_home)
        def _():
            @pl.when(u < N)
            def _():
                attention(u)

            @pl.when((u >= 1) & (u <= N))
            def _():
                s1_outer(u - 1).wait_send()
                s1_peer(u - 1).wait_send()

            @pl.when(u < N)
            def _():
                s1_peer(u).start()
                s1_outer(u).start()

            @pl.when((u >= 1) & (u <= N))
            def _():
                mlp_home(u - 1)

            @pl.when(u >= N)
            def _():
                finish(u)

            @pl.when((u >= 1) & (u <= N))
            def _():
                combine(u - 1)

            forward(u)

        @pl.when(is_outer & (u < N))
        def _():
            for k in (0, 1):
                b = inner - 1 if k == 0 else 2 - inner
                with jax.named_scope('w_ag_outer'):
                    ag_wait(b, u)

                @pl.when(u >= 2)
                def _():
                    s3_copy(u - 2, b).wait_send()
                mlp_outer(u, b)
                s3_copy(u, b).start()

        return carry

    def out_fwd(mb, p, sem):
        return rcopy(out_ref.at[mb], out_ref.at[mb], ofs.at[mb, p], sem, pp=p)

    lax.fori_loop(0, N + 2, body, 0)

    last_here = (s == n_stages - 1) & (z == NJ - 1)

    @pl.when(last_here)
    def _():
        for mb in (n_mb - 2, n_mb - 1):
            local(out_ref.at[mb], out_ref.at[mb], outr.at[mb]).wait()
            out_fwd(mb, 2, outf).start()

    def od_copy(v):
        return rcopy(hin_hbm.at[v], out_ref.at[2 * (v // NJ) + hb], od.at[v], outr.at[2 * (v // NJ) + hb], tp=lax.rem(v, NJ))

    @pl.when(s == 1)
    def _():
        def spread(v, carry):
            vj = lax.rem(v, NJ)
            mine = 2 * (v // NJ) + hb

            @pl.when(is_home)
            def _():
                local(hin_hbm.at[v], hin_hbm.at[v], op.at[v]).wait()

            @pl.when(is_home & (vj != z))
            def _():
                od_copy(v).start()

            @pl.when(is_home & (vj == z))
            def _():
                c = local(hin_hbm.at[v], hin.at[0], hv_sem)
                c.start()
                c.wait()
                c = local(hin.at[0], out_ref.at[mine], hv_sem)
                c.start()
                c.wait()

            @pl.when(vj == z)
            def _():
                for b in (0, 1):
                    mb = 2 * (v // NJ) + b

                    @pl.when(z - 1 != b)
                    def _(mb=mb):
                        local(out_ref.at[mb], out_ref.at[mb], outr.at[mb]).wait()
                    out_fwd(mb, 0, outf).start()

                    @pl.when(v < N - 1)
                    def _(mb=mb):
                        out_fwd(mb, 3, outf).start()
                        out_fwd(mb, 2, outf).start()
            return carry
        lax.fori_loop(0, N, spread, 0)

    @pl.when(is_home)
    def _():
        s4_copy(N - 1).wait_send()
        hin_copy(N - 1).wait_send()

        @pl.when(s == n_stages - 1)
        def _():
            last_copy().wait_send()

    @pl.when(is_outer)
    def _():
        for b in (0, 1):
            s3_copy(N - 2, b).wait_send()
            s3_copy(N - 1, b).wait_send()

    @pl.when(is_outer)
    def _():
        for k in range(5, 8):
            o_send(k).wait_send()

    @pl.when(is_home)
    def _():
        for m in range(4):
            p_send(m).wait_send()
            f_send(m).wait_send()
            x_send(1, m).wait_send()
            x_send(2, m).wait_send()

        @pl.when(s == 2)
        def _():
            for w in range(1, NW):
                for j in range(NJ):
                    @pl.when(z != j)
                    def _():
                        x_pass(w, j).wait_send()

        @pl.when(s == 1)
        def _():
            def spread_done(v, carry):
                @pl.when(lax.rem(v, NJ) != z)
                def _():
                    od_copy(v).wait_send()
                return carry
            lax.fori_loop(0, N, spread_done, 0)

    for w in range(NW):
        x_each(w, lambda c: c.wait_send())

    @pl.when(s == 1)
    def _():
        for mb in range(n_mb):
            out_fwd(mb, 0, outf).wait_send()
            if mb < n_mb - 2:
                out_fwd(mb, 3, outf).wait_send()
                out_fwd(mb, 2, outf).wait_send()
            else:
                @pl.when(z < NJ - 1)
                def _(mb=mb):
                    out_fwd(mb, 3, outf).wait_send()
                    out_fwd(mb, 2, outf).wait_send()

    @pl.when(last_here)
    def _():
        for mb in (n_mb - 2, n_mb - 1):
            out_fwd(mb, 2, outf).wait_send()
        early = out_ref.at[pl.ds(0, n_mb - 2)]
        local(early, early, outf).wait()

    @pl.when((s == n_stages - 1) & (z < NJ - 1))
    def _():
        local(out_ref, out_ref, outf).wait()

    @pl.when((s == 0) | (s == 2))
    def _():
        local(out_ref, out_ref, outf).wait()


def solution(mesh):
    n_stages = mesh.shape['pp']

    def stage_program(hidden_in, seg_ids, positions, attn_norm, w_query, w_key, w_value, w_out, mlp_norm, w_gate, w_up, w_down):
        n_mb, T, D = hidden_in.shape
        S = seg_ids.shape[1]
        QL = w_query.shape[2]
        FL = w_gate.shape[2]
        NJ = S // T
        N = (n_mb // 2) * NJ
        NB = max(1, FL // 512)
        invf = jnp.asarray(np.tile(rope_freqs(), 2)[None, :], F32)
        any_spec = pl.BlockSpec(memory_space=pl.ANY)
        vmem = pl.BlockSpec(memory_space=pltpu.VMEM)
        dma = pltpu.SemaphoreType.DMA
        scratch = [
            pltpu.VMEM((NB, D, FL // NB), BF16), pltpu.VMEM((NB, D, FL // NB), BF16), pltpu.VMEM((NB, FL, D // NB), BF16),
            pltpu.VMEM((3, D, QL), BF16), pltpu.VMEM((2, 3, D, QL), BF16),
            pltpu.VMEM((3, 2 * T, D), BF16),
            pltpu.VMEM((2, 2 * T, D), BF16),
            pltpu.VMEM((2, T, D), BF16),
            pltpu.VMEM((4, S, QL), BF16), pltpu.VMEM((4, S, QL), BF16),
            pltpu.VMEM((4, T, D), BF16),
            pltpu.VMEM((3, T, D), BF16),
            pltpu.VMEM((2 * T, D), F32),
            pltpu.VMEM((T, D), F32),
            pltpu.VMEM((T, D), BF16),
            pltpu.VMEM((T, D), BF16),
            pltpu.VMEM((2 * T, max(D, FL, 4 * QL)), BF16),
            pltpu.VMEM((T, D), BF16),
            pltpu.VMEM((2, T, QL), BF16),
            pltpu.VMEM((n_mb // 2, S, HEAD_DIM), F32),
            pltpu.VMEM((T, S), F32), pltpu.VMEM((QL // HEAD_DIM, T, S), BF16),
            dma((3, 8)), dma((2, 4)), dma((8,)), dma((4,)), dma((2, 4)),
            dma((N,)), dma((n_mb // 2, 2)), dma((2, 3)), dma((2,)), dma, dma((2, 2)), dma((2, 2)), dma((2,)), dma, dma,
            dma((n_mb,)), dma, dma((n_mb, n_stages)),
            dma((3,)), dma((2, 3)), dma, dma((3, NB)), dma, dma, dma((N,)), dma((n_mb // 2, NJ)), dma((N,)), dma((N,)),
            pltpu.SemaphoreType.REGULAR, pltpu.SemaphoreType.REGULAR,
        ]
        return pl.pallas_call(
            functools.partial(kernel, n_stages),
            out_shape=[jax.ShapeDtypeStruct(hidden_in.shape, BF16), jax.ShapeDtypeStruct((3, 3, D, QL), BF16),
                       jax.ShapeDtypeStruct((4 * QL, D), BF16), jax.ShapeDtypeStruct((N, T, D), BF16)],
            in_specs=[any_spec, vmem, vmem, vmem, vmem, vmem] + [any_spec] * 7,
            out_specs=[any_spec] * 4,
            scratch_shapes=scratch,
            compiler_params=pltpu.CompilerParams(has_side_effects=True, vmem_limit_bytes=67_043_328),
        )(hidden_in, seg_ids, positions, invf, attn_norm, mlp_norm, w_query, w_key, w_value, w_out, w_gate, w_up, w_down)[0]

    act_spec = P('dp', 'tp', None)
    row_spec = P('dp', None)
    gain_spec = P('pp', None)
    col_spec = P('pp', None, 'tp')
    rows_spec = P('pp', 'tp', None)
    return jax.shard_map(stage_program, mesh=mesh,
                         in_specs=(act_spec, row_spec, row_spec, gain_spec, col_spec, col_spec, col_spec, rows_spec, gain_spec, col_spec, col_spec, rows_spec),
                         out_specs=act_spec, check_vma=False)
```

```python
import functools
import math

import jax
import jax.numpy as jnp
import numpy as np
from jax import lax
from jax.experimental import pallas as pl
from jax.experimental.pallas import tpu as pltpu
from jax.sharding import PartitionSpec as P

HEAD_DIM = 128
NORM_EPS = 1e-5
ROPE_THETA = 500000.0
ROPE_FACTOR = 8.0
LOW_FREQ = 1.0
HIGH_FREQ = 4.0
ORIG_CTX = 8192.0
NEG = -1e30
MESH = pl.DeviceIdType.MESH
F32 = jnp.float32
BF16 = jnp.bfloat16


def rope_freqs():
    base_freq = 1.0 / (ROPE_THETA ** (np.arange(0, HEAD_DIM, 2) / HEAD_DIM))
    wavelen = 2.0 * np.pi / base_freq
    smooth = (ORIG_CTX / wavelen - LOW_FREQ) / (HIGH_FREQ - LOW_FREQ)
    blended = (1.0 - smooth) * base_freq / ROPE_FACTOR + smooth * base_freq
    scaled = np.where(wavelen > ORIG_CTX / LOW_FREQ, base_freq / ROPE_FACTOR, blended)
    return np.where(wavelen < ORIG_CTX / HIGH_FREQ, base_freq, scaled)


def kernel(n_stages, x_ref, seg_ref, pos_ref, invf_ref, ga_ref, gm_ref,
           wq_ref, wk_ref, wv_ref, wo_ref, wg_ref, wu_ref, wd_ref,
           out_ref,
           wqkv_hbm, wo_hbm, hin_hbm,
           wg_s, wu_s, wd_s, wres, wst, gb, px, ps, kc, vc, hin, h1b, pacc, oacc, sendb, h2b, act, abuf, qb,
           table, mask, pbuf,
           wr, wx, wsnd, wfwd, wxs, hin_sem, xs, ag, s1s, s2s, pxr, pxs, psr, s4s, s5s, outr, outf, ofs,
           wres_sem, wst_sem, wo_sem, mlp_sem, hv_sem, s6s, xp, xq, op, od, gate, cred):
    n_mb, T, D = x_ref.shape
    QL = wq_ref.shape[2]
    FL = wg_ref.shape[2]
    NB = wg_s.shape[0]
    FB = FL // NB
    S = seg_ref.shape[1]
    NJ = S // T
    NH = QL // HEAD_DIM
    N = (n_mb // 2) * NJ
    DB = D // NB
    scale = HEAD_DIM ** -0.5
    RB = 16
    NR = 32
    HS = hin.shape[0]
    OB = wst.shape[3]
    NO = D // OB

    hx = lax.axis_index("dp")
    z = lax.axis_index("tp")
    s = lax.axis_index("pp")
    is_home = (z == 1) | (z == 2)
    is_outer = (z == 0) | (z == 3)
    hb = lax.rem(z + 1, 2) * 0 + (z - 1)
    peer = 3 - z
    outer = 3 * (z - 1)
    inner = 1 + z // 2
    odd = lax.rem(s, 2)

    def rcopy(src, dst, ssem, rsem, **dev):
        return pltpu.make_async_remote_copy(src_ref=src, dst_ref=dst, send_sem=ssem, recv_sem=rsem,
                                            device_id=dev, device_id_type=MESH)

    def local(src, dst, sem):
        return pltpu.make_async_copy(src, dst, sem)

    def column(ref, mb, j):
        row = ref[pl.ds(mb, 1), :]
        part = row[:, 0:T]
        for c in range(1, NJ):
            part = jnp.where(j == c, row[:, c * T:(c + 1) * T], part)
        return jnp.broadcast_to(part, (HEAD_DIM, T)).T

    wqkv_own = (wq_ref, wk_ref, wv_ref, wo_ref)

    def mlp_copies():
        cps = []
        for n in range(NB):
            cps.append(local(wg_ref.at[0, :, pl.ds(n * FB, FB)], wg_s.at[n], mlp_sem.at[0, n]))
            cps.append(local(wu_ref.at[0, :, pl.ds(n * FB, FB)], wu_s.at[n], mlp_sem.at[1, n]))
            cps.append(local(wd_ref.at[0, :, pl.ds(n * DB, DB)], wd_s.at[n], mlp_sem.at[2, n]))
        return cps

    NW = n_mb // 2

    def x_copy(w, home):
        u = w * NJ + z
        return rcopy(x_ref.at[2 * w + (home - 1)], hin_hbm.at[u], xs.at[w, home - 1], (hin_sem if w == 0 else xp).at[u], tp=home)

    def x_each(w, act):
        for home in (1, 2):
            @pl.when((s == (0 if w == 0 else 2)) & (z != home))
            def _():
                act(x_copy(w, home))

    def x_pass(w, j):
        u = w * NJ + j
        return rcopy(hin_hbm.at[u], hin_hbm.at[u], xq.at[w, j], hin_sem.at[u], pp=0)

    def half(ref, m, h):
        rows = (D if m < 3 else QL) // 2
        return ref.at[pl.ds(h * rows, rows), :]

    def wslot(r, m):
        return wqkv_hbm.at[r, m] if m < 3 else wo_hbm.at[pl.ds((r + 1) * QL, QL)]

    def own_w(m):
        return wqkv_own[m].at[0]

    def wo_own():
        return local(own_w(3), wo_hbm.at[pl.ds(0, QL)], wo_sem)

    def o_send(k):
        h = hx if k < 4 else 1 - hx
        return rcopy(half(own_w(k % 4), k % 4, h), half(wslot(0, k % 4), k % 4, h), wsnd.at[k], wr.at[0, k], tp=inner)

    def p_send(m):
        return rcopy(half(own_w(m), m, hx), half(wslot(1, m), m, hx), wsnd.at[m], wr.at[1, m], tp=peer)

    def f_send(m):
        return rcopy(half(wslot(0, m), m, hx), half(wslot(2, m), m, hx), wfwd.at[m], wr.at[2, m], tp=peer)

    def x_send(r, m):
        return rcopy(half(wslot(r, m), m, hx), half(wslot(r, m), m, hx), wxs.at[r - 1, m], wx.at[r - 1, m], dp=1 - hx)

    def w_ready(rs, ms):
        for m in ms:
            if 0 in rs:
                o_send(4 + m).wait_recv()
            for r in (1, 2):
                if r in rs:
                    x_send(r, m).wait_recv()

    def release():
        @pl.when(odd == 0)
        def _():
            pl.semaphore_signal(gate, inc=1, device_id={"pp": s + 1}, device_id_type=MESH)

    @pl.when(odd == 1)
    def _():
        for c in mlp_copies():
            c.start()
        with jax.named_scope('w_gate'):
            pl.semaphore_wait(gate, 1)

    @pl.when(is_outer)
    def _():
        for k in range(8):
            o_send(k).start()

        @pl.when(odd == 0)
        def _():
            x_each(0, lambda c: c.start())
            for c in mlp_copies():
                c.start()
        for k in range(5):
            o_send(k).wait_send()
        release()
        for w in range(1, NW):
            x_each(w, lambda c: c.start())

    @pl.when(is_home)
    def _():
        for m in range(4):
            p_send(m).start()
        wo_own().start()

        @pl.when(odd == 0)
        def _():
            for c in mlp_copies():
                c.start()
        def zero_rows(b, carry):
            for i in range(4):
                kc[i, pl.ds(b * RB, RB), :] = jnp.zeros((RB, QL), BF16)
                vc[i, pl.ds(b * RB, RB), :] = jnp.zeros((RB, QL), BF16)
            return carry
        lax.fori_loop(0, S // RB, zero_rows, 0)

        def tables(w):
            lane = lax.broadcasted_iota(jnp.int32, (T, HEAD_DIM), 1)

            def table_rows(b, carry):
                rows = pl.ds(pl.multiple_of(b * T, T), T)
                ang = column(pos_ref, 2 * w + hb, b).astype(F32) * invf_ref[0:1, :]
                table[w, rows, :] = jnp.where(lane < HEAD_DIM // 2, jnp.cos(ang), jnp.sin(ang))
                return carry
            with jax.named_scope('table'):
                lax.fori_loop(0, NJ, table_rows, 0)

        steps = [("o", 0), ("p", 0), ("t", 0), ("o", 1), ("p", 1), ("t", 1), ("o", 2), ("p", 2), ("t", 2), ("o", 3), ("p", 3), ("t", 3),
                 ("f", 0), ("g", 0), ("f", 1), ("f", 2), ("f", 3)]
        for kind, m in steps:
          with jax.named_scope('w_' + kind + str(m)):
            if kind == "o":
                o_send(m).wait_recv()
                f_send(m).start()
            elif kind == "p":
                p_send(m).wait_recv()
                x_send(1, m).start()
            elif kind == "f":
                f_send(m).wait_recv()
                x_send(2, m).start()
            elif kind == "g":
                release()
            elif m < n_mb // 2:
                tables(m)
        for w in range(NW):
            x_each(w, lambda c: c.start())
        w_ready([0, 1], range(3))

        @pl.when(s == 2)
        def _():
            for w in range(1, NW):
                for j in range(NJ):
                    @pl.when(z != j)
                    def _():
                        local(hin_hbm.at[w * NJ + j], hin_hbm.at[w * NJ + j], xp.at[w * NJ + j]).wait()
                        x_pass(w, j).start()

    def gslot(g, u):
        return lax.rem(g - 1 + u, 2)

    def group_copies(g, u):
        if g == 0:
            return [local(own_w(m), wres.at[m], wres_sem.at[m]) for m in range(3)]
        p = gslot(g, u)
        if g < 4:
            return [local(wqkv_hbm.at[g - 1], wst.at[p], wst_sem.at[p, 0])]
        return [local(wo_hbm.at[:, pl.ds(((g - 4) * 3 + m) * OB, OB)], wst.at[p, m], wst_sem.at[p, m]) for m in range(3 if g == 4 else 1)]

    def group_start(g, u):
        for c in group_copies(g, u):
            c.start()

    def group_wait(g, u):
        for c in group_copies(g, u):
            c.wait()

    def h_fetch(u):
        mb = 2 * (u // NJ) + hb
        here = lax.rem(u, NJ) == z
        dst = hin.at[lax.rem(u, HS)]

        @pl.when((s == 0) & here)
        def _():
            local(x_ref.at[mb], dst, hv_sem).start()

        @pl.when((s == 0) & jnp.logical_not(here))
        def _():
            local(hin_hbm.at[u], hin_hbm.at[u], hin_sem.at[u]).wait()
            local(hin_hbm.at[u], dst, hv_sem).start()

    @pl.when(is_home)
    def _():
        group_start(0, 0)
        group_start(1, 0)
        group_start(2, 0)
        h_fetch(0)

    for c in mlp_copies():
        c.wait()

    def hin_copy(u):
        return rcopy(h2b, hin.at[lax.rem(u, HS)], s5s, hin_sem.at[u], pp=lax.rem(s + 1, n_stages))

    def s1_outer(u):
        blk = gb.at[lax.rem(u, 3), pl.ds(pl.multiple_of(hb * T, T), T), :]
        return rcopy(blk, blk, s1s.at[0], ag.at[hb, lax.rem(u, 3)], tp=outer)

    def s1_peer(u):
        blk = gb.at[lax.rem(u, 3), pl.ds(pl.multiple_of(hb * T, T), T), :]
        return rcopy(blk, blk, s1s.at[1], ag.at[hb, lax.rem(u, 3)], tp=peer)

    def s2_copy(u):
        blk = gb.at[lax.rem(u, 3), pl.ds(pl.multiple_of((1 - hb) * T, T), T), :]
        return rcopy(blk, blk, s2s, ag.at[1 - hb, lax.rem(u, 3)], tp=outer)

    def ag_wait(b, u):
        blk = gb.at[lax.rem(u, 3), pl.ds(pl.multiple_of(b * T, T), T), :]
        local(blk, blk, ag.at[b, lax.rem(u, 3)]).wait()

    def s3_copy(u, b):
        sl = lax.rem(u, 2)
        blk = px.at[sl, pl.ds(pl.multiple_of(b * T, T), T), :]
        return rcopy(blk, blk, pxs.at[sl, b], pxr.at[sl, b], tp=inner)

    def s4_copy(u):
        return rcopy(sendb, ps.at[lax.rem(u, 2)], s4s, psr.at[lax.rem(u, 2)], tp=peer)

    def park_copy(u):
        return rcopy(h2b, hin_hbm.at[u], s5s, op.at[u], pp=1)

    def last_copy():
        mb = n_mb - 2 + hb
        return rcopy(h2b, out_ref.at[mb], s6s, outr.at[mb], tp=NJ - 1)

    def norm_rows(src, gain, dst):
        hf = src.astype(F32)
        inv = lax.rsqrt(jnp.mean(hf * hf, axis=-1, keepdims=True) + NORM_EPS)
        return (hf * inv * gain.astype(F32)).astype(BF16)

    def attention(u):
      with jax.named_scope('attn'):
        attention_(u)

    def attention_(u):
        w = u // NJ
        j = lax.rem(u, NJ)
        mb = 2 * w + hb
        row0 = pl.multiple_of(j * T, T)
        hs = lax.rem(u, HS)

        with jax.named_scope('w_hin'):
            @pl.when(s == 0)
            def _():
                local(x_ref.at[mb], hin.at[hs], hv_sem).wait()

            @pl.when(s > 0)
            def _():
                hin_copy(u).wait_recv()

        def norm_a(b, carry):
            rows = pl.ds(b * NR, NR)
            abuf[rows, :] = norm_rows(hin[hs, rows, :], ga_ref[0:1, :], None)
            return carry
        lax.fori_loop(0, T // NR, norm_a, 0)

        segrow = seg_ref[pl.ds(mb, 1), :]
        segc = column(seg_ref, mb, j)
        ti = lax.broadcasted_iota(jnp.int32, (T, HEAD_DIM), 0) + row0
        for c in range(0, S, HEAD_DIM):
            segr = segrow[:, c:c + HEAD_DIM]
            ui = lax.broadcasted_iota(jnp.int32, (T, HEAD_DIM), 1) + c
            mask[:, c:c + HEAD_DIM] = jnp.where((segc == segr) & (ui <= ti), 1.0, 0.0)

        def rope(val):
            pk = table[w, pl.ds(row0, T), :]
            lane = lax.broadcasted_iota(jnp.int32, (T, HEAD_DIM), 1)
            swapped = pltpu.roll(pk, HEAD_DIM // 2, 1)
            cosw = jnp.where(lane < HEAD_DIM // 2, pk, swapped)
            sinw = jnp.where(lane < HEAD_DIM // 2, -swapped, pk)
            outs = []
            for h in range(NH):
                v = val[:, h * HEAD_DIM:(h + 1) * HEAD_DIM]
                outs.append((v * cosw + pltpu.roll(v, HEAD_DIM // 2, 1) * sinw).astype(BF16))
            return outs

        def hcols(h):
            return slice(h * HEAD_DIM, (h + 1) * HEAD_DIM)

        def proj(i):
            p = i % 2

            def w(m):
                return wres[m] if i == 0 else wst[gslot(i, u), m]
            for h, val in enumerate(rope(jnp.dot(abuf[...], w(0), preferred_element_type=F32))):
                qb[p, :, hcols(h)] = val
            for h, val in enumerate(rope(jnp.dot(abuf[...], w(1), preferred_element_type=F32))):
                kc[i, pl.ds(row0, T), hcols(h)] = val
            vc[i, pl.ds(row0, T), :] = jnp.dot(abuf[...], w(2), preferred_element_type=F32).astype(BF16)

        def heads(i):
            for h in range(NH):
                sc = lax.dot_general(qb[i % 2, :, hcols(h)], kc[i, :, hcols(h)], (((1,), (1,)), ((), ())),
                                     preferred_element_type=F32) * scale
                pacc[0:T, h * S:(h + 1) * S] = jnp.where(mask[...] > 0.5, sc, NEG)
            for h in range(NH):
                for r in range(0, T, 32):
                    sc = pacc[r:r + 32, h * S:(h + 1) * S]
                    e = jnp.exp(sc - jnp.max(sc, axis=-1, keepdims=True))
                    pbuf[h, r:r + 32, :] = (e * (1.0 / jnp.sum(e, axis=-1, keepdims=True))).astype(BF16)
            for h in range(NH):
                act[0:T, i * QL + h * HEAD_DIM:i * QL + (h + 1) * HEAD_DIM] = jnp.dot(
                    pbuf[h], vc[i, :, hcols(h)], preferred_element_type=F32).astype(BF16)

        with jax.named_scope('shards'):
            @pl.when(u == 0)
            def _():
                group_wait(0, u)
            proj(0)
            for i in range(3):
                group_wait(i + 1, u)
                proj(i + 1)
                if i < 2:
                    @pl.when(u == 0)
                    def _():
                        if i == 0:
                            w_ready([2], range(3))
                        else:
                            w_ready([0, 1, 2], [3])
                            wo_own().wait()
                group_start(i + 3, u)
                heads(i)
                if i == 0:
                    @pl.when(u < N - 1)
                    def _():
                        h_fetch(u + 1)
            heads(3)

        with jax.named_scope('wo'):
            def wo_block(n, w):
                act[T:2 * T, n * OB:(n + 1) * OB] = jnp.dot(act[0:T, 0:4 * QL], w, preferred_element_type=F32).astype(BF16)

            group_wait(4, u)
            group_wait(5, u)
            for n in range(3):
                wo_block(n, wst[gslot(4, u), n])

            wo_block(3, wst[gslot(5, u), 0])

            @pl.when(u < N - 1)
            def _():
                group_start(1, u + 1)
                group_start(2, u + 1)

        def norm_b(b, carry):
            rows = pl.ds(b * NR, NR)
            h1 = (hin[hs, rows, :].astype(F32) + act[pl.ds(pl.multiple_of(T + b * NR, NR), NR), 0:D].astype(F32)).astype(BF16)
            h1b[lax.rem(u, 3), rows, :] = h1
            gb[lax.rem(u, 3), pl.ds(pl.multiple_of(hb * T + b * NR, NR), NR), :] = norm_rows(h1, gm_ref[0:1, :], None)
            return carry
        lax.fori_loop(0, T // NR, norm_b, 0)

        @pl.when((s > 0) & (u < N - HS))
        def _():
            pl.semaphore_signal(cred, inc=1, device_id={"pp": s - 1}, device_id_type=MESH)

    def mlp(sl, row0, rows, store):
        UN = 2 if NB % 2 == 0 else 1

        def up(q, carry):
            for n in [q * UN + k for k in range(UN)]:
                xin = gb[sl, pl.ds(row0, rows), :]
                g = jnp.dot(xin, wg_s[n], preferred_element_type=F32)
                u_ = jnp.dot(xin, wu_s[n], preferred_element_type=F32)
                act[0:rows, pl.ds(pl.multiple_of(n * FB, FB), FB)] = (jax.nn.silu(g) * u_).astype(BF16)
            return carry
        lax.fori_loop(0, NB // UN, up, 0)

        def down(q, carry):
            for n in [q * UN + k for k in range(UN)]:
                store(pl.ds(pl.multiple_of(n * DB, DB), DB), jnp.dot(act[0:rows, 0:FL], wd_s[n], preferred_element_type=F32))
            return carry
        lax.fori_loop(0, NB // UN, down, 0)

    def mlp_home(u):
        def store(c, val):
            pacc[:, c] = val
        with jax.named_scope('mlp'):
            mlp(lax.rem(u, 3), 0, 2 * T, store)

    def mlp_outer(u, b):
        def store(c, val):
            px[lax.rem(u, 2), pl.ds(pl.multiple_of(b * T, T), T), c] = val.astype(BF16)
        with jax.named_scope('mlp_o'):
            mlp(lax.rem(u, 3), pl.multiple_of(b * T, T), T, store)

    def forward(u):
        @pl.when((u >= 1) & (u <= N))
        def _():
            s2_copy(u - 1).wait_send()

        @pl.when(u < N)
        def _():
            with jax.named_scope('w_ag'):
                ag_wait(1 - hb, u)
            s2_copy(u).start()

    def combine(v):
        sl = lax.rem(v, 2)
        with jax.named_scope('w_s3'):
            s3_copy(v, 0).wait_recv()
            s3_copy(v, 1).wait_recv()

        @pl.when(v >= 1)
        def _():
            s4_copy(v - 1).wait_send()

        def comb(b, carry):
            rows = pl.ds(b * RB, RB)
            mine = pl.ds(pl.multiple_of(hb * T + b * RB, RB), RB)
            theirs = pl.ds(pl.multiple_of((1 - hb) * T + b * RB, RB), RB)
            oacc[rows, :] = pacc[mine, :] + px[sl, mine, :].astype(F32)
            sendb[rows, :] = (pacc[theirs, :] + px[sl, theirs, :].astype(F32)).astype(BF16)
            return carry
        lax.fori_loop(0, T // RB, comb, 0)
        s4_copy(v).start()

    def finish(u):
        @pl.when((u >= 2) & (u < N + 2))
        def _():
            v = u - 2
            with jax.named_scope('w_s4'):
                s4_copy(v).wait_recv()
            vw = v // NJ
            vj = lax.rem(v, NJ)

            @pl.when(v >= 1)
            def _():
                hin_copy(v).wait_send()

            def fin(b, carry):
                rows = pl.ds(b * RB, RB)
                d = (oacc[rows, :] + ps[lax.rem(v, 2), rows, :].astype(F32)).astype(BF16)
                h2b[rows, :] = (h1b[lax.rem(v, 3), rows, :].astype(F32) + d.astype(F32)).astype(BF16)
                return carry
            lax.fori_loop(0, T // RB, fin, 0)

            @pl.when((s < n_stages - 1) & (v >= HS))
            def _():
                with jax.named_scope('w_cred'):
                    pl.semaphore_wait(cred, 1)

            @pl.when(s < n_stages - 1)
            def _():
                hin_copy(v).start()

            @pl.when(s == n_stages - 1)
            def _():
                park_copy(v).start()

            @pl.when((s == n_stages - 1) & (v == N - 1))
            def _():
                last_copy().start()

    def body(u, carry):
        @pl.when(is_home)
        def _():
            @pl.when(u < N)
            def _():
                attention(u)

            @pl.when((u >= 1) & (u <= N))
            def _():
                s1_outer(u - 1).wait_send()
                s1_peer(u - 1).wait_send()

            @pl.when(u < N)
            def _():
                s1_peer(u).start()
                s1_outer(u).start()

            @pl.when((u >= 1) & (u <= N))
            def _():
                mlp_home(u - 1)

            finish(u)
            forward(u)

            @pl.when((u >= 1) & (u <= N))
            def _():
                combine(u - 1)

        @pl.when(is_outer & (u < N))
        def _():
            for k in (0, 1):
                b = inner - 1 if k == 0 else 2 - inner
                with jax.named_scope('w_ag_outer'):
                    ag_wait(b, u)

                @pl.when(u >= 2)
                def _():
                    s3_copy(u - 2, b).wait_send()
                mlp_outer(u, b)
                s3_copy(u, b).start()

        return carry

    def out_fwd(mb, p, sem):
        return rcopy(out_ref.at[mb], out_ref.at[mb], ofs.at[mb, p], sem, pp=p)

    lax.fori_loop(0, N + 2, body, 0)

    last_here = (s == n_stages - 1) & (z == NJ - 1)

    @pl.when(last_here)
    def _():
        for mb in (n_mb - 2, n_mb - 1):
            local(out_ref.at[mb], out_ref.at[mb], outr.at[mb]).wait()
            out_fwd(mb, 2, outf).start()

    def od_copy(v):
        return rcopy(hin_hbm.at[v], out_ref.at[2 * (v // NJ) + hb], od.at[v], outr.at[2 * (v // NJ) + hb], tp=lax.rem(v, NJ))

    @pl.when(s == 1)
    def _():
        def spread(v, carry):
            vj = lax.rem(v, NJ)
            mine = 2 * (v // NJ) + hb

            @pl.when(is_home)
            def _():
                local(hin_hbm.at[v], hin_hbm.at[v], op.at[v]).wait()

            @pl.when(is_home & (vj != z))
            def _():
                od_copy(v).start()

            @pl.when(is_home & (vj == z))
            def _():
                c = local(hin_hbm.at[v], hin.at[0], hv_sem)
                c.start()
                c.wait()
                c = local(hin.at[0], out_ref.at[mine], hv_sem)
                c.start()
                c.wait()

            @pl.when(vj == z)
            def _():
                for b in (0, 1):
                    mb = 2 * (v // NJ) + b

                    @pl.when(z - 1 != b)
                    def _(mb=mb):
                        local(out_ref.at[mb], out_ref.at[mb], outr.at[mb]).wait()
                    out_fwd(mb, 0, outf).start()

                    @pl.when(v < N - 1)
                    def _(mb=mb):
                        out_fwd(mb, 3, outf).start()
                        out_fwd(mb, 2, outf).start()
            return carry
        lax.fori_loop(0, N, spread, 0)

    @pl.when(is_home)
    def _():
        s4_copy(N - 1).wait_send()
        hin_copy(N - 1).wait_send()

        @pl.when(s == n_stages - 1)
        def _():
            last_copy().wait_send()

    @pl.when(is_outer)
    def _():
        for b in (0, 1):
            s3_copy(N - 2, b).wait_send()
            s3_copy(N - 1, b).wait_send()

    @pl.when(is_outer)
    def _():
        for k in range(5, 8):
            o_send(k).wait_send()

    @pl.when(is_home)
    def _():
        for m in range(4):
            p_send(m).wait_send()
            f_send(m).wait_send()
            x_send(1, m).wait_send()
            x_send(2, m).wait_send()

        @pl.when(s == 2)
        def _():
            for w in range(1, NW):
                for j in range(NJ):
                    @pl.when(z != j)
                    def _():
                        x_pass(w, j).wait_send()

        @pl.when(s == 1)
        def _():
            def spread_done(v, carry):
                @pl.when(lax.rem(v, NJ) != z)
                def _():
                    od_copy(v).wait_send()
                return carry
            lax.fori_loop(0, N, spread_done, 0)

    for w in range(NW):
        x_each(w, lambda c: c.wait_send())

    @pl.when(s == 1)
    def _():
        for mb in range(n_mb):
            out_fwd(mb, 0, outf).wait_send()
            if mb < n_mb - 2:
                out_fwd(mb, 3, outf).wait_send()
                out_fwd(mb, 2, outf).wait_send()
            else:
                @pl.when(z < NJ - 1)
                def _(mb=mb):
                    out_fwd(mb, 3, outf).wait_send()
                    out_fwd(mb, 2, outf).wait_send()

    @pl.when(last_here)
    def _():
        for mb in (n_mb - 2, n_mb - 1):
            out_fwd(mb, 2, outf).wait_send()
        early = out_ref.at[pl.ds(0, n_mb - 2)]
        local(early, early, outf).wait()

    @pl.when((s == n_stages - 1) & (z < NJ - 1))
    def _():
        local(out_ref, out_ref, outf).wait()

    @pl.when((s == 0) | (s == 2))
    def _():
        local(out_ref, out_ref, outf).wait()


def solution(mesh):
    n_stages = mesh.shape['pp']

    def stage_program(hidden_in, seg_ids, positions, attn_norm, w_query, w_key, w_value, w_out, mlp_norm, w_gate, w_up, w_down):
        n_mb, T, D = hidden_in.shape
        S = seg_ids.shape[1]
        QL = w_query.shape[2]
        FL = w_gate.shape[2]
        NJ = S // T
        N = (n_mb // 2) * NJ
        NB = max(1, FL // 512)
        invf = jnp.asarray(np.tile(rope_freqs(), 2)[None, :], F32)
        any_spec = pl.BlockSpec(memory_space=pl.ANY)
        vmem = pl.BlockSpec(memory_space=pltpu.VMEM)
        dma = pltpu.SemaphoreType.DMA
        scratch = [
            pltpu.VMEM((NB, D, FL // NB), BF16), pltpu.VMEM((NB, D, FL // NB), BF16), pltpu.VMEM((NB, FL, D // NB), BF16),
            pltpu.VMEM((3, D, QL), BF16), pltpu.VMEM((2, 3, D, QL), BF16),
            pltpu.VMEM((3, 2 * T, D), BF16),
            pltpu.VMEM((2, 2 * T, D), BF16),
            pltpu.VMEM((2, T, D), BF16),
            pltpu.VMEM((4, S, QL), BF16), pltpu.VMEM((4, S, QL), BF16),
            pltpu.VMEM((4, T, D), BF16),
            pltpu.VMEM((3, T, D), BF16),
            pltpu.VMEM((2 * T, D), F32),
            pltpu.VMEM((T, D), F32),
            pltpu.VMEM((T, D), BF16),
            pltpu.VMEM((T, D), BF16),
            pltpu.VMEM((2 * T, max(D, FL, 4 * QL)), BF16),
            pltpu.VMEM((T, D), BF16),
            pltpu.VMEM((2, T, QL), BF16),
            pltpu.VMEM((n_mb // 2, S, HEAD_DIM), F32),
            pltpu.VMEM((T, S), F32), pltpu.VMEM((QL // HEAD_DIM, T, S), BF16),
            dma((3, 8)), dma((2, 4)), dma((8,)), dma((4,)), dma((2, 4)),
            dma((N,)), dma((n_mb // 2, 2)), dma((2, 3)), dma((2,)), dma, dma((2, 2)), dma((2, 2)), dma((2,)), dma, dma,
            dma((n_mb,)), dma, dma((n_mb, n_stages)),
            dma((3,)), dma((2, 3)), dma, dma((3, NB)), dma, dma, dma((N,)), dma((n_mb // 2, NJ)), dma((N,)), dma((N,)),
            pltpu.SemaphoreType.REGULAR, pltpu.SemaphoreType.REGULAR,
        ]
        return pl.pallas_call(
            functools.partial(kernel, n_stages),
            out_shape=[jax.ShapeDtypeStruct(hidden_in.shape, BF16), jax.ShapeDtypeStruct((3, 3, D, QL), BF16),
                       jax.ShapeDtypeStruct((4 * QL, D), BF16), jax.ShapeDtypeStruct((N, T, D), BF16)],
            in_specs=[any_spec, vmem, vmem, vmem, vmem, vmem] + [any_spec] * 7,
            out_specs=[any_spec] * 4,
            scratch_shapes=scratch,
            compiler_params=pltpu.CompilerParams(has_side_effects=True, vmem_limit_bytes=67_043_328),
        )(hidden_in, seg_ids, positions, invf, attn_norm, mlp_norm, w_query, w_key, w_value, w_out, w_gate, w_up, w_down)[0]

    act_spec = P('dp', 'tp', None)
    row_spec = P('dp', None)
    gain_spec = P('pp', None)
    col_spec = P('pp', None, 'tp')
    rows_spec = P('pp', 'tp', None)
    return jax.shard_map(stage_program, mesh=mesh,
                         in_specs=(act_spec, row_spec, row_spec, gain_spec, col_spec, col_spec, col_spec, rows_spec, gain_spec, col_spec, col_spec, rows_spec),
                         out_specs=act_spec, check_vma=False)
```

```python
import functools
import math

import jax
import jax.numpy as jnp
import numpy as np
from jax import lax
from jax.experimental import pallas as pl
from jax.experimental.pallas import tpu as pltpu
from jax.sharding import PartitionSpec as P

HEAD_DIM = 128
NORM_EPS = 1e-5
ROPE_THETA = 500000.0
ROPE_FACTOR = 8.0
LOW_FREQ = 1.0
HIGH_FREQ = 4.0
ORIG_CTX = 8192.0
NEG = -1e30
MESH = pl.DeviceIdType.MESH
F32 = jnp.float32
BF16 = jnp.bfloat16


def rope_freqs():
    base_freq = 1.0 / (ROPE_THETA ** (np.arange(0, HEAD_DIM, 2) / HEAD_DIM))
    wavelen = 2.0 * np.pi / base_freq
    smooth = (ORIG_CTX / wavelen - LOW_FREQ) / (HIGH_FREQ - LOW_FREQ)
    blended = (1.0 - smooth) * base_freq / ROPE_FACTOR + smooth * base_freq
    scaled = np.where(wavelen > ORIG_CTX / LOW_FREQ, base_freq / ROPE_FACTOR, blended)
    return np.where(wavelen < ORIG_CTX / HIGH_FREQ, base_freq, scaled)


def kernel(n_stages, x_ref, seg_ref, pos_ref, invf_ref, ga_ref, gm_ref,
           wq_ref, wk_ref, wv_ref, wo_ref, wg_ref, wu_ref, wd_ref,
           out_ref,
           wqkv_hbm, wo_hbm, hin_hbm, pv_hbm, po_hbm,
           wg_s, wu_s, wd_s, wres, wst, gb, px, ps, kc, vc, hin, h1b, pacc, oacc, sendb, h2b, act, abuf, qb,
           table, mask, pbuf,
           wr, wx, wsnd, wfwd, wxs, hin_sem, xs, ag, s1s, s2s, pxr, pxs, psr, s4s, s5s, outr, outf, ofs,
           wres_sem, wst_sem, wo_sem, mlp_sem, hv_sem, s6s, xp, xq, op, od,
           ysn, yrc, pos, por, pps, ppr, pfs, pfr, pxfs, pxfr, pds, gate, cred):
    n_mb, T, D = x_ref.shape
    QL = wq_ref.shape[2]
    FL = wg_ref.shape[2]
    NB = wg_s.shape[0]
    FB = FL // NB
    S = seg_ref.shape[1]
    NJ = S // T
    NH = QL // HEAD_DIM
    N = (n_mb // 2) * NJ
    DB = D // NB
    scale = HEAD_DIM ** -0.5
    RB = 16
    NR = 32
    HS = hin.shape[0]
    OB = wst.shape[3]
    NO = D // OB

    hx = lax.axis_index("dp")
    z = lax.axis_index("tp")
    s = lax.axis_index("pp")
    is_home = (z == 1) | (z == 2)
    is_outer = (z == 0) | (z == 3)
    hb = lax.rem(z + 1, 2) * 0 + (z - 1)
    peer = 3 - z
    outer = 3 * (z - 1)
    inner = 1 + z // 2
    odd = lax.rem(s, 2)

    def rcopy(src, dst, ssem, rsem, **dev):
        return pltpu.make_async_remote_copy(src_ref=src, dst_ref=dst, send_sem=ssem, recv_sem=rsem,
                                            device_id=dev, device_id_type=MESH)

    def local(src, dst, sem):
        return pltpu.make_async_copy(src, dst, sem)

    def column(ref, mb, j):
        row = ref[pl.ds(mb, 1), :]
        part = row[:, 0:T]
        for c in range(1, NJ):
            part = jnp.where(j == c, row[:, c * T:(c + 1) * T], part)
        return jnp.broadcast_to(part, (HEAD_DIM, T)).T

    wqkv_own = (wq_ref, wk_ref, wv_ref, wo_ref)

    def mlp_copies():
        cps = []
        for n in range(NB):
            cps.append(local(wg_ref.at[0, :, pl.ds(n * FB, FB)], wg_s.at[n], mlp_sem.at[0, n]))
            cps.append(local(wu_ref.at[0, :, pl.ds(n * FB, FB)], wu_s.at[n], mlp_sem.at[1, n]))
            cps.append(local(wd_ref.at[0, :, pl.ds(n * DB, DB)], wd_s.at[n], mlp_sem.at[2, n]))
        return cps

    NW = n_mb // 2

    def x_copy(w, home):
        u = w * NJ + z
        return rcopy(x_ref.at[2 * w + (home - 1)], hin_hbm.at[u], xs.at[w, home - 1], (hin_sem if w == 0 else xp).at[u], tp=home)

    def x_each(w, act):
        for home in (1, 2):
            @pl.when((s == (0 if w == 0 else 2)) & (z != home))
            def _():
                act(x_copy(w, home))

    def x_pass(w, j):
        u = w * NJ + j
        return rcopy(hin_hbm.at[u], hin_hbm.at[u], xq.at[w, j], hin_sem.at[u], pp=0)

    def half(ref, m, h):
        rows = (D if m < 3 else QL) // 2
        return ref.at[pl.ds(h * rows, rows), :]

    def wslot(r, m):
        return wqkv_hbm.at[r, m] if m < 3 else wo_hbm.at[pl.ds((r + 1) * QL, QL)]

    def own_w(m):
        return wqkv_own[m].at[0]

    def wo_own():
        return local(own_w(3), wo_hbm.at[pl.ds(0, QL)], wo_sem)

    def o_send(k):
        h = hx if k < 4 else 1 - hx
        return rcopy(half(own_w(k % 4), k % 4, h), half(wslot(0, k % 4), k % 4, h), wsnd.at[k], wr.at[0, k], tp=inner)

    def p_send(m):
        return rcopy(half(own_w(m), m, hx), half(wslot(1, m), m, hx), wsnd.at[m], wr.at[1, m], tp=peer)

    def f_send(m):
        return rcopy(half(wslot(0, m), m, hx), half(wslot(2, m), m, hx), wfwd.at[m], wr.at[2, m], tp=peer)

    def x_send(r, m):
        return rcopy(half(wslot(r, m), m, hx), half(wslot(r, m), m, hx), wxs.at[r - 1, m], wx.at[r - 1, m], dp=1 - hx)

    def w_ready(rs, ms):
        def pushed(m):
            if 0 in rs:
                o_send(m).wait_recv()
            if 1 in rs:
                p_send(m).wait_recv()
            if 2 in rs:
                f_send(m).wait_recv()
        for m in ms:
            if m in PM:
                pl.when(s == 1)(functools.partial(pushed, m))
            if 0 in rs:
                o_send(4 + m).wait_recv()
            for r in (1, 2):
                if r in rs:
                    x_send(r, m).wait_recv()

    PM = (2, 3)

    def pb(r, m):
        return pv_hbm.at[r] if m == 2 else po_hbm.at[pl.ds(r * QL, QL)]

    def hh(i):
        return hx if i == 0 else 1 - hx

    def y_send(i, m):
        return rcopy(half(own_w(m), m, hh(i)), half(pb(3, m), m, hh(i)), ysn.at[2 * i + m - 2], yrc.at[2 * i + m - 2], pp=3)

    def po_send(i, m):
        return rcopy(half(pb(3, m), m, hh(i)), half(pb(0, m), m, hh(i)), pos.at[2 * i + m - 2], por.at[2 * i + m - 2], tp=inner)

    def pp_send(m):
        return rcopy(half(pb(3, m), m, hx), half(pb(1, m), m, hx), pps.at[m - 2], ppr.at[m - 2], tp=peer)

    def pf_send(m):
        return rcopy(half(pb(0, m), m, hx), half(pb(2, m), m, hx), pfs.at[m - 2], pfr.at[m - 2], tp=peer)

    def pxf_send(r, m):
        return rcopy(half(pb(r, m), m, hx), half(pb(r, m), m, hx), pxfs.at[r - 1, m - 2], pxfr.at[r - 1, m - 2], dp=1 - hx)

    def push(r, m, i):
        rsem = wr.at[0, 4 * i + m] if r == 0 else (wr.at[r, m] if i == 0 else wx.at[r - 1, m])
        return rcopy(half(pb(r, m), m, hh(i)), half(wslot(r, m), m, hh(i)), pds.at[r, m - 2, i], rsem, pp=1)

    def direct(m, f):
        if m in PM:
            pl.when(s != 1)(f)
        else:
            f()

    @pl.when(s == 1)
    def _():
        for m in PM:
            y_send(0, m).start()

        @pl.when(is_outer)
        def _():
            for m in PM:
                y_send(1, m).start()

    @pl.when((s == 3) & is_outer)
    def _():
        for i in (0, 1):
            for m in PM:
                y_send(i, m).wait_recv()
                po_send(i, m).start()
        for i in (0, 1):
            for m in PM:
                po_send(i, m).wait_send()

    @pl.when((s == 3) & is_home)
    def _():
        for m in PM:
            y_send(0, m).wait_recv()
            pp_send(m).start()
        for kind, m, a in (("p", 2, 0), ("o", 2, 0), ("p", 3, 0), ("o", 3, 0), ("f", 2, 0), ("o", 2, 1), ("x", 2, 1), ("x", 3, 1),
                           ("f", 3, 0), ("o", 3, 1), ("x", 2, 2), ("x", 3, 2)):
            with jax.named_scope('wp_' + kind + str(m) + str(a)):
                if kind == "p":
                    pp_send(m).wait_recv()
                    pxf_send(1, m).start()
                    push(1, m, 0).start()
                elif kind == "o":
                    po_send(a, m).wait_recv()
                    if a == 0:
                        pf_send(m).start()
                    push(0, m, a).start()
                elif kind == "f":
                    pf_send(m).wait_recv()
                    pxf_send(2, m).start()
                    push(2, m, 0).start()
                else:
                    pxf_send(a, m).wait_recv()
                    push(a, m, 1).start()

    @pl.when(s == 3)
    def _():
        pl.semaphore_signal(gate, inc=1, device_id={"pp": 2}, device_id_type=MESH)

    def release():
        @pl.when(odd == 0)
        def _():
            pl.semaphore_signal(gate, inc=1, device_id={"pp": s + 1}, device_id_type=MESH)

    @pl.when(s != 0)
    def _():
        for c in mlp_copies():
            c.start()
        with jax.named_scope('w_gate'):
            pl.semaphore_wait(gate, 1)

    def x_relay(ws):
        @pl.when((s == 2) & is_home)
        def _():
            for w in ws:
                for j in range(NJ):
                    @pl.when(z != j)
                    def _():
                        local(hin_hbm.at[w * NJ + j], hin_hbm.at[w * NJ + j], xp.at[w * NJ + j]).wait()
                        x_pass(w, j).start()

    if NW > 1:
        x_each(1, lambda c: c.start())

    @pl.when(is_outer)
    def _():
        for k in range(8):
            direct(k % 4, lambda k=k: o_send(k).start())
        x_each(0, lambda c: c.start())

        @pl.when(s == 0)
        def _():
            for c in mlp_copies():
                c.start()
        for k in range(8):
            direct(k % 4, lambda k=k: o_send(k).wait_send())
        release()
        for w in range(2, NW):
            x_each(w, lambda c: c.start())

    @pl.when(is_home)
    def _():
        for m in range(4):
            direct(m, lambda m=m: p_send(m).start())
        wo_own().start()

        @pl.when(s == 0)
        def _():
            for c in mlp_copies():
                c.start()
        def zero_rows(b, carry):
            for i in range(4):
                kc[i, pl.ds(b * RB, RB), :] = jnp.zeros((RB, QL), BF16)
                vc[i, pl.ds(b * RB, RB), :] = jnp.zeros((RB, QL), BF16)
            return carry
        lax.fori_loop(0, S // RB, zero_rows, 0)

        def tables(w):
            lane = lax.broadcasted_iota(jnp.int32, (T, HEAD_DIM), 1)

            def table_rows(b, carry):
                rows = pl.ds(pl.multiple_of(b * T, T), T)
                ang = column(pos_ref, 2 * w + hb, b).astype(F32) * invf_ref[0:1, :]
                table[w, rows, :] = jnp.where(lane < HEAD_DIM // 2, jnp.cos(ang), jnp.sin(ang))
                return carry
            with jax.named_scope('table'):
                lax.fori_loop(0, NJ, table_rows, 0)

        steps = [("o", 0), ("p", 0), ("t", 0), ("o", 1), ("p", 1), ("t", 1), ("o", 2), ("p", 2), ("t", 2), ("o", 3), ("p", 3), ("t", 3),
                 ("r", 0), ("f", 0), ("f", 1), ("f", 2), ("f", 3), ("g", 0)]

        def step(kind, m):
            if kind == "o":
                o_send(m).wait_recv()
                f_send(m).start()
            elif kind == "p":
                p_send(m).wait_recv()
                x_send(1, m).start()
            else:
                f_send(m).wait_recv()
                x_send(2, m).start()

        for kind, m in steps:
            with jax.named_scope('w_' + kind + str(m)):
                if kind in "opf":
                    direct(m, lambda kind=kind, m=m: step(kind, m))
                elif kind == "g":
                    release()
                elif kind == "r":
                    x_relay([1] if NW > 1 else [])
                elif m < n_mb // 2:
                    tables(m)
        x_each(0, lambda c: c.start())
        for w in range(2, NW):
            x_each(w, lambda c: c.start())
        w_ready([0, 1], range(3))
        x_relay(range(2, NW))

    def gslot(g, u):
        return lax.rem(g - 1 + u, 2)

    def group_copies(g, u):
        if g == 0:
            return [local(own_w(m), wres.at[m], wres_sem.at[m]) for m in range(3)]
        p = gslot(g, u)
        if g < 4:
            return [local(wqkv_hbm.at[g - 1], wst.at[p], wst_sem.at[p, 0])]
        return [local(wo_hbm.at[:, pl.ds(((g - 4) * 3 + m) * OB, OB)], wst.at[p, m], wst_sem.at[p, m]) for m in range(3 if g == 4 else 1)]

    def group_start(g, u):
        for c in group_copies(g, u):
            c.start()

    def group_wait(g, u):
        for c in group_copies(g, u):
            c.wait()

    def h_fetch(u):
        mb = 2 * (u // NJ) + hb
        here = lax.rem(u, NJ) == z
        dst = hin.at[lax.rem(u, HS)]

        @pl.when((s == 0) & here)
        def _():
            local(x_ref.at[mb], dst, hv_sem).start()

        @pl.when((s == 0) & jnp.logical_not(here))
        def _():
            local(hin_hbm.at[u], hin_hbm.at[u], hin_sem.at[u]).wait()
            local(hin_hbm.at[u], dst, hv_sem).start()

    @pl.when(is_home)
    def _():
        group_start(0, 0)
        group_start(1, 0)
        group_start(2, 0)
        h_fetch(0)

    for c in mlp_copies():
        c.wait()

    def hin_copy(u):
        return rcopy(h2b, hin.at[lax.rem(u, HS)], s5s, hin_sem.at[u], pp=lax.rem(s + 1, n_stages))

    def s1_outer(u):
        blk = gb.at[lax.rem(u, 3), pl.ds(pl.multiple_of(hb * T, T), T), :]
        return rcopy(blk, blk, s1s.at[0], ag.at[hb, lax.rem(u, 3)], tp=outer)

    def s1_peer(u):
        blk = gb.at[lax.rem(u, 3), pl.ds(pl.multiple_of(hb * T, T), T), :]
        return rcopy(blk, blk, s1s.at[1], ag.at[hb, lax.rem(u, 3)], tp=peer)

    def s2_copy(u):
        blk = gb.at[lax.rem(u, 3), pl.ds(pl.multiple_of((1 - hb) * T, T), T), :]
        return rcopy(blk, blk, s2s, ag.at[1 - hb, lax.rem(u, 3)], tp=outer)

    def ag_wait(b, u):
        blk = gb.at[lax.rem(u, 3), pl.ds(pl.multiple_of(b * T, T), T), :]
        local(blk, blk, ag.at[b, lax.rem(u, 3)]).wait()

    def s3_copy(u, b):
        sl = lax.rem(u, 2)
        blk = px.at[sl, pl.ds(pl.multiple_of(b * T, T), T), :]
        return rcopy(blk, blk, pxs.at[sl, b], pxr.at[sl, b], tp=inner)

    def s4_copy(u):
        return rcopy(sendb, ps.at[lax.rem(u, 2)], s4s, psr.at[lax.rem(u, 2)], tp=peer)

    def park_copy(u):
        return rcopy(h2b, hin_hbm.at[u], s5s, op.at[u], pp=1)

    def last_copy():
        mb = n_mb - 2 + hb
        return rcopy(h2b, out_ref.at[mb], s6s, outr.at[mb], tp=NJ - 1)

    def norm_rows(src, gain, dst):
        hf = src.astype(F32)
        inv = lax.rsqrt(jnp.mean(hf * hf, axis=-1, keepdims=True) + NORM_EPS)
        return (hf * inv * gain.astype(F32)).astype(BF16)

    def attention(u):
      with jax.named_scope('attn'):
        attention_(u)

    def attention_(u):
        w = u // NJ
        j = lax.rem(u, NJ)
        mb = 2 * w + hb
        row0 = pl.multiple_of(j * T, T)
        hs = lax.rem(u, HS)

        with jax.named_scope('w_hin'):
            @pl.when(s == 0)
            def _():
                local(x_ref.at[mb], hin.at[hs], hv_sem).wait()

            @pl.when(s > 0)
            def _():
                hin_copy(u).wait_recv()

        def norm_a(b, carry):
            rows = pl.ds(b * NR, NR)
            abuf[rows, :] = norm_rows(hin[hs, rows, :], ga_ref[0:1, :], None)
            return carry
        lax.fori_loop(0, T // NR, norm_a, 0)

        segrow = seg_ref[pl.ds(mb, 1), :]
        segc = column(seg_ref, mb, j)
        ti = lax.broadcasted_iota(jnp.int32, (T, HEAD_DIM), 0) + row0
        for c in range(0, S, HEAD_DIM):
            segr = segrow[:, c:c + HEAD_DIM]
            ui = lax.broadcasted_iota(jnp.int32, (T, HEAD_DIM), 1) + c
            mask[:, c:c + HEAD_DIM] = jnp.where((segc == segr) & (ui <= ti), 1.0, 0.0)

        def rope(val):
            pk = table[w, pl.ds(row0, T), :]
            lane = lax.broadcasted_iota(jnp.int32, (T, HEAD_DIM), 1)
            swapped = pltpu.roll(pk, HEAD_DIM // 2, 1)
            cosw = jnp.where(lane < HEAD_DIM // 2, pk, swapped)
            sinw = jnp.where(lane < HEAD_DIM // 2, -swapped, pk)
            outs = []
            for h in range(NH):
                v = val[:, h * HEAD_DIM:(h + 1) * HEAD_DIM]
                outs.append((v * cosw + pltpu.roll(v, HEAD_DIM // 2, 1) * sinw).astype(BF16))
            return outs

        def hcols(h):
            return slice(h * HEAD_DIM, (h + 1) * HEAD_DIM)

        def proj(i):
            p = i % 2

            def w(m):
                return wres[m] if i == 0 else wst[gslot(i, u), m]
            for h, val in enumerate(rope(jnp.dot(abuf[...], w(0), preferred_element_type=F32))):
                qb[p, :, hcols(h)] = val
            for h, val in enumerate(rope(jnp.dot(abuf[...], w(1), preferred_element_type=F32))):
                kc[i, pl.ds(row0, T), hcols(h)] = val
            vc[i, pl.ds(row0, T), :] = jnp.dot(abuf[...], w(2), preferred_element_type=F32).astype(BF16)

        def heads(i):
            for h in range(NH):
                sc = lax.dot_general(qb[i % 2, :, hcols(h)], kc[i, :, hcols(h)], (((1,), (1,)), ((), ())),
                                     preferred_element_type=F32) * scale
                pacc[0:T, h * S:(h + 1) * S] = jnp.where(mask[...] > 0.5, sc, NEG)
            for h in range(NH):
                for r in range(0, T, 32):
                    sc = pacc[r:r + 32, h * S:(h + 1) * S]
                    e = jnp.exp(sc - jnp.max(sc, axis=-1, keepdims=True))
                    pbuf[h, r:r + 32, :] = (e * (1.0 / jnp.sum(e, axis=-1, keepdims=True))).astype(BF16)
            for h in range(NH):
                act[0:T, i * QL + h * HEAD_DIM:i * QL + (h + 1) * HEAD_DIM] = jnp.dot(
                    pbuf[h], vc[i, :, hcols(h)], preferred_element_type=F32).astype(BF16)

        with jax.named_scope('shards'):
            @pl.when(u == 0)
            def _():
                group_wait(0, u)
            proj(0)
            for i in range(3):
                group_wait(i + 1, u)
                proj(i + 1)
                if i < 2:
                    @pl.when(u == 0)
                    def _():
                        if i == 0:
                            w_ready([2], range(3))
                        else:
                            w_ready([0, 1, 2], [3])
                            wo_own().wait()
                group_start(i + 3, u)
                heads(i)
                if i == 0:
                    @pl.when(u < N - 1)
                    def _():
                        h_fetch(u + 1)
            heads(3)

        with jax.named_scope('wo'):
            def wo_block(n, w):
                act[T:2 * T, n * OB:(n + 1) * OB] = jnp.dot(act[0:T, 0:4 * QL], w, preferred_element_type=F32).astype(BF16)

            group_wait(4, u)
            group_wait(5, u)
            for n in range(3):
                wo_block(n, wst[gslot(4, u), n])

            wo_block(3, wst[gslot(5, u), 0])

            @pl.when(u < N - 1)
            def _():
                group_start(1, u + 1)
                group_start(2, u + 1)

        def norm_b(b, carry):
            rows = pl.ds(b * NR, NR)
            h1 = (hin[hs, rows, :].astype(F32) + act[pl.ds(pl.multiple_of(T + b * NR, NR), NR), 0:D].astype(F32)).astype(BF16)
            h1b[lax.rem(u, 3), rows, :] = h1
            gb[lax.rem(u, 3), pl.ds(pl.multiple_of(hb * T + b * NR, NR), NR), :] = norm_rows(h1, gm_ref[0:1, :], None)
            return carry
        lax.fori_loop(0, T // NR, norm_b, 0)

        @pl.when((s > 0) & (u < N - HS))
        def _():
            pl.semaphore_signal(cred, inc=1, device_id={"pp": s - 1}, device_id_type=MESH)

    def mlp(sl, row0, rows, store):
        UN = 2 if NB % 2 == 0 else 1

        def up(q, carry):
            for n in [q * UN + k for k in range(UN)]:
                xin = gb[sl, pl.ds(row0, rows), :]
                g = jnp.dot(xin, wg_s[n], preferred_element_type=F32)
                u_ = jnp.dot(xin, wu_s[n], preferred_element_type=F32)
                act[0:rows, pl.ds(pl.multiple_of(n * FB, FB), FB)] = (jax.nn.silu(g) * u_).astype(BF16)
            return carry
        lax.fori_loop(0, NB // UN, up, 0)

        def down(q, carry):
            for n in [q * UN + k for k in range(UN)]:
                store(pl.ds(pl.multiple_of(n * DB, DB), DB), jnp.dot(act[0:rows, 0:FL], wd_s[n], preferred_element_type=F32))
            return carry
        lax.fori_loop(0, NB // UN, down, 0)

    def mlp_home(u):
        def store(c, val):
            pacc[:, c] = val
        with jax.named_scope('mlp'):
            mlp(lax.rem(u, 3), 0, 2 * T, store)

    def mlp_outer(u, b):
        def store(c, val):
            px[lax.rem(u, 2), pl.ds(pl.multiple_of(b * T, T), T), c] = val.astype(BF16)
        with jax.named_scope('mlp_o'):
            mlp(lax.rem(u, 3), pl.multiple_of(b * T, T), T, store)

    def forward(u):
        @pl.when((u >= 1) & (u <= N))
        def _():
            s2_copy(u - 1).wait_send()

        @pl.when(u < N)
        def _():
            with jax.named_scope('w_ag'):
                ag_wait(1 - hb, u)
            s2_copy(u).start()

    def combine(v):
        sl = lax.rem(v, 2)
        with jax.named_scope('w_s3'):
            s3_copy(v, 0).wait_recv()
            s3_copy(v, 1).wait_recv()

        @pl.when(v >= 1)
        def _():
            s4_copy(v - 1).wait_send()

        def comb(b, carry):
            rows = pl.ds(b * RB, RB)
            mine = pl.ds(pl.multiple_of(hb * T + b * RB, RB), RB)
            theirs = pl.ds(pl.multiple_of((1 - hb) * T + b * RB, RB), RB)
            oacc[rows, :] = pacc[mine, :] + px[sl, mine, :].astype(F32)
            sendb[rows, :] = (pacc[theirs, :] + px[sl, theirs, :].astype(F32)).astype(BF16)
            return carry
        lax.fori_loop(0, T // RB, comb, 0)
        s4_copy(v).start()

    def finish(u):
        @pl.when((u >= 2) & (u < N + 2))
        def _():
            v = u - 2
            with jax.named_scope('w_s4'):
                s4_copy(v).wait_recv()
            vw = v // NJ
            vj = lax.rem(v, NJ)

            @pl.when(v >= 1)
            def _():
                hin_copy(v).wait_send()

            def fin(b, carry):
                rows = pl.ds(b * RB, RB)
                d = (oacc[rows, :] + ps[lax.rem(v, 2), rows, :].astype(F32)).astype(BF16)
                h2b[rows, :] = (h1b[lax.rem(v, 3), rows, :].astype(F32) + d.astype(F32)).astype(BF16)
                return carry
            lax.fori_loop(0, T // RB, fin, 0)

            @pl.when((s < n_stages - 1) & (v >= HS))
            def _():
                with jax.named_scope('w_cred'):
                    pl.semaphore_wait(cred, 1)

            @pl.when(s < n_stages - 1)
            def _():
                hin_copy(v).start()

            @pl.when(s == n_stages - 1)
            def _():
                park_copy(v).start()

            @pl.when((s == n_stages - 1) & (v == N - 1))
            def _():
                last_copy().start()

    def body(u, carry):
        @pl.when(is_home)
        def _():
            @pl.when(u < N)
            def _():
                attention(u)

            @pl.when((u >= 1) & (u <= N))
            def _():
                s1_outer(u - 1).wait_send()
                s1_peer(u - 1).wait_send()

            @pl.when(u < N)
            def _():
                s1_peer(u).start()
                s1_outer(u).start()

            @pl.when((u >= 1) & (u <= N))
            def _():
                mlp_home(u - 1)

            finish(u)
            forward(u)

            @pl.when((u >= 1) & (u <= N))
            def _():
                combine(u - 1)

        @pl.when(is_outer & (u < N))
        def _():
            for k in (0, 1):
                b = inner - 1 if k == 0 else 2 - inner
                with jax.named_scope('w_ag_outer'):
                    ag_wait(b, u)

                @pl.when(u >= 2)
                def _():
                    s3_copy(u - 2, b).wait_send()
                mlp_outer(u, b)
                s3_copy(u, b).start()

        return carry

    def out_fwd(mb, p, sem):
        return rcopy(out_ref.at[mb], out_ref.at[mb], ofs.at[mb, p], sem, pp=p)

    lax.fori_loop(0, N + 2, body, 0)

    last_here = (s == n_stages - 1) & (z == NJ - 1)

    @pl.when(last_here)
    def _():
        for mb in (n_mb - 2, n_mb - 1):
            local(out_ref.at[mb], out_ref.at[mb], outr.at[mb]).wait()
            out_fwd(mb, 2, outf).start()

    def od_copy(v):
        return rcopy(hin_hbm.at[v], out_ref.at[2 * (v // NJ) + hb], od.at[v], outr.at[2 * (v // NJ) + hb], tp=lax.rem(v, NJ))

    @pl.when(s == 1)
    def _():
        def spread(v, carry):
            vj = lax.rem(v, NJ)
            mine = 2 * (v // NJ) + hb

            @pl.when(is_home)
            def _():
                local(hin_hbm.at[v], hin_hbm.at[v], op.at[v]).wait()

            @pl.when(is_home & (vj != z))
            def _():
                od_copy(v).start()

            @pl.when(is_home & (vj == z))
            def _():
                c = local(hin_hbm.at[v], hin.at[0], hv_sem)
                c.start()
                c.wait()
                c = local(hin.at[0], out_ref.at[mine], hv_sem)
                c.start()
                c.wait()

            @pl.when(vj == z)
            def _():
                for b in (0, 1):
                    mb = 2 * (v // NJ) + b

                    @pl.when(z - 1 != b)
                    def _(mb=mb):
                        local(out_ref.at[mb], out_ref.at[mb], outr.at[mb]).wait()
                    out_fwd(mb, 0, outf).start()

                    @pl.when(v < N - 1)
                    def _(mb=mb):
                        out_fwd(mb, 3, outf).start()
                        out_fwd(mb, 2, outf).start()
            return carry
        lax.fori_loop(0, N, spread, 0)

    @pl.when(is_home)
    def _():
        s4_copy(N - 1).wait_send()
        hin_copy(N - 1).wait_send()

        @pl.when(s == n_stages - 1)
        def _():
            last_copy().wait_send()

    @pl.when(is_outer)
    def _():
        for b in (0, 1):
            s3_copy(N - 2, b).wait_send()
            s3_copy(N - 1, b).wait_send()

    @pl.when(s == 1)
    def _():
        for m in PM:
            y_send(0, m).wait_send()

        @pl.when(is_outer)
        def _():
            for m in PM:
                y_send(1, m).wait_send()

    @pl.when((s == 3) & is_home)
    def _():
        for m in PM:
            pp_send(m).wait_send()
            pf_send(m).wait_send()
            for r in (1, 2):
                pxf_send(r, m).wait_send()
            for r in (0, 1, 2):
                for i in (0, 1):
                    push(r, m, i).wait_send()

    @pl.when(is_home)
    def _():
        def sent(m):
            p_send(m).wait_send()
            f_send(m).wait_send()
            x_send(1, m).wait_send()
            x_send(2, m).wait_send()
        for m in range(4):
            direct(m, functools.partial(sent, m))

        @pl.when(s == 2)
        def _():
            for w in range(1, NW):
                for j in range(NJ):
                    @pl.when(z != j)
                    def _():
                        x_pass(w, j).wait_send()

        @pl.when(s == 1)
        def _():
            def spread_done(v, carry):
                @pl.when(lax.rem(v, NJ) != z)
                def _():
                    od_copy(v).wait_send()
                return carry
            lax.fori_loop(0, N, spread_done, 0)

    for w in range(NW):
        x_each(w, lambda c: c.wait_send())

    @pl.when(s == 1)
    def _():
        for mb in range(n_mb):
            out_fwd(mb, 0, outf).wait_send()
            if mb < n_mb - 2:
                out_fwd(mb, 3, outf).wait_send()
                out_fwd(mb, 2, outf).wait_send()
            else:
                @pl.when(z < NJ - 1)
                def _(mb=mb):
                    out_fwd(mb, 3, outf).wait_send()
                    out_fwd(mb, 2, outf).wait_send()

    @pl.when(last_here)
    def _():
        for mb in (n_mb - 2, n_mb - 1):
            out_fwd(mb, 2, outf).wait_send()
        early = out_ref.at[pl.ds(0, n_mb - 2)]
        local(early, early, outf).wait()

    @pl.when((s == n_stages - 1) & (z < NJ - 1))
    def _():
        local(out_ref, out_ref, outf).wait()

    @pl.when((s == 0) | (s == 2))
    def _():
        local(out_ref, out_ref, outf).wait()


def solution(mesh):
    n_stages = mesh.shape['pp']

    def stage_program(hidden_in, seg_ids, positions, attn_norm, w_query, w_key, w_value, w_out, mlp_norm, w_gate, w_up, w_down):
        n_mb, T, D = hidden_in.shape
        S = seg_ids.shape[1]
        QL = w_query.shape[2]
        FL = w_gate.shape[2]
        NJ = S // T
        N = (n_mb // 2) * NJ
        NB = max(1, FL // 512)
        invf = jnp.asarray(np.tile(rope_freqs(), 2)[None, :], F32)
        any_spec = pl.BlockSpec(memory_space=pl.ANY)
        vmem = pl.BlockSpec(memory_space=pltpu.VMEM)
        dma = pltpu.SemaphoreType.DMA
        scratch = [
            pltpu.VMEM((NB, D, FL // NB), BF16), pltpu.VMEM((NB, D, FL // NB), BF16), pltpu.VMEM((NB, FL, D // NB), BF16),
            pltpu.VMEM((3, D, QL), BF16), pltpu.VMEM((2, 3, D, QL), BF16),
            pltpu.VMEM((3, 2 * T, D), BF16),
            pltpu.VMEM((2, 2 * T, D), BF16),
            pltpu.VMEM((2, T, D), BF16),
            pltpu.VMEM((4, S, QL), BF16), pltpu.VMEM((4, S, QL), BF16),
            pltpu.VMEM((4, T, D), BF16),
            pltpu.VMEM((3, T, D), BF16),
            pltpu.VMEM((2 * T, D), F32),
            pltpu.VMEM((T, D), F32),
            pltpu.VMEM((T, D), BF16),
            pltpu.VMEM((T, D), BF16),
            pltpu.VMEM((2 * T, max(D, FL, 4 * QL)), BF16),
            pltpu.VMEM((T, D), BF16),
            pltpu.VMEM((2, T, QL), BF16),
            pltpu.VMEM((n_mb // 2, S, HEAD_DIM), F32),
            pltpu.VMEM((T, S), F32), pltpu.VMEM((QL // HEAD_DIM, T, S), BF16),
            dma((3, 8)), dma((2, 4)), dma((8,)), dma((4,)), dma((2, 4)),
            dma((N,)), dma((n_mb // 2, 2)), dma((2, 3)), dma((2,)), dma, dma((2, 2)), dma((2, 2)), dma((2,)), dma, dma,
            dma((n_mb,)), dma, dma((n_mb, n_stages)),
            dma((3,)), dma((2, 3)), dma, dma((3, NB)), dma, dma, dma((N,)), dma((n_mb // 2, NJ)), dma((N,)), dma((N,)),
            dma((4,)), dma((4,)), dma((4,)), dma((4,)), dma((2,)), dma((2,)), dma((2,)), dma((2,)), dma((2, 2)), dma((2, 2)), dma((3, 2, 2)),
            pltpu.SemaphoreType.REGULAR, pltpu.SemaphoreType.REGULAR,
        ]
        return pl.pallas_call(
            functools.partial(kernel, n_stages),
            out_shape=[jax.ShapeDtypeStruct(hidden_in.shape, BF16), jax.ShapeDtypeStruct((3, 3, D, QL), BF16),
                       jax.ShapeDtypeStruct((4 * QL, D), BF16), jax.ShapeDtypeStruct((N, T, D), BF16),
                       jax.ShapeDtypeStruct((4, D, QL), BF16), jax.ShapeDtypeStruct((4 * QL, D), BF16)],
            in_specs=[any_spec, vmem, vmem, vmem, vmem, vmem] + [any_spec] * 7,
            out_specs=[any_spec] * 6,
            scratch_shapes=scratch,
            compiler_params=pltpu.CompilerParams(has_side_effects=True, vmem_limit_bytes=67_043_328),
        )(hidden_in, seg_ids, positions, invf, attn_norm, mlp_norm, w_query, w_key, w_value, w_out, w_gate, w_up, w_down)[0]

    act_spec = P('dp', 'tp', None)
    row_spec = P('dp', None)
    gain_spec = P('pp', None)
    col_spec = P('pp', None, 'tp')
    rows_spec = P('pp', 'tp', None)
    return jax.shard_map(stage_program, mesh=mesh,
                         in_specs=(act_spec, row_spec, row_spec, gain_spec, col_spec, col_spec, col_spec, rows_spec, gain_spec, col_spec, col_spec, rows_spec),
                         out_specs=act_spec, check_vma=False)
```

```python
import functools
import math

import jax
import jax.numpy as jnp
import numpy as np
from jax import lax
from jax.experimental import pallas as pl
from jax.experimental.pallas import tpu as pltpu
from jax.sharding import PartitionSpec as P

HEAD_DIM = 128
NORM_EPS = 1e-5
ROPE_THETA = 500000.0
ROPE_FACTOR = 8.0
LOW_FREQ = 1.0
HIGH_FREQ = 4.0
ORIG_CTX = 8192.0
NEG = -1e30
MESH = pl.DeviceIdType.MESH
F32 = jnp.float32
BF16 = jnp.bfloat16


def rope_freqs():
    base_freq = 1.0 / (ROPE_THETA ** (np.arange(0, HEAD_DIM, 2) / HEAD_DIM))
    wavelen = 2.0 * np.pi / base_freq
    smooth = (ORIG_CTX / wavelen - LOW_FREQ) / (HIGH_FREQ - LOW_FREQ)
    blended = (1.0 - smooth) * base_freq / ROPE_FACTOR + smooth * base_freq
    scaled = np.where(wavelen > ORIG_CTX / LOW_FREQ, base_freq / ROPE_FACTOR, blended)
    return np.where(wavelen < ORIG_CTX / HIGH_FREQ, base_freq, scaled)


def kernel(n_stages, x_ref, seg_ref, pos_ref, invf_ref, ga_ref, gm_ref,
           wq_ref, wk_ref, wv_ref, wo_ref, wg_ref, wu_ref, wd_ref,
           out_ref,
           wqkv_hbm, wo_hbm, hin_hbm, po_hbm,
           wg_s, wu_s, wd_s, wres, wst, gb, px, ps, kc, vc, hin, h1b, pacc, oacc, sendb, h2b, act, abuf, qb,
           table, mask, pbuf,
           wr, wx, wsnd, wfwd, wxs, hin_sem, xs, ag, s1s, s2s, pxr, pxs, psr, s4s, s5s, outr, outf, ofs,
           wres_sem, wst_sem, wo_sem, mlp_sem, hv_sem, s6s, xp, xq, op, od,
           ysn, yrc, pos, por, pps, ppr, pfs, pfr, pxfs, pxfr, pds, gate, cred):
    n_mb, T, D = x_ref.shape
    QL = wq_ref.shape[2]
    FL = wg_ref.shape[2]
    NB = wg_s.shape[0]
    FB = FL // NB
    S = seg_ref.shape[1]
    NJ = S // T
    NH = QL // HEAD_DIM
    N = (n_mb // 2) * NJ
    DB = D // NB
    scale = HEAD_DIM ** -0.5
    RB = 16
    NR = 32
    HS = hin.shape[0]
    OB = wst.shape[3]
    NO = D // OB

    hx = lax.axis_index("dp")
    z = lax.axis_index("tp")
    s = lax.axis_index("pp")
    is_home = (z == 1) | (z == 2)
    is_outer = (z == 0) | (z == 3)
    hb = lax.rem(z + 1, 2) * 0 + (z - 1)
    peer = 3 - z
    outer = 3 * (z - 1)
    inner = 1 + z // 2
    odd = lax.rem(s, 2)

    def rcopy(src, dst, ssem, rsem, **dev):
        return pltpu.make_async_remote_copy(src_ref=src, dst_ref=dst, send_sem=ssem, recv_sem=rsem,
                                            device_id=dev, device_id_type=MESH)

    def local(src, dst, sem):
        return pltpu.make_async_copy(src, dst, sem)

    def column(ref, mb, j):
        row = ref[pl.ds(mb, 1), :]
        part = row[:, 0:T]
        for c in range(1, NJ):
            part = jnp.where(j == c, row[:, c * T:(c + 1) * T], part)
        return jnp.broadcast_to(part, (HEAD_DIM, T)).T

    wqkv_own = (wq_ref, wk_ref, wv_ref, wo_ref)

    def mlp_copies():
        cps = []
        for n in range(NB):
            cps.append(local(wg_ref.at[0, :, pl.ds(n * FB, FB)], wg_s.at[n], mlp_sem.at[0, n]))
            cps.append(local(wu_ref.at[0, :, pl.ds(n * FB, FB)], wu_s.at[n], mlp_sem.at[1, n]))
            cps.append(local(wd_ref.at[0, :, pl.ds(n * DB, DB)], wd_s.at[n], mlp_sem.at[2, n]))
        return cps

    NW = n_mb // 2

    def x_copy(w, home):
        u = w * NJ + z
        return rcopy(x_ref.at[2 * w + (home - 1)], hin_hbm.at[u], xs.at[w, home - 1], (hin_sem if w == 0 else xp).at[u], tp=home)

    def x_each(w, act):
        for home in (1, 2):
            @pl.when((s == (0 if w == 0 else 2)) & (z != home))
            def _():
                act(x_copy(w, home))

    def x_pass(w, j):
        u = w * NJ + j
        return rcopy(hin_hbm.at[u], hin_hbm.at[u], xq.at[w, j], hin_sem.at[u], pp=0)

    def half(ref, m, h):
        rows = (D if m < 3 else QL) // 2
        return ref.at[pl.ds(h * rows, rows), :]

    def wslot(r, m):
        return wqkv_hbm.at[r, m] if m < 3 else wo_hbm.at[pl.ds((r + 1) * QL, QL)]

    def own_w(m):
        return wqkv_own[m].at[0]

    def wo_own():
        return local(own_w(3), wo_hbm.at[pl.ds(0, QL)], wo_sem)

    def o_send(k):
        h = hx if k < 4 else 1 - hx
        return rcopy(half(own_w(k % 4), k % 4, h), half(wslot(0, k % 4), k % 4, h), wsnd.at[k], wr.at[0, k], tp=inner)

    def p_send(m):
        return rcopy(half(own_w(m), m, hx), half(wslot(1, m), m, hx), wsnd.at[m], wr.at[1, m], tp=peer)

    def f_send(m):
        return rcopy(half(wslot(0, m), m, hx), half(wslot(2, m), m, hx), wfwd.at[m], wr.at[2, m], tp=peer)

    def x_send(r, m):
        return rcopy(half(wslot(r, m), m, hx), half(wslot(r, m), m, hx), wxs.at[r - 1, m], wx.at[r - 1, m], dp=1 - hx)

    def w_ready(rs, ms):
        def pushed(m):
            if 0 in rs:
                o_send(m).wait_recv()
            if 1 in rs:
                p_send(m).wait_recv()
            if 2 in rs:
                f_send(m).wait_recv()
        for m in ms:
            if m == 3:
                pl.when(s < 2)(functools.partial(pushed, m))
            if 0 in rs:
                o_send(4 + m).wait_recv()
            for r in (1, 2):
                if r in rs:
                    x_send(r, m).wait_recv()

    def pb(r):
        return po_hbm.at[pl.ds(r * QL, QL)]

    def hh(i):
        return hx if i == 0 else 1 - hx

    def y_send(i):
        return rcopy(half(own_w(3), 3, hh(i)), half(pb(3), 3, hh(i)), ysn.at[i], yrc.at[i], pp=lax.rem(s + 2, 4))

    def po_send(i):
        return rcopy(half(pb(3), 3, hh(i)), half(pb(0), 3, hh(i)), pos.at[i], por.at[i], tp=inner)

    def pp_send():
        return rcopy(half(pb(3), 3, hx), half(pb(1), 3, hx), pps, ppr, tp=peer)

    def pf_send():
        return rcopy(half(pb(0), 3, hx), half(pb(2), 3, hx), pfs, pfr, tp=peer)

    def pxf_send(r):
        return rcopy(half(pb(r), 3, hx), half(pb(r), 3, hx), pxfs.at[r - 1], pxfr.at[r - 1], dp=1 - hx)

    def push(r, i):
        rsem = wr.at[0, 4 * i + 3] if r == 0 else (wr.at[r, 3] if i == 0 else wx.at[r - 1, 3])
        return rcopy(half(pb(r), 3, hh(i)), half(wslot(r, 3), 3, hh(i)), pds.at[r, i], rsem, pp=lax.rem(s + 2, 4))

    def direct(m, f):
        if m == 3:
            pl.when(s >= 2)(f)
        else:
            f()

    def hand_over():
        y_send(0).start()

        @pl.when(is_outer)
        def _():
            y_send(1).start()

    pl.when(s == 0)(hand_over)

    @pl.when((s >= 2) & is_outer)
    def _():
        for i in (0, 1):
            y_send(i).wait_recv()
            po_send(i).start()
        for i in (0, 1):
            po_send(i).wait_send()

    @pl.when((s >= 2) & is_home)
    def _():
        y_send(0).wait_recv()
        pp_send().start()
        for kind, a in (("p", 0), ("o", 0), ("f", 0), ("o", 1), ("x", 1), ("x", 2)):
            with jax.named_scope('wp_' + kind + str(a)):
                if kind == "p":
                    pp_send().wait_recv()
                    pxf_send(1).start()
                    push(1, 0).start()
                elif kind == "o":
                    po_send(a).wait_recv()
                    if a == 0:
                        pf_send().start()
                    push(0, a).start()
                elif kind == "f":
                    pf_send().wait_recv()
                    pxf_send(2).start()
                    push(2, 0).start()
                else:
                    pxf_send(a).wait_recv()
                    push(a, 1).start()

    def release():
        @pl.when(odd == 0)
        def _():
            pl.semaphore_signal(gate, inc=1, device_id={"pp": s + 1}, device_id_type=MESH)

    @pl.when(s != 0)
    def _():
        for c in mlp_copies():
            c.start()
        with jax.named_scope('w_gate'):
            @pl.when(odd == 1)
            def _():
                pl.semaphore_wait(gate, 1)

    pl.when(s == 1)(hand_over)

    def x_relay(ws):
        @pl.when((s == 2) & is_home)
        def _():
            for w in ws:
                for j in range(NJ):
                    @pl.when(z != j)
                    def _():
                        local(hin_hbm.at[w * NJ + j], hin_hbm.at[w * NJ + j], xp.at[w * NJ + j]).wait()
                        x_pass(w, j).start()

    if NW > 1:
        x_each(1, lambda c: c.start())

    @pl.when(is_outer)
    def _():
        for k in range(8):
            direct(k % 4, lambda k=k: o_send(k).start())
        x_each(0, lambda c: c.start())

        @pl.when(s == 0)
        def _():
            for c in mlp_copies():
                c.start()
        for k in range(8):
            direct(k % 4, lambda k=k: o_send(k).wait_send())
        release()
        for w in range(2, NW):
            x_each(w, lambda c: c.start())

    @pl.when(is_home)
    def _():
        for m in range(4):
            direct(m, lambda m=m: p_send(m).start())
        wo_own().start()
        x_relay([1] if NW > 1 else [])

        @pl.when(s == 0)
        def _():
            for c in mlp_copies():
                c.start()
        def zero_rows(b, carry):
            for i in range(4):
                kc[i, pl.ds(b * RB, RB), :] = jnp.zeros((RB, QL), BF16)
                vc[i, pl.ds(b * RB, RB), :] = jnp.zeros((RB, QL), BF16)
            return carry
        lax.fori_loop(0, S // RB, zero_rows, 0)

        def tables(w):
            lane = lax.broadcasted_iota(jnp.int32, (T, HEAD_DIM), 1)

            def table_rows(b, carry):
                rows = pl.ds(pl.multiple_of(b * T, T), T)
                ang = column(pos_ref, 2 * w + hb, b).astype(F32) * invf_ref[0:1, :]
                table[w, rows, :] = jnp.where(lane < HEAD_DIM // 2, jnp.cos(ang), jnp.sin(ang))
                return carry
            with jax.named_scope('table'):
                lax.fori_loop(0, NJ, table_rows, 0)

        steps = [("o", 0), ("p", 0), ("t", 0), ("o", 1), ("p", 1), ("t", 1), ("o", 2), ("p", 2), ("t", 2), ("o", 3), ("p", 3), ("t", 3),
                 ("f", 0), ("f", 1), ("f", 2), ("f", 3), ("g", 0)]

        def step(kind, m):
            if kind == "o":
                o_send(m).wait_recv()
                f_send(m).start()
            elif kind == "p":
                p_send(m).wait_recv()
                x_send(1, m).start()
            else:
                f_send(m).wait_recv()
                x_send(2, m).start()

        for kind, m in steps:
            with jax.named_scope('w_' + kind + str(m)):
                if kind in "opf":
                    direct(m, lambda kind=kind, m=m: step(kind, m))
                elif kind == "g":
                    release()
                elif m < n_mb // 2:
                    tables(m)
        x_each(0, lambda c: c.start())
        for w in range(2, NW):
            x_each(w, lambda c: c.start())
        with jax.named_scope('w_rdy0'):
            w_ready([0], range(3))
        with jax.named_scope('w_rdy1'):
            w_ready([1], range(3))
        x_relay(range(2, NW))

    def gslot(g, u):
        return lax.rem(g - 1 + u, 2)

    def group_copies(g, u):
        if g == 0:
            return [local(own_w(m), wres.at[m], wres_sem.at[m]) for m in range(3)]
        p = gslot(g, u)
        if g < 4:
            return [local(wqkv_hbm.at[g - 1], wst.at[p], wst_sem.at[p, 0])]
        return [local(wo_hbm.at[:, pl.ds(((g - 4) * 3 + m) * OB, OB)], wst.at[p, m], wst_sem.at[p, m]) for m in range(3 if g == 4 else 1)]

    def group_start(g, u):
        for c in group_copies(g, u):
            c.start()

    def group_wait(g, u):
        for c in group_copies(g, u):
            c.wait()

    def h_fetch(u):
        mb = 2 * (u // NJ) + hb
        here = lax.rem(u, NJ) == z
        dst = hin.at[lax.rem(u, HS)]

        @pl.when((s == 0) & here)
        def _():
            local(x_ref.at[mb], dst, hv_sem).start()

        @pl.when((s == 0) & jnp.logical_not(here))
        def _():
            local(hin_hbm.at[u], hin_hbm.at[u], hin_sem.at[u]).wait()
            local(hin_hbm.at[u], dst, hv_sem).start()

    @pl.when(is_home)
    def _():
        group_start(0, 0)
        group_start(1, 0)
        group_start(2, 0)
        h_fetch(0)

    for c in mlp_copies():
        c.wait()

    def hin_copy(u):
        return rcopy(h2b, hin.at[lax.rem(u, HS)], s5s, hin_sem.at[u], pp=lax.rem(s + 1, n_stages))

    def s1_outer(u):
        blk = gb.at[lax.rem(u, 3), pl.ds(pl.multiple_of(hb * T, T), T), :]
        return rcopy(blk, blk, s1s.at[0], ag.at[hb, lax.rem(u, 3)], tp=outer)

    def s1_peer(u):
        blk = gb.at[lax.rem(u, 3), pl.ds(pl.multiple_of(hb * T, T), T), :]
        return rcopy(blk, blk, s1s.at[1], ag.at[hb, lax.rem(u, 3)], tp=peer)

    def s2_copy(u):
        blk = gb.at[lax.rem(u, 3), pl.ds(pl.multiple_of((1 - hb) * T, T), T), :]
        return rcopy(blk, blk, s2s, ag.at[1 - hb, lax.rem(u, 3)], tp=outer)

    def ag_wait(b, u):
        blk = gb.at[lax.rem(u, 3), pl.ds(pl.multiple_of(b * T, T), T), :]
        local(blk, blk, ag.at[b, lax.rem(u, 3)]).wait()

    def s3_copy(u, b):
        sl = lax.rem(u, 2)
        blk = px.at[sl, pl.ds(pl.multiple_of(b * T, T), T), :]
        return rcopy(blk, blk, pxs.at[sl, b], pxr.at[sl, b], tp=inner)

    def s4_copy(u):
        return rcopy(sendb, ps.at[lax.rem(u, 2)], s4s, psr.at[lax.rem(u, 2)], tp=peer)

    def park_copy(u):
        return rcopy(h2b, hin_hbm.at[u], s5s, op.at[u], pp=1)

    def last_copy():
        mb = n_mb - 2 + hb
        return rcopy(h2b, out_ref.at[mb], s6s, outr.at[mb], tp=NJ - 1)

    def norm_rows(src, gain, dst):
        hf = src.astype(F32)
        inv = lax.rsqrt(jnp.mean(hf * hf, axis=-1, keepdims=True) + NORM_EPS)
        return (hf * inv * gain.astype(F32)).astype(BF16)

    def attention(u):
      with jax.named_scope('attn'):
        attention_(u)

    def attention_(u):
        w = u // NJ
        j = lax.rem(u, NJ)
        mb = 2 * w + hb
        row0 = pl.multiple_of(j * T, T)
        hs = lax.rem(u, HS)

        with jax.named_scope('w_hin'):
            @pl.when(s == 0)
            def _():
                local(x_ref.at[mb], hin.at[hs], hv_sem).wait()

            @pl.when(s > 0)
            def _():
                hin_copy(u).wait_recv()

        def norm_a(b, carry):
            rows = pl.ds(b * NR, NR)
            abuf[rows, :] = norm_rows(hin[hs, rows, :], ga_ref[0:1, :], None)
            return carry
        lax.fori_loop(0, T // NR, norm_a, 0)

        segrow = seg_ref[pl.ds(mb, 1), :]
        segc = column(seg_ref, mb, j)
        ti = lax.broadcasted_iota(jnp.int32, (T, HEAD_DIM), 0) + row0
        for c in range(0, S, HEAD_DIM):
            segr = segrow[:, c:c + HEAD_DIM]
            ui = lax.broadcasted_iota(jnp.int32, (T, HEAD_DIM), 1) + c
            mask[:, c:c + HEAD_DIM] = jnp.where((segc == segr) & (ui <= ti), 1.0, 0.0)

        def rope(val):
            pk = table[w, pl.ds(row0, T), :]
            lane = lax.broadcasted_iota(jnp.int32, (T, HEAD_DIM), 1)
            swapped = pltpu.roll(pk, HEAD_DIM // 2, 1)
            cosw = jnp.where(lane < HEAD_DIM // 2, pk, swapped)
            sinw = jnp.where(lane < HEAD_DIM // 2, -swapped, pk)
            outs = []
            for h in range(NH):
                v = val[:, h * HEAD_DIM:(h + 1) * HEAD_DIM]
                outs.append((v * cosw + pltpu.roll(v, HEAD_DIM // 2, 1) * sinw).astype(BF16))
            return outs

        def hcols(h):
            return slice(h * HEAD_DIM, (h + 1) * HEAD_DIM)

        def proj(i):
            p = i % 2

            def w(m):
                return wres[m] if i == 0 else wst[gslot(i, u), m]
            for h, val in enumerate(rope(jnp.dot(abuf[...], w(0), preferred_element_type=F32))):
                qb[p, :, hcols(h)] = val
            for h, val in enumerate(rope(jnp.dot(abuf[...], w(1), preferred_element_type=F32))):
                kc[i, pl.ds(row0, T), hcols(h)] = val
            vc[i, pl.ds(row0, T), :] = jnp.dot(abuf[...], w(2), preferred_element_type=F32).astype(BF16)

        def heads(i):
            for h in range(NH):
                sc = lax.dot_general(qb[i % 2, :, hcols(h)], kc[i, :, hcols(h)], (((1,), (1,)), ((), ())),
                                     preferred_element_type=F32) * scale
                pacc[0:T, h * S:(h + 1) * S] = jnp.where(mask[...] > 0.5, sc, NEG)
            for h in range(NH):
                for r in range(0, T, 32):
                    sc = pacc[r:r + 32, h * S:(h + 1) * S]
                    e = jnp.exp(sc - jnp.max(sc, axis=-1, keepdims=True))
                    pbuf[h, r:r + 32, :] = (e * (1.0 / jnp.sum(e, axis=-1, keepdims=True))).astype(BF16)
            for h in range(NH):
                act[0:T, i * QL + h * HEAD_DIM:i * QL + (h + 1) * HEAD_DIM] = jnp.dot(
                    pbuf[h], vc[i, :, hcols(h)], preferred_element_type=F32).astype(BF16)

        with jax.named_scope('shards'):
            @pl.when(u == 0)
            def _():
                group_wait(0, u)
            proj(0)
            for i in range(3):
                group_wait(i + 1, u)
                proj(i + 1)
                if i < 2:
                    @pl.when(u == 0)
                    def _():
                        if i == 0:
                            w_ready([2], range(3))
                        else:
                            w_ready([0, 1, 2], [3])
                            wo_own().wait()
                group_start(i + 3, u)
                heads(i)
                if i == 0:
                    @pl.when(u < N - 1)
                    def _():
                        h_fetch(u + 1)
            heads(3)

        with jax.named_scope('wo'):
            def wo_block(n, w):
                act[T:2 * T, n * OB:(n + 1) * OB] = jnp.dot(act[0:T, 0:4 * QL], w, preferred_element_type=F32).astype(BF16)

            group_wait(4, u)
            group_wait(5, u)
            for n in range(3):
                wo_block(n, wst[gslot(4, u), n])

            wo_block(3, wst[gslot(5, u), 0])

            @pl.when(u < N - 1)
            def _():
                group_start(1, u + 1)
                group_start(2, u + 1)

        def norm_b(b, carry):
            rows = pl.ds(b * NR, NR)
            h1 = (hin[hs, rows, :].astype(F32) + act[pl.ds(pl.multiple_of(T + b * NR, NR), NR), 0:D].astype(F32)).astype(BF16)
            h1b[lax.rem(u, 3), rows, :] = h1
            gb[lax.rem(u, 3), pl.ds(pl.multiple_of(hb * T + b * NR, NR), NR), :] = norm_rows(h1, gm_ref[0:1, :], None)
            return carry
        lax.fori_loop(0, T // NR, norm_b, 0)

        @pl.when((s > 0) & (u < N - HS))
        def _():
            pl.semaphore_signal(cred, inc=1, device_id={"pp": s - 1}, device_id_type=MESH)

    def mlp(sl, row0, rows, store):
        UN = 2 if NB % 2 == 0 else 1

        def up(q, carry):
            for n in [q * UN + k for k in range(UN)]:
                xin = gb[sl, pl.ds(row0, rows), :]
                g = jnp.dot(xin, wg_s[n], preferred_element_type=F32)
                u_ = jnp.dot(xin, wu_s[n], preferred_element_type=F32)
                act[0:rows, pl.ds(pl.multiple_of(n * FB, FB), FB)] = (jax.nn.silu(g) * u_).astype(BF16)
            return carry
        lax.fori_loop(0, NB // UN, up, 0)

        def down(q, carry):
            for n in [q * UN + k for k in range(UN)]:
                store(pl.ds(pl.multiple_of(n * DB, DB), DB), jnp.dot(act[0:rows, 0:FL], wd_s[n], preferred_element_type=F32))
            return carry
        lax.fori_loop(0, NB // UN, down, 0)

    def mlp_home(u):
        def store(c, val):
            pacc[:, c] = val
        with jax.named_scope('mlp'):
            mlp(lax.rem(u, 3), 0, 2 * T, store)

    def mlp_outer(u, b):
        def store(c, val):
            px[lax.rem(u, 2), pl.ds(pl.multiple_of(b * T, T), T), c] = val.astype(BF16)
        with jax.named_scope('mlp_o'):
            mlp(lax.rem(u, 3), pl.multiple_of(b * T, T), T, store)

    def forward(u):
        @pl.when((u >= 1) & (u <= N))
        def _():
            s2_copy(u - 1).wait_send()

        @pl.when(u < N)
        def _():
            with jax.named_scope('w_ag'):
                ag_wait(1 - hb, u)
            s2_copy(u).start()

    def combine(v):
        sl = lax.rem(v, 2)
        with jax.named_scope('w_s3'):
            s3_copy(v, 0).wait_recv()
            s3_copy(v, 1).wait_recv()

        @pl.when(v >= 1)
        def _():
            s4_copy(v - 1).wait_send()

        def comb(b, carry):
            rows = pl.ds(b * RB, RB)
            mine = pl.ds(pl.multiple_of(hb * T + b * RB, RB), RB)
            theirs = pl.ds(pl.multiple_of((1 - hb) * T + b * RB, RB), RB)
            oacc[rows, :] = pacc[mine, :] + px[sl, mine, :].astype(F32)
            sendb[rows, :] = (pacc[theirs, :] + px[sl, theirs, :].astype(F32)).astype(BF16)
            return carry
        lax.fori_loop(0, T // RB, comb, 0)
        s4_copy(v).start()

    def finish(u):
        @pl.when((u >= 2) & (u < N + 2))
        def _():
            v = u - 2
            with jax.named_scope('w_s4'):
                s4_copy(v).wait_recv()
            vw = v // NJ
            vj = lax.rem(v, NJ)

            @pl.when(v >= 1)
            def _():
                hin_copy(v).wait_send()

            def fin(b, carry):
                rows = pl.ds(b * RB, RB)
                d = (oacc[rows, :] + ps[lax.rem(v, 2), rows, :].astype(F32)).astype(BF16)
                h2b[rows, :] = (h1b[lax.rem(v, 3), rows, :].astype(F32) + d.astype(F32)).astype(BF16)
                return carry
            lax.fori_loop(0, T // RB, fin, 0)

            @pl.when((s < n_stages - 1) & (v >= HS))
            def _():
                with jax.named_scope('w_cred'):
                    pl.semaphore_wait(cred, 1)

            @pl.when(s < n_stages - 1)
            def _():
                hin_copy(v).start()

            @pl.when(s == n_stages - 1)
            def _():
                park_copy(v).start()

            @pl.when((s == n_stages - 1) & (v == N - 1))
            def _():
                last_copy().start()

    def body(u, carry):
        @pl.when(is_home)
        def _():
            @pl.when(u < N)
            def _():
                attention(u)

            @pl.when((u >= 1) & (u <= N))
            def _():
                s1_outer(u - 1).wait_send()
                s1_peer(u - 1).wait_send()

            @pl.when(u < N)
            def _():
                s1_peer(u).start()
                s1_outer(u).start()

            @pl.when((u >= 1) & (u <= N))
            def _():
                mlp_home(u - 1)

            finish(u)
            forward(u)

            @pl.when((u >= 1) & (u <= N))
            def _():
                combine(u - 1)

        @pl.when(is_outer & (u < N))
        def _():
            for k in (0, 1):
                b = inner - 1 if k == 0 else 2 - inner
                with jax.named_scope('w_ag_outer'):
                    ag_wait(b, u)

                @pl.when(u >= 2)
                def _():
                    s3_copy(u - 2, b).wait_send()
                mlp_outer(u, b)
                s3_copy(u, b).start()

        return carry

    def out_fwd(mb, p, sem):
        return rcopy(out_ref.at[mb], out_ref.at[mb], ofs.at[mb, p], sem, pp=p)

    lax.fori_loop(0, N + 2, body, 0)

    last_here = (s == n_stages - 1) & (z == NJ - 1)

    @pl.when(last_here)
    def _():
        for mb in (n_mb - 2, n_mb - 1):
            local(out_ref.at[mb], out_ref.at[mb], outr.at[mb]).wait()
            out_fwd(mb, 2, outf).start()

    def od_copy(v):
        return rcopy(hin_hbm.at[v], out_ref.at[2 * (v // NJ) + hb], od.at[v], outr.at[2 * (v // NJ) + hb], tp=lax.rem(v, NJ))

    @pl.when(s == 1)
    def _():
        def spread(v, carry):
            vj = lax.rem(v, NJ)
            mine = 2 * (v // NJ) + hb

            @pl.when(is_home)
            def _():
                local(hin_hbm.at[v], hin_hbm.at[v], op.at[v]).wait()

            @pl.when(is_home & (vj != z))
            def _():
                od_copy(v).start()

            @pl.when(is_home & (vj == z))
            def _():
                c = local(hin_hbm.at[v], hin.at[0], hv_sem)
                c.start()
                c.wait()
                c = local(hin.at[0], out_ref.at[mine], hv_sem)
                c.start()
                c.wait()

            @pl.when(vj == z)
            def _():
                for b in (0, 1):
                    mb = 2 * (v // NJ) + b

                    @pl.when(z - 1 != b)
                    def _(mb=mb):
                        local(out_ref.at[mb], out_ref.at[mb], outr.at[mb]).wait()
                    out_fwd(mb, 0, outf).start()

                    @pl.when(v < N - 1)
                    def _(mb=mb):
                        out_fwd(mb, 3, outf).start()
                        out_fwd(mb, 2, outf).start()
            return carry
        lax.fori_loop(0, N, spread, 0)

    @pl.when(is_home)
    def _():
        s4_copy(N - 1).wait_send()
        hin_copy(N - 1).wait_send()

        @pl.when(s == n_stages - 1)
        def _():
            last_copy().wait_send()

    @pl.when(is_outer)
    def _():
        for b in (0, 1):
            s3_copy(N - 2, b).wait_send()
            s3_copy(N - 1, b).wait_send()

    @pl.when(s < 2)
    def _():
        y_send(0).wait_send()

        @pl.when(is_outer)
        def _():
            y_send(1).wait_send()

    @pl.when((s >= 2) & is_home)
    def _():
        pp_send().wait_send()
        pf_send().wait_send()
        for r in (1, 2):
            pxf_send(r).wait_send()
        for r in (0, 1, 2):
            for i in (0, 1):
                push(r, i).wait_send()

    @pl.when(is_home)
    def _():
        def sent(m):
            p_send(m).wait_send()
            f_send(m).wait_send()
            x_send(1, m).wait_send()
            x_send(2, m).wait_send()
        for m in range(4):
            direct(m, functools.partial(sent, m))

        @pl.when(s == 2)
        def _():
            for w in range(1, NW):
                for j in range(NJ):
                    @pl.when(z != j)
                    def _():
                        x_pass(w, j).wait_send()

        @pl.when(s == 1)
        def _():
            def spread_done(v, carry):
                @pl.when(lax.rem(v, NJ) != z)
                def _():
                    od_copy(v).wait_send()
                return carry
            lax.fori_loop(0, N, spread_done, 0)

    for w in range(NW):
        x_each(w, lambda c: c.wait_send())

    @pl.when(s == 1)
    def _():
        for mb in range(n_mb):
            out_fwd(mb, 0, outf).wait_send()
            if mb < n_mb - 2:
                out_fwd(mb, 3, outf).wait_send()
                out_fwd(mb, 2, outf).wait_send()
            else:
                @pl.when(z < NJ - 1)
                def _(mb=mb):
                    out_fwd(mb, 3, outf).wait_send()
                    out_fwd(mb, 2, outf).wait_send()

    @pl.when(last_here)
    def _():
        for mb in (n_mb - 2, n_mb - 1):
            out_fwd(mb, 2, outf).wait_send()
        early = out_ref.at[pl.ds(0, n_mb - 2)]
        local(early, early, outf).wait()

    @pl.when((s == n_stages - 1) & (z < NJ - 1))
    def _():
        local(out_ref, out_ref, outf).wait()

    @pl.when((s == 0) | (s == 2))
    def _():
        local(out_ref, out_ref, outf).wait()


def solution(mesh):
    n_stages = mesh.shape['pp']

    def stage_program(hidden_in, seg_ids, positions, attn_norm, w_query, w_key, w_value, w_out, mlp_norm, w_gate, w_up, w_down):
        n_mb, T, D = hidden_in.shape
        S = seg_ids.shape[1]
        QL = w_query.shape[2]
        FL = w_gate.shape[2]
        NJ = S // T
        N = (n_mb // 2) * NJ
        NB = max(1, FL // 512)
        invf = jnp.asarray(np.tile(rope_freqs(), 2)[None, :], F32)
        any_spec = pl.BlockSpec(memory_space=pl.ANY)
        vmem = pl.BlockSpec(memory_space=pltpu.VMEM)
        dma = pltpu.SemaphoreType.DMA
        scratch = [
            pltpu.VMEM((NB, D, FL // NB), BF16), pltpu.VMEM((NB, D, FL // NB), BF16), pltpu.VMEM((NB, FL, D // NB), BF16),
            pltpu.VMEM((3, D, QL), BF16), pltpu.VMEM((2, 3, D, QL), BF16),
            pltpu.VMEM((3, 2 * T, D), BF16),
            pltpu.VMEM((2, 2 * T, D), BF16),
            pltpu.VMEM((2, T, D), BF16),
            pltpu.VMEM((4, S, QL), BF16), pltpu.VMEM((4, S, QL), BF16),
            pltpu.VMEM((4, T, D), BF16),
            pltpu.VMEM((3, T, D), BF16),
            pltpu.VMEM((2 * T, D), F32),
            pltpu.VMEM((T, D), F32),
            pltpu.VMEM((T, D), BF16),
            pltpu.VMEM((T, D), BF16),
            pltpu.VMEM((2 * T, max(D, FL, 4 * QL)), BF16),
            pltpu.VMEM((T, D), BF16),
            pltpu.VMEM((2, T, QL), BF16),
            pltpu.VMEM((n_mb // 2, S, HEAD_DIM), F32),
            pltpu.VMEM((T, S), F32), pltpu.VMEM((QL // HEAD_DIM, T, S), BF16),
            dma((3, 8)), dma((2, 4)), dma((8,)), dma((4,)), dma((2, 4)),
            dma((N,)), dma((n_mb // 2, 2)), dma((2, 3)), dma((2,)), dma, dma((2, 2)), dma((2, 2)), dma((2,)), dma, dma,
            dma((n_mb,)), dma, dma((n_mb, n_stages)),
            dma((3,)), dma((2, 3)), dma, dma((3, NB)), dma, dma, dma((N,)), dma((n_mb // 2, NJ)), dma((N,)), dma((N,)),
            dma((2,)), dma((2,)), dma((2,)), dma((2,)), dma, dma, dma, dma, dma((2,)), dma((2,)), dma((3, 2)),
            pltpu.SemaphoreType.REGULAR, pltpu.SemaphoreType.REGULAR,
        ]
        return pl.pallas_call(
            functools.partial(kernel, n_stages),
            out_shape=[jax.ShapeDtypeStruct(hidden_in.shape, BF16), jax.ShapeDtypeStruct((3, 3, D, QL), BF16),
                       jax.ShapeDtypeStruct((4 * QL, D), BF16), jax.ShapeDtypeStruct((N, T, D), BF16),
                       jax.ShapeDtypeStruct((4 * QL, D), BF16)],
            in_specs=[any_spec, vmem, vmem, vmem, vmem, vmem] + [any_spec] * 7,
            out_specs=[any_spec] * 5,
            scratch_shapes=scratch,
            compiler_params=pltpu.CompilerParams(has_side_effects=True, vmem_limit_bytes=67_043_328),
        )(hidden_in, seg_ids, positions, invf, attn_norm, mlp_norm, w_query, w_key, w_value, w_out, w_gate, w_up, w_down)[0]

    act_spec = P('dp', 'tp', None)
    row_spec = P('dp', None)
    gain_spec = P('pp', None)
    col_spec = P('pp', None, 'tp')
    rows_spec = P('pp', 'tp', None)
    return jax.shard_map(stage_program, mesh=mesh,
                         in_specs=(act_spec, row_spec, row_spec, gain_spec, col_spec, col_spec, col_spec, rows_spec, gain_spec, col_spec, col_spec, rows_spec),
                         out_specs=act_spec, check_vma=False)
```

```python
import functools
import math

import jax
import jax.numpy as jnp
import numpy as np
from jax import lax
from jax.experimental import pallas as pl
from jax.experimental.pallas import tpu as pltpu
from jax.sharding import PartitionSpec as P

HEAD_DIM = 128
NORM_EPS = 1e-5
ROPE_THETA = 500000.0
ROPE_FACTOR = 8.0
LOW_FREQ = 1.0
HIGH_FREQ = 4.0
ORIG_CTX = 8192.0
NEG = -1e30
MESH = pl.DeviceIdType.MESH
F32 = jnp.float32
BF16 = jnp.bfloat16


def rope_freqs():
    base_freq = 1.0 / (ROPE_THETA ** (np.arange(0, HEAD_DIM, 2) / HEAD_DIM))
    wavelen = 2.0 * np.pi / base_freq
    smooth = (ORIG_CTX / wavelen - LOW_FREQ) / (HIGH_FREQ - LOW_FREQ)
    blended = (1.0 - smooth) * base_freq / ROPE_FACTOR + smooth * base_freq
    scaled = np.where(wavelen > ORIG_CTX / LOW_FREQ, base_freq / ROPE_FACTOR, blended)
    return np.where(wavelen < ORIG_CTX / HIGH_FREQ, base_freq, scaled)


def kernel(n_stages, x_ref, seg_ref, pos_ref, invf_ref, ga_ref, gm_ref,
           wq_ref, wk_ref, wv_ref, wo_ref, wg_ref, wu_ref, wd_ref,
           out_ref,
           wqkv_hbm, wo_hbm, hin_hbm, pv_hbm, po_hbm,
           wg_s, wu_s, wd_s, wres, wst, gb, px, ps, kc, vc, hin, h1b, pacc, oacc, sendb, h2b, act, abuf, qb,
           table, mask, pbuf,
           wr, wx, wsnd, wfwd, wxs, hin_sem, xs, ag, s1s, s2s, pxr, pxs, psr, s4s, s5s, outr, outf, ofs,
           wres_sem, wst_sem, wo_sem, mlp_sem, hv_sem, s6s, xp, xq, op, od,
           ysn, yrc, pos, por, pps, ppr, pfs, pfr, pxfs, pxfr, pds, gate, cred):
    n_mb, T, D = x_ref.shape
    QL = wq_ref.shape[2]
    FL = wg_ref.shape[2]
    NB = wg_s.shape[0]
    FB = FL // NB
    S = seg_ref.shape[1]
    NJ = S // T
    NH = QL // HEAD_DIM
    N = (n_mb // 2) * NJ
    DB = D // NB
    scale = HEAD_DIM ** -0.5
    RB = 16
    NR = 32
    HS = hin.shape[0]
    OB = wst.shape[3]
    NO = D // OB

    hx = lax.axis_index("dp")
    z = lax.axis_index("tp")
    s = lax.axis_index("pp")
    is_home = (z == 1) | (z == 2)
    is_outer = (z == 0) | (z == 3)
    hb = lax.rem(z + 1, 2) * 0 + (z - 1)
    peer = 3 - z
    outer = 3 * (z - 1)
    inner = 1 + z // 2
    odd = lax.rem(s, 2)

    def rcopy(src, dst, ssem, rsem, **dev):
        return pltpu.make_async_remote_copy(src_ref=src, dst_ref=dst, send_sem=ssem, recv_sem=rsem,
                                            device_id=dev, device_id_type=MESH)

    def local(src, dst, sem):
        return pltpu.make_async_copy(src, dst, sem)

    def column(ref, mb, j):
        row = ref[pl.ds(mb, 1), :]
        part = row[:, 0:T]
        for c in range(1, NJ):
            part = jnp.where(j == c, row[:, c * T:(c + 1) * T], part)
        return jnp.broadcast_to(part, (HEAD_DIM, T)).T

    barrier = pltpu.get_barrier_semaphore()
    for k in range(1, 4):
        pl.semaphore_signal(barrier, inc=1, device_id={"tp": lax.rem(z + k, 4)}, device_id_type=MESH)
        pl.semaphore_signal(barrier, inc=1, device_id={"pp": lax.rem(s + k, 4)}, device_id_type=MESH)
    pl.semaphore_signal(barrier, inc=1, device_id={"dp": 1 - hx}, device_id_type=MESH)
    pl.semaphore_wait(barrier, 7)

    wqkv_own = (wq_ref, wk_ref, wv_ref, wo_ref)

    def mlp_copies():
        cps = []
        for n in range(NB):
            cps.append(local(wg_ref.at[0, :, pl.ds(n * FB, FB)], wg_s.at[n], mlp_sem.at[0, n]))
            cps.append(local(wu_ref.at[0, :, pl.ds(n * FB, FB)], wu_s.at[n], mlp_sem.at[1, n]))
            cps.append(local(wd_ref.at[0, :, pl.ds(n * DB, DB)], wd_s.at[n], mlp_sem.at[2, n]))
        return cps

    NW = n_mb // 2

    def x_copy(w, home):
        u = w * NJ + z
        return rcopy(x_ref.at[2 * w + (home - 1)], hin_hbm.at[u], xs.at[w, home - 1], xp.at[u], tp=home)

    def x_each(w, act):
        for home in (1, 2):
            @pl.when((s == 2) & (z != home))
            def _():
                act(x_copy(w, home))

    def x_pass(w, j):
        u = w * NJ + j
        return rcopy(hin_hbm.at[u], hin_hbm.at[u], xq.at[w, j], hin_sem.at[u], pp=0)

    def x_relay(ws):
        @pl.when((s == 2) & is_home)
        def _():
            for w in ws:
                for j in range(NJ):
                    @pl.when(z != j)
                    def _():
                        local(hin_hbm.at[w * NJ + j], hin_hbm.at[w * NJ + j], xp.at[w * NJ + j]).wait()
                        x_pass(w, j).start()

    x_each(0, lambda c: c.start())
    x_relay([0])

    def half(ref, m, h):
        rows = (D if m < 3 else QL) // 2
        return ref.at[pl.ds(h * rows, rows), :]

    def wslot(r, m):
        return wqkv_hbm.at[r, m] if m < 3 else wo_hbm.at[pl.ds((r + 1) * QL, QL)]

    def own_w(m):
        return wqkv_own[m].at[0]

    def wo_own():
        return local(own_w(3), wo_hbm.at[pl.ds(0, QL)], wo_sem)

    def o_send(k):
        h = hx if k < 4 else 1 - hx
        return rcopy(half(own_w(k % 4), k % 4, h), half(wslot(0, k % 4), k % 4, h), wsnd.at[k], wr.at[0, k], tp=inner)

    def p_send(m):
        return rcopy(half(own_w(m), m, hx), half(wslot(1, m), m, hx), wsnd.at[m], wr.at[1, m], tp=peer)

    def f_send(m):
        return rcopy(half(wslot(0, m), m, hx), half(wslot(2, m), m, hx), wfwd.at[m], wr.at[2, m], tp=peer)

    def x_send(r, m):
        return rcopy(half(wslot(r, m), m, hx), half(wslot(r, m), m, hx), wxs.at[r - 1, m], wx.at[r - 1, m], dp=1 - hx)

    def w_ready(rs, ms):
        def pushed(m):
            if 0 in rs:
                o_send(m).wait_recv()
            if 1 in rs:
                p_send(m).wait_recv()
            if 2 in rs:
                f_send(m).wait_recv()
        for m in ms:
            if m in PM:
                pl.when(s == 1)(functools.partial(pushed, m))
            if 0 in rs:
                o_send(4 + m).wait_recv()
            for r in (1, 2):
                if r in rs:
                    x_send(r, m).wait_recv()

    PM = (2, 3)

    def pb(r, m):
        return pv_hbm.at[r] if m == 2 else po_hbm.at[pl.ds(r * QL, QL)]

    def hh(i):
        return hx if i == 0 else 1 - hx

    def y_send(i, m):
        return rcopy(half(own_w(m), m, hh(i)), half(pb(3, m), m, hh(i)), ysn.at[2 * i + m - 2], yrc.at[2 * i + m - 2], pp=3)

    def po_send(i, m):
        return rcopy(half(pb(3, m), m, hh(i)), half(pb(0, m), m, hh(i)), pos.at[2 * i + m - 2], por.at[2 * i + m - 2], tp=inner)

    def pp_send(m):
        return rcopy(half(pb(3, m), m, hx), half(pb(1, m), m, hx), pps.at[m - 2], ppr.at[m - 2], tp=peer)

    def pf_send(m):
        return rcopy(half(pb(0, m), m, hx), half(pb(2, m), m, hx), pfs.at[m - 2], pfr.at[m - 2], tp=peer)

    def pxf_send(r, m):
        return rcopy(half(pb(r, m), m, hx), half(pb(r, m), m, hx), pxfs.at[r - 1, m - 2], pxfr.at[r - 1, m - 2], dp=1 - hx)

    def push(r, m, i):
        rsem = wr.at[0, 4 * i + m] if r == 0 else (wr.at[r, m] if i == 0 else wx.at[r - 1, m])
        return rcopy(half(pb(r, m), m, hh(i)), half(wslot(r, m), m, hh(i)), pds.at[r, m - 2, i], rsem, pp=1)

    def direct(m, f):
        if m in PM:
            pl.when(s != 1)(f)
        else:
            f()

    @pl.when(s == 1)
    def _():
        for m in PM:
            y_send(0, m).start()

        @pl.when(is_outer)
        def _():
            for m in PM:
                y_send(1, m).start()

    @pl.when((s == 3) & is_outer)
    def _():
        for i in (0, 1):
            for m in PM:
                y_send(i, m).wait_recv()
                po_send(i, m).start()
        for i in (0, 1):
            for m in PM:
                po_send(i, m).wait_send()

    @pl.when((s == 3) & is_home)
    def _():
        for m in PM:
            y_send(0, m).wait_recv()
            pp_send(m).start()
        for kind, m, a in (("p", 2, 0), ("o", 2, 0), ("p", 3, 0), ("o", 3, 0), ("f", 2, 0), ("o", 2, 1), ("x", 2, 1), ("x", 3, 1),
                           ("f", 3, 0), ("o", 3, 1), ("x", 2, 2), ("x", 3, 2)):
            with jax.named_scope('wp_' + kind + str(m) + str(a)):
                if kind == "p":
                    pp_send(m).wait_recv()
                    pxf_send(1, m).start()
                    push(1, m, 0).start()
                elif kind == "o":
                    po_send(a, m).wait_recv()
                    if a == 0:
                        pf_send(m).start()
                    push(0, m, a).start()
                elif kind == "f":
                    pf_send(m).wait_recv()
                    pxf_send(2, m).start()
                    push(2, m, 0).start()
                else:
                    pxf_send(a, m).wait_recv()
                    push(a, m, 1).start()

    @pl.when(s == 3)
    def _():
        pl.semaphore_signal(gate, inc=1, device_id={"pp": 2}, device_id_type=MESH)

    def release():
        @pl.when(odd == 0)
        def _():
            pl.semaphore_signal(gate, inc=1, device_id={"pp": s + 1}, device_id_type=MESH)

    @pl.when(s != 0)
    def _():
        for c in mlp_copies():
            c.start()
        with jax.named_scope('w_gate'):
            pl.semaphore_wait(gate, 1)

    if NW > 1:
        x_each(1, lambda c: c.start())

    @pl.when(is_outer)
    def _():
        for k in range(8):
            direct(k % 4, lambda k=k: o_send(k).start())

        @pl.when(s == 0)
        def _():
            for c in mlp_copies():
                c.start()
        for k in range(8):
            direct(k % 4, lambda k=k: o_send(k).wait_send())
        release()
        for w in range(2, NW):
            x_each(w, lambda c: c.start())

    @pl.when(is_home)
    def _():
        for m in range(4):
            direct(m, lambda m=m: p_send(m).start())
        wo_own().start()

        @pl.when(s == 0)
        def _():
            for c in mlp_copies():
                c.start()
        def zero_rows(b, carry):
            for i in range(4):
                kc[i, pl.ds(b * RB, RB), :] = jnp.zeros((RB, QL), BF16)
                vc[i, pl.ds(b * RB, RB), :] = jnp.zeros((RB, QL), BF16)
            return carry
        lax.fori_loop(0, S // RB, zero_rows, 0)

        def tables(w):
            lane = lax.broadcasted_iota(jnp.int32, (T, HEAD_DIM), 1)

            def table_rows(b, carry):
                rows = pl.ds(pl.multiple_of(b * T, T), T)
                ang = column(pos_ref, 2 * w + hb, b).astype(F32) * invf_ref[0:1, :]
                table[w, rows, :] = jnp.where(lane < HEAD_DIM // 2, jnp.cos(ang), jnp.sin(ang))
                return carry
            with jax.named_scope('table'):
                lax.fori_loop(0, NJ, table_rows, 0)

        steps = [("o", 0), ("p", 0), ("t", 0), ("o", 1), ("p", 1), ("t", 1), ("o", 2), ("p", 2), ("t", 2), ("o", 3), ("p", 3), ("t", 3),
                 ("r", 0), ("f", 0), ("f", 1), ("f", 2), ("f", 3), ("g", 0)]

        def step(kind, m):
            if kind == "o":
                o_send(m).wait_recv()
                f_send(m).start()
            elif kind == "p":
                p_send(m).wait_recv()
                x_send(1, m).start()
            else:
                f_send(m).wait_recv()
                x_send(2, m).start()

        for kind, m in steps:
            with jax.named_scope('w_' + kind + str(m)):
                if kind in "opf":
                    direct(m, lambda kind=kind, m=m: step(kind, m))
                elif kind == "g":
                    release()
                elif kind == "r":
                    x_relay([1] if NW > 1 else [])
                elif m < n_mb // 2:
                    tables(m)
        for w in range(2, NW):
            x_each(w, lambda c: c.start())
        w_ready([0, 1], range(3))
        x_relay(range(2, NW))

    def gslot(g, u):
        return lax.rem(g - 1 + u, 2)

    def group_copies(g, u):
        if g == 0:
            return [local(own_w(m), wres.at[m], wres_sem.at[m]) for m in range(3)]
        p = gslot(g, u)
        if g < 4:
            return [local(wqkv_hbm.at[g - 1], wst.at[p], wst_sem.at[p, 0])]
        return [local(wo_hbm.at[:, pl.ds(((g - 4) * 3 + m) * OB, OB)], wst.at[p, m], wst_sem.at[p, m]) for m in range(3 if g == 4 else 1)]

    def group_start(g, u):
        for c in group_copies(g, u):
            c.start()

    def group_wait(g, u):
        for c in group_copies(g, u):
            c.wait()

    def h_fetch(u):
        mb = 2 * (u // NJ) + hb
        here = lax.rem(u, NJ) == z
        dst = hin.at[lax.rem(u, HS)]

        @pl.when((s == 0) & here)
        def _():
            local(x_ref.at[mb], dst, hv_sem).start()

        @pl.when((s == 0) & jnp.logical_not(here))
        def _():
            local(hin_hbm.at[u], hin_hbm.at[u], hin_sem.at[u]).wait()
            local(hin_hbm.at[u], dst, hv_sem).start()

    @pl.when(is_home)
    def _():
        group_start(0, 0)
        group_start(1, 0)
        group_start(2, 0)
        h_fetch(0)

    for c in mlp_copies():
        c.wait()

    def hin_copy(u):
        return rcopy(h2b, hin.at[lax.rem(u, HS)], s5s, hin_sem.at[u], pp=lax.rem(s + 1, n_stages))

    def s1_outer(u):
        blk = gb.at[lax.rem(u, 3), pl.ds(pl.multiple_of(hb * T, T), T), :]
        return rcopy(blk, blk, s1s.at[0], ag.at[hb, lax.rem(u, 3)], tp=outer)

    def s1_peer(u):
        blk = gb.at[lax.rem(u, 3), pl.ds(pl.multiple_of(hb * T, T), T), :]
        return rcopy(blk, blk, s1s.at[1], ag.at[hb, lax.rem(u, 3)], tp=peer)

    def s2_copy(u):
        blk = gb.at[lax.rem(u, 3), pl.ds(pl.multiple_of((1 - hb) * T, T), T), :]
        return rcopy(blk, blk, s2s, ag.at[1 - hb, lax.rem(u, 3)], tp=outer)

    def ag_wait(b, u):
        blk = gb.at[lax.rem(u, 3), pl.ds(pl.multiple_of(b * T, T), T), :]
        local(blk, blk, ag.at[b, lax.rem(u, 3)]).wait()

    def s3_copy(u, b):
        sl = lax.rem(u, 2)
        blk = px.at[sl, pl.ds(pl.multiple_of(b * T, T), T), :]
        return rcopy(blk, blk, pxs.at[sl, b], pxr.at[sl, b], tp=inner)

    def s4_copy(u):
        return rcopy(sendb, ps.at[lax.rem(u, 2)], s4s, psr.at[lax.rem(u, 2)], tp=peer)

    def park_copy(u):
        return rcopy(h2b, hin_hbm.at[u], s5s, op.at[u], pp=1)

    def last_copy():
        mb = n_mb - 2 + hb
        return rcopy(h2b, out_ref.at[mb], s6s, outr.at[mb], tp=NJ - 1)

    def norm_rows(src, gain, dst):
        hf = src.astype(F32)
        inv = lax.rsqrt(jnp.mean(hf * hf, axis=-1, keepdims=True) + NORM_EPS)
        return (hf * inv * gain.astype(F32)).astype(BF16)

    def attention(u):
      with jax.named_scope('attn'):
        attention_(u)

    def attention_(u):
        w = u // NJ
        j = lax.rem(u, NJ)
        mb = 2 * w + hb
        row0 = pl.multiple_of(j * T, T)
        hs = lax.rem(u, HS)

        with jax.named_scope('w_hin'):
            @pl.when(s == 0)
            def _():
                local(x_ref.at[mb], hin.at[hs], hv_sem).wait()

            @pl.when(s > 0)
            def _():
                hin_copy(u).wait_recv()

        def norm_a(b, carry):
            rows = pl.ds(b * NR, NR)
            abuf[rows, :] = norm_rows(hin[hs, rows, :], ga_ref[0:1, :], None)
            return carry
        lax.fori_loop(0, T // NR, norm_a, 0)

        segrow = seg_ref[pl.ds(mb, 1), :]
        segc = column(seg_ref, mb, j)
        ti = lax.broadcasted_iota(jnp.int32, (T, HEAD_DIM), 0) + row0
        for c in range(0, S, HEAD_DIM):
            segr = segrow[:, c:c + HEAD_DIM]
            ui = lax.broadcasted_iota(jnp.int32, (T, HEAD_DIM), 1) + c
            mask[:, c:c + HEAD_DIM] = jnp.where((segc == segr) & (ui <= ti), 1.0, 0.0)

        def rope(val):
            pk = table[w, pl.ds(row0, T), :]
            lane = lax.broadcasted_iota(jnp.int32, (T, HEAD_DIM), 1)
            swapped = pltpu.roll(pk, HEAD_DIM // 2, 1)
            cosw = jnp.where(lane < HEAD_DIM // 2, pk, swapped)
            sinw = jnp.where(lane < HEAD_DIM // 2, -swapped, pk)
            outs = []
            for h in range(NH):
                v = val[:, h * HEAD_DIM:(h + 1) * HEAD_DIM]
                outs.append((v * cosw + pltpu.roll(v, HEAD_DIM // 2, 1) * sinw).astype(BF16))
            return outs

        def hcols(h):
            return slice(h * HEAD_DIM, (h + 1) * HEAD_DIM)

        def proj(i):
            p = i % 2

            def w(m):
                return wres[m] if i == 0 else wst[gslot(i, u), m]
            for h, val in enumerate(rope(jnp.dot(abuf[...], w(0), preferred_element_type=F32))):
                qb[p, :, hcols(h)] = val
            for h, val in enumerate(rope(jnp.dot(abuf[...], w(1), preferred_element_type=F32))):
                kc[i, pl.ds(row0, T), hcols(h)] = val
            vc[i, pl.ds(row0, T), :] = jnp.dot(abuf[...], w(2), preferred_element_type=F32).astype(BF16)

        def heads(i):
            for h in range(NH):
                sc = lax.dot_general(qb[i % 2, :, hcols(h)], kc[i, :, hcols(h)], (((1,), (1,)), ((), ())),
                                     preferred_element_type=F32) * scale
                pacc[0:T, h * S:(h + 1) * S] = jnp.where(mask[...] > 0.5, sc, NEG)
            for h in range(NH):
                for r in range(0, T, 32):
                    sc = pacc[r:r + 32, h * S:(h + 1) * S]
                    e = jnp.exp(sc - jnp.max(sc, axis=-1, keepdims=True))
                    pbuf[h, r:r + 32, :] = (e * (1.0 / jnp.sum(e, axis=-1, keepdims=True))).astype(BF16)
            for h in range(NH):
                act[0:T, i * QL + h * HEAD_DIM:i * QL + (h + 1) * HEAD_DIM] = jnp.dot(
                    pbuf[h], vc[i, :, hcols(h)], preferred_element_type=F32).astype(BF16)

        with jax.named_scope('shards'):
            @pl.when(u == 0)
            def _():
                group_wait(0, u)
            proj(0)
            for i in range(3):
                group_wait(i + 1, u)
                proj(i + 1)
                if i < 2:
                    @pl.when(u == 0)
                    def _():
                        if i == 0:
                            w_ready([2], range(3))
                        else:
                            w_ready([0, 1, 2], [3])
                            wo_own().wait()
                group_start(i + 3, u)
                heads(i)
                if i == 0:
                    @pl.when(u < N - 1)
                    def _():
                        h_fetch(u + 1)
            heads(3)

        with jax.named_scope('wo'):
            def wo_block(n, w):
                act[T:2 * T, n * OB:(n + 1) * OB] = jnp.dot(act[0:T, 0:4 * QL], w, preferred_element_type=F32).astype(BF16)

            group_wait(4, u)
            group_wait(5, u)
            for n in range(3):
                wo_block(n, wst[gslot(4, u), n])

            wo_block(3, wst[gslot(5, u), 0])

            @pl.when(u < N - 1)
            def _():
                group_start(1, u + 1)
                group_start(2, u + 1)

        def norm_b(b, carry):
            rows = pl.ds(b * NR, NR)
            h1 = (hin[hs, rows, :].astype(F32) + act[pl.ds(pl.multiple_of(T + b * NR, NR), NR), 0:D].astype(F32)).astype(BF16)
            h1b[lax.rem(u, 3), rows, :] = h1
            gb[lax.rem(u, 3), pl.ds(pl.multiple_of(hb * T + b * NR, NR), NR), :] = norm_rows(h1, gm_ref[0:1, :], None)
            return carry
        lax.fori_loop(0, T // NR, norm_b, 0)

        @pl.when((s > 0) & (u < N - HS))
        def _():
            pl.semaphore_signal(cred, inc=1, device_id={"pp": s - 1}, device_id_type=MESH)

    def mlp(sl, row0, rows, store):
        UN = 2 if NB % 2 == 0 else 1

        def up(q, carry):
            for n in [q * UN + k for k in range(UN)]:
                xin = gb[sl, pl.ds(row0, rows), :]
                g = jnp.dot(xin, wg_s[n], preferred_element_type=F32)
                u_ = jnp.dot(xin, wu_s[n], preferred_element_type=F32)
                act[0:rows, pl.ds(pl.multiple_of(n * FB, FB), FB)] = (jax.nn.silu(g) * u_).astype(BF16)
            return carry
        lax.fori_loop(0, NB // UN, up, 0)

        def down(q, carry):
            for n in [q * UN + k for k in range(UN)]:
                store(pl.ds(pl.multiple_of(n * DB, DB), DB), jnp.dot(act[0:rows, 0:FL], wd_s[n], preferred_element_type=F32))
            return carry
        lax.fori_loop(0, NB // UN, down, 0)

    def mlp_home(u):
        def store(c, val):
            pacc[:, c] = val
        with jax.named_scope('mlp'):
            mlp(lax.rem(u, 3), 0, 2 * T, store)

    def mlp_outer(u, b):
        def store(c, val):
            px[lax.rem(u, 2), pl.ds(pl.multiple_of(b * T, T), T), c] = val.astype(BF16)
        with jax.named_scope('mlp_o'):
            mlp(lax.rem(u, 3), pl.multiple_of(b * T, T), T, store)

    def forward(u):
        @pl.when((u >= 1) & (u <= N))
        def _():
            s2_copy(u - 1).wait_send()

        @pl.when(u < N)
        def _():
            with jax.named_scope('w_ag'):
                ag_wait(1 - hb, u)
            s2_copy(u).start()

    def combine(v):
        sl = lax.rem(v, 2)
        with jax.named_scope('w_s3'):
            s3_copy(v, 0).wait_recv()
            s3_copy(v, 1).wait_recv()

        @pl.when(v >= 1)
        def _():
            s4_copy(v - 1).wait_send()

        def comb(b, carry):
            rows = pl.ds(b * RB, RB)
            mine = pl.ds(pl.multiple_of(hb * T + b * RB, RB), RB)
            theirs = pl.ds(pl.multiple_of((1 - hb) * T + b * RB, RB), RB)
            oacc[rows, :] = pacc[mine, :] + px[sl, mine, :].astype(F32)
            sendb[rows, :] = (pacc[theirs, :] + px[sl, theirs, :].astype(F32)).astype(BF16)
            return carry
        lax.fori_loop(0, T // RB, comb, 0)
        s4_copy(v).start()

    def finish(u):
        @pl.when((u >= 2) & (u < N + 2))
        def _():
            v = u - 2
            with jax.named_scope('w_s4'):
                s4_copy(v).wait_recv()
            vw = v // NJ
            vj = lax.rem(v, NJ)

            @pl.when(v >= 1)
            def _():
                hin_copy(v).wait_send()

            def fin(b, carry):
                rows = pl.ds(b * RB, RB)
                d = (oacc[rows, :] + ps[lax.rem(v, 2), rows, :].astype(F32)).astype(BF16)
                h2b[rows, :] = (h1b[lax.rem(v, 3), rows, :].astype(F32) + d.astype(F32)).astype(BF16)
                return carry
            lax.fori_loop(0, T // RB, fin, 0)

            @pl.when((s < n_stages - 1) & (v >= HS))
            def _():
                with jax.named_scope('w_cred'):
                    pl.semaphore_wait(cred, 1)

            @pl.when(s < n_stages - 1)
            def _():
                hin_copy(v).start()

            @pl.when(s == n_stages - 1)
            def _():
                park_copy(v).start()

            @pl.when((s == n_stages - 1) & (v == N - 1))
            def _():
                last_copy().start()

    def body(u, carry):
        @pl.when(is_home)
        def _():
            @pl.when(u < N)
            def _():
                attention(u)

            @pl.when((u >= 1) & (u <= N))
            def _():
                s1_outer(u - 1).wait_send()
                s1_peer(u - 1).wait_send()

            @pl.when(u < N)
            def _():
                s1_peer(u).start()
                s1_outer(u).start()

            @pl.when((u >= 1) & (u <= N))
            def _():
                mlp_home(u - 1)

            finish(u)
            forward(u)

            @pl.when((u >= 1) & (u <= N))
            def _():
                combine(u - 1)

        @pl.when(is_outer & (u < N))
        def _():
            for k in (0, 1):
                b = inner - 1 if k == 0 else 2 - inner
                with jax.named_scope('w_ag_outer'):
                    ag_wait(b, u)

                @pl.when(u >= 2)
                def _():
                    s3_copy(u - 2, b).wait_send()
                mlp_outer(u, b)
                s3_copy(u, b).start()

        return carry

    def out_fwd(mb, p, sem):
        return rcopy(out_ref.at[mb], out_ref.at[mb], ofs.at[mb, p], sem, pp=p)

    lax.fori_loop(0, N + 2, body, 0)

    last_here = (s == n_stages - 1) & (z == NJ - 1)

    @pl.when(last_here)
    def _():
        for mb in (n_mb - 2, n_mb - 1):
            local(out_ref.at[mb], out_ref.at[mb], outr.at[mb]).wait()
            out_fwd(mb, 2, outf).start()

    def od_copy(v):
        return rcopy(hin_hbm.at[v], out_ref.at[2 * (v // NJ) + hb], od.at[v], outr.at[2 * (v // NJ) + hb], tp=lax.rem(v, NJ))

    @pl.when(s == 1)
    def _():
        def spread(v, carry):
            vj = lax.rem(v, NJ)
            mine = 2 * (v // NJ) + hb

            @pl.when(is_home)
            def _():
                local(hin_hbm.at[v], hin_hbm.at[v], op.at[v]).wait()

            @pl.when(is_home & (vj != z))
            def _():
                od_copy(v).start()

            @pl.when(is_home & (vj == z))
            def _():
                c = local(hin_hbm.at[v], hin.at[0], hv_sem)
                c.start()
                c.wait()
                c = local(hin.at[0], out_ref.at[mine], hv_sem)
                c.start()
                c.wait()

            @pl.when(vj == z)
            def _():
                for b in (0, 1):
                    mb = 2 * (v // NJ) + b

                    @pl.when(z - 1 != b)
                    def _(mb=mb):
                        local(out_ref.at[mb], out_ref.at[mb], outr.at[mb]).wait()
                    out_fwd(mb, 0, outf).start()

                    @pl.when(v < N - 1)
                    def _(mb=mb):
                        out_fwd(mb, 3, outf).start()
                        out_fwd(mb, 2, outf).start()
            return carry
        lax.fori_loop(0, N, spread, 0)

    @pl.when(is_home)
    def _():
        s4_copy(N - 1).wait_send()
        hin_copy(N - 1).wait_send()

        @pl.when(s == n_stages - 1)
        def _():
            last_copy().wait_send()

    @pl.when(is_outer)
    def _():
        for b in (0, 1):
            s3_copy(N - 2, b).wait_send()
            s3_copy(N - 1, b).wait_send()

    @pl.when(s == 1)
    def _():
        for m in PM:
            y_send(0, m).wait_send()

        @pl.when(is_outer)
        def _():
            for m in PM:
                y_send(1, m).wait_send()

    @pl.when((s == 3) & is_home)
    def _():
        for m in PM:
            pp_send(m).wait_send()
            pf_send(m).wait_send()
            for r in (1, 2):
                pxf_send(r, m).wait_send()
            for r in (0, 1, 2):
                for i in (0, 1):
                    push(r, m, i).wait_send()

    @pl.when(is_home)
    def _():
        def sent(m):
            p_send(m).wait_send()
            f_send(m).wait_send()
            x_send(1, m).wait_send()
            x_send(2, m).wait_send()
        for m in range(4):
            direct(m, functools.partial(sent, m))

        @pl.when(s == 2)
        def _():
            for w in range(NW):
                for j in range(NJ):
                    @pl.when(z != j)
                    def _():
                        x_pass(w, j).wait_send()

        @pl.when(s == 1)
        def _():
            def spread_done(v, carry):
                @pl.when(lax.rem(v, NJ) != z)
                def _():
                    od_copy(v).wait_send()
                return carry
            lax.fori_loop(0, N, spread_done, 0)

    for w in range(NW):
        x_each(w, lambda c: c.wait_send())

    @pl.when(s == 1)
    def _():
        for mb in range(n_mb):
            out_fwd(mb, 0, outf).wait_send()
            if mb < n_mb - 2:
                out_fwd(mb, 3, outf).wait_send()
                out_fwd(mb, 2, outf).wait_send()
            else:
                @pl.when(z < NJ - 1)
                def _(mb=mb):
                    out_fwd(mb, 3, outf).wait_send()
                    out_fwd(mb, 2, outf).wait_send()

    @pl.when(last_here)
    def _():
        for mb in (n_mb - 2, n_mb - 1):
            out_fwd(mb, 2, outf).wait_send()
        early = out_ref.at[pl.ds(0, n_mb - 2)]
        local(early, early, outf).wait()

    @pl.when((s == n_stages - 1) & (z < NJ - 1))
    def _():
        local(out_ref, out_ref, outf).wait()

    @pl.when((s == 0) | (s == 2))
    def _():
        local(out_ref, out_ref, outf).wait()


def solution(mesh):
    n_stages = mesh.shape['pp']

    def stage_program(hidden_in, seg_ids, positions, attn_norm, w_query, w_key, w_value, w_out, mlp_norm, w_gate, w_up, w_down):
        n_mb, T, D = hidden_in.shape
        S = seg_ids.shape[1]
        QL = w_query.shape[2]
        FL = w_gate.shape[2]
        NJ = S // T
        N = (n_mb // 2) * NJ
        NB = max(1, FL // 512)
        invf = jnp.asarray(np.tile(rope_freqs(), 2)[None, :], F32)
        any_spec = pl.BlockSpec(memory_space=pl.ANY)
        vmem = pl.BlockSpec(memory_space=pltpu.VMEM)
        dma = pltpu.SemaphoreType.DMA
        scratch = [
            pltpu.VMEM((NB, D, FL // NB), BF16), pltpu.VMEM((NB, D, FL // NB), BF16), pltpu.VMEM((NB, FL, D // NB), BF16),
            pltpu.VMEM((3, D, QL), BF16), pltpu.VMEM((2, 3, D, QL), BF16),
            pltpu.VMEM((3, 2 * T, D), BF16),
            pltpu.VMEM((2, 2 * T, D), BF16),
            pltpu.VMEM((2, T, D), BF16),
            pltpu.VMEM((4, S, QL), BF16), pltpu.VMEM((4, S, QL), BF16),
            pltpu.VMEM((4, T, D), BF16),
            pltpu.VMEM((3, T, D), BF16),
            pltpu.VMEM((2 * T, D), F32),
            pltpu.VMEM((T, D), F32),
            pltpu.VMEM((T, D), BF16),
            pltpu.VMEM((T, D), BF16),
            pltpu.VMEM((2 * T, max(D, FL, 4 * QL)), BF16),
            pltpu.VMEM((T, D), BF16),
            pltpu.VMEM((2, T, QL), BF16),
            pltpu.VMEM((n_mb // 2, S, HEAD_DIM), F32),
            pltpu.VMEM((T, S), F32), pltpu.VMEM((QL // HEAD_DIM, T, S), BF16),
            dma((3, 8)), dma((2, 4)), dma((8,)), dma((4,)), dma((2, 4)),
            dma((N,)), dma((n_mb // 2, 2)), dma((2, 3)), dma((2,)), dma, dma((2, 2)), dma((2, 2)), dma((2,)), dma, dma,
            dma((n_mb,)), dma, dma((n_mb, n_stages)),
            dma((3,)), dma((2, 3)), dma, dma((3, NB)), dma, dma, dma((N,)), dma((n_mb // 2, NJ)), dma((N,)), dma((N,)),
            dma((4,)), dma((4,)), dma((4,)), dma((4,)), dma((2,)), dma((2,)), dma((2,)), dma((2,)), dma((2, 2)), dma((2, 2)), dma((3, 2, 2)),
            pltpu.SemaphoreType.REGULAR, pltpu.SemaphoreType.REGULAR,
        ]
        return pl.pallas_call(
            functools.partial(kernel, n_stages),
            out_shape=[jax.ShapeDtypeStruct(hidden_in.shape, BF16), jax.ShapeDtypeStruct((3, 3, D, QL), BF16),
                       jax.ShapeDtypeStruct((4 * QL, D), BF16), jax.ShapeDtypeStruct((N, T, D), BF16),
                       jax.ShapeDtypeStruct((4, D, QL), BF16), jax.ShapeDtypeStruct((4 * QL, D), BF16)],
            in_specs=[any_spec, vmem, vmem, vmem, vmem, vmem] + [any_spec] * 7,
            out_specs=[any_spec] * 6,
            scratch_shapes=scratch,
            compiler_params=pltpu.CompilerParams(collective_id=0, has_side_effects=True, vmem_limit_bytes=67_043_328),
        )(hidden_in, seg_ids, positions, invf, attn_norm, mlp_norm, w_query, w_key, w_value, w_out, w_gate, w_up, w_down)[0]

    act_spec = P('dp', 'tp', None)
    row_spec = P('dp', None)
    gain_spec = P('pp', None)
    col_spec = P('pp', None, 'tp')
    rows_spec = P('pp', 'tp', None)
    return jax.shard_map(stage_program, mesh=mesh,
                         in_specs=(act_spec, row_spec, row_spec, gain_spec, col_spec, col_spec, col_spec, rows_spec, gain_spec, col_spec, col_spec, rows_spec),
                         out_specs=act_spec, check_vma=False)
```

```python
import functools
import math

import jax
import jax.numpy as jnp
import numpy as np
from jax import lax
from jax.experimental import pallas as pl
from jax.experimental.pallas import tpu as pltpu
from jax.sharding import PartitionSpec as P

HEAD_DIM = 128
NORM_EPS = 1e-5
ROPE_THETA = 500000.0
ROPE_FACTOR = 8.0
LOW_FREQ = 1.0
HIGH_FREQ = 4.0
ORIG_CTX = 8192.0
NEG = -1e30
MESH = pl.DeviceIdType.MESH
F32 = jnp.float32
BF16 = jnp.bfloat16


def rope_freqs():
    base_freq = 1.0 / (ROPE_THETA ** (np.arange(0, HEAD_DIM, 2) / HEAD_DIM))
    wavelen = 2.0 * np.pi / base_freq
    smooth = (ORIG_CTX / wavelen - LOW_FREQ) / (HIGH_FREQ - LOW_FREQ)
    blended = (1.0 - smooth) * base_freq / ROPE_FACTOR + smooth * base_freq
    scaled = np.where(wavelen > ORIG_CTX / LOW_FREQ, base_freq / ROPE_FACTOR, blended)
    return np.where(wavelen < ORIG_CTX / HIGH_FREQ, base_freq, scaled)


def kernel(n_stages, x_ref, seg_ref, pos_ref, invf_ref, ga_ref, gm_ref,
           wq_ref, wk_ref, wv_ref, wo_ref, wg_ref, wu_ref, wd_ref,
           out_ref,
           wqkv_hbm, wo_hbm, hin_hbm, pv_hbm, po_hbm,
           wg_s, wu_s, wd_s, wres, wst, gb, px, ps, kc, vc, hin, h1b, pacc, oacc, sendb, h2b, act, abuf, qb,
           table, mask, pbuf,
           wr, wx, wsnd, wfwd, wxs, hin_sem, xs, ag, s1s, s2s, pxr, pxs, psr, s4s, s5s, outr, outf, ofs,
           wres_sem, wst_sem, wo_sem, mlp_sem, hv_sem, s6s, xp, xq, op, od,
           ysn, yrc, pos, por, pps, ppr, pfs, pfr, pxfs, pxfr, pds, gate, cred):
    n_mb, T, D = x_ref.shape
    QL = wq_ref.shape[2]
    FL = wg_ref.shape[2]
    NB = wg_s.shape[0]
    FB = FL // NB
    S = seg_ref.shape[1]
    NJ = S // T
    NH = QL // HEAD_DIM
    N = (n_mb // 2) * NJ
    DB = D // NB
    scale = HEAD_DIM ** -0.5
    RB = 16
    NR = 32
    HS = hin.shape[0]
    OB = wst.shape[3]
    NO = D // OB

    hx = lax.axis_index("dp")
    z = lax.axis_index("tp")
    s = lax.axis_index("pp")
    is_home = (z == 1) | (z == 2)
    is_outer = (z == 0) | (z == 3)
    hb = lax.rem(z + 1, 2) * 0 + (z - 1)
    peer = 3 - z
    outer = 3 * (z - 1)
    inner = 1 + z // 2
    odd = lax.rem(s, 2)

    def rcopy(src, dst, ssem, rsem, **dev):
        return pltpu.make_async_remote_copy(src_ref=src, dst_ref=dst, send_sem=ssem, recv_sem=rsem,
                                            device_id=dev, device_id_type=MESH)

    def local(src, dst, sem):
        return pltpu.make_async_copy(src, dst, sem)

    def column(ref, mb, j):
        row = ref[pl.ds(mb, 1), :]
        part = row[:, 0:T]
        for c in range(1, NJ):
            part = jnp.where(j == c, row[:, c * T:(c + 1) * T], part)
        return jnp.broadcast_to(part, (HEAD_DIM, T)).T

    barrier = pltpu.get_barrier_semaphore()
    for k in range(1, 4):
        pl.semaphore_signal(barrier, inc=1, device_id={"tp": lax.rem(z + k, 4)}, device_id_type=MESH)
        pl.semaphore_signal(barrier, inc=1, device_id={"pp": lax.rem(s + k, 4)}, device_id_type=MESH)
    pl.semaphore_signal(barrier, inc=1, device_id={"dp": 1 - hx}, device_id_type=MESH)
    pl.semaphore_wait(barrier, 7)

    wqkv_own = (wq_ref, wk_ref, wv_ref, wo_ref)

    def mlp_copies():
        cps = []
        for n in range(NB):
            cps.append(local(wg_ref.at[0, :, pl.ds(n * FB, FB)], wg_s.at[n], mlp_sem.at[0, n]))
            cps.append(local(wu_ref.at[0, :, pl.ds(n * FB, FB)], wu_s.at[n], mlp_sem.at[1, n]))
            cps.append(local(wd_ref.at[0, :, pl.ds(n * DB, DB)], wd_s.at[n], mlp_sem.at[2, n]))
        return cps

    NW = n_mb // 2

    def x_copy(w, home):
        u = w * NJ + z
        return rcopy(x_ref.at[2 * w + (home - 1)], hin_hbm.at[u], xs.at[w, home - 1], xp.at[u], tp=home)

    def x_each(w, act):
        for home in (1, 2):
            @pl.when((s == 2) & (z != home))
            def _():
                act(x_copy(w, home))

    def x_pass(w, j):
        u = w * NJ + j
        return rcopy(hin_hbm.at[u], hin_hbm.at[u], xq.at[w, j], hin_sem.at[u], pp=0)

    def x_relay(ws):
        @pl.when((s == 2) & is_home)
        def _():
            for w in ws:
                for j in range(NJ):
                    @pl.when(z != j)
                    def _():
                        local(hin_hbm.at[w * NJ + j], hin_hbm.at[w * NJ + j], xp.at[w * NJ + j]).wait()
                        x_pass(w, j).start()

    x_each(0, lambda c: c.start())
    x_relay([0])

    def half(ref, m, h):
        rows = (D if m < 3 else QL) // 2
        return ref.at[pl.ds(h * rows, rows), :]

    def wslot(r, m):
        return wqkv_hbm.at[r, m] if m < 3 else wo_hbm.at[pl.ds((r + 1) * QL, QL)]

    def own_w(m):
        return wqkv_own[m].at[0]

    def wo_own():
        return local(own_w(3), wo_hbm.at[pl.ds(0, QL)], wo_sem)

    def o_send(k):
        h = hx if k < 4 else 1 - hx
        return rcopy(half(own_w(k % 4), k % 4, h), half(wslot(0, k % 4), k % 4, h), wsnd.at[k], wr.at[0, k], tp=inner)

    def p_send(m):
        return rcopy(half(own_w(m), m, hx), half(wslot(1, m), m, hx), wsnd.at[m], wr.at[1, m], tp=peer)

    def f_send(m):
        return rcopy(half(wslot(0, m), m, hx), half(wslot(2, m), m, hx), wfwd.at[m], wr.at[2, m], tp=peer)

    def x_send(r, m):
        return rcopy(half(wslot(r, m), m, hx), half(wslot(r, m), m, hx), wxs.at[r - 1, m], wx.at[r - 1, m], dp=1 - hx)

    def w_ready(rs, ms):
        def pushed(m):
            if 0 in rs:
                o_send(m).wait_recv()
            if 1 in rs:
                p_send(m).wait_recv()
        for m in ms:
            if m in PM:
                pl.when(s == 1)(functools.partial(pushed, m))
            if 0 in rs:
                o_send(4 + m).wait_recv()
            for r in (1, 2):
                if r in rs:
                    x_send(r, m).wait_recv()

    PM = (2, 3)

    def pb(r, m):
        return pv_hbm.at[r] if m == 2 else po_hbm.at[pl.ds(r * QL, QL)]

    def hh(i):
        return hx if i == 0 else 1 - hx

    def y_send(i, m):
        return rcopy(half(own_w(m), m, hh(i)), half(pb(3, m), m, hh(i)), ysn.at[2 * i + m - 2], yrc.at[2 * i + m - 2], pp=3)

    def po_send(i, m):
        return rcopy(half(pb(3, m), m, hh(i)), half(pb(0, m), m, hh(i)), pos.at[2 * i + m - 2], por.at[2 * i + m - 2], tp=inner)

    def pp_send(m):
        return rcopy(half(pb(3, m), m, hx), half(pb(1, m), m, hx), pps.at[m - 2], ppr.at[m - 2], tp=peer)

    def pf_send(m):
        return rcopy(half(pb(0, m), m, hx), half(pb(2, m), m, hx), pfs.at[m - 2], pfr.at[m - 2], tp=peer)

    def pxf_send(r, m):
        return rcopy(half(pb(r, m), m, hx), half(pb(r, m), m, hx), pxfs.at[r - 1, m - 2], pxfr.at[r - 1, m - 2], dp=1 - hx)

    def push(r, m, i):
        rsem = wr.at[0, 4 * i + m] if r == 0 else (wr.at[r, m] if i == 0 else wx.at[r - 1, m])
        return rcopy(half(pb(r, m), m, hh(i)), half(wslot(r, m), m, hh(i)), pds.at[r, m - 2, i], rsem, pp=1)

    def direct(m, f):
        if m in PM:
            pl.when(s != 1)(f)
        else:
            f()

    @pl.when(s == 1)
    def _():
        for m in PM:
            y_send(0, m).start()

        @pl.when(is_outer)
        def _():
            for m in PM:
                y_send(1, m).start()

    @pl.when((s == 3) & is_outer)
    def _():
        for i in (0, 1):
            for m in PM:
                y_send(i, m).wait_recv()
                po_send(i, m).start()
        for i in (0, 1):
            for m in PM:
                po_send(i, m).wait_send()

    @pl.when((s == 3) & is_home)
    def _():
        for m in PM:
            y_send(0, m).wait_recv()
            pp_send(m).start()
        for kind, m, a in (("p", 2, 0), ("o", 2, 0), ("p", 3, 0), ("o", 3, 0), ("f", 2, 0), ("f", 3, 0), ("o", 2, 1), ("x", 2, 1),
                           ("o", 3, 1), ("x", 3, 1)):
            with jax.named_scope('wp_' + kind + str(m) + str(a)):
                if kind == "p":
                    pp_send(m).wait_recv()
                    pxf_send(1, m).start()
                    push(1, m, 0).start()
                elif kind == "o":
                    po_send(a, m).wait_recv()
                    if a == 0:
                        pf_send(m).start()
                    push(0, m, a).start()
                elif kind == "f":
                    pf_send(m).wait_recv()
                    push(2, m, 0).start()
                else:
                    pxf_send(a, m).wait_recv()
                    push(a, m, 1).start()

    @pl.when(s == 3)
    def _():
        pl.semaphore_signal(gate, inc=1, device_id={"pp": 2}, device_id_type=MESH)

    def release():
        @pl.when(odd == 0)
        def _():
            pl.semaphore_signal(gate, inc=1, device_id={"pp": s + 1}, device_id_type=MESH)

    @pl.when(s != 0)
    def _():
        for c in mlp_copies():
            c.start()
        with jax.named_scope('w_gate'):
            pl.semaphore_wait(gate, 1)

    if NW > 1:
        x_each(1, lambda c: c.start())

    @pl.when(is_outer)
    def _():
        for k in range(8):
            direct(k % 4, lambda k=k: o_send(k).start())

        @pl.when(s == 0)
        def _():
            for c in mlp_copies():
                c.start()
        for k in range(8):
            direct(k % 4, lambda k=k: o_send(k).wait_send())
        release()
        for w in range(2, NW):
            x_each(w, lambda c: c.start())

    @pl.when(is_home)
    def _():
        for m in range(4):
            direct(m, lambda m=m: p_send(m).start())
        wo_own().start()

        @pl.when(s == 0)
        def _():
            for c in mlp_copies():
                c.start()
        def zero_rows(b, carry):
            for i in range(4):
                kc[i, pl.ds(b * RB, RB), :] = jnp.zeros((RB, QL), BF16)
                vc[i, pl.ds(b * RB, RB), :] = jnp.zeros((RB, QL), BF16)
            return carry
        lax.fori_loop(0, S // RB, zero_rows, 0)

        def tables(w):
            lane = lax.broadcasted_iota(jnp.int32, (T, HEAD_DIM), 1)

            def table_rows(b, carry):
                rows = pl.ds(pl.multiple_of(b * T, T), T)
                ang = column(pos_ref, 2 * w + hb, b).astype(F32) * invf_ref[0:1, :]
                table[w, rows, :] = jnp.where(lane < HEAD_DIM // 2, jnp.cos(ang), jnp.sin(ang))
                return carry
            with jax.named_scope('table'):
                lax.fori_loop(0, NJ, table_rows, 0)

        steps = [("o", 0), ("p", 0), ("t", 0), ("o", 1), ("p", 1), ("t", 1), ("o", 2), ("p", 2), ("t", 2), ("o", 3), ("p", 3), ("t", 3),
                 ("r", 0), ("f", 0), ("f", 1), ("f", 2), ("f", 3), ("g", 0)]

        def step(kind, m):
            if kind == "o":
                o_send(m).wait_recv()
                f_send(m).start()
            elif kind == "p":
                p_send(m).wait_recv()
                x_send(1, m).start()
            else:
                f_send(m).wait_recv()
                x_send(2, m).start()

        for kind, m in steps:
            with jax.named_scope('w_' + kind + str(m)):
                if kind in "op":
                    direct(m, lambda kind=kind, m=m: step(kind, m))
                elif kind == "f":
                    step(kind, m)
                elif kind == "g":
                    release()
                elif kind == "r":
                    x_relay([1] if NW > 1 else [])
                elif m < n_mb // 2:
                    tables(m)
        for w in range(2, NW):
            x_each(w, lambda c: c.start())
        w_ready([0, 1], range(3))
        x_relay(range(2, NW))

    def gslot(g, u):
        return lax.rem(g - 1 + u, 2)

    def group_copies(g, u):
        if g == 0:
            return [local(own_w(m), wres.at[m], wres_sem.at[m]) for m in range(3)]
        p = gslot(g, u)
        if g < 4:
            return [local(wqkv_hbm.at[g - 1], wst.at[p], wst_sem.at[p, 0])]
        return [local(wo_hbm.at[:, pl.ds(((g - 4) * 3 + m) * OB, OB)], wst.at[p, m], wst_sem.at[p, m]) for m in range(3 if g == 4 else 1)]

    def group_start(g, u):
        for c in group_copies(g, u):
            c.start()

    def group_wait(g, u):
        for c in group_copies(g, u):
            c.wait()

    def h_fetch(u):
        mb = 2 * (u // NJ) + hb
        here = lax.rem(u, NJ) == z
        dst = hin.at[lax.rem(u, HS)]

        @pl.when((s == 0) & here)
        def _():
            local(x_ref.at[mb], dst, hv_sem).start()

        @pl.when((s == 0) & jnp.logical_not(here))
        def _():
            local(hin_hbm.at[u], hin_hbm.at[u], hin_sem.at[u]).wait()
            local(hin_hbm.at[u], dst, hv_sem).start()

    @pl.when(is_home)
    def _():
        group_start(0, 0)
        group_start(1, 0)
        group_start(2, 0)
        h_fetch(0)

    for c in mlp_copies():
        c.wait()

    def hin_copy(u):
        return rcopy(h2b, hin.at[lax.rem(u, HS)], s5s, hin_sem.at[u], pp=lax.rem(s + 1, n_stages))

    def s1_outer(u):
        blk = gb.at[lax.rem(u, 3), pl.ds(pl.multiple_of(hb * T, T), T), :]
        return rcopy(blk, blk, s1s.at[0], ag.at[hb, lax.rem(u, 3)], tp=outer)

    def s1_peer(u):
        blk = gb.at[lax.rem(u, 3), pl.ds(pl.multiple_of(hb * T, T), T), :]
        return rcopy(blk, blk, s1s.at[1], ag.at[hb, lax.rem(u, 3)], tp=peer)

    def s2_copy(u):
        blk = gb.at[lax.rem(u, 3), pl.ds(pl.multiple_of((1 - hb) * T, T), T), :]
        return rcopy(blk, blk, s2s, ag.at[1 - hb, lax.rem(u, 3)], tp=outer)

    def ag_wait(b, u):
        blk = gb.at[lax.rem(u, 3), pl.ds(pl.multiple_of(b * T, T), T), :]
        local(blk, blk, ag.at[b, lax.rem(u, 3)]).wait()

    def s3_copy(u, b):
        sl = lax.rem(u, 2)
        blk = px.at[sl, pl.ds(pl.multiple_of(b * T, T), T), :]
        return rcopy(blk, blk, pxs.at[sl, b], pxr.at[sl, b], tp=inner)

    def s4_copy(u):
        return rcopy(sendb, ps.at[lax.rem(u, 2)], s4s, psr.at[lax.rem(u, 2)], tp=peer)

    def park_copy(u):
        return rcopy(h2b, hin_hbm.at[u], s5s, op.at[u], pp=1)

    def last_copy():
        mb = n_mb - 2 + hb
        return rcopy(h2b, out_ref.at[mb], s6s, outr.at[mb], tp=NJ - 1)

    def norm_rows(src, gain, dst):
        hf = src.astype(F32)
        inv = lax.rsqrt(jnp.mean(hf * hf, axis=-1, keepdims=True) + NORM_EPS)
        return (hf * inv * gain.astype(F32)).astype(BF16)

    def attention(u):
      with jax.named_scope('attn'):
        attention_(u)

    def attention_(u):
        w = u // NJ
        j = lax.rem(u, NJ)
        mb = 2 * w + hb
        row0 = pl.multiple_of(j * T, T)
        hs = lax.rem(u, HS)

        with jax.named_scope('w_hin'):
            @pl.when(s == 0)
            def _():
                local(x_ref.at[mb], hin.at[hs], hv_sem).wait()

            @pl.when(s > 0)
            def _():
                hin_copy(u).wait_recv()

        def norm_a(b, carry):
            rows = pl.ds(b * NR, NR)
            abuf[rows, :] = norm_rows(hin[hs, rows, :], ga_ref[0:1, :], None)
            return carry
        lax.fori_loop(0, T // NR, norm_a, 0)

        segrow = seg_ref[pl.ds(mb, 1), :]
        segc = column(seg_ref, mb, j)
        ti = lax.broadcasted_iota(jnp.int32, (T, HEAD_DIM), 0) + row0
        for c in range(0, S, HEAD_DIM):
            segr = segrow[:, c:c + HEAD_DIM]
            ui = lax.broadcasted_iota(jnp.int32, (T, HEAD_DIM), 1) + c
            mask[:, c:c + HEAD_DIM] = jnp.where((segc == segr) & (ui <= ti), 1.0, 0.0)

        def rope(val):
            pk = table[w, pl.ds(row0, T), :]
            lane = lax.broadcasted_iota(jnp.int32, (T, HEAD_DIM), 1)
            swapped = pltpu.roll(pk, HEAD_DIM // 2, 1)
            cosw = jnp.where(lane < HEAD_DIM // 2, pk, swapped)
            sinw = jnp.where(lane < HEAD_DIM // 2, -swapped, pk)
            outs = []
            for h in range(NH):
                v = val[:, h * HEAD_DIM:(h + 1) * HEAD_DIM]
                outs.append((v * cosw + pltpu.roll(v, HEAD_DIM // 2, 1) * sinw).astype(BF16))
            return outs

        def hcols(h):
            return slice(h * HEAD_DIM, (h + 1) * HEAD_DIM)

        def proj(i):
            p = i % 2

            def w(m):
                return wres[m] if i == 0 else wst[gslot(i, u), m]
            for h, val in enumerate(rope(jnp.dot(abuf[...], w(0), preferred_element_type=F32))):
                qb[p, :, hcols(h)] = val
            for h, val in enumerate(rope(jnp.dot(abuf[...], w(1), preferred_element_type=F32))):
                kc[i, pl.ds(row0, T), hcols(h)] = val
            vc[i, pl.ds(row0, T), :] = jnp.dot(abuf[...], w(2), preferred_element_type=F32).astype(BF16)

        def heads(i):
            for h in range(NH):
                sc = lax.dot_general(qb[i % 2, :, hcols(h)], kc[i, :, hcols(h)], (((1,), (1,)), ((), ())),
                                     preferred_element_type=F32) * scale
                pacc[0:T, h * S:(h + 1) * S] = jnp.where(mask[...] > 0.5, sc, NEG)
            for h in range(NH):
                for r in range(0, T, 32):
                    sc = pacc[r:r + 32, h * S:(h + 1) * S]
                    e = jnp.exp(sc - jnp.max(sc, axis=-1, keepdims=True))
                    pbuf[h, r:r + 32, :] = (e * (1.0 / jnp.sum(e, axis=-1, keepdims=True))).astype(BF16)
            for h in range(NH):
                act[0:T, i * QL + h * HEAD_DIM:i * QL + (h + 1) * HEAD_DIM] = jnp.dot(
                    pbuf[h], vc[i, :, hcols(h)], preferred_element_type=F32).astype(BF16)

        with jax.named_scope('shards'):
            @pl.when(u == 0)
            def _():
                group_wait(0, u)
            proj(0)
            for i in range(3):
                group_wait(i + 1, u)
                proj(i + 1)
                if i < 2:
                    @pl.when(u == 0)
                    def _():
                        if i == 0:
                            w_ready([2], range(3))
                        else:
                            w_ready([0, 1, 2], [3])
                            wo_own().wait()
                group_start(i + 3, u)
                heads(i)
                if i == 0:
                    @pl.when(u < N - 1)
                    def _():
                        h_fetch(u + 1)
            heads(3)

        with jax.named_scope('wo'):
            def wo_block(n, w):
                act[T:2 * T, n * OB:(n + 1) * OB] = jnp.dot(act[0:T, 0:4 * QL], w, preferred_element_type=F32).astype(BF16)

            group_wait(4, u)
            group_wait(5, u)
            for n in range(3):
                wo_block(n, wst[gslot(4, u), n])

            wo_block(3, wst[gslot(5, u), 0])

            @pl.when(u < N - 1)
            def _():
                group_start(1, u + 1)
                group_start(2, u + 1)

        def norm_b(b, carry):
            rows = pl.ds(b * NR, NR)
            h1 = (hin[hs, rows, :].astype(F32) + act[pl.ds(pl.multiple_of(T + b * NR, NR), NR), 0:D].astype(F32)).astype(BF16)
            h1b[lax.rem(u, 3), rows, :] = h1
            gb[lax.rem(u, 3), pl.ds(pl.multiple_of(hb * T + b * NR, NR), NR), :] = norm_rows(h1, gm_ref[0:1, :], None)
            return carry
        lax.fori_loop(0, T // NR, norm_b, 0)

        @pl.when((s > 0) & (u < N - HS))
        def _():
            pl.semaphore_signal(cred, inc=1, device_id={"pp": s - 1}, device_id_type=MESH)

    def mlp(sl, row0, rows, store):
        UN = 2 if NB % 2 == 0 else 1

        def up(q, carry):
            for n in [q * UN + k for k in range(UN)]:
                xin = gb[sl, pl.ds(row0, rows), :]
                g = jnp.dot(xin, wg_s[n], preferred_element_type=F32)
                u_ = jnp.dot(xin, wu_s[n], preferred_element_type=F32)
                act[0:rows, pl.ds(pl.multiple_of(n * FB, FB), FB)] = (jax.nn.silu(g) * u_).astype(BF16)
            return carry
        lax.fori_loop(0, NB // UN, up, 0)

        def down(q, carry):
            for n in [q * UN + k for k in range(UN)]:
                store(pl.ds(pl.multiple_of(n * DB, DB), DB), jnp.dot(act[0:rows, 0:FL], wd_s[n], preferred_element_type=F32))
            return carry
        lax.fori_loop(0, NB // UN, down, 0)

    def mlp_home(u):
        def store(c, val):
            pacc[:, c] = val
        with jax.named_scope('mlp'):
            mlp(lax.rem(u, 3), 0, 2 * T, store)

    def mlp_outer(u, b):
        def store(c, val):
            px[lax.rem(u, 2), pl.ds(pl.multiple_of(b * T, T), T), c] = val.astype(BF16)
        with jax.named_scope('mlp_o'):
            mlp(lax.rem(u, 3), pl.multiple_of(b * T, T), T, store)

    def forward(u):
        @pl.when((u >= 1) & (u <= N))
        def _():
            s2_copy(u - 1).wait_send()

        @pl.when(u < N)
        def _():
            with jax.named_scope('w_ag'):
                ag_wait(1 - hb, u)
            s2_copy(u).start()

    def combine(v):
        sl = lax.rem(v, 2)
        with jax.named_scope('w_s3'):
            s3_copy(v, 0).wait_recv()
            s3_copy(v, 1).wait_recv()

        @pl.when(v >= 1)
        def _():
            s4_copy(v - 1).wait_send()

        def comb(b, carry):
            rows = pl.ds(b * RB, RB)
            mine = pl.ds(pl.multiple_of(hb * T + b * RB, RB), RB)
            theirs = pl.ds(pl.multiple_of((1 - hb) * T + b * RB, RB), RB)
            oacc[rows, :] = pacc[mine, :] + px[sl, mine, :].astype(F32)
            sendb[rows, :] = (pacc[theirs, :] + px[sl, theirs, :].astype(F32)).astype(BF16)
            return carry
        lax.fori_loop(0, T // RB, comb, 0)
        s4_copy(v).start()

    def finish(u):
        @pl.when((u >= 2) & (u < N + 2))
        def _():
            v = u - 2
            with jax.named_scope('w_s4'):
                s4_copy(v).wait_recv()
            vw = v // NJ
            vj = lax.rem(v, NJ)

            @pl.when(v >= 1)
            def _():
                hin_copy(v).wait_send()

            def fin(b, carry):
                rows = pl.ds(b * RB, RB)
                d = (oacc[rows, :] + ps[lax.rem(v, 2), rows, :].astype(F32)).astype(BF16)
                h2b[rows, :] = (h1b[lax.rem(v, 3), rows, :].astype(F32) + d.astype(F32)).astype(BF16)
                return carry
            lax.fori_loop(0, T // RB, fin, 0)

            @pl.when((s < n_stages - 1) & (v >= HS))
            def _():
                with jax.named_scope('w_cred'):
                    pl.semaphore_wait(cred, 1)

            @pl.when(s < n_stages - 1)
            def _():
                hin_copy(v).start()

            @pl.when(s == n_stages - 1)
            def _():
                park_copy(v).start()

            @pl.when((s == n_stages - 1) & (v == N - 1))
            def _():
                last_copy().start()

    def body(u, carry):
        @pl.when(is_home)
        def _():
            @pl.when(u < N)
            def _():
                attention(u)

            @pl.when((u >= 1) & (u <= N))
            def _():
                s1_outer(u - 1).wait_send()
                s1_peer(u - 1).wait_send()

            @pl.when(u < N)
            def _():
                s1_peer(u).start()
                s1_outer(u).start()

            finish(u)

            @pl.when((u >= 1) & (u <= N))
            def _():
                mlp_home(u - 1)

            forward(u)

            @pl.when((u >= 1) & (u <= N))
            def _():
                combine(u - 1)

        @pl.when(is_outer & (u < N))
        def _():
            for k in (0, 1):
                b = inner - 1 if k == 0 else 2 - inner
                with jax.named_scope('w_ag_outer'):
                    ag_wait(b, u)

                @pl.when(u >= 2)
                def _():
                    s3_copy(u - 2, b).wait_send()
                mlp_outer(u, b)
                s3_copy(u, b).start()

        return carry

    def out_fwd(mb, p, sem):
        return rcopy(out_ref.at[mb], out_ref.at[mb], ofs.at[mb, p], sem, pp=p)

    lax.fori_loop(0, N + 2, body, 0)

    last_here = (s == n_stages - 1) & (z == NJ - 1)

    @pl.when(last_here)
    def _():
        for mb in (n_mb - 2, n_mb - 1):
            local(out_ref.at[mb], out_ref.at[mb], outr.at[mb]).wait()
            out_fwd(mb, 2, outf).start()

    def od_copy(v):
        return rcopy(hin_hbm.at[v], out_ref.at[2 * (v // NJ) + hb], od.at[v], outr.at[2 * (v // NJ) + hb], tp=lax.rem(v, NJ))

    @pl.when(s == 1)
    def _():
        def spread(v, carry):
            vj = lax.rem(v, NJ)
            mine = 2 * (v // NJ) + hb

            @pl.when(is_home)
            def _():
                local(hin_hbm.at[v], hin_hbm.at[v], op.at[v]).wait()

            @pl.when(is_home & (vj != z))
            def _():
                od_copy(v).start()

            @pl.when(is_home & (vj == z))
            def _():
                c = local(hin_hbm.at[v], hin.at[0], hv_sem)
                c.start()
                c.wait()
                c = local(hin.at[0], out_ref.at[mine], hv_sem)
                c.start()
                c.wait()

            @pl.when(vj == z)
            def _():
                for b in (0, 1):
                    mb = 2 * (v // NJ) + b

                    @pl.when(z - 1 != b)
                    def _(mb=mb):
                        local(out_ref.at[mb], out_ref.at[mb], outr.at[mb]).wait()
                    out_fwd(mb, 0, outf).start()

                    @pl.when(v < N - 1)
                    def _(mb=mb):
                        out_fwd(mb, 3, outf).start()
                        out_fwd(mb, 2, outf).start()
            return carry
        lax.fori_loop(0, N, spread, 0)

    @pl.when(is_home)
    def _():
        s4_copy(N - 1).wait_send()
        hin_copy(N - 1).wait_send()

        @pl.when(s == n_stages - 1)
        def _():
            last_copy().wait_send()

    @pl.when(is_outer)
    def _():
        for b in (0, 1):
            s3_copy(N - 2, b).wait_send()
            s3_copy(N - 1, b).wait_send()

    @pl.when(s == 1)
    def _():
        for m in PM:
            y_send(0, m).wait_send()

        @pl.when(is_outer)
        def _():
            for m in PM:
                y_send(1, m).wait_send()

    @pl.when((s == 3) & is_home)
    def _():
        for m in PM:
            pp_send(m).wait_send()
            pf_send(m).wait_send()
            pxf_send(1, m).wait_send()
            for r, i in ((0, 0), (0, 1), (1, 0), (1, 1), (2, 0)):
                push(r, m, i).wait_send()

    @pl.when(is_home)
    def _():
        def sent(m):
            p_send(m).wait_send()
            f_send(m).wait_send()
            x_send(1, m).wait_send()
        for m in range(4):
            direct(m, functools.partial(sent, m))
            x_send(2, m).wait_send()

        @pl.when(s == 2)
        def _():
            for w in range(NW):
                for j in range(NJ):
                    @pl.when(z != j)
                    def _():
                        x_pass(w, j).wait_send()

        @pl.when(s == 1)
        def _():
            def spread_done(v, carry):
                @pl.when(lax.rem(v, NJ) != z)
                def _():
                    od_copy(v).wait_send()
                return carry
            lax.fori_loop(0, N, spread_done, 0)

    for w in range(NW):
        x_each(w, lambda c: c.wait_send())

    @pl.when(s == 1)
    def _():
        for mb in range(n_mb):
            out_fwd(mb, 0, outf).wait_send()
            if mb < n_mb - 2:
                out_fwd(mb, 3, outf).wait_send()
                out_fwd(mb, 2, outf).wait_send()
            else:
                @pl.when(z < NJ - 1)
                def _(mb=mb):
                    out_fwd(mb, 3, outf).wait_send()
                    out_fwd(mb, 2, outf).wait_send()

    @pl.when(last_here)
    def _():
        for mb in (n_mb - 2, n_mb - 1):
            out_fwd(mb, 2, outf).wait_send()
        early = out_ref.at[pl.ds(0, n_mb - 2)]
        local(early, early, outf).wait()

    @pl.when((s == n_stages - 1) & (z < NJ - 1))
    def _():
        local(out_ref, out_ref, outf).wait()

    @pl.when((s == 0) | (s == 2))
    def _():
        local(out_ref, out_ref, outf).wait()


def solution(mesh):
    n_stages = mesh.shape['pp']

    def stage_program(hidden_in, seg_ids, positions, attn_norm, w_query, w_key, w_value, w_out, mlp_norm, w_gate, w_up, w_down):
        n_mb, T, D = hidden_in.shape
        S = seg_ids.shape[1]
        QL = w_query.shape[2]
        FL = w_gate.shape[2]
        NJ = S // T
        N = (n_mb // 2) * NJ
        NB = max(1, FL // 512)
        invf = jnp.asarray(np.tile(rope_freqs(), 2)[None, :], F32)
        any_spec = pl.BlockSpec(memory_space=pl.ANY)
        vmem = pl.BlockSpec(memory_space=pltpu.VMEM)
        dma = pltpu.SemaphoreType.DMA
        scratch = [
            pltpu.VMEM((NB, D, FL // NB), BF16), pltpu.VMEM((NB, D, FL // NB), BF16), pltpu.VMEM((NB, FL, D // NB), BF16),
            pltpu.VMEM((3, D, QL), BF16), pltpu.VMEM((2, 3, D, QL), BF16),
            pltpu.VMEM((3, 2 * T, D), BF16),
            pltpu.VMEM((2, 2 * T, D), BF16),
            pltpu.VMEM((2, T, D), BF16),
            pltpu.VMEM((4, S, QL), BF16), pltpu.VMEM((4, S, QL), BF16),
            pltpu.VMEM((4, T, D), BF16),
            pltpu.VMEM((3, T, D), BF16),
            pltpu.VMEM((2 * T, D), F32),
            pltpu.VMEM((T, D), F32),
            pltpu.VMEM((T, D), BF16),
            pltpu.VMEM((T, D), BF16),
            pltpu.VMEM((2 * T, max(D, FL, 4 * QL)), BF16),
            pltpu.VMEM((T, D), BF16),
            pltpu.VMEM((2, T, QL), BF16),
            pltpu.VMEM((n_mb // 2, S, HEAD_DIM), F32),
            pltpu.VMEM((T, S), F32), pltpu.VMEM((QL // HEAD_DIM, T, S), BF16),
            dma((3, 8)), dma((2, 4)), dma((8,)), dma((4,)), dma((2, 4)),
            dma((N,)), dma((n_mb // 2, 2)), dma((2, 3)), dma((2,)), dma, dma((2, 2)), dma((2, 2)), dma((2,)), dma, dma,
            dma((n_mb,)), dma, dma((n_mb, n_stages)),
            dma((3,)), dma((2, 3)), dma, dma((3, NB)), dma, dma, dma((N,)), dma((n_mb // 2, NJ)), dma((N,)), dma((N,)),
            dma((4,)), dma((4,)), dma((4,)), dma((4,)), dma((2,)), dma((2,)), dma((2,)), dma((2,)), dma((2, 2)), dma((2, 2)), dma((3, 2, 2)),
            pltpu.SemaphoreType.REGULAR, pltpu.SemaphoreType.REGULAR,
        ]
        return pl.pallas_call(
            functools.partial(kernel, n_stages),
            out_shape=[jax.ShapeDtypeStruct(hidden_in.shape, BF16), jax.ShapeDtypeStruct((3, 3, D, QL), BF16),
                       jax.ShapeDtypeStruct((4 * QL, D), BF16), jax.ShapeDtypeStruct((N, T, D), BF16),
                       jax.ShapeDtypeStruct((4, D, QL), BF16), jax.ShapeDtypeStruct((4 * QL, D), BF16)],
            in_specs=[any_spec, vmem, vmem, vmem, vmem, vmem] + [any_spec] * 7,
            out_specs=[any_spec] * 6,
            scratch_shapes=scratch,
            compiler_params=pltpu.CompilerParams(collective_id=0, has_side_effects=True, vmem_limit_bytes=67_043_328),
        )(hidden_in, seg_ids, positions, invf, attn_norm, mlp_norm, w_query, w_key, w_value, w_out, w_gate, w_up, w_down)[0]

    act_spec = P('dp', 'tp', None)
    row_spec = P('dp', None)
    gain_spec = P('pp', None)
    col_spec = P('pp', None, 'tp')
    rows_spec = P('pp', 'tp', None)
    return jax.shard_map(stage_program, mesh=mesh,
                         in_specs=(act_spec, row_spec, row_spec, gain_spec, col_spec, col_spec, col_spec, rows_spec, gain_spec, col_spec, col_spec, rows_spec),
                         out_specs=act_spec, check_vma=False)
```

```python
import functools
import math

import jax
import jax.numpy as jnp
import numpy as np
from jax import lax
from jax.experimental import pallas as pl
from jax.experimental.pallas import tpu as pltpu
from jax.sharding import PartitionSpec as P

HEAD_DIM = 128
NORM_EPS = 1e-5
ROPE_THETA = 500000.0
ROPE_FACTOR = 8.0
LOW_FREQ = 1.0
HIGH_FREQ = 4.0
ORIG_CTX = 8192.0
NEG = -1e30
MESH = pl.DeviceIdType.MESH
F32 = jnp.float32
BF16 = jnp.bfloat16


def rope_freqs():
    base_freq = 1.0 / (ROPE_THETA ** (np.arange(0, HEAD_DIM, 2) / HEAD_DIM))
    wavelen = 2.0 * np.pi / base_freq
    smooth = (ORIG_CTX / wavelen - LOW_FREQ) / (HIGH_FREQ - LOW_FREQ)
    blended = (1.0 - smooth) * base_freq / ROPE_FACTOR + smooth * base_freq
    scaled = np.where(wavelen > ORIG_CTX / LOW_FREQ, base_freq / ROPE_FACTOR, blended)
    return np.where(wavelen < ORIG_CTX / HIGH_FREQ, base_freq, scaled)


def kernel(n_stages, x_ref, seg_ref, pos_ref, invf_ref, ga_ref, gm_ref,
           wq_ref, wk_ref, wv_ref, wo_ref, wg_ref, wu_ref, wd_ref,
           out_ref,
           wqkv_hbm, wo_hbm, hin_hbm, pv_hbm, po_hbm,
           wg_s, wu_s, wd_s, wres, wst, gb, px, ps, kc, vc, hin, h1b, pacc, oacc, sendb, h2b, act, qb,
           table, mask, sbuf, pbuf,
           wr, wx, wsnd, wfwd, wxs, hin_sem, xs, ag, s1s, s2s, pxr, pxs, psr, s4s, s5s, outr, outf, ofs,
           wres_sem, wst_sem, wo_sem, mlp_sem, hv_sem, s6s, xp, xq, op, od,
           ysn, yrc, pos, por, pps, ppr, pfs, pfr, pxfs, pxfr, pds, gate, cred):
    n_mb, T, D = x_ref.shape
    QL = wq_ref.shape[2]
    FL = wg_ref.shape[2]
    NB = wg_s.shape[0]
    FB = FL // NB
    S = seg_ref.shape[1]
    NJ = S // T
    NH = QL // HEAD_DIM
    N = (n_mb // 2) * NJ
    DB = D // NB
    scale = HEAD_DIM ** -0.5
    RB = 16
    NR = 32
    HS = hin.shape[0]
    OB = wst.shape[3]
    NO = D // OB

    hx = lax.axis_index("dp")
    z = lax.axis_index("tp")
    s = lax.axis_index("pp")
    is_home = (z == 1) | (z == 2)
    is_outer = (z == 0) | (z == 3)
    hb = lax.rem(z + 1, 2) * 0 + (z - 1)
    peer = 3 - z
    outer = 3 * (z - 1)
    inner = 1 + z // 2
    odd = lax.rem(s, 2)

    def rcopy(src, dst, ssem, rsem, **dev):
        return pltpu.make_async_remote_copy(src_ref=src, dst_ref=dst, send_sem=ssem, recv_sem=rsem,
                                            device_id=dev, device_id_type=MESH)

    def local(src, dst, sem):
        return pltpu.make_async_copy(src, dst, sem)

    def column(ref, mb, j):
        row = ref[pl.ds(mb, 1), :]
        part = row[:, 0:T]
        for c in range(1, NJ):
            part = jnp.where(j == c, row[:, c * T:(c + 1) * T], part)
        return jnp.broadcast_to(part, (HEAD_DIM, T)).T

    barrier = pltpu.get_barrier_semaphore()
    for k in range(1, 4):
        pl.semaphore_signal(barrier, inc=1, device_id={"tp": lax.rem(z + k, 4)}, device_id_type=MESH)
        pl.semaphore_signal(barrier, inc=1, device_id={"pp": lax.rem(s + k, 4)}, device_id_type=MESH)
    pl.semaphore_signal(barrier, inc=1, device_id={"dp": 1 - hx}, device_id_type=MESH)
    pl.semaphore_wait(barrier, 7)

    wqkv_own = (wq_ref, wk_ref, wv_ref, wo_ref)

    def mlp_copies():
        cps = []
        for n in range(NB):
            cps.append(local(wg_ref.at[0, :, pl.ds(n * FB, FB)], wg_s.at[n], mlp_sem.at[0, n]))
            cps.append(local(wu_ref.at[0, :, pl.ds(n * FB, FB)], wu_s.at[n], mlp_sem.at[1, n]))
            cps.append(local(wd_ref.at[0, :, pl.ds(n * DB, DB)], wd_s.at[n], mlp_sem.at[2, n]))
        return cps

    NW = n_mb // 2

    def x_copy(w, home):
        u = w * NJ + z
        return rcopy(x_ref.at[2 * w + (home - 1)], hin_hbm.at[u], xs.at[w, home - 1], xp.at[u], tp=home)

    def x_each(w, act):
        for home in (1, 2):
            @pl.when((s == 2) & (z != home))
            def _():
                act(x_copy(w, home))

    def x_pass(w, j):
        u = w * NJ + j
        return rcopy(hin_hbm.at[u], hin_hbm.at[u], xq.at[w, j], hin_sem.at[u], pp=0)

    def x_relay(ws):
        @pl.when((s == 2) & is_home)
        def _():
            for w in ws:
                for j in range(NJ):
                    @pl.when(z != j)
                    def _():
                        local(hin_hbm.at[w * NJ + j], hin_hbm.at[w * NJ + j], xp.at[w * NJ + j]).wait()
                        x_pass(w, j).start()

    x_each(0, lambda c: c.start())
    x_relay([0])

    def half(ref, m, h):
        rows = (D if m < 3 else QL) // 2
        return ref.at[pl.ds(h * rows, rows), :]

    def wslot(r, m):
        return wqkv_hbm.at[r, m] if m < 3 else wo_hbm.at[pl.ds((r + 1) * QL, QL)]

    def own_w(m):
        return wqkv_own[m].at[0]

    def wo_own():
        return local(own_w(3), wo_hbm.at[pl.ds(0, QL)], wo_sem)

    def o_send(k):
        h = hx if k < 4 else 1 - hx
        return rcopy(half(own_w(k % 4), k % 4, h), half(wslot(0, k % 4), k % 4, h), wsnd.at[k], wr.at[0, k], tp=inner)

    def p_send(m):
        return rcopy(half(own_w(m), m, hx), half(wslot(1, m), m, hx), wsnd.at[m], wr.at[1, m], tp=peer)

    def f_send(m):
        return rcopy(half(wslot(0, m), m, hx), half(wslot(2, m), m, hx), wfwd.at[m], wr.at[2, m], tp=peer)

    def x_send(r, m):
        return rcopy(half(wslot(r, m), m, hx), half(wslot(r, m), m, hx), wxs.at[r - 1, m], wx.at[r - 1, m], dp=1 - hx)

    def w_ready(rs, ms):
        def pushed(m):
            if 0 in rs:
                o_send(m).wait_recv()
            if 1 in rs:
                p_send(m).wait_recv()
            if 2 in rs:
                f_send(m).wait_recv()
        for m in ms:
            if m in PM:
                pl.when(s == 1)(functools.partial(pushed, m))
            if 0 in rs:
                o_send(4 + m).wait_recv()
            for r in (1, 2):
                if r in rs:
                    x_send(r, m).wait_recv()

    PM = (2, 3)

    def pb(r, m):
        return pv_hbm.at[r] if m == 2 else po_hbm.at[pl.ds(r * QL, QL)]

    def hh(i):
        return hx if i == 0 else 1 - hx

    def y_send(i, m):
        return rcopy(half(own_w(m), m, hh(i)), half(pb(3, m), m, hh(i)), ysn.at[2 * i + m - 2], yrc.at[2 * i + m - 2], pp=3)

    def po_send(i, m):
        return rcopy(half(pb(3, m), m, hh(i)), half(pb(0, m), m, hh(i)), pos.at[2 * i + m - 2], por.at[2 * i + m - 2], tp=inner)

    def pp_send(m):
        return rcopy(half(pb(3, m), m, hx), half(pb(1, m), m, hx), pps.at[m - 2], ppr.at[m - 2], tp=peer)

    def pf_send(m):
        return rcopy(half(pb(0, m), m, hx), half(pb(2, m), m, hx), pfs.at[m - 2], pfr.at[m - 2], tp=peer)

    def pxf_send(r, m):
        return rcopy(half(pb(r, m), m, hx), half(pb(r, m), m, hx), pxfs.at[r - 1, m - 2], pxfr.at[r - 1, m - 2], dp=1 - hx)

    def push(r, m, i):
        rsem = wr.at[0, 4 * i + m] if r == 0 else (wr.at[r, m] if i == 0 else wx.at[r - 1, m])
        return rcopy(half(pb(r, m), m, hh(i)), half(wslot(r, m), m, hh(i)), pds.at[r, m - 2, i], rsem, pp=1)

    def direct(m, f):
        if m in PM:
            pl.when(s != 1)(f)
        else:
            f()

    @pl.when(s == 1)
    def _():
        for m in PM:
            y_send(0, m).start()

        @pl.when(is_outer)
        def _():
            for m in PM:
                y_send(1, m).start()

    @pl.when((s == 3) & is_outer)
    def _():
        for i in (0, 1):
            for m in PM:
                y_send(i, m).wait_recv()
                po_send(i, m).start()
        for i in (0, 1):
            for m in PM:
                po_send(i, m).wait_send()

    @pl.when((s == 3) & is_home)
    def _():
        for m in PM:
            y_send(0, m).wait_recv()
            pp_send(m).start()
        for kind, m, a in (("p", 2, 0), ("o", 2, 0), ("p", 3, 0), ("o", 3, 0), ("f", 2, 0), ("o", 2, 1), ("x", 2, 1), ("x", 3, 1),
                           ("f", 3, 0), ("o", 3, 1), ("x", 2, 2), ("x", 3, 2)):
            with jax.named_scope('wp_' + kind + str(m) + str(a)):
                if kind == "p":
                    pp_send(m).wait_recv()
                    pxf_send(1, m).start()
                    push(1, m, 0).start()
                elif kind == "o":
                    po_send(a, m).wait_recv()
                    if a == 0:
                        pf_send(m).start()
                    push(0, m, a).start()
                elif kind == "f":
                    pf_send(m).wait_recv()
                    pxf_send(2, m).start()
                    push(2, m, 0).start()
                else:
                    pxf_send(a, m).wait_recv()
                    push(a, m, 1).start()

    @pl.when(s == 3)
    def _():
        pl.semaphore_signal(gate, inc=1, device_id={"pp": 2}, device_id_type=MESH)

    def release():
        @pl.when(odd == 0)
        def _():
            pl.semaphore_signal(gate, inc=1, device_id={"pp": s + 1}, device_id_type=MESH)

    @pl.when(s != 0)
    def _():
        for c in mlp_copies():
            c.start()
        with jax.named_scope('w_gate'):
            pl.semaphore_wait(gate, 1)

    if NW > 1:
        x_each(1, lambda c: c.start())

    @pl.when(is_outer)
    def _():
        for k in range(8):
            direct(k % 4, lambda k=k: o_send(k).start())

        @pl.when(s == 0)
        def _():
            for c in mlp_copies():
                c.start()
        for k in range(8):
            direct(k % 4, lambda k=k: o_send(k).wait_send())
        release()
        for w in range(2, NW):
            x_each(w, lambda c: c.start())

    @pl.when(is_home)
    def _():
        for m in range(4):
            direct(m, lambda m=m: p_send(m).start())
        wo_own().start()

        @pl.when(s == 0)
        def _():
            for c in mlp_copies():
                c.start()
        def zero_rows(b, carry):
            for i in range(4):
                kc[i, pl.ds(b * RB, RB), :] = jnp.zeros((RB, QL), BF16)
                vc[i, pl.ds(b * RB, RB), :] = jnp.zeros((RB, QL), BF16)
            return carry
        lax.fori_loop(0, S // RB, zero_rows, 0)

        def tables(w):
            lane = lax.broadcasted_iota(jnp.int32, (T, HEAD_DIM), 1)

            def table_rows(b, carry):
                rows = pl.ds(pl.multiple_of(b * T, T), T)
                ang = column(pos_ref, 2 * w + hb, b).astype(F32) * invf_ref[0:1, :]
                table[w, rows, :] = jnp.where(lane < HEAD_DIM // 2, jnp.cos(ang), jnp.sin(ang))
                return carry
            with jax.named_scope('table'):
                lax.fori_loop(0, NJ, table_rows, 0)

        steps = [("o", 0), ("p", 0), ("t", 0), ("o", 1), ("p", 1), ("t", 1), ("o", 2), ("p", 2), ("t", 2), ("o", 3), ("p", 3), ("t", 3),
                 ("r", 0), ("f", 0), ("f", 1), ("f", 2), ("f", 3), ("g", 0)]

        def step(kind, m):
            if kind == "o":
                o_send(m).wait_recv()
                f_send(m).start()
            elif kind == "p":
                p_send(m).wait_recv()
                x_send(1, m).start()
            else:
                f_send(m).wait_recv()
                x_send(2, m).start()

        for kind, m in steps:
            with jax.named_scope('w_' + kind + str(m)):
                if kind in "opf":
                    direct(m, lambda kind=kind, m=m: step(kind, m))
                elif kind == "g":
                    release()
                elif kind == "r":
                    x_relay([1] if NW > 1 else [])
                elif m < n_mb // 2:
                    tables(m)
        for w in range(2, NW):
            x_each(w, lambda c: c.start())
        w_ready([0, 1], range(3))
        x_relay(range(2, NW))

    def gslot(g, u):
        return lax.rem(g - 1 + u, 2)

    def group_copies(g, u):
        if g == 0:
            return [local(own_w(m), wres.at[m], wres_sem.at[m]) for m in range(3)]
        p = gslot(g, u)
        if g < 4:
            return [local(wqkv_hbm.at[g - 1], wst.at[p], wst_sem.at[p, 0])]
        return [local(wo_hbm.at[:, pl.ds(((g - 4) * 3 + m) * OB, OB)], wst.at[p, m], wst_sem.at[p, m]) for m in range(3 if g == 4 else 1)]

    def group_start(g, u):
        for c in group_copies(g, u):
            c.start()

    def group_wait(g, u):
        for c in group_copies(g, u):
            c.wait()

    def h_fetch(u):
        mb = 2 * (u // NJ) + hb
        here = lax.rem(u, NJ) == z
        dst = hin.at[lax.rem(u, HS)]

        @pl.when((s == 0) & here)
        def _():
            local(x_ref.at[mb], dst, hv_sem).start()

        @pl.when((s == 0) & jnp.logical_not(here))
        def _():
            local(hin_hbm.at[u], hin_hbm.at[u], hin_sem.at[u]).wait()
            local(hin_hbm.at[u], dst, hv_sem).start()

    @pl.when(is_home)
    def _():
        group_start(0, 0)
        group_start(1, 0)
        group_start(2, 0)
        h_fetch(0)

    for c in mlp_copies():
        c.wait()

    def hin_copy(u):
        return rcopy(h2b, hin.at[lax.rem(u, HS)], s5s, hin_sem.at[u], pp=lax.rem(s + 1, n_stages))

    def s1_outer(u):
        blk = gb.at[lax.rem(u, 3), pl.ds(pl.multiple_of(hb * T, T), T), :]
        return rcopy(blk, blk, s1s.at[0], ag.at[hb, lax.rem(u, 3)], tp=outer)

    def s1_peer(u):
        blk = gb.at[lax.rem(u, 3), pl.ds(pl.multiple_of(hb * T, T), T), :]
        return rcopy(blk, blk, s1s.at[1], ag.at[hb, lax.rem(u, 3)], tp=peer)

    def s2_copy(u):
        blk = gb.at[lax.rem(u, 3), pl.ds(pl.multiple_of((1 - hb) * T, T), T), :]
        return rcopy(blk, blk, s2s, ag.at[1 - hb, lax.rem(u, 3)], tp=outer)

    def ag_wait(b, u):
        blk = gb.at[lax.rem(u, 3), pl.ds(pl.multiple_of(b * T, T), T), :]
        local(blk, blk, ag.at[b, lax.rem(u, 3)]).wait()

    def s3_copy(u, b):
        sl = lax.rem(u, 2)
        blk = px.at[sl, pl.ds(pl.multiple_of(b * T, T), T), :]
        return rcopy(blk, blk, pxs.at[sl, b], pxr.at[sl, b], tp=inner)

    def s4_copy(u):
        return rcopy(sendb, ps.at[lax.rem(u, 2)], s4s, psr.at[lax.rem(u, 2)], tp=peer)

    def park_copy(u):
        return rcopy(h2b, hin_hbm.at[u], s5s, op.at[u], pp=1)

    def last_copy():
        mb = n_mb - 2 + hb
        return rcopy(h2b, out_ref.at[mb], s6s, outr.at[mb], tp=NJ - 1)

    def norm_rows(src, gain, dst):
        hf = src.astype(F32)
        inv = lax.rsqrt(jnp.mean(hf * hf, axis=-1, keepdims=True) + NORM_EPS)
        return (hf * inv * gain.astype(F32)).astype(BF16)

    def attention(u):
      with jax.named_scope('attn'):
        attention_(u)

    def attention_(u):
        w = u // NJ
        j = lax.rem(u, NJ)
        mb = 2 * w + hb
        row0 = pl.multiple_of(j * T, T)
        hs = lax.rem(u, HS)

        with jax.named_scope('w_hin'):
            @pl.when(s == 0)
            def _():
                local(x_ref.at[mb], hin.at[hs], hv_sem).wait()

            @pl.when(s > 0)
            def _():
                hin_copy(u).wait_recv()

        def norm_a(b, carry):
            rows = pl.ds(b * NR, NR)
            act[pl.ds(pl.multiple_of(T + b * NR, NR), NR), 0:D] = norm_rows(hin[hs, rows, :], ga_ref[0:1, :], None)
            return carry
        lax.fori_loop(0, T // NR, norm_a, 0)

        segrow = seg_ref[pl.ds(mb, 1), :]
        segc = column(seg_ref, mb, j)
        ti = lax.broadcasted_iota(jnp.int32, (T, HEAD_DIM), 0) + row0
        for c in range(0, S, HEAD_DIM):
            segr = segrow[:, c:c + HEAD_DIM]
            ui = lax.broadcasted_iota(jnp.int32, (T, HEAD_DIM), 1) + c
            mask[:, c:c + HEAD_DIM] = jnp.where((segc == segr) & (ui <= ti), 1.0, 0.0)

        def rope(val):
            pk = table[w, pl.ds(row0, T), :]
            lane = lax.broadcasted_iota(jnp.int32, (T, HEAD_DIM), 1)
            swapped = pltpu.roll(pk, HEAD_DIM // 2, 1)
            cosw = jnp.where(lane < HEAD_DIM // 2, pk, swapped)
            sinw = jnp.where(lane < HEAD_DIM // 2, -swapped, pk)
            outs = []
            for h in range(NH):
                v = val[:, h * HEAD_DIM:(h + 1) * HEAD_DIM]
                outs.append((v * cosw + pltpu.roll(v, HEAD_DIM // 2, 1) * sinw).astype(BF16))
            return outs

        def hcols(h):
            return slice(h * HEAD_DIM, (h + 1) * HEAD_DIM)

        def proj(i):
            p = i % 2

            def w(m):
                return wres[m] if i == 0 else wst[gslot(i, u), m]
            for h, val in enumerate(rope(jnp.dot(act[T:2 * T, 0:D], w(0), preferred_element_type=F32))):
                qb[p, :, hcols(h)] = val
            for h, val in enumerate(rope(jnp.dot(act[T:2 * T, 0:D], w(1), preferred_element_type=F32))):
                kc[i, pl.ds(row0, T), hcols(h)] = val
            vc[i, pl.ds(row0, T), :] = jnp.dot(act[T:2 * T, 0:D], w(2), preferred_element_type=F32).astype(BF16)

        def heads(i):
            for h in range(NH):
                sc = lax.dot_general(qb[i % 2, :, hcols(h)], kc[i, :, hcols(h)], (((1,), (1,)), ((), ())),
                                     preferred_element_type=F32) * scale
                sbuf[h] = jnp.where(mask[...] > 0.5, sc, NEG)
            for h in range(NH):
                for r in range(0, T, 32):
                    sc = sbuf[h, r:r + 32, :]
                    e = jnp.exp(sc - jnp.max(sc, axis=-1, keepdims=True))
                    pbuf[h, r:r + 32, :] = (e * (1.0 / jnp.sum(e, axis=-1, keepdims=True))).astype(BF16)
            for h in range(NH):
                act[0:T, i * QL + h * HEAD_DIM:i * QL + (h + 1) * HEAD_DIM] = jnp.dot(
                    pbuf[h], vc[i, :, hcols(h)], preferred_element_type=F32).astype(BF16)

        with jax.named_scope('shards'):
            @pl.when(u == 0)
            def _():
                group_wait(0, u)
            proj(0)
            for i in range(3):
                group_wait(i + 1, u)
                proj(i + 1)
                if i < 2:
                    @pl.when(u == 0)
                    def _():
                        if i == 0:
                            w_ready([2], range(3))
                        else:
                            w_ready([0, 1, 2], [3])
                            wo_own().wait()
                group_start(i + 3, u)
                heads(i)
                if i == 0:
                    @pl.when(u >= 2)
                    def _():
                        combine(u - 2)
                if i == 0:
                    @pl.when(u < N - 1)
                    def _():
                        h_fetch(u + 1)
            heads(3)

        with jax.named_scope('wo'):
            def wo_block(n, w):
                act[T:2 * T, n * OB:(n + 1) * OB] = jnp.dot(act[0:T, 0:4 * QL], w, preferred_element_type=F32).astype(BF16)

            group_wait(4, u)
            group_wait(5, u)
            for n in range(3):
                wo_block(n, wst[gslot(4, u), n])

            wo_block(3, wst[gslot(5, u), 0])

            @pl.when(u < N - 1)
            def _():
                group_start(1, u + 1)
                group_start(2, u + 1)

        def norm_b(b, carry):
            rows = pl.ds(b * NR, NR)
            h1 = (hin[hs, rows, :].astype(F32) + act[pl.ds(pl.multiple_of(T + b * NR, NR), NR), 0:D].astype(F32)).astype(BF16)
            h1b[lax.rem(u, 3), rows, :] = h1
            gb[lax.rem(u, 3), pl.ds(pl.multiple_of(hb * T + b * NR, NR), NR), :] = norm_rows(h1, gm_ref[0:1, :], None)
            return carry
        lax.fori_loop(0, T // NR, norm_b, 0)

        @pl.when((s > 0) & (u < N - HS))
        def _():
            pl.semaphore_signal(cred, inc=1, device_id={"pp": s - 1}, device_id_type=MESH)

    def mlp(sl, row0, rows, store):
        UN = 2 if NB % 2 == 0 else 1

        def up(q, carry):
            for n in [q * UN + k for k in range(UN)]:
                xin = gb[sl, pl.ds(row0, rows), :]
                g = jnp.dot(xin, wg_s[n], preferred_element_type=F32)
                u_ = jnp.dot(xin, wu_s[n], preferred_element_type=F32)
                act[0:rows, pl.ds(pl.multiple_of(n * FB, FB), FB)] = (jax.nn.silu(g) * u_).astype(BF16)
            return carry
        lax.fori_loop(0, NB // UN, up, 0)

        def down(q, carry):
            for n in [q * UN + k for k in range(UN)]:
                store(pl.ds(pl.multiple_of(n * DB, DB), DB), jnp.dot(act[0:rows, 0:FL], wd_s[n], preferred_element_type=F32))
            return carry
        lax.fori_loop(0, NB // UN, down, 0)

    def mlp_home(u):
        def store(c, val):
            pacc[:, c] = val
        with jax.named_scope('mlp'):
            mlp(lax.rem(u, 3), 0, 2 * T, store)

    def mlp_outer(u, b):
        def store(c, val):
            px[lax.rem(u, 2), pl.ds(pl.multiple_of(b * T, T), T), c] = val.astype(BF16)
        with jax.named_scope('mlp_o'):
            mlp(lax.rem(u, 3), pl.multiple_of(b * T, T), T, store)

    def forward(u):
        @pl.when((u >= 1) & (u <= N))
        def _():
            s2_copy(u - 1).wait_send()

        @pl.when(u < N)
        def _():
            with jax.named_scope('w_ag'):
                ag_wait(1 - hb, u)
            s2_copy(u).start()

    def combine(v):
        sl = lax.rem(v, 2)
        with jax.named_scope('w_s3'):
            s3_copy(v, 0).wait_recv()
            s3_copy(v, 1).wait_recv()

        @pl.when(v >= 1)
        def _():
            s4_copy(v - 1).wait_send()

        def comb(b, carry):
            rows = pl.ds(b * RB, RB)
            mine = pl.ds(pl.multiple_of(hb * T + b * RB, RB), RB)
            theirs = pl.ds(pl.multiple_of((1 - hb) * T + b * RB, RB), RB)
            oacc[rows, :] = pacc[mine, :] + px[sl, mine, :].astype(F32)
            sendb[rows, :] = (pacc[theirs, :] + px[sl, theirs, :].astype(F32)).astype(BF16)
            return carry
        lax.fori_loop(0, T // RB, comb, 0)
        s4_copy(v).start()

    def finish(u):
        @pl.when((u >= 2) & (u < N + 2))
        def _():
            v = u - 2
            with jax.named_scope('w_s4'):
                s4_copy(v).wait_recv()
            vw = v // NJ
            vj = lax.rem(v, NJ)

            @pl.when(v >= 1)
            def _():
                hin_copy(v).wait_send()

            def fin(b, carry):
                rows = pl.ds(b * RB, RB)
                d = (oacc[rows, :] + ps[lax.rem(v, 2), rows, :].astype(F32)).astype(BF16)
                h2b[rows, :] = (h1b[lax.rem(v, 3), rows, :].astype(F32) + d.astype(F32)).astype(BF16)
                return carry
            lax.fori_loop(0, T // RB, fin, 0)

            @pl.when((s < n_stages - 1) & (v >= HS))
            def _():
                with jax.named_scope('w_cred'):
                    pl.semaphore_wait(cred, 1)

            @pl.when(s < n_stages - 1)
            def _():
                hin_copy(v).start()

            @pl.when(s == n_stages - 1)
            def _():
                park_copy(v).start()

            @pl.when((s == n_stages - 1) & (v == N - 1))
            def _():
                last_copy().start()

    def body(u, carry):
        @pl.when(is_home)
        def _():
            @pl.when(u < N)
            def _():
                attention(u)

            @pl.when((u >= 1) & (u <= N))
            def _():
                s1_outer(u - 1).wait_send()
                s1_peer(u - 1).wait_send()

            @pl.when(u < N)
            def _():
                s1_peer(u).start()
                s1_outer(u).start()

            @pl.when((u >= N) & (u < N + 2))
            def _():
                combine(u - 2)

            finish(u)

            @pl.when((u >= 1) & (u <= N))
            def _():
                mlp_home(u - 1)

            forward(u)

        @pl.when(is_outer & (u < N))
        def _():
            for k in (0, 1):
                b = inner - 1 if k == 0 else 2 - inner
                with jax.named_scope('w_ag_outer'):
                    ag_wait(b, u)

                @pl.when(u >= 2)
                def _():
                    s3_copy(u - 2, b).wait_send()
                mlp_outer(u, b)
                s3_copy(u, b).start()

        return carry

    def out_fwd(mb, p, sem):
        return rcopy(out_ref.at[mb], out_ref.at[mb], ofs.at[mb, p], sem, pp=p)

    lax.fori_loop(0, N + 2, body, 0)

    last_here = (s == n_stages - 1) & (z == NJ - 1)

    @pl.when(last_here)
    def _():
        for mb in (n_mb - 2, n_mb - 1):
            local(out_ref.at[mb], out_ref.at[mb], outr.at[mb]).wait()
            out_fwd(mb, 2, outf).start()

    def od_copy(v):
        return rcopy(hin_hbm.at[v], out_ref.at[2 * (v // NJ) + hb], od.at[v], outr.at[2 * (v // NJ) + hb], tp=lax.rem(v, NJ))

    @pl.when(s == 1)
    def _():
        def spread(v, carry):
            vj = lax.rem(v, NJ)
            mine = 2 * (v // NJ) + hb

            @pl.when(is_home)
            def _():
                local(hin_hbm.at[v], hin_hbm.at[v], op.at[v]).wait()

            @pl.when(is_home & (vj != z))
            def _():
                od_copy(v).start()

            @pl.when(is_home & (vj == z))
            def _():
                c = local(hin_hbm.at[v], hin.at[0], hv_sem)
                c.start()
                c.wait()
                c = local(hin.at[0], out_ref.at[mine], hv_sem)
                c.start()
                c.wait()

            @pl.when(vj == z)
            def _():
                for b in (0, 1):
                    mb = 2 * (v // NJ) + b

                    @pl.when(z - 1 != b)
                    def _(mb=mb):
                        local(out_ref.at[mb], out_ref.at[mb], outr.at[mb]).wait()
                    out_fwd(mb, 0, outf).start()

                    @pl.when(v < N - 1)
                    def _(mb=mb):
                        out_fwd(mb, 3, outf).start()
                        out_fwd(mb, 2, outf).start()
            return carry
        lax.fori_loop(0, N, spread, 0)

    @pl.when(is_home)
    def _():
        s4_copy(N - 1).wait_send()
        hin_copy(N - 1).wait_send()

        @pl.when(s == n_stages - 1)
        def _():
            last_copy().wait_send()

    @pl.when(is_outer)
    def _():
        for b in (0, 1):
            s3_copy(N - 2, b).wait_send()
            s3_copy(N - 1, b).wait_send()

    @pl.when(s == 1)
    def _():
        for m in PM:
            y_send(0, m).wait_send()

        @pl.when(is_outer)
        def _():
            for m in PM:
                y_send(1, m).wait_send()

    @pl.when((s == 3) & is_home)
    def _():
        for m in PM:
            pp_send(m).wait_send()
            pf_send(m).wait_send()
            for r in (1, 2):
                pxf_send(r, m).wait_send()
            for r in (0, 1, 2):
                for i in (0, 1):
                    push(r, m, i).wait_send()

    @pl.when(is_home)
    def _():
        def sent(m):
            p_send(m).wait_send()
            f_send(m).wait_send()
            x_send(1, m).wait_send()
            x_send(2, m).wait_send()
        for m in range(4):
            direct(m, functools.partial(sent, m))

        @pl.when(s == 2)
        def _():
            for w in range(NW):
                for j in range(NJ):
                    @pl.when(z != j)
                    def _():
                        x_pass(w, j).wait_send()

        @pl.when(s == 1)
        def _():
            def spread_done(v, carry):
                @pl.when(lax.rem(v, NJ) != z)
                def _():
                    od_copy(v).wait_send()
                return carry
            lax.fori_loop(0, N, spread_done, 0)

    for w in range(NW):
        x_each(w, lambda c: c.wait_send())

    @pl.when(s == 1)
    def _():
        for mb in range(n_mb):
            out_fwd(mb, 0, outf).wait_send()
            if mb < n_mb - 2:
                out_fwd(mb, 3, outf).wait_send()
                out_fwd(mb, 2, outf).wait_send()
            else:
                @pl.when(z < NJ - 1)
                def _(mb=mb):
                    out_fwd(mb, 3, outf).wait_send()
                    out_fwd(mb, 2, outf).wait_send()

    @pl.when(last_here)
    def _():
        for mb in (n_mb - 2, n_mb - 1):
            out_fwd(mb, 2, outf).wait_send()
        early = out_ref.at[pl.ds(0, n_mb - 2)]
        local(early, early, outf).wait()

    @pl.when((s == n_stages - 1) & (z < NJ - 1))
    def _():
        local(out_ref, out_ref, outf).wait()

    @pl.when((s == 0) | (s == 2))
    def _():
        local(out_ref, out_ref, outf).wait()


def solution(mesh):
    n_stages = mesh.shape['pp']

    def stage_program(hidden_in, seg_ids, positions, attn_norm, w_query, w_key, w_value, w_out, mlp_norm, w_gate, w_up, w_down):
        n_mb, T, D = hidden_in.shape
        S = seg_ids.shape[1]
        QL = w_query.shape[2]
        FL = w_gate.shape[2]
        NJ = S // T
        N = (n_mb // 2) * NJ
        NB = max(1, FL // 512)
        invf = jnp.asarray(np.tile(rope_freqs(), 2)[None, :], F32)
        any_spec = pl.BlockSpec(memory_space=pl.ANY)
        vmem = pl.BlockSpec(memory_space=pltpu.VMEM)
        dma = pltpu.SemaphoreType.DMA
        scratch = [
            pltpu.VMEM((NB, D, FL // NB), BF16), pltpu.VMEM((NB, D, FL // NB), BF16), pltpu.VMEM((NB, FL, D // NB), BF16),
            pltpu.VMEM((3, D, QL), BF16), pltpu.VMEM((2, 3, D, QL), BF16),
            pltpu.VMEM((3, 2 * T, D), BF16),
            pltpu.VMEM((2, 2 * T, D), BF16),
            pltpu.VMEM((2, T, D), BF16),
            pltpu.VMEM((4, S, QL), BF16), pltpu.VMEM((4, S, QL), BF16),
            pltpu.VMEM((3, T, D), BF16),
            pltpu.VMEM((3, T, D), BF16),
            pltpu.VMEM((2 * T, D), F32),
            pltpu.VMEM((T, D), F32),
            pltpu.VMEM((T, D), BF16),
            pltpu.VMEM((T, D), BF16),
            pltpu.VMEM((2 * T, max(D, FL, 4 * QL)), BF16),
            pltpu.VMEM((2, T, QL), BF16),
            pltpu.VMEM((n_mb // 2, S, HEAD_DIM), F32),
            pltpu.VMEM((T, S), F32), pltpu.VMEM((QL // HEAD_DIM, T, S), F32), pltpu.VMEM((QL // HEAD_DIM, T, S), BF16),
            dma((3, 8)), dma((2, 4)), dma((8,)), dma((4,)), dma((2, 4)),
            dma((N,)), dma((n_mb // 2, 2)), dma((2, 3)), dma((2,)), dma, dma((2, 2)), dma((2, 2)), dma((2,)), dma, dma,
            dma((n_mb,)), dma, dma((n_mb, n_stages)),
            dma((3,)), dma((2, 3)), dma, dma((3, NB)), dma, dma, dma((N,)), dma((n_mb // 2, NJ)), dma((N,)), dma((N,)),
            dma((4,)), dma((4,)), dma((4,)), dma((4,)), dma((2,)), dma((2,)), dma((2,)), dma((2,)), dma((2, 2)), dma((2, 2)), dma((3, 2, 2)),
            pltpu.SemaphoreType.REGULAR, pltpu.SemaphoreType.REGULAR,
        ]
        return pl.pallas_call(
            functools.partial(kernel, n_stages),
            out_shape=[jax.ShapeDtypeStruct(hidden_in.shape, BF16), jax.ShapeDtypeStruct((3, 3, D, QL), BF16),
                       jax.ShapeDtypeStruct((4 * QL, D), BF16), jax.ShapeDtypeStruct((N, T, D), BF16),
                       jax.ShapeDtypeStruct((4, D, QL), BF16), jax.ShapeDtypeStruct((4 * QL, D), BF16)],
            in_specs=[any_spec, vmem, vmem, vmem, vmem, vmem] + [any_spec] * 7,
            out_specs=[any_spec] * 6,
            scratch_shapes=scratch,
            compiler_params=pltpu.CompilerParams(collective_id=0, has_side_effects=True, vmem_limit_bytes=67_043_328),
        )(hidden_in, seg_ids, positions, invf, attn_norm, mlp_norm, w_query, w_key, w_value, w_out, w_gate, w_up, w_down)[0]

    act_spec = P('dp', 'tp', None)
    row_spec = P('dp', None)
    gain_spec = P('pp', None)
    col_spec = P('pp', None, 'tp')
    rows_spec = P('pp', 'tp', None)
    return jax.shard_map(stage_program, mesh=mesh,
                         in_specs=(act_spec, row_spec, row_spec, gain_spec, col_spec, col_spec, col_spec, rows_spec, gain_spec, col_spec, col_spec, rows_spec),
                         out_specs=act_spec, check_vma=False)
```

```python
import functools
import math

import jax
import jax.numpy as jnp
import numpy as np
from jax import lax
from jax.experimental import pallas as pl
from jax.experimental.pallas import tpu as pltpu
from jax.sharding import PartitionSpec as P

HEAD_DIM = 128
NORM_EPS = 1e-5
ROPE_THETA = 500000.0
ROPE_FACTOR = 8.0
LOW_FREQ = 1.0
HIGH_FREQ = 4.0
ORIG_CTX = 8192.0
NEG = -1e30
MESH = pl.DeviceIdType.MESH
F32 = jnp.float32
BF16 = jnp.bfloat16


def rope_freqs():
    base_freq = 1.0 / (ROPE_THETA ** (np.arange(0, HEAD_DIM, 2) / HEAD_DIM))
    wavelen = 2.0 * np.pi / base_freq
    smooth = (ORIG_CTX / wavelen - LOW_FREQ) / (HIGH_FREQ - LOW_FREQ)
    blended = (1.0 - smooth) * base_freq / ROPE_FACTOR + smooth * base_freq
    scaled = np.where(wavelen > ORIG_CTX / LOW_FREQ, base_freq / ROPE_FACTOR, blended)
    return np.where(wavelen < ORIG_CTX / HIGH_FREQ, base_freq, scaled)


def kernel(n_stages, x_ref, seg_ref, pos_ref, invf_ref, ga_ref, gm_ref,
           wq_ref, wk_ref, wv_ref, wo_ref, wg_ref, wu_ref, wd_ref,
           out_ref,
           wqkv_hbm, wo_hbm, hin_hbm, pv_hbm, po_hbm,
           wg_s, wu_s, wd_s, wres, wst, gb, px, ps, kc, vc, hin, h1b, pacc, oacc, sendb, h2b, act, qb,
           table, mask, sbuf, pbuf,
           wr, wx, wsnd, wfwd, wxs, hin_sem, xs, ag, s1s, s2s, pxr, pxs, psr, s4s, s5s, outr, outf, ofs,
           wres_sem, wst_sem, wo_sem, mlp_sem, hv_sem, s6s, xp, xq, op, od,
           ysn, yrc, pos, por, pps, ppr, pfs, pfr, pxfs, pxfr, pds, gate, cred):
    n_mb, T, D = x_ref.shape
    QL = wq_ref.shape[2]
    FL = wg_ref.shape[2]
    NB = wg_s.shape[0]
    FB = FL // NB
    S = seg_ref.shape[1]
    NJ = S // T
    NH = QL // HEAD_DIM
    N = (n_mb // 2) * NJ
    DB = D // NB
    scale = HEAD_DIM ** -0.5
    RB = 16
    NR = 32
    HS = hin.shape[0]
    OB = wst.shape[3]
    NO = D // OB

    hx = lax.axis_index("dp")
    z = lax.axis_index("tp")
    s = lax.axis_index("pp")
    is_home = (z == 1) | (z == 2)
    is_outer = (z == 0) | (z == 3)
    hb = lax.rem(z + 1, 2) * 0 + (z - 1)
    peer = 3 - z
    outer = 3 * (z - 1)
    inner = 1 + z // 2
    odd = lax.rem(s, 2)

    def rcopy(src, dst, ssem, rsem, **dev):
        return pltpu.make_async_remote_copy(src_ref=src, dst_ref=dst, send_sem=ssem, recv_sem=rsem,
                                            device_id=dev, device_id_type=MESH)

    def local(src, dst, sem):
        return pltpu.make_async_copy(src, dst, sem)

    def column(ref, mb, j):
        row = ref[pl.ds(mb, 1), :]
        part = row[:, 0:T]
        for c in range(1, NJ):
            part = jnp.where(j == c, row[:, c * T:(c + 1) * T], part)
        return jnp.broadcast_to(part, (HEAD_DIM, T)).T

    barrier = pltpu.get_barrier_semaphore()
    for k in range(1, 4):
        pl.semaphore_signal(barrier, inc=1, device_id={"tp": lax.rem(z + k, 4)}, device_id_type=MESH)
        pl.semaphore_signal(barrier, inc=1, device_id={"pp": lax.rem(s + k, 4)}, device_id_type=MESH)
    pl.semaphore_signal(barrier, inc=1, device_id={"dp": 1 - hx}, device_id_type=MESH)
    pl.semaphore_wait(barrier, 7)

    wqkv_own = (wq_ref, wk_ref, wv_ref, wo_ref)

    def mlp_copies():
        cps = []
        for n in range(NB):
            cps.append(local(wg_ref.at[0, :, pl.ds(n * FB, FB)], wg_s.at[n], mlp_sem.at[0, n]))
            cps.append(local(wu_ref.at[0, :, pl.ds(n * FB, FB)], wu_s.at[n], mlp_sem.at[1, n]))
            cps.append(local(wd_ref.at[0, :, pl.ds(n * DB, DB)], wd_s.at[n], mlp_sem.at[2, n]))
        return cps

    NW = n_mb // 2

    def x_copy(w, home):
        u = w * NJ + z
        return rcopy(x_ref.at[2 * w + (home - 1)], hin_hbm.at[u], xs.at[w, home - 1], xp.at[u], tp=home)

    def x_each(w, act):
        for home in (1, 2):
            @pl.when((s == 2) & (z != home))
            def _():
                act(x_copy(w, home))

    def x_pass(w, j):
        u = w * NJ + j
        return rcopy(hin_hbm.at[u], hin_hbm.at[u], xq.at[w, j], hin_sem.at[u], pp=0)

    def x_relay(ws):
        @pl.when((s == 2) & is_home)
        def _():
            for w in ws:
                for j in range(NJ):
                    @pl.when(z != j)
                    def _():
                        local(hin_hbm.at[w * NJ + j], hin_hbm.at[w * NJ + j], xp.at[w * NJ + j]).wait()
                        x_pass(w, j).start()

    x_each(0, lambda c: c.start())
    x_relay([0])

    def half(ref, m, h):
        rows = (D if m < 3 else QL) // 2
        return ref.at[pl.ds(h * rows, rows), :]

    def wslot(r, m):
        return wqkv_hbm.at[r, m] if m < 3 else wo_hbm.at[pl.ds((r + 1) * QL, QL)]

    def own_w(m):
        return wqkv_own[m].at[0]

    def wo_own():
        return local(own_w(3), wo_hbm.at[pl.ds(0, QL)], wo_sem)

    def o_send(k):
        h = hx if k < 4 else 1 - hx
        return rcopy(half(own_w(k % 4), k % 4, h), half(wslot(0, k % 4), k % 4, h), wsnd.at[k], wr.at[0, k], tp=inner)

    def p_send(m):
        return rcopy(half(own_w(m), m, hx), half(wslot(1, m), m, hx), wsnd.at[m], wr.at[1, m], tp=peer)

    def f_send(m):
        return rcopy(half(wslot(0, m), m, hx), half(wslot(2, m), m, hx), wfwd.at[m], wr.at[2, m], tp=peer)

    def x_send(r, m):
        return rcopy(half(wslot(r, m), m, hx), half(wslot(r, m), m, hx), wxs.at[r - 1, m], wx.at[r - 1, m], dp=1 - hx)

    def w_ready(rs, ms):
        def pushed(m):
            if 0 in rs:
                o_send(m).wait_recv()
            if 1 in rs:
                p_send(m).wait_recv()
        for m in ms:
            if m in PM:
                pl.when(s == 1)(functools.partial(pushed, m))
            if 0 in rs:
                o_send(4 + m).wait_recv()
            for r in (1, 2):
                if r in rs:
                    x_send(r, m).wait_recv()

    PM = (2, 3)

    def pb(r, m):
        return pv_hbm.at[r] if m == 2 else po_hbm.at[pl.ds(r * QL, QL)]

    def hh(i):
        return hx if i == 0 else 1 - hx

    def y_send(i, m):
        return rcopy(half(own_w(m), m, hh(i)), half(pb(3, m), m, hh(i)), ysn.at[2 * i + m - 2], yrc.at[2 * i + m - 2], pp=3)

    def po_send(i, m):
        return rcopy(half(pb(3, m), m, hh(i)), half(pb(0, m), m, hh(i)), pos.at[2 * i + m - 2], por.at[2 * i + m - 2], tp=inner)

    def pp_send(m):
        return rcopy(half(pb(3, m), m, hx), half(pb(1, m), m, hx), pps.at[m - 2], ppr.at[m - 2], tp=peer)

    def pf_send(m):
        return rcopy(half(pb(0, m), m, hx), half(pb(2, m), m, hx), pfs.at[m - 2], pfr.at[m - 2], tp=peer)

    def pxf_send(r, m):
        return rcopy(half(pb(r, m), m, hx), half(pb(r, m), m, hx), pxfs.at[r - 1, m - 2], pxfr.at[r - 1, m - 2], dp=1 - hx)

    def push(r, m, i):
        rsem = wr.at[0, 4 * i + m] if r == 0 else (wr.at[r, m] if i == 0 else wx.at[r - 1, m])
        return rcopy(half(pb(r, m), m, hh(i)), half(wslot(r, m), m, hh(i)), pds.at[r, m - 2, i], rsem, pp=1)

    def direct(m, f):
        if m in PM:
            pl.when(s != 1)(f)
        else:
            f()

    @pl.when(s == 1)
    def _():
        for m in PM:
            y_send(0, m).start()

        @pl.when(is_outer)
        def _():
            for m in PM:
                y_send(1, m).start()

    @pl.when((s == 3) & is_outer)
    def _():
        for i in (0, 1):
            for m in PM:
                y_send(i, m).wait_recv()
                po_send(i, m).start()
        for i in (0, 1):
            for m in PM:
                po_send(i, m).wait_send()

    @pl.when((s == 3) & is_home)
    def _():
        for m in PM:
            y_send(0, m).wait_recv()
            pp_send(m).start()
        for kind, m, a in (("p", 2, 0), ("o", 2, 0), ("p", 3, 0), ("o", 3, 0), ("f", 2, 0), ("f", 3, 0), ("o", 2, 1), ("x", 2, 1),
                           ("o", 3, 1), ("x", 3, 1)):
            with jax.named_scope('wp_' + kind + str(m) + str(a)):
                if kind == "p":
                    pp_send(m).wait_recv()
                    pxf_send(1, m).start()
                    push(1, m, 0).start()
                elif kind == "o":
                    po_send(a, m).wait_recv()
                    if a == 0:
                        pf_send(m).start()
                    push(0, m, a).start()
                elif kind == "f":
                    pf_send(m).wait_recv()
                    push(2, m, 0).start()
                else:
                    pxf_send(a, m).wait_recv()
                    push(a, m, 1).start()

    @pl.when(s == 3)
    def _():
        pl.semaphore_signal(gate, inc=1, device_id={"pp": 2}, device_id_type=MESH)

    def release():
        @pl.when(odd == 0)
        def _():
            pl.semaphore_signal(gate, inc=1, device_id={"pp": s + 1}, device_id_type=MESH)

    @pl.when(s != 0)
    def _():
        for c in mlp_copies():
            c.start()
        with jax.named_scope('w_gate'):
            pl.semaphore_wait(gate, 1)

    if NW > 1:
        x_each(1, lambda c: c.start())

    @pl.when(is_outer)
    def _():
        for k in range(8):
            direct(k % 4, lambda k=k: o_send(k).start())

        @pl.when(s == 0)
        def _():
            for c in mlp_copies():
                c.start()
        for k in range(8):
            direct(k % 4, lambda k=k: o_send(k).wait_send())
        release()
        for w in range(2, NW):
            x_each(w, lambda c: c.start())

    @pl.when(is_home)
    def _():
        for m in range(4):
            direct(m, lambda m=m: p_send(m).start())
        wo_own().start()

        @pl.when(s == 0)
        def _():
            for c in mlp_copies():
                c.start()
        def zero_rows(b, carry):
            for i in range(4):
                kc[i, pl.ds(b * RB, RB), :] = jnp.zeros((RB, QL), BF16)
                vc[i, pl.ds(b * RB, RB), :] = jnp.zeros((RB, QL), BF16)
            return carry
        lax.fori_loop(0, S // RB, zero_rows, 0)

        def tables(w):
            lane = lax.broadcasted_iota(jnp.int32, (T, HEAD_DIM), 1)

            def table_rows(b, carry):
                rows = pl.ds(pl.multiple_of(b * T, T), T)
                ang = column(pos_ref, 2 * w + hb, b).astype(F32) * invf_ref[0:1, :]
                table[w, rows, :] = jnp.where(lane < HEAD_DIM // 2, jnp.cos(ang), jnp.sin(ang))
                return carry
            with jax.named_scope('table'):
                lax.fori_loop(0, NJ, table_rows, 0)

        steps = [("o", 0), ("p", 0), ("t", 0), ("o", 1), ("p", 1), ("t", 1), ("o", 2), ("p", 2), ("t", 2), ("o", 3), ("p", 3), ("t", 3),
                 ("f", 0), ("f", 1), ("f", 2), ("f", 3), ("g", 0), ("r", 0)]

        def step(kind, m):
            if kind == "o":
                o_send(m).wait_recv()
                f_send(m).start()
            elif kind == "p":
                p_send(m).wait_recv()
                x_send(1, m).start()
            else:
                f_send(m).wait_recv()
                x_send(2, m).start()

        for kind, m in steps:
            with jax.named_scope('w_' + kind + str(m)):
                if kind in "op":
                    direct(m, lambda kind=kind, m=m: step(kind, m))
                elif kind == "f" and m in PM:
                    pl.when(s != 1)(functools.partial(step, kind, m))
                elif kind == "f":
                    pl.when(s == 1)(functools.partial(step, kind, m + 2))
                    step(kind, m)
                elif kind == "g":
                    release()
                elif kind == "r":
                    x_relay([1] if NW > 1 else [])
                elif m < n_mb // 2:
                    tables(m)
        for w in range(2, NW):
            x_each(w, lambda c: c.start())
        w_ready([0, 1], range(3))
        x_relay(range(2, NW))

    def gslot(g, u):
        return lax.rem(g - 1 + u, 2)

    def group_copies(g, u):
        if g == 0:
            return [local(own_w(m), wres.at[m], wres_sem.at[m]) for m in range(3)]
        p = gslot(g, u)
        if g < 4:
            return [local(wqkv_hbm.at[g - 1], wst.at[p], wst_sem.at[p, 0])]
        return [local(wo_hbm.at[:, pl.ds(((g - 4) * 3 + m) * OB, OB)], wst.at[p, m], wst_sem.at[p, m]) for m in range(3 if g == 4 else 1)]

    def group_start(g, u):
        for c in group_copies(g, u):
            c.start()

    def group_wait(g, u):
        for c in group_copies(g, u):
            c.wait()

    def h_fetch(u):
        mb = 2 * (u // NJ) + hb
        here = lax.rem(u, NJ) == z
        dst = hin.at[lax.rem(u, HS)]

        @pl.when((s == 0) & here)
        def _():
            local(x_ref.at[mb], dst, hv_sem).start()

        @pl.when((s == 0) & jnp.logical_not(here))
        def _():
            local(hin_hbm.at[u], hin_hbm.at[u], hin_sem.at[u]).wait()
            local(hin_hbm.at[u], dst, hv_sem).start()

    @pl.when(is_home)
    def _():
        group_start(0, 0)
        group_start(1, 0)
        group_start(2, 0)
        h_fetch(0)

    for c in mlp_copies():
        c.wait()

    def hin_copy(u):
        return rcopy(h2b, hin.at[lax.rem(u, HS)], s5s, hin_sem.at[u], pp=lax.rem(s + 1, n_stages))

    def s1_outer(u):
        blk = gb.at[lax.rem(u, 3), pl.ds(pl.multiple_of(hb * T, T), T), :]
        return rcopy(blk, blk, s1s.at[0], ag.at[hb, lax.rem(u, 3)], tp=outer)

    def s1_peer(u):
        blk = gb.at[lax.rem(u, 3), pl.ds(pl.multiple_of(hb * T, T), T), :]
        return rcopy(blk, blk, s1s.at[1], ag.at[hb, lax.rem(u, 3)], tp=peer)

    def s2_copy(u):
        blk = gb.at[lax.rem(u, 3), pl.ds(pl.multiple_of((1 - hb) * T, T), T), :]
        return rcopy(blk, blk, s2s, ag.at[1 - hb, lax.rem(u, 3)], tp=outer)

    def ag_wait(b, u):
        blk = gb.at[lax.rem(u, 3), pl.ds(pl.multiple_of(b * T, T), T), :]
        local(blk, blk, ag.at[b, lax.rem(u, 3)]).wait()

    def s3_copy(u, b):
        sl = lax.rem(u, 2)
        blk = px.at[sl, pl.ds(pl.multiple_of(b * T, T), T), :]
        return rcopy(blk, blk, pxs.at[sl, b], pxr.at[sl, b], tp=inner)

    def s4_copy(u):
        return rcopy(sendb, ps.at[lax.rem(u, 2)], s4s, psr.at[lax.rem(u, 2)], tp=peer)

    def park_copy(u):
        return rcopy(h2b, hin_hbm.at[u], s5s, op.at[u], pp=1)

    def last_copy():
        mb = n_mb - 2 + hb
        return rcopy(h2b, out_ref.at[mb], s6s, outr.at[mb], tp=NJ - 1)

    def norm_rows(src, gain, dst):
        hf = src.astype(F32)
        inv = lax.rsqrt(jnp.mean(hf * hf, axis=-1, keepdims=True) + NORM_EPS)
        return (hf * inv * gain.astype(F32)).astype(BF16)

    def attention(u):
      with jax.named_scope('attn'):
        attention_(u)

    def attention_(u):
        w = u // NJ
        j = lax.rem(u, NJ)
        mb = 2 * w + hb
        row0 = pl.multiple_of(j * T, T)
        hs = lax.rem(u, HS)

        with jax.named_scope('w_hin'):
            @pl.when(s == 0)
            def _():
                local(x_ref.at[mb], hin.at[hs], hv_sem).wait()

            @pl.when(s > 0)
            def _():
                hin_copy(u).wait_recv()

        def norm_a(b, carry):
            rows = pl.ds(b * NR, NR)
            act[pl.ds(pl.multiple_of(T + b * NR, NR), NR), 0:D] = norm_rows(hin[hs, rows, :], ga_ref[0:1, :], None)
            return carry
        lax.fori_loop(0, T // NR, norm_a, 0)

        segrow = seg_ref[pl.ds(mb, 1), :]
        segc = column(seg_ref, mb, j)
        ti = lax.broadcasted_iota(jnp.int32, (T, HEAD_DIM), 0) + row0
        for c in range(0, S, HEAD_DIM):
            segr = segrow[:, c:c + HEAD_DIM]
            ui = lax.broadcasted_iota(jnp.int32, (T, HEAD_DIM), 1) + c
            mask[:, c:c + HEAD_DIM] = jnp.where((segc == segr) & (ui <= ti), 1.0, 0.0)

        def rope(val):
            pk = table[w, pl.ds(row0, T), :]
            lane = lax.broadcasted_iota(jnp.int32, (T, HEAD_DIM), 1)
            swapped = pltpu.roll(pk, HEAD_DIM // 2, 1)
            cosw = jnp.where(lane < HEAD_DIM // 2, pk, swapped)
            sinw = jnp.where(lane < HEAD_DIM // 2, -swapped, pk)
            outs = []
            for h in range(NH):
                v = val[:, h * HEAD_DIM:(h + 1) * HEAD_DIM]
                outs.append((v * cosw + pltpu.roll(v, HEAD_DIM // 2, 1) * sinw).astype(BF16))
            return outs

        def hcols(h):
            return slice(h * HEAD_DIM, (h + 1) * HEAD_DIM)

        def proj(i):
            p = i % 2

            def w(m):
                return wres[m] if i == 0 else wst[gslot(i, u), m]
            for h, val in enumerate(rope(jnp.dot(act[T:2 * T, 0:D], w(0), preferred_element_type=F32))):
                qb[p, :, hcols(h)] = val
            for h, val in enumerate(rope(jnp.dot(act[T:2 * T, 0:D], w(1), preferred_element_type=F32))):
                kc[i, pl.ds(row0, T), hcols(h)] = val
            vc[i, pl.ds(row0, T), :] = jnp.dot(act[T:2 * T, 0:D], w(2), preferred_element_type=F32).astype(BF16)

        def heads(i):
            for h in range(NH):
                sc = lax.dot_general(qb[i % 2, :, hcols(h)], kc[i, :, hcols(h)], (((1,), (1,)), ((), ())),
                                     preferred_element_type=F32) * scale
                sbuf[h] = jnp.where(mask[...] > 0.5, sc, NEG)
            for h in range(NH):
                for r in range(0, T, 32):
                    sc = sbuf[h, r:r + 32, :]
                    e = jnp.exp(sc - jnp.max(sc, axis=-1, keepdims=True))
                    pbuf[h, r:r + 32, :] = (e * (1.0 / jnp.sum(e, axis=-1, keepdims=True))).astype(BF16)
            for h in range(NH):
                act[0:T, i * QL + h * HEAD_DIM:i * QL + (h + 1) * HEAD_DIM] = jnp.dot(
                    pbuf[h], vc[i, :, hcols(h)], preferred_element_type=F32).astype(BF16)

        with jax.named_scope('shards'):
            @pl.when(u == 0)
            def _():
                group_wait(0, u)
            proj(0)
            for i in range(3):
                group_wait(i + 1, u)
                proj(i + 1)
                if i < 2:
                    @pl.when(u == 0)
                    def _():
                        if i == 0:
                            w_ready([2], range(3))
                        else:
                            w_ready([0, 1, 2], [3])
                            wo_own().wait()
                group_start(i + 3, u)
                heads(i)
                if i == 0:
                    @pl.when(u >= 2)
                    def _():
                        combine(u - 2)
                if i == 0:
                    @pl.when(u < N - 1)
                    def _():
                        h_fetch(u + 1)
            heads(3)

        with jax.named_scope('wo'):
            def wo_block(n, w):
                act[T:2 * T, n * OB:(n + 1) * OB] = jnp.dot(act[0:T, 0:4 * QL], w, preferred_element_type=F32).astype(BF16)

            group_wait(4, u)
            for n in range(3):
                wo_block(n, wst[gslot(4, u), n])

            group_wait(5, u)
            wo_block(3, wst[gslot(5, u), 0])

            @pl.when(u < N - 1)
            def _():
                group_start(1, u + 1)
                group_start(2, u + 1)

        def norm_b(b, carry):
            rows = pl.ds(b * NR, NR)
            h1 = (hin[hs, rows, :].astype(F32) + act[pl.ds(pl.multiple_of(T + b * NR, NR), NR), 0:D].astype(F32)).astype(BF16)
            h1b[lax.rem(u, 3), rows, :] = h1
            gb[lax.rem(u, 3), pl.ds(pl.multiple_of(hb * T + b * NR, NR), NR), :] = norm_rows(h1, gm_ref[0:1, :], None)
            return carry
        lax.fori_loop(0, T // NR, norm_b, 0)

        @pl.when((s > 0) & (u < N - HS))
        def _():
            pl.semaphore_signal(cred, inc=1, device_id={"pp": s - 1}, device_id_type=MESH)

    def mlp(sl, row0, rows, store):
        UN = 2 if NB % 2 == 0 else 1

        def up(q, carry):
            for n in [q * UN + k for k in range(UN)]:
                xin = gb[sl, pl.ds(row0, rows), :]
                g = jnp.dot(xin, wg_s[n], preferred_element_type=F32)
                u_ = jnp.dot(xin, wu_s[n], preferred_element_type=F32)
                act[0:rows, pl.ds(pl.multiple_of(n * FB, FB), FB)] = (jax.nn.silu(g) * u_).astype(BF16)
            return carry
        lax.fori_loop(0, NB // UN, up, 0)

        def down(q, carry):
            for n in [q * UN + k for k in range(UN)]:
                store(pl.ds(pl.multiple_of(n * DB, DB), DB), jnp.dot(act[0:rows, 0:FL], wd_s[n], preferred_element_type=F32))
            return carry
        lax.fori_loop(0, NB // UN, down, 0)

    def mlp_home(u):
        def store(c, val):
            pacc[:, c] = val
        with jax.named_scope('mlp'):
            mlp(lax.rem(u, 3), 0, 2 * T, store)

    def mlp_outer(u, b):
        def store(c, val):
            px[lax.rem(u, 2), pl.ds(pl.multiple_of(b * T, T), T), c] = val.astype(BF16)
        with jax.named_scope('mlp_o'):
            mlp(lax.rem(u, 3), pl.multiple_of(b * T, T), T, store)

    def forward(u):
        @pl.when((u >= 1) & (u <= N))
        def _():
            s2_copy(u - 1).wait_send()

        @pl.when(u < N)
        def _():
            with jax.named_scope('w_ag'):
                ag_wait(1 - hb, u)
            s2_copy(u).start()

    def combine(v):
        sl = lax.rem(v, 2)
        with jax.named_scope('w_s3'):
            s3_copy(v, 0).wait_recv()
            s3_copy(v, 1).wait_recv()

        @pl.when(v >= 1)
        def _():
            s4_copy(v - 1).wait_send()

        def comb(b, carry):
            rows = pl.ds(b * RB, RB)
            mine = pl.ds(pl.multiple_of(hb * T + b * RB, RB), RB)
            theirs = pl.ds(pl.multiple_of((1 - hb) * T + b * RB, RB), RB)
            oacc[rows, :] = pacc[mine, :] + px[sl, mine, :].astype(F32)
            sendb[rows, :] = (pacc[theirs, :] + px[sl, theirs, :].astype(F32)).astype(BF16)
            return carry
        lax.fori_loop(0, T // RB, comb, 0)
        s4_copy(v).start()

    def finish(u):
        @pl.when((u >= 2) & (u < N + 2))
        def _():
            v = u - 2
            with jax.named_scope('w_s4'):
                s4_copy(v).wait_recv()
            vw = v // NJ
            vj = lax.rem(v, NJ)

            @pl.when(v >= 1)
            def _():
                hin_copy(v).wait_send()

            def fin(b, carry):
                rows = pl.ds(b * RB, RB)
                d = (oacc[rows, :] + ps[lax.rem(v, 2), rows, :].astype(F32)).astype(BF16)
                h2b[rows, :] = (h1b[lax.rem(v, 3), rows, :].astype(F32) + d.astype(F32)).astype(BF16)
                return carry
            lax.fori_loop(0, T // RB, fin, 0)

            @pl.when((s < n_stages - 1) & (v >= HS))
            def _():
                with jax.named_scope('w_cred'):
                    pl.semaphore_wait(cred, 1)

            @pl.when(s < n_stages - 1)
            def _():
                hin_copy(v).start()

            @pl.when(s == n_stages - 1)
            def _():
                park_copy(v).start()

            @pl.when((s == n_stages - 1) & (v == N - 1))
            def _():
                last_copy().start()

    def body(u, carry):
        @pl.when(is_home)
        def _():
            @pl.when(u < N)
            def _():
                attention(u)

            @pl.when((u >= 1) & (u <= N))
            def _():
                s1_outer(u - 1).wait_send()
                s1_peer(u - 1).wait_send()

            @pl.when(u < N)
            def _():
                s1_peer(u).start()
                s1_outer(u).start()

            @pl.when((u >= N) & (u < N + 2))
            def _():
                combine(u - 2)

            finish(u)

            @pl.when((u >= 1) & (u <= N))
            def _():
                mlp_home(u - 1)

            forward(u)

        @pl.when(is_outer & (u < N))
        def _():
            for k in (0, 1):
                b = inner - 1 if k == 0 else 2 - inner
                with jax.named_scope('w_ag_outer'):
                    ag_wait(b, u)

                @pl.when(u >= 2)
                def _():
                    s3_copy(u - 2, b).wait_send()
                mlp_outer(u, b)
                s3_copy(u, b).start()

        return carry

    def out_fwd(mb, p, sem):
        return rcopy(out_ref.at[mb], out_ref.at[mb], ofs.at[mb, p], sem, pp=p)

    lax.fori_loop(0, N + 2, body, 0)

    last_here = (s == n_stages - 1) & (z == NJ - 1)

    @pl.when(last_here)
    def _():
        for mb in (n_mb - 2, n_mb - 1):
            local(out_ref.at[mb], out_ref.at[mb], outr.at[mb]).wait()
            out_fwd(mb, 2, outf).start()

    def od_copy(v):
        return rcopy(hin_hbm.at[v], out_ref.at[2 * (v // NJ) + hb], od.at[v], outr.at[2 * (v // NJ) + hb], tp=lax.rem(v, NJ))

    @pl.when(s == 1)
    def _():
        def spread(v, carry):
            vj = lax.rem(v, NJ)
            mine = 2 * (v // NJ) + hb

            @pl.when(is_home)
            def _():
                local(hin_hbm.at[v], hin_hbm.at[v], op.at[v]).wait()

            @pl.when(is_home & (vj != z))
            def _():
                od_copy(v).start()

            @pl.when(is_home & (vj == z))
            def _():
                c = local(hin_hbm.at[v], hin.at[0], hv_sem)
                c.start()
                c.wait()
                c = local(hin.at[0], out_ref.at[mine], hv_sem)
                c.start()
                c.wait()

            @pl.when(vj == z)
            def _():
                for b in (0, 1):
                    mb = 2 * (v // NJ) + b

                    @pl.when(z - 1 != b)
                    def _(mb=mb):
                        local(out_ref.at[mb], out_ref.at[mb], outr.at[mb]).wait()
                    out_fwd(mb, 0, outf).start()

                    @pl.when(v < N - 1)
                    def _(mb=mb):
                        out_fwd(mb, 3, outf).start()
                        out_fwd(mb, 2, outf).start()
            return carry
        lax.fori_loop(0, N, spread, 0)

    @pl.when(is_home)
    def _():
        s4_copy(N - 1).wait_send()
        hin_copy(N - 1).wait_send()

        @pl.when(s == n_stages - 1)
        def _():
            last_copy().wait_send()

    @pl.when(is_outer)
    def _():
        for b in (0, 1):
            s3_copy(N - 2, b).wait_send()
            s3_copy(N - 1, b).wait_send()

    @pl.when(s == 1)
    def _():
        for m in PM:
            y_send(0, m).wait_send()

        @pl.when(is_outer)
        def _():
            for m in PM:
                y_send(1, m).wait_send()

    @pl.when((s == 3) & is_home)
    def _():
        for m in PM:
            pp_send(m).wait_send()
            pf_send(m).wait_send()
            pxf_send(1, m).wait_send()
            for r, i in ((0, 0), (0, 1), (1, 0), (1, 1), (2, 0)):
                push(r, m, i).wait_send()

    @pl.when(is_home)
    def _():
        def sent(m):
            p_send(m).wait_send()
            f_send(m).wait_send()
            x_send(1, m).wait_send()
        for m in range(4):
            direct(m, functools.partial(sent, m))
            x_send(2, m).wait_send()

        @pl.when(s == 2)
        def _():
            for w in range(NW):
                for j in range(NJ):
                    @pl.when(z != j)
                    def _():
                        x_pass(w, j).wait_send()

        @pl.when(s == 1)
        def _():
            def spread_done(v, carry):
                @pl.when(lax.rem(v, NJ) != z)
                def _():
                    od_copy(v).wait_send()
                return carry
            lax.fori_loop(0, N, spread_done, 0)

    for w in range(NW):
        x_each(w, lambda c: c.wait_send())

    @pl.when(s == 1)
    def _():
        for mb in range(n_mb):
            out_fwd(mb, 0, outf).wait_send()
            if mb < n_mb - 2:
                out_fwd(mb, 3, outf).wait_send()
                out_fwd(mb, 2, outf).wait_send()
            else:
                @pl.when(z < NJ - 1)
                def _(mb=mb):
                    out_fwd(mb, 3, outf).wait_send()
                    out_fwd(mb, 2, outf).wait_send()

    @pl.when(last_here)
    def _():
        for mb in (n_mb - 2, n_mb - 1):
            out_fwd(mb, 2, outf).wait_send()
        early = out_ref.at[pl.ds(0, n_mb - 2)]
        local(early, early, outf).wait()

    @pl.when((s == n_stages - 1) & (z < NJ - 1))
    def _():
        local(out_ref, out_ref, outf).wait()

    @pl.when((s == 0) | (s == 2))
    def _():
        local(out_ref, out_ref, outf).wait()


def solution(mesh):
    n_stages = mesh.shape['pp']

    def stage_program(hidden_in, seg_ids, positions, attn_norm, w_query, w_key, w_value, w_out, mlp_norm, w_gate, w_up, w_down):
        n_mb, T, D = hidden_in.shape
        S = seg_ids.shape[1]
        QL = w_query.shape[2]
        FL = w_gate.shape[2]
        NJ = S // T
        N = (n_mb // 2) * NJ
        NB = max(1, FL // 512)
        invf = jnp.asarray(np.tile(rope_freqs(), 2)[None, :], F32)
        any_spec = pl.BlockSpec(memory_space=pl.ANY)
        vmem = pl.BlockSpec(memory_space=pltpu.VMEM)
        dma = pltpu.SemaphoreType.DMA
        scratch = [
            pltpu.VMEM((NB, D, FL // NB), BF16), pltpu.VMEM((NB, D, FL // NB), BF16), pltpu.VMEM((NB, FL, D // NB), BF16),
            pltpu.VMEM((3, D, QL), BF16), pltpu.VMEM((2, 3, D, QL), BF16),
            pltpu.VMEM((3, 2 * T, D), BF16),
            pltpu.VMEM((2, 2 * T, D), BF16),
            pltpu.VMEM((2, T, D), BF16),
            pltpu.VMEM((4, S, QL), BF16), pltpu.VMEM((4, S, QL), BF16),
            pltpu.VMEM((3, T, D), BF16),
            pltpu.VMEM((3, T, D), BF16),
            pltpu.VMEM((2 * T, D), F32),
            pltpu.VMEM((T, D), F32),
            pltpu.VMEM((T, D), BF16),
            pltpu.VMEM((T, D), BF16),
            pltpu.VMEM((2 * T, max(D, FL, 4 * QL)), BF16),
            pltpu.VMEM((2, T, QL), BF16),
            pltpu.VMEM((n_mb // 2, S, HEAD_DIM), F32),
            pltpu.VMEM((T, S), F32), pltpu.VMEM((QL // HEAD_DIM, T, S), F32), pltpu.VMEM((QL // HEAD_DIM, T, S), BF16),
            dma((3, 8)), dma((2, 4)), dma((8,)), dma((4,)), dma((2, 4)),
            dma((N,)), dma((n_mb // 2, 2)), dma((2, 3)), dma((2,)), dma, dma((2, 2)), dma((2, 2)), dma((2,)), dma, dma,
            dma((n_mb,)), dma, dma((n_mb, n_stages)),
            dma((3,)), dma((2, 3)), dma, dma((3, NB)), dma, dma, dma((N,)), dma((n_mb // 2, NJ)), dma((N,)), dma((N,)),
            dma((4,)), dma((4,)), dma((4,)), dma((4,)), dma((2,)), dma((2,)), dma((2,)), dma((2,)), dma((2, 2)), dma((2, 2)), dma((3, 2, 2)),
            pltpu.SemaphoreType.REGULAR, pltpu.SemaphoreType.REGULAR,
        ]
        return pl.pallas_call(
            functools.partial(kernel, n_stages),
            out_shape=[jax.ShapeDtypeStruct(hidden_in.shape, BF16), jax.ShapeDtypeStruct((3, 3, D, QL), BF16),
                       jax.ShapeDtypeStruct((4 * QL, D), BF16), jax.ShapeDtypeStruct((N, T, D), BF16),
                       jax.ShapeDtypeStruct((4, D, QL), BF16), jax.ShapeDtypeStruct((4 * QL, D), BF16)],
            in_specs=[any_spec, vmem, vmem, vmem, vmem, vmem] + [any_spec] * 7,
            out_specs=[any_spec] * 6,
            scratch_shapes=scratch,
            compiler_params=pltpu.CompilerParams(collective_id=0, has_side_effects=True, vmem_limit_bytes=67_043_328),
        )(hidden_in, seg_ids, positions, invf, attn_norm, mlp_norm, w_query, w_key, w_value, w_out, w_gate, w_up, w_down)[0]

    act_spec = P('dp', 'tp', None)
    row_spec = P('dp', None)
    gain_spec = P('pp', None)
    col_spec = P('pp', None, 'tp')
    rows_spec = P('pp', 'tp', None)
    return jax.shard_map(stage_program, mesh=mesh,
                         in_specs=(act_spec, row_spec, row_spec, gain_spec, col_spec, col_spec, col_spec, rows_spec, gain_spec, col_spec, col_spec, rows_spec),
                         out_specs=act_spec, check_vma=False)
```

```python
import functools
import math

import jax
import jax.numpy as jnp
import numpy as np
from jax import lax
from jax.experimental import pallas as pl
from jax.experimental.pallas import tpu as pltpu
from jax.sharding import PartitionSpec as P

HEAD_DIM = 128
NORM_EPS = 1e-5
ROPE_THETA = 500000.0
ROPE_FACTOR = 8.0
LOW_FREQ = 1.0
HIGH_FREQ = 4.0
ORIG_CTX = 8192.0
NEG = -1e30
MESH = pl.DeviceIdType.MESH
F32 = jnp.float32
BF16 = jnp.bfloat16


def rope_freqs():
    base_freq = 1.0 / (ROPE_THETA ** (np.arange(0, HEAD_DIM, 2) / HEAD_DIM))
    wavelen = 2.0 * np.pi / base_freq
    smooth = (ORIG_CTX / wavelen - LOW_FREQ) / (HIGH_FREQ - LOW_FREQ)
    blended = (1.0 - smooth) * base_freq / ROPE_FACTOR + smooth * base_freq
    scaled = np.where(wavelen > ORIG_CTX / LOW_FREQ, base_freq / ROPE_FACTOR, blended)
    return np.where(wavelen < ORIG_CTX / HIGH_FREQ, base_freq, scaled)


def kernel(n_stages, x_ref, seg_ref, pos_ref, invf_ref, ga_ref, gm_ref,
           wq_ref, wk_ref, wv_ref, wo_ref, wg_ref, wu_ref, wd_ref,
           out_ref,
           wqkv_hbm, wo_hbm, hin_hbm, pv_hbm, po_hbm,
           wg_s, wu_s, wd_s, wres, wst, gb, px, ps, kc, vc, hin, h1b, pacc, oacc, sendb, h2b, act, qb,
           table, mask, sbuf, pbuf,
           wr, wx, wsnd, wfwd, wxs, hin_sem, xs, ag, s1s, s2s, pxr, pxs, psr, s4s, s5s, outr, outf, ofs,
           wres_sem, wst_sem, wo_sem, mlp_sem, hv_sem, s6s, xp, xq, op, od,
           ysn, yrc, pos, por, pps, ppr, pfs, pfr, pxfs, pxfr, pds, gate, cred):
    n_mb, T, D = x_ref.shape
    QL = wq_ref.shape[2]
    FL = wg_ref.shape[2]
    NB = wg_s.shape[0]
    FB = FL // NB
    S = seg_ref.shape[1]
    NJ = S // T
    NH = QL // HEAD_DIM
    N = (n_mb // 2) * NJ
    DB = D // NB
    scale = HEAD_DIM ** -0.5
    RB = 16
    NR = 32
    HS = hin.shape[0]
    OB = wst.shape[3]
    NO = D // OB

    hx = lax.axis_index("dp")
    z = lax.axis_index("tp")
    s = lax.axis_index("pp")
    is_home = (z == 1) | (z == 2)
    is_outer = (z == 0) | (z == 3)
    hb = lax.rem(z + 1, 2) * 0 + (z - 1)
    peer = 3 - z
    outer = 3 * (z - 1)
    inner = 1 + z // 2
    odd = lax.rem(s, 2)

    def rcopy(src, dst, ssem, rsem, **dev):
        return pltpu.make_async_remote_copy(src_ref=src, dst_ref=dst, send_sem=ssem, recv_sem=rsem,
                                            device_id=dev, device_id_type=MESH)

    def local(src, dst, sem):
        return pltpu.make_async_copy(src, dst, sem)

    def column(ref, mb, j):
        row = ref[pl.ds(mb, 1), :]
        part = row[:, 0:T]
        for c in range(1, NJ):
            part = jnp.where(j == c, row[:, c * T:(c + 1) * T], part)
        return jnp.broadcast_to(part, (HEAD_DIM, T)).T

    barrier = pltpu.get_barrier_semaphore()
    for k in range(1, 4):
        pl.semaphore_signal(barrier, inc=1, device_id={"tp": lax.rem(z + k, 4)}, device_id_type=MESH)
        pl.semaphore_signal(barrier, inc=1, device_id={"pp": lax.rem(s + k, 4)}, device_id_type=MESH)
    pl.semaphore_signal(barrier, inc=1, device_id={"dp": 1 - hx}, device_id_type=MESH)
    pl.semaphore_wait(barrier, 7)

    wqkv_own = (wq_ref, wk_ref, wv_ref, wo_ref)

    def mlp_copies():
        cps = []
        for n in range(NB):
            cps.append(local(wg_ref.at[0, :, pl.ds(n * FB, FB)], wg_s.at[n], mlp_sem.at[0, n]))
            cps.append(local(wu_ref.at[0, :, pl.ds(n * FB, FB)], wu_s.at[n], mlp_sem.at[1, n]))
            cps.append(local(wd_ref.at[0, :, pl.ds(n * DB, DB)], wd_s.at[n], mlp_sem.at[2, n]))
        return cps

    NW = n_mb // 2

    def x_copy(w, home):
        u = w * NJ + z
        return rcopy(x_ref.at[2 * w + (home - 1)], hin_hbm.at[u], xs.at[w, home - 1], xp.at[u], tp=home)

    def x_each(w, act):
        for home in (1, 2):
            @pl.when((s == 2) & (z != home))
            def _():
                act(x_copy(w, home))

    def x_pass(w, j):
        u = w * NJ + j
        return rcopy(hin_hbm.at[u], hin_hbm.at[u], xq.at[w, j], hin_sem.at[u], pp=0)

    def x_relay(ws):
        @pl.when((s == 2) & is_home)
        def _():
            for w in ws:
                for j in range(NJ):
                    @pl.when(z != j)
                    def _():
                        local(hin_hbm.at[w * NJ + j], hin_hbm.at[w * NJ + j], xp.at[w * NJ + j]).wait()
                        x_pass(w, j).start()

    x_each(0, lambda c: c.start())
    x_relay([0])

    def half(ref, m, h):
        rows = (D if m < 3 else QL) // 2
        return ref.at[pl.ds(h * rows, rows), :]

    def wslot(r, m):
        return wqkv_hbm.at[r, m] if m < 3 else wo_hbm.at[pl.ds((r + 1) * QL, QL)]

    def own_w(m):
        return wqkv_own[m].at[0]

    def wo_own():
        return local(own_w(3), wo_hbm.at[pl.ds(0, QL)], wo_sem)

    def o_send(k):
        h = hx if k < 4 else 1 - hx
        return rcopy(half(own_w(k % 4), k % 4, h), half(wslot(0, k % 4), k % 4, h), wsnd.at[k], wr.at[0, k], tp=inner)

    def p_send(m):
        return rcopy(half(own_w(m), m, hx), half(wslot(1, m), m, hx), wsnd.at[m], wr.at[1, m], tp=peer)

    def f_send(m):
        return rcopy(half(wslot(0, m), m, hx), half(wslot(2, m), m, hx), wfwd.at[m], wr.at[2, m], tp=peer)

    def x_send(r, m):
        return rcopy(half(wslot(r, m), m, hx), half(wslot(r, m), m, hx), wxs.at[r - 1, m], wx.at[r - 1, m], dp=1 - hx)

    def w_ready(rs, ms):
        def pushed(m):
            if 0 in rs:
                o_send(m).wait_recv()
            if 1 in rs:
                p_send(m).wait_recv()
        for m in ms:
            if m in PM:
                pl.when(s == 1)(functools.partial(pushed, m))
            if 0 in rs:
                o_send(4 + m).wait_recv()
            for r in (1, 2):
                if r in rs:
                    x_send(r, m).wait_recv()

    PM = (2, 3)

    def pb(r, m):
        return pv_hbm.at[r] if m == 2 else po_hbm.at[pl.ds(r * QL, QL)]

    def hh(i):
        return hx if i == 0 else 1 - hx

    def y_send(i, m):
        return rcopy(half(own_w(m), m, hh(i)), half(pb(3, m), m, hh(i)), ysn.at[2 * i + m - 2], yrc.at[2 * i + m - 2], pp=3)

    def po_send(i, m):
        return rcopy(half(pb(3, m), m, hh(i)), half(pb(0, m), m, hh(i)), pos.at[2 * i + m - 2], por.at[2 * i + m - 2], tp=inner)

    def pp_send(m):
        return rcopy(half(pb(3, m), m, hx), half(pb(1, m), m, hx), pps.at[m - 2], ppr.at[m - 2], tp=peer)

    def pf_send(m):
        return rcopy(half(pb(0, m), m, hx), half(pb(2, m), m, hx), pfs.at[m - 2], pfr.at[m - 2], tp=peer)

    def pxf_send(r, m):
        return rcopy(half(pb(r, m), m, hx), half(pb(r, m), m, hx), pxfs.at[r - 1, m - 2], pxfr.at[r - 1, m - 2], dp=1 - hx)

    def push(r, m, i):
        rsem = wr.at[0, 4 * i + m] if r == 0 else (wr.at[r, m] if i == 0 else wx.at[r - 1, m])
        return rcopy(half(pb(r, m), m, hh(i)), half(wslot(r, m), m, hh(i)), pds.at[r, m - 2, i], rsem, pp=1)

    def direct(m, f):
        if m in PM:
            pl.when(s != 1)(f)
        else:
            f()

    @pl.when(s == 1)
    def _():
        for m in PM:
            y_send(0, m).start()

        @pl.when(is_outer)
        def _():
            for m in PM:
                y_send(1, m).start()

    @pl.when((s == 3) & is_outer)
    def _():
        for i in (0, 1):
            for m in PM:
                y_send(i, m).wait_recv()
                po_send(i, m).start()
        for i in (0, 1):
            for m in PM:
                po_send(i, m).wait_send()

    @pl.when((s == 3) & is_home)
    def _():
        for m in PM:
            y_send(0, m).wait_recv()
            pp_send(m).start()
        for kind, m, a in (("p", 2, 0), ("o", 2, 0), ("p", 3, 0), ("o", 3, 0), ("f", 2, 0), ("f", 3, 0), ("o", 2, 1), ("x", 2, 1),
                           ("o", 3, 1), ("x", 3, 1)):
            with jax.named_scope('wp_' + kind + str(m) + str(a)):
                if kind == "p":
                    pp_send(m).wait_recv()
                    pxf_send(1, m).start()
                    push(1, m, 0).start()
                elif kind == "o":
                    po_send(a, m).wait_recv()
                    if a == 0:
                        pf_send(m).start()
                    push(0, m, a).start()
                elif kind == "f":
                    pf_send(m).wait_recv()
                    push(2, m, 0).start()
                else:
                    pxf_send(a, m).wait_recv()
                    push(a, m, 1).start()

    @pl.when(s == 3)
    def _():
        pl.semaphore_signal(gate, inc=1, device_id={"pp": 2}, device_id_type=MESH)

    def release():
        @pl.when(odd == 0)
        def _():
            pl.semaphore_signal(gate, inc=1, device_id={"pp": s + 1}, device_id_type=MESH)

    @pl.when(s != 0)
    def _():
        for c in mlp_copies():
            c.start()
        with jax.named_scope('w_gate'):
            pl.semaphore_wait(gate, 1)

    if NW > 1:
        x_each(1, lambda c: c.start())

    @pl.when(is_outer)
    def _():
        for k in range(8):
            direct(k % 4, lambda k=k: o_send(k).start())

        @pl.when(s == 0)
        def _():
            for c in mlp_copies():
                c.start()
        for k in range(8):
            direct(k % 4, lambda k=k: o_send(k).wait_send())
        release()
        for w in range(2, NW):
            x_each(w, lambda c: c.start())

    @pl.when(is_home)
    def _():
        for m in range(4):
            direct(m, lambda m=m: p_send(m).start())
        wo_own().start()

        @pl.when(s == 0)
        def _():
            for c in mlp_copies():
                c.start()
        def zero_rows(b, carry):
            for i in range(4):
                kc[i, pl.ds(b * RB, RB), :] = jnp.zeros((RB, QL), BF16)
                vc[i, pl.ds(b * RB, RB), :] = jnp.zeros((RB, QL), BF16)
            return carry
        lax.fori_loop(0, S // RB, zero_rows, 0)

        def tables(w):
            lane = lax.broadcasted_iota(jnp.int32, (T, HEAD_DIM), 1)

            def table_rows(b, carry):
                rows = pl.ds(pl.multiple_of(b * T, T), T)
                ang = column(pos_ref, 2 * w + hb, b).astype(F32) * invf_ref[0:1, :]
                table[w, rows, :] = jnp.where(lane < HEAD_DIM // 2, jnp.cos(ang), jnp.sin(ang))
                return carry
            with jax.named_scope('table'):
                lax.fori_loop(0, NJ, table_rows, 0)

        steps = [("o", 0), ("p", 0), ("t", 0), ("o", 1), ("p", 1), ("t", 1), ("o", 2), ("p", 2), ("t", 2), ("o", 3), ("p", 3), ("t", 3),
                 ("f", 0), ("f", 1), ("f", 2), ("f", 3), ("g", 0), ("r", 0)]

        def step(kind, m):
            if kind == "o":
                o_send(m).wait_recv()
                f_send(m).start()
            elif kind == "p":
                p_send(m).wait_recv()
                x_send(1, m).start()
            else:
                f_send(m).wait_recv()
                x_send(2, m).start()

        @pl.when(s == 1)
        def _():
            for m in PM:
                step("f", m)

        for kind, m in steps:
            with jax.named_scope('w_' + kind + str(m)):
                if kind in "op":
                    direct(m, lambda kind=kind, m=m: step(kind, m))
                elif kind == "f" and m in PM:
                    pl.when(s != 1)(functools.partial(step, kind, m))
                elif kind == "f":
                    step(kind, m)
                elif kind == "g":
                    release()
                elif kind == "r":
                    x_relay([1] if NW > 1 else [])
                elif m < n_mb // 2:
                    tables(m)
        for w in range(2, NW):
            x_each(w, lambda c: c.start())
        w_ready([0, 1], range(3))
        x_relay(range(2, NW))

    def gslot(g, u):
        return lax.rem(g - 1 + u, 2)

    def group_copies(g, u):
        if g == 0:
            return [local(own_w(m), wres.at[m], wres_sem.at[m]) for m in range(3)]
        p = gslot(g, u)
        if g < 4:
            return [local(wqkv_hbm.at[g - 1], wst.at[p], wst_sem.at[p, 0])]
        return [local(wo_hbm.at[:, pl.ds(((g - 4) * 3 + m) * OB, OB)], wst.at[p, m], wst_sem.at[p, m]) for m in range(3 if g == 4 else 1)]

    def group_start(g, u):
        for c in group_copies(g, u):
            c.start()

    def group_wait(g, u):
        for c in group_copies(g, u):
            c.wait()

    def h_fetch(u):
        mb = 2 * (u // NJ) + hb
        here = lax.rem(u, NJ) == z
        dst = hin.at[lax.rem(u, HS)]

        @pl.when((s == 0) & here)
        def _():
            local(x_ref.at[mb], dst, hv_sem).start()

        @pl.when((s == 0) & jnp.logical_not(here))
        def _():
            local(hin_hbm.at[u], hin_hbm.at[u], hin_sem.at[u]).wait()
            local(hin_hbm.at[u], dst, hv_sem).start()

    @pl.when(is_home)
    def _():
        group_start(0, 0)
        group_start(1, 0)
        group_start(2, 0)
        h_fetch(0)

    for c in mlp_copies():
        c.wait()

    def hin_copy(u):
        return rcopy(h2b, hin.at[lax.rem(u, HS)], s5s, hin_sem.at[u], pp=lax.rem(s + 1, n_stages))

    def s1_outer(u):
        blk = gb.at[lax.rem(u, 3), pl.ds(pl.multiple_of(hb * T, T), T), :]
        return rcopy(blk, blk, s1s.at[0], ag.at[hb, lax.rem(u, 3)], tp=outer)

    def s1_peer(u):
        blk = gb.at[lax.rem(u, 3), pl.ds(pl.multiple_of(hb * T, T), T), :]
        return rcopy(blk, blk, s1s.at[1], ag.at[hb, lax.rem(u, 3)], tp=peer)

    def s2_copy(u):
        blk = gb.at[lax.rem(u, 3), pl.ds(pl.multiple_of((1 - hb) * T, T), T), :]
        return rcopy(blk, blk, s2s, ag.at[1 - hb, lax.rem(u, 3)], tp=outer)

    def ag_wait(b, u):
        blk = gb.at[lax.rem(u, 3), pl.ds(pl.multiple_of(b * T, T), T), :]
        local(blk, blk, ag.at[b, lax.rem(u, 3)]).wait()

    def s3_copy(u, b):
        sl = lax.rem(u, 2)
        blk = px.at[sl, pl.ds(pl.multiple_of(b * T, T), T), :]
        return rcopy(blk, blk, pxs.at[sl, b], pxr.at[sl, b], tp=inner)

    def s4_copy(u):
        return rcopy(sendb, ps.at[lax.rem(u, 2)], s4s, psr.at[lax.rem(u, 2)], tp=peer)

    def park_copy(u):
        return rcopy(h2b, hin_hbm.at[u], s5s, op.at[u], pp=1)

    def last_copy():
        mb = n_mb - 2 + hb
        return rcopy(h2b, out_ref.at[mb], s6s, outr.at[mb], tp=NJ - 1)

    def norm_rows(src, gain, dst):
        hf = src.astype(F32)
        inv = lax.rsqrt(jnp.mean(hf * hf, axis=-1, keepdims=True) + NORM_EPS)
        return (hf * inv * gain.astype(F32)).astype(BF16)

    def attention(u):
      with jax.named_scope('attn'):
        attention_(u)

    def attention_(u):
        w = u // NJ
        j = lax.rem(u, NJ)
        mb = 2 * w + hb
        row0 = pl.multiple_of(j * T, T)
        hs = lax.rem(u, HS)

        with jax.named_scope('w_hin'):
            @pl.when(s == 0)
            def _():
                local(x_ref.at[mb], hin.at[hs], hv_sem).wait()

            @pl.when(s > 0)
            def _():
                hin_copy(u).wait_recv()

        def norm_a(b, carry):
            rows = pl.ds(b * NR, NR)
            act[pl.ds(pl.multiple_of(T + b * NR, NR), NR), 0:D] = norm_rows(hin[hs, rows, :], ga_ref[0:1, :], None)
            return carry
        lax.fori_loop(0, T // NR, norm_a, 0)

        segrow = seg_ref[pl.ds(mb, 1), :]
        segc = column(seg_ref, mb, j)
        ti = lax.broadcasted_iota(jnp.int32, (T, HEAD_DIM), 0) + row0
        for c in range(0, S, HEAD_DIM):
            segr = segrow[:, c:c + HEAD_DIM]
            ui = lax.broadcasted_iota(jnp.int32, (T, HEAD_DIM), 1) + c
            mask[:, c:c + HEAD_DIM] = jnp.where((segc == segr) & (ui <= ti), 1.0, 0.0)

        def rope(val):
            pk = table[w, pl.ds(row0, T), :]
            lane = lax.broadcasted_iota(jnp.int32, (T, HEAD_DIM), 1)
            swapped = pltpu.roll(pk, HEAD_DIM // 2, 1)
            cosw = jnp.where(lane < HEAD_DIM // 2, pk, swapped)
            sinw = jnp.where(lane < HEAD_DIM // 2, -swapped, pk)
            outs = []
            for h in range(NH):
                v = val[:, h * HEAD_DIM:(h + 1) * HEAD_DIM]
                outs.append((v * cosw + pltpu.roll(v, HEAD_DIM // 2, 1) * sinw).astype(BF16))
            return outs

        def hcols(h):
            return slice(h * HEAD_DIM, (h + 1) * HEAD_DIM)

        def proj(i):
            p = i % 2

            def w(m):
                return wres[m] if i == 0 else wst[gslot(i, u), m]
            for h, val in enumerate(rope(jnp.dot(act[T:2 * T, 0:D], w(0), preferred_element_type=F32))):
                qb[p, :, hcols(h)] = val
            for h, val in enumerate(rope(jnp.dot(act[T:2 * T, 0:D], w(1), preferred_element_type=F32))):
                kc[i, pl.ds(row0, T), hcols(h)] = val
            vc[i, pl.ds(row0, T), :] = jnp.dot(act[T:2 * T, 0:D], w(2), preferred_element_type=F32).astype(BF16)

        def heads(i):
            for h in range(NH):
                sc = lax.dot_general(qb[i % 2, :, hcols(h)], kc[i, :, hcols(h)], (((1,), (1,)), ((), ())),
                                     preferred_element_type=F32) * scale
                sbuf[h] = jnp.where(mask[...] > 0.5, sc, NEG)
            for h in range(NH):
                for r in range(0, T, 32):
                    sc = sbuf[h, r:r + 32, :]
                    e = jnp.exp(sc - jnp.max(sc, axis=-1, keepdims=True))
                    pbuf[h, r:r + 32, :] = (e * (1.0 / jnp.sum(e, axis=-1, keepdims=True))).astype(BF16)
            for h in range(NH):
                act[0:T, i * QL + h * HEAD_DIM:i * QL + (h + 1) * HEAD_DIM] = jnp.dot(
                    pbuf[h], vc[i, :, hcols(h)], preferred_element_type=F32).astype(BF16)

        with jax.named_scope('shards'):
            @pl.when(u == 0)
            def _():
                group_wait(0, u)
            proj(0)

            @pl.when(u >= 2)
            def _():
                combine(u - 2)
            for i in range(3):
                group_wait(i + 1, u)
                proj(i + 1)
                if i < 2:
                    @pl.when(u == 0)
                    def _():
                        if i == 0:
                            w_ready([2], range(3))
                        else:
                            w_ready([0, 1, 2], [3])
                            wo_own().wait()
                group_start(i + 3, u)
                heads(i)
                if i == 0:
                    @pl.when(u < N - 1)
                    def _():
                        h_fetch(u + 1)
            heads(3)

        with jax.named_scope('wo'):
            def wo_block(n, w):
                act[T:2 * T, n * OB:(n + 1) * OB] = jnp.dot(act[0:T, 0:4 * QL], w, preferred_element_type=F32).astype(BF16)

            group_wait(4, u)
            for n in range(3):
                wo_block(n, wst[gslot(4, u), n])

            group_wait(5, u)
            wo_block(3, wst[gslot(5, u), 0])

            @pl.when(u < N - 1)
            def _():
                group_start(1, u + 1)
                group_start(2, u + 1)

        def norm_b(b, carry):
            rows = pl.ds(b * NR, NR)
            h1 = (hin[hs, rows, :].astype(F32) + act[pl.ds(pl.multiple_of(T + b * NR, NR), NR), 0:D].astype(F32)).astype(BF16)
            h1b[lax.rem(u, 3), rows, :] = h1
            gb[lax.rem(u, 3), pl.ds(pl.multiple_of(hb * T + b * NR, NR), NR), :] = norm_rows(h1, gm_ref[0:1, :], None)
            return carry
        lax.fori_loop(0, T // NR, norm_b, 0)

        @pl.when((s > 0) & (u < N - HS))
        def _():
            pl.semaphore_signal(cred, inc=1, device_id={"pp": s - 1}, device_id_type=MESH)

    def mlp(sl, row0, rows, store):
        UN = 2 if NB % 2 == 0 else 1

        def up(q, carry):
            for n in [q * UN + k for k in range(UN)]:
                xin = gb[sl, pl.ds(row0, rows), :]
                g = jnp.dot(xin, wg_s[n], preferred_element_type=F32)
                u_ = jnp.dot(xin, wu_s[n], preferred_element_type=F32)
                act[0:rows, pl.ds(pl.multiple_of(n * FB, FB), FB)] = (jax.nn.silu(g) * u_).astype(BF16)
            return carry
        lax.fori_loop(0, NB // UN, up, 0)

        def down(q, carry):
            for n in [q * UN + k for k in range(UN)]:
                store(pl.ds(pl.multiple_of(n * DB, DB), DB), jnp.dot(act[0:rows, 0:FL], wd_s[n], preferred_element_type=F32))
            return carry
        lax.fori_loop(0, NB // UN, down, 0)

    def mlp_home(u):
        def store(c, val):
            pacc[:, c] = val
        with jax.named_scope('mlp'):
            mlp(lax.rem(u, 3), 0, 2 * T, store)

    def mlp_outer(u, b):
        def store(c, val):
            px[lax.rem(u, 2), pl.ds(pl.multiple_of(b * T, T), T), c] = val.astype(BF16)
        with jax.named_scope('mlp_o'):
            mlp(lax.rem(u, 3), pl.multiple_of(b * T, T), T, store)

    def forward(u):
        @pl.when((u >= 1) & (u <= N))
        def _():
            s2_copy(u - 1).wait_send()

        @pl.when(u < N)
        def _():
            with jax.named_scope('w_ag'):
                ag_wait(1 - hb, u)
            s2_copy(u).start()

    def combine(v):
        sl = lax.rem(v, 2)
        with jax.named_scope('w_s3'):
            s3_copy(v, 0).wait_recv()
            s3_copy(v, 1).wait_recv()

        @pl.when(v >= 1)
        def _():
            s4_copy(v - 1).wait_send()

        def comb(b, carry):
            rows = pl.ds(b * RB, RB)
            mine = pl.ds(pl.multiple_of(hb * T + b * RB, RB), RB)
            theirs = pl.ds(pl.multiple_of((1 - hb) * T + b * RB, RB), RB)
            oacc[rows, :] = pacc[mine, :] + px[sl, mine, :].astype(F32)
            sendb[rows, :] = (pacc[theirs, :] + px[sl, theirs, :].astype(F32)).astype(BF16)
            return carry
        lax.fori_loop(0, T // RB, comb, 0)
        s4_copy(v).start()

    def finish(u):
        @pl.when((u >= 2) & (u < N + 2))
        def _():
            v = u - 2
            with jax.named_scope('w_s4'):
                s4_copy(v).wait_recv()
            vw = v // NJ
            vj = lax.rem(v, NJ)

            @pl.when(v >= 1)
            def _():
                hin_copy(v).wait_send()

            def fin(b, carry):
                rows = pl.ds(b * RB, RB)
                d = (oacc[rows, :] + ps[lax.rem(v, 2), rows, :].astype(F32)).astype(BF16)
                h2b[rows, :] = (h1b[lax.rem(v, 3), rows, :].astype(F32) + d.astype(F32)).astype(BF16)
                return carry
            lax.fori_loop(0, T // RB, fin, 0)

            @pl.when((s < n_stages - 1) & (v >= HS))
            def _():
                with jax.named_scope('w_cred'):
                    pl.semaphore_wait(cred, 1)

            @pl.when(s < n_stages - 1)
            def _():
                hin_copy(v).start()

            @pl.when(s == n_stages - 1)
            def _():
                park_copy(v).start()

            @pl.when((s == n_stages - 1) & (v == N - 1))
            def _():
                last_copy().start()

    def body(u, carry):
        @pl.when(is_home)
        def _():
            @pl.when(u < N)
            def _():
                attention(u)

            @pl.when((u >= 1) & (u <= N))
            def _():
                s1_outer(u - 1).wait_send()
                s1_peer(u - 1).wait_send()

            @pl.when(u < N)
            def _():
                s1_peer(u).start()
                s1_outer(u).start()

            @pl.when((u >= N) & (u < N + 2))
            def _():
                combine(u - 2)

            finish(u)

            @pl.when((u >= 1) & (u <= N))
            def _():
                mlp_home(u - 1)

            forward(u)

        @pl.when(is_outer & (u < N))
        def _():
            for k in (0, 1):
                b = inner - 1 if k == 0 else 2 - inner
                with jax.named_scope('w_ag_outer'):
                    ag_wait(b, u)

                @pl.when(u >= 2)
                def _():
                    s3_copy(u - 2, b).wait_send()
                mlp_outer(u, b)
                s3_copy(u, b).start()

        return carry

    def out_fwd(mb, p, sem):
        return rcopy(out_ref.at[mb], out_ref.at[mb], ofs.at[mb, p], sem, pp=p)

    lax.fori_loop(0, N + 2, body, 0)

    last_here = (s == n_stages - 1) & (z == NJ - 1)

    @pl.when(last_here)
    def _():
        for mb in (n_mb - 2, n_mb - 1):
            local(out_ref.at[mb], out_ref.at[mb], outr.at[mb]).wait()
            out_fwd(mb, 2, outf).start()

    def od_copy(v):
        return rcopy(hin_hbm.at[v], out_ref.at[2 * (v // NJ) + hb], od.at[v], outr.at[2 * (v // NJ) + hb], tp=lax.rem(v, NJ))

    @pl.when(s == 1)
    def _():
        def spread(v, carry):
            vj = lax.rem(v, NJ)
            mine = 2 * (v // NJ) + hb

            @pl.when(is_home)
            def _():
                local(hin_hbm.at[v], hin_hbm.at[v], op.at[v]).wait()

            @pl.when(is_home & (vj != z))
            def _():
                od_copy(v).start()

            @pl.when(is_home & (vj == z))
            def _():
                c = local(hin_hbm.at[v], hin.at[0], hv_sem)
                c.start()
                c.wait()
                c = local(hin.at[0], out_ref.at[mine], hv_sem)
                c.start()
                c.wait()

            @pl.when(vj == z)
            def _():
                for b in (0, 1):
                    mb = 2 * (v // NJ) + b

                    @pl.when(z - 1 != b)
                    def _(mb=mb):
                        local(out_ref.at[mb], out_ref.at[mb], outr.at[mb]).wait()
                    out_fwd(mb, 0, outf).start()

                    @pl.when(v < N - 1)
                    def _(mb=mb):
                        out_fwd(mb, 3, outf).start()
                        out_fwd(mb, 2, outf).start()
            return carry
        lax.fori_loop(0, N, spread, 0)

    @pl.when(is_home)
    def _():
        s4_copy(N - 1).wait_send()
        hin_copy(N - 1).wait_send()

        @pl.when(s == n_stages - 1)
        def _():
            last_copy().wait_send()

    @pl.when(is_outer)
    def _():
        for b in (0, 1):
            s3_copy(N - 2, b).wait_send()
            s3_copy(N - 1, b).wait_send()

    @pl.when(s == 1)
    def _():
        for m in PM:
            y_send(0, m).wait_send()

        @pl.when(is_outer)
        def _():
            for m in PM:
                y_send(1, m).wait_send()

    @pl.when((s == 3) & is_home)
    def _():
        for m in PM:
            pp_send(m).wait_send()
            pf_send(m).wait_send()
            pxf_send(1, m).wait_send()
            for r, i in ((0, 0), (0, 1), (1, 0), (1, 1), (2, 0)):
                push(r, m, i).wait_send()

    @pl.when(is_home)
    def _():
        def sent(m):
            p_send(m).wait_send()
            f_send(m).wait_send()
            x_send(1, m).wait_send()
        for m in range(4):
            direct(m, functools.partial(sent, m))
            x_send(2, m).wait_send()

        @pl.when(s == 2)
        def _():
            for w in range(NW):
                for j in range(NJ):
                    @pl.when(z != j)
                    def _():
                        x_pass(w, j).wait_send()

        @pl.when(s == 1)
        def _():
            def spread_done(v, carry):
                @pl.when(lax.rem(v, NJ) != z)
                def _():
                    od_copy(v).wait_send()
                return carry
            lax.fori_loop(0, N, spread_done, 0)

    for w in range(NW):
        x_each(w, lambda c: c.wait_send())

    @pl.when(s == 1)
    def _():
        for mb in range(n_mb):
            out_fwd(mb, 0, outf).wait_send()
            if mb < n_mb - 2:
                out_fwd(mb, 3, outf).wait_send()
                out_fwd(mb, 2, outf).wait_send()
            else:
                @pl.when(z < NJ - 1)
                def _(mb=mb):
                    out_fwd(mb, 3, outf).wait_send()
                    out_fwd(mb, 2, outf).wait_send()

    @pl.when(last_here)
    def _():
        for mb in (n_mb - 2, n_mb - 1):
            out_fwd(mb, 2, outf).wait_send()
        early = out_ref.at[pl.ds(0, n_mb - 2)]
        local(early, early, outf).wait()

    @pl.when((s == n_stages - 1) & (z < NJ - 1))
    def _():
        local(out_ref, out_ref, outf).wait()

    @pl.when((s == 0) | (s == 2))
    def _():
        local(out_ref, out_ref, outf).wait()


def solution(mesh):
    n_stages = mesh.shape['pp']

    def stage_program(hidden_in, seg_ids, positions, attn_norm, w_query, w_key, w_value, w_out, mlp_norm, w_gate, w_up, w_down):
        n_mb, T, D = hidden_in.shape
        S = seg_ids.shape[1]
        QL = w_query.shape[2]
        FL = w_gate.shape[2]
        NJ = S // T
        N = (n_mb // 2) * NJ
        NB = max(1, FL // 512)
        invf = jnp.asarray(np.tile(rope_freqs(), 2)[None, :], F32)
        any_spec = pl.BlockSpec(memory_space=pl.ANY)
        vmem = pl.BlockSpec(memory_space=pltpu.VMEM)
        dma = pltpu.SemaphoreType.DMA
        scratch = [
            pltpu.VMEM((NB, D, FL // NB), BF16), pltpu.VMEM((NB, D, FL // NB), BF16), pltpu.VMEM((NB, FL, D // NB), BF16),
            pltpu.VMEM((3, D, QL), BF16), pltpu.VMEM((2, 3, D, QL), BF16),
            pltpu.VMEM((3, 2 * T, D), BF16),
            pltpu.VMEM((2, 2 * T, D), BF16),
            pltpu.VMEM((2, T, D), BF16),
            pltpu.VMEM((4, S, QL), BF16), pltpu.VMEM((4, S, QL), BF16),
            pltpu.VMEM((3, T, D), BF16),
            pltpu.VMEM((3, T, D), BF16),
            pltpu.VMEM((2 * T, D), F32),
            pltpu.VMEM((T, D), F32),
            pltpu.VMEM((T, D), BF16),
            pltpu.VMEM((T, D), BF16),
            pltpu.VMEM((2 * T, max(D, FL, 4 * QL)), BF16),
            pltpu.VMEM((2, T, QL), BF16),
            pltpu.VMEM((n_mb // 2, S, HEAD_DIM), F32),
            pltpu.VMEM((T, S), F32), pltpu.VMEM((QL // HEAD_DIM, T, S), F32), pltpu.VMEM((QL // HEAD_DIM, T, S), BF16),
            dma((3, 8)), dma((2, 4)), dma((8,)), dma((4,)), dma((2, 4)),
            dma((N,)), dma((n_mb // 2, 2)), dma((2, 3)), dma((2,)), dma, dma((2, 2)), dma((2, 2)), dma((2,)), dma, dma,
            dma((n_mb,)), dma, dma((n_mb, n_stages)),
            dma((3,)), dma((2, 3)), dma, dma((3, NB)), dma, dma, dma((N,)), dma((n_mb // 2, NJ)), dma((N,)), dma((N,)),
            dma((4,)), dma((4,)), dma((4,)), dma((4,)), dma((2,)), dma((2,)), dma((2,)), dma((2,)), dma((2, 2)), dma((2, 2)), dma((3, 2, 2)),
            pltpu.SemaphoreType.REGULAR, pltpu.SemaphoreType.REGULAR,
        ]
        return pl.pallas_call(
            functools.partial(kernel, n_stages),
            out_shape=[jax.ShapeDtypeStruct(hidden_in.shape, BF16), jax.ShapeDtypeStruct((3, 3, D, QL), BF16),
                       jax.ShapeDtypeStruct((4 * QL, D), BF16), jax.ShapeDtypeStruct((N, T, D), BF16),
                       jax.ShapeDtypeStruct((4, D, QL), BF16), jax.ShapeDtypeStruct((4 * QL, D), BF16)],
            in_specs=[any_spec, vmem, vmem, vmem, vmem, vmem] + [any_spec] * 7,
            out_specs=[any_spec] * 6,
            scratch_shapes=scratch,
            compiler_params=pltpu.CompilerParams(collective_id=0, has_side_effects=True, vmem_limit_bytes=67_043_328),
        )(hidden_in, seg_ids, positions, invf, attn_norm, mlp_norm, w_query, w_key, w_value, w_out, w_gate, w_up, w_down)[0]

    act_spec = P('dp', 'tp', None)
    row_spec = P('dp', None)
    gain_spec = P('pp', None)
    col_spec = P('pp', None, 'tp')
    rows_spec = P('pp', 'tp', None)
    return jax.shard_map(stage_program, mesh=mesh,
                         in_specs=(act_spec, row_spec, row_spec, gain_spec, col_spec, col_spec, col_spec, rows_spec, gain_spec, col_spec, col_spec, rows_spec),
                         out_specs=act_spec, check_vma=False)
```

```python
import functools
import math

import jax
import jax.numpy as jnp
import numpy as np
from jax import lax
from jax.experimental import pallas as pl
from jax.experimental.pallas import tpu as pltpu
from jax.sharding import PartitionSpec as P

HEAD_DIM = 128
NORM_EPS = 1e-5
ROPE_THETA = 500000.0
ROPE_FACTOR = 8.0
LOW_FREQ = 1.0
HIGH_FREQ = 4.0
ORIG_CTX = 8192.0
NEG = -1e30
MESH = pl.DeviceIdType.MESH
F32 = jnp.float32
BF16 = jnp.bfloat16


def rope_freqs():
    base_freq = 1.0 / (ROPE_THETA ** (np.arange(0, HEAD_DIM, 2) / HEAD_DIM))
    wavelen = 2.0 * np.pi / base_freq
    smooth = (ORIG_CTX / wavelen - LOW_FREQ) / (HIGH_FREQ - LOW_FREQ)
    blended = (1.0 - smooth) * base_freq / ROPE_FACTOR + smooth * base_freq
    scaled = np.where(wavelen > ORIG_CTX / LOW_FREQ, base_freq / ROPE_FACTOR, blended)
    return np.where(wavelen < ORIG_CTX / HIGH_FREQ, base_freq, scaled)


def kernel(n_stages, x_ref, seg_ref, pos_ref, invf_ref, ga_ref, gm_ref,
           wq_ref, wk_ref, wv_ref, wo_ref, wg_ref, wu_ref, wd_ref,
           out_ref,
           wqkv_hbm, wo_hbm, hin_hbm, pv_hbm, po_hbm,
           wg_s, wu_s, wd_s, wres, wst, gb, px, ps, kc, vc, hin, h1b, pacc, oacc, sendb, h2b, act, qb,
           table, mask, sbuf, pbuf,
           wr, wx, wsnd, wfwd, wxs, hin_sem, xs, ag, s1s, s2s, pxr, pxs, psr, s4s, s5s, outr, outf, ofs,
           wres_sem, wst_sem, wo_sem, mlp_sem, hv_sem, s6s, xp, xq, op, od,
           ysn, yrc, pos, por, pps, ppr, pfs, pfr, pxfs, pxfr, pds, gate, cred):
    n_mb, T, D = x_ref.shape
    QL = wq_ref.shape[2]
    FL = wg_ref.shape[2]
    NB = wg_s.shape[0]
    FB = FL // NB
    S = seg_ref.shape[1]
    NJ = S // T
    NH = QL // HEAD_DIM
    N = (n_mb // 2) * NJ
    DB = D // NB
    scale = HEAD_DIM ** -0.5
    RB = 16
    NR = 32
    HS = hin.shape[0]
    OB = wst.shape[3]
    NO = D // OB

    hx = lax.axis_index("dp")
    z = lax.axis_index("tp")
    s = lax.axis_index("pp")
    is_home = (z == 1) | (z == 2)
    is_outer = (z == 0) | (z == 3)
    hb = lax.rem(z + 1, 2) * 0 + (z - 1)
    peer = 3 - z
    outer = 3 * (z - 1)
    inner = 1 + z // 2
    odd = lax.rem(s, 2)

    def rcopy(src, dst, ssem, rsem, **dev):
        return pltpu.make_async_remote_copy(src_ref=src, dst_ref=dst, send_sem=ssem, recv_sem=rsem,
                                            device_id=dev, device_id_type=MESH)

    def local(src, dst, sem):
        return pltpu.make_async_copy(src, dst, sem)

    def column(ref, mb, j):
        row = ref[pl.ds(mb, 1), :]
        part = row[:, 0:T]
        for c in range(1, NJ):
            part = jnp.where(j == c, row[:, c * T:(c + 1) * T], part)
        return jnp.broadcast_to(part, (HEAD_DIM, T)).T

    barrier = pltpu.get_barrier_semaphore()
    for k in range(1, 4):
        pl.semaphore_signal(barrier, inc=1, device_id={"tp": lax.rem(z + k, 4)}, device_id_type=MESH)
        pl.semaphore_signal(barrier, inc=1, device_id={"pp": lax.rem(s + k, 4)}, device_id_type=MESH)
    pl.semaphore_signal(barrier, inc=1, device_id={"dp": 1 - hx}, device_id_type=MESH)
    pl.semaphore_wait(barrier, 7)

    wqkv_own = (wq_ref, wk_ref, wv_ref, wo_ref)

    def mlp_copies():
        cps = []
        for n in range(NB):
            cps.append(local(wg_ref.at[0, :, pl.ds(n * FB, FB)], wg_s.at[n], mlp_sem.at[0, n]))
            cps.append(local(wu_ref.at[0, :, pl.ds(n * FB, FB)], wu_s.at[n], mlp_sem.at[1, n]))
            cps.append(local(wd_ref.at[0, :, pl.ds(n * DB, DB)], wd_s.at[n], mlp_sem.at[2, n]))
        return cps

    NW = n_mb // 2

    def x_copy(w, home):
        u = w * NJ + z
        return rcopy(x_ref.at[2 * w + (home - 1)], hin_hbm.at[u], xs.at[w, home - 1], xp.at[u], tp=home)

    def x_each(w, act):
        for home in (1, 2):
            @pl.when((s == 2) & (z != home))
            def _():
                act(x_copy(w, home))

    def x_pass(w, j):
        u = w * NJ + j
        return rcopy(hin_hbm.at[u], hin_hbm.at[u], xq.at[w, j], hin_sem.at[u], pp=0)

    def x_relay(ws):
        @pl.when((s == 2) & is_home)
        def _():
            for w in ws:
                for j in range(NJ):
                    @pl.when(z != j)
                    def _():
                        local(hin_hbm.at[w * NJ + j], hin_hbm.at[w * NJ + j], xp.at[w * NJ + j]).wait()
                        x_pass(w, j).start()

    x_each(0, lambda c: c.start())
    x_relay([0])

    def half(ref, m, h):
        rows = (D if m < 3 else QL) // 2
        return ref.at[pl.ds(h * rows, rows), :]

    def wslot(r, m):
        return wqkv_hbm.at[r, m] if m < 3 else wo_hbm.at[pl.ds((r + 1) * QL, QL)]

    def own_w(m):
        return wqkv_own[m].at[0]

    def wo_own():
        return local(own_w(3), wo_hbm.at[pl.ds(0, QL)], wo_sem)

    def o_send(k):
        h = hx if k < 4 else 1 - hx
        return rcopy(half(own_w(k % 4), k % 4, h), half(wslot(0, k % 4), k % 4, h), wsnd.at[k], wr.at[0, k], tp=inner)

    def p_send(m):
        return rcopy(half(own_w(m), m, hx), half(wslot(1, m), m, hx), wsnd.at[m], wr.at[1, m], tp=peer)

    def f_send(m):
        return rcopy(half(wslot(0, m), m, hx), half(wslot(2, m), m, hx), wfwd.at[m], wr.at[2, m], tp=peer)

    def x_send(r, m):
        return rcopy(half(wslot(r, m), m, hx), half(wslot(r, m), m, hx), wxs.at[r - 1, m], wx.at[r - 1, m], dp=1 - hx)

    def w_ready(rs, ms):
        def pushed(m):
            if 0 in rs:
                o_send(m).wait_recv()
            if 1 in rs:
                p_send(m).wait_recv()
        for m in ms:
            if m in PM:
                pl.when(s == 1)(functools.partial(pushed, m))
            if 0 in rs:
                o_send(4 + m).wait_recv()
            for r in (1, 2):
                if r in rs:
                    x_send(r, m).wait_recv()

    PM = (2, 3)

    def pb(r, m):
        return pv_hbm.at[r] if m == 2 else po_hbm.at[pl.ds(r * QL, QL)]

    def hh(i):
        return hx if i == 0 else 1 - hx

    def y_send(i, m):
        return rcopy(half(own_w(m), m, hh(i)), half(pb(3, m), m, hh(i)), ysn.at[2 * i + m - 2], yrc.at[2 * i + m - 2], pp=3)

    def po_send(i, m):
        return rcopy(half(pb(3, m), m, hh(i)), half(pb(0, m), m, hh(i)), pos.at[2 * i + m - 2], por.at[2 * i + m - 2], tp=inner)

    def pp_send(m):
        return rcopy(half(pb(3, m), m, hx), half(pb(1, m), m, hx), pps.at[m - 2], ppr.at[m - 2], tp=peer)

    def pf_send(m):
        return rcopy(half(pb(0, m), m, hx), half(pb(2, m), m, hx), pfs.at[m - 2], pfr.at[m - 2], tp=peer)

    def pxf_send(r, m):
        return rcopy(half(pb(r, m), m, hx), half(pb(r, m), m, hx), pxfs.at[r - 1, m - 2], pxfr.at[r - 1, m - 2], dp=1 - hx)

    def push(r, m, i):
        rsem = wr.at[0, 4 * i + m] if r == 0 else (wr.at[r, m] if i == 0 else wx.at[r - 1, m])
        return rcopy(half(pb(r, m), m, hh(i)), half(wslot(r, m), m, hh(i)), pds.at[r, m - 2, i], rsem, pp=1)

    def direct(m, f):
        if m in PM:
            pl.when(s != 1)(f)
        else:
            f()

    @pl.when(s == 1)
    def _():
        for m in PM:
            y_send(0, m).start()

        @pl.when(is_outer)
        def _():
            for m in PM:
                y_send(1, m).start()

    @pl.when((s == 3) & is_outer)
    def _():
        for i in (0, 1):
            for m in PM:
                y_send(i, m).wait_recv()
                po_send(i, m).start()
        for i in (0, 1):
            for m in PM:
                po_send(i, m).wait_send()

    @pl.when((s == 3) & is_home)
    def _():
        for m in PM:
            y_send(0, m).wait_recv()
            pp_send(m).start()
        for kind, m, a in (("p", 2, 0), ("o", 2, 0), ("p", 3, 0), ("o", 3, 0), ("f", 2, 0), ("f", 3, 0), ("o", 2, 1), ("x", 2, 1),
                           ("o", 3, 1), ("x", 3, 1)):
            with jax.named_scope('wp_' + kind + str(m) + str(a)):
                if kind == "p":
                    pp_send(m).wait_recv()
                    pxf_send(1, m).start()
                    push(1, m, 0).start()
                elif kind == "o":
                    po_send(a, m).wait_recv()
                    if a == 0:
                        pf_send(m).start()
                    push(0, m, a).start()
                elif kind == "f":
                    pf_send(m).wait_recv()
                    push(2, m, 0).start()
                else:
                    pxf_send(a, m).wait_recv()
                    push(a, m, 1).start()

    @pl.when(s == 3)
    def _():
        pl.semaphore_signal(gate, inc=1, device_id={"pp": 2}, device_id_type=MESH)

    def release():
        @pl.when(odd == 0)
        def _():
            pl.semaphore_signal(gate, inc=1, device_id={"pp": s + 1}, device_id_type=MESH)

    @pl.when(s != 0)
    def _():
        for c in mlp_copies():
            c.start()
        with jax.named_scope('w_gate'):
            pl.semaphore_wait(gate, 1)

    if NW > 1:
        x_each(1, lambda c: c.start())

    @pl.when(is_outer)
    def _():
        for k in range(8):
            direct(k % 4, lambda k=k: o_send(k).start())

        @pl.when(s == 0)
        def _():
            for c in mlp_copies():
                c.start()
        for k in range(8):
            direct(k % 4, lambda k=k: o_send(k).wait_send())
            if k == 5:
                pl.when(s == 2)(release)
        pl.when(s == 0)(release)
        for w in range(2, NW):
            x_each(w, lambda c: c.start())

    @pl.when(is_home)
    def _():
        for m in range(4):
            direct(m, lambda m=m: p_send(m).start())
        wo_own().start()

        @pl.when(s == 0)
        def _():
            for c in mlp_copies():
                c.start()
        def zero_rows(b, carry):
            for i in range(4):
                kc[i, pl.ds(b * RB, RB), :] = jnp.zeros((RB, QL), BF16)
                vc[i, pl.ds(b * RB, RB), :] = jnp.zeros((RB, QL), BF16)
            return carry
        lax.fori_loop(0, S // RB, zero_rows, 0)

        def tables(w):
            lane = lax.broadcasted_iota(jnp.int32, (T, HEAD_DIM), 1)

            def table_rows(b, carry):
                rows = pl.ds(pl.multiple_of(b * T, T), T)
                ang = column(pos_ref, 2 * w + hb, b).astype(F32) * invf_ref[0:1, :]
                table[w, rows, :] = jnp.where(lane < HEAD_DIM // 2, jnp.cos(ang), jnp.sin(ang))
                return carry
            with jax.named_scope('table'):
                lax.fori_loop(0, NJ, table_rows, 0)

        steps = [("o", 0), ("p", 0), ("t", 0), ("y", 2), ("o", 1), ("p", 1), ("t", 1), ("y", 3), ("o", 2), ("p", 2), ("t", 2), ("o", 3), ("p", 3), ("t", 3),
                 ("f", 0), ("f", 1), ("g", 2), ("f", 2), ("f", 3), ("g", 0), ("r", 0)]

        def step(kind, m):
            if kind == "o":
                o_send(m).wait_recv()
                f_send(m).start()
            elif kind == "p":
                p_send(m).wait_recv()
                x_send(1, m).start()
            else:
                f_send(m).wait_recv()
                x_send(2, m).start()

        for kind, m in steps:
            with jax.named_scope('w_' + kind + str(m)):
                if kind in "op":
                    direct(m, lambda kind=kind, m=m: step(kind, m))
                elif kind == "f" and m in PM:
                    pl.when(s != 1)(functools.partial(step, kind, m))
                elif kind == "f":
                    step(kind, m)
                elif kind == "y":
                    pl.when(s == 1)(functools.partial(step, "f", m))
                elif kind == "g":
                    pl.when(s == (0 if m == 0 else 2))(release)
                elif kind == "r":
                    x_relay([1] if NW > 1 else [])
                elif m < n_mb // 2:
                    tables(m)
        for w in range(2, NW):
            x_each(w, lambda c: c.start())
        w_ready([0, 1], range(3))
        x_relay(range(2, NW))

    def gslot(g, u):
        return lax.rem(g - 1 + u, 2)

    def group_copies(g, u):
        if g == 0:
            return [local(own_w(m), wres.at[m], wres_sem.at[m]) for m in range(3)]
        p = gslot(g, u)
        if g < 4:
            return [local(wqkv_hbm.at[g - 1], wst.at[p], wst_sem.at[p, 0])]
        return [local(wo_hbm.at[:, pl.ds(((g - 4) * 3 + m) * OB, OB)], wst.at[p, m], wst_sem.at[p, m]) for m in range(3 if g == 4 else 1)]

    def group_start(g, u):
        for c in group_copies(g, u):
            c.start()

    def group_wait(g, u):
        for c in group_copies(g, u):
            c.wait()

    def h_fetch(u):
        mb = 2 * (u // NJ) + hb
        here = lax.rem(u, NJ) == z
        dst = hin.at[lax.rem(u, HS)]

        @pl.when((s == 0) & here)
        def _():
            local(x_ref.at[mb], dst, hv_sem).start()

        @pl.when((s == 0) & jnp.logical_not(here))
        def _():
            local(hin_hbm.at[u], hin_hbm.at[u], hin_sem.at[u]).wait()
            local(hin_hbm.at[u], dst, hv_sem).start()

    @pl.when(is_home)
    def _():
        group_start(0, 0)
        group_start(1, 0)
        group_start(2, 0)
        h_fetch(0)

    for c in mlp_copies():
        c.wait()

    def hin_copy(u):
        return rcopy(h2b, hin.at[lax.rem(u, HS)], s5s, hin_sem.at[u], pp=lax.rem(s + 1, n_stages))

    def s1_outer(u):
        blk = gb.at[lax.rem(u, 3), pl.ds(pl.multiple_of(hb * T, T), T), :]
        return rcopy(blk, blk, s1s.at[0], ag.at[hb, lax.rem(u, 3)], tp=outer)

    def s1_peer(u):
        blk = gb.at[lax.rem(u, 3), pl.ds(pl.multiple_of(hb * T, T), T), :]
        return rcopy(blk, blk, s1s.at[1], ag.at[hb, lax.rem(u, 3)], tp=peer)

    def s2_copy(u):
        blk = gb.at[lax.rem(u, 3), pl.ds(pl.multiple_of((1 - hb) * T, T), T), :]
        return rcopy(blk, blk, s2s, ag.at[1 - hb, lax.rem(u, 3)], tp=outer)

    def ag_wait(b, u):
        blk = gb.at[lax.rem(u, 3), pl.ds(pl.multiple_of(b * T, T), T), :]
        local(blk, blk, ag.at[b, lax.rem(u, 3)]).wait()

    def s3_copy(u, b):
        sl = lax.rem(u, 2)
        blk = px.at[sl, pl.ds(pl.multiple_of(b * T, T), T), :]
        return rcopy(blk, blk, pxs.at[sl, b], pxr.at[sl, b], tp=inner)

    def s4_copy(u):
        return rcopy(sendb, ps.at[lax.rem(u, 2)], s4s, psr.at[lax.rem(u, 2)], tp=peer)

    def park_copy(u):
        return rcopy(h2b, hin_hbm.at[u], s5s, op.at[u], pp=1)

    def last_copy():
        mb = n_mb - 2 + hb
        return rcopy(h2b, out_ref.at[mb], s6s, outr.at[mb], tp=NJ - 1)

    def norm_rows(src, gain, dst):
        hf = src.astype(F32)
        inv = lax.rsqrt(jnp.mean(hf * hf, axis=-1, keepdims=True) + NORM_EPS)
        return (hf * inv * gain.astype(F32)).astype(BF16)

    def attention(u):
      with jax.named_scope('attn'):
        attention_(u)

    def attention_(u):
        w = u // NJ
        j = lax.rem(u, NJ)
        mb = 2 * w + hb
        row0 = pl.multiple_of(j * T, T)
        hs = lax.rem(u, HS)

        with jax.named_scope('w_hin'):
            @pl.when(s == 0)
            def _():
                local(x_ref.at[mb], hin.at[hs], hv_sem).wait()

            @pl.when(s > 0)
            def _():
                hin_copy(u).wait_recv()

        def norm_a(b, carry):
            rows = pl.ds(b * NR, NR)
            act[pl.ds(pl.multiple_of(T + b * NR, NR), NR), 0:D] = norm_rows(hin[hs, rows, :], ga_ref[0:1, :], None)
            return carry
        lax.fori_loop(0, T // NR, norm_a, 0)

        segrow = seg_ref[pl.ds(mb, 1), :]
        segc = column(seg_ref, mb, j)
        ti = lax.broadcasted_iota(jnp.int32, (T, HEAD_DIM), 0) + row0
        for c in range(0, S, HEAD_DIM):
            segr = segrow[:, c:c + HEAD_DIM]
            ui = lax.broadcasted_iota(jnp.int32, (T, HEAD_DIM), 1) + c
            mask[:, c:c + HEAD_DIM] = jnp.where((segc == segr) & (ui <= ti), 1.0, 0.0)

        def rope(val):
            pk = table[w, pl.ds(row0, T), :]
            lane = lax.broadcasted_iota(jnp.int32, (T, HEAD_DIM), 1)
            swapped = pltpu.roll(pk, HEAD_DIM // 2, 1)
            cosw = jnp.where(lane < HEAD_DIM // 2, pk, swapped)
            sinw = jnp.where(lane < HEAD_DIM // 2, -swapped, pk)
            outs = []
            for h in range(NH):
                v = val[:, h * HEAD_DIM:(h + 1) * HEAD_DIM]
                outs.append((v * cosw + pltpu.roll(v, HEAD_DIM // 2, 1) * sinw).astype(BF16))
            return outs

        def hcols(h):
            return slice(h * HEAD_DIM, (h + 1) * HEAD_DIM)

        def proj(i):
            p = i % 2

            def w(m):
                return wres[m] if i == 0 else wst[gslot(i, u), m]
            for h, val in enumerate(rope(jnp.dot(act[T:2 * T, 0:D], w(0), preferred_element_type=F32))):
                qb[p, :, hcols(h)] = val
            for h, val in enumerate(rope(jnp.dot(act[T:2 * T, 0:D], w(1), preferred_element_type=F32))):
                kc[i, pl.ds(row0, T), hcols(h)] = val
            vc[i, pl.ds(row0, T), :] = jnp.dot(act[T:2 * T, 0:D], w(2), preferred_element_type=F32).astype(BF16)

        def heads(i):
            for h in range(NH):
                sc = lax.dot_general(qb[i % 2, :, hcols(h)], kc[i, :, hcols(h)], (((1,), (1,)), ((), ())),
                                     preferred_element_type=F32) * scale
                sbuf[h] = jnp.where(mask[...] > 0.5, sc, NEG)
            for h in range(NH):
                for r in range(0, T, 32):
                    sc = sbuf[h, r:r + 32, :]
                    e = jnp.exp(sc - jnp.max(sc, axis=-1, keepdims=True))
                    pbuf[h, r:r + 32, :] = (e * (1.0 / jnp.sum(e, axis=-1, keepdims=True))).astype(BF16)
            for h in range(NH):
                act[0:T, i * QL + h * HEAD_DIM:i * QL + (h + 1) * HEAD_DIM] = jnp.dot(
                    pbuf[h], vc[i, :, hcols(h)], preferred_element_type=F32).astype(BF16)

        with jax.named_scope('shards'):
            @pl.when(u == 0)
            def _():
                group_wait(0, u)
            proj(0)

            @pl.when(u >= 2)
            def _():
                combine(u - 2)
            for i in range(3):
                group_wait(i + 1, u)
                proj(i + 1)
                if i < 2:
                    @pl.when(u == 0)
                    def _():
                        if i == 0:
                            w_ready([2], range(3))
                        else:
                            w_ready([0, 1, 2], [3])
                            wo_own().wait()
                group_start(i + 3, u)
                heads(i)
                if i == 0:
                    @pl.when(u < N - 1)
                    def _():
                        h_fetch(u + 1)
            heads(3)

        with jax.named_scope('wo'):
            def wo_block(n, w):
                act[T:2 * T, n * OB:(n + 1) * OB] = jnp.dot(act[0:T, 0:4 * QL], w, preferred_element_type=F32).astype(BF16)

            group_wait(4, u)
            for n in range(3):
                wo_block(n, wst[gslot(4, u), n])

            group_wait(5, u)
            wo_block(3, wst[gslot(5, u), 0])

            @pl.when(u < N - 1)
            def _():
                group_start(1, u + 1)
                group_start(2, u + 1)

        def norm_b(b, carry):
            rows = pl.ds(b * NR, NR)
            h1 = (hin[hs, rows, :].astype(F32) + act[pl.ds(pl.multiple_of(T + b * NR, NR), NR), 0:D].astype(F32)).astype(BF16)
            h1b[lax.rem(u, 3), rows, :] = h1
            gb[lax.rem(u, 3), pl.ds(pl.multiple_of(hb * T + b * NR, NR), NR), :] = norm_rows(h1, gm_ref[0:1, :], None)
            return carry
        lax.fori_loop(0, T // NR, norm_b, 0)

        @pl.when((s > 0) & (u < N - HS))
        def _():
            pl.semaphore_signal(cred, inc=1, device_id={"pp": s - 1}, device_id_type=MESH)

    def mlp(sl, row0, rows, store):
        UN = 2 if NB % 2 == 0 else 1

        def up(q, carry):
            for n in [q * UN + k for k in range(UN)]:
                xin = gb[sl, pl.ds(row0, rows), :]
                g = jnp.dot(xin, wg_s[n], preferred_element_type=F32)
                u_ = jnp.dot(xin, wu_s[n], preferred_element_type=F32)
                act[0:rows, pl.ds(pl.multiple_of(n * FB, FB), FB)] = (jax.nn.silu(g) * u_).astype(BF16)
            return carry
        lax.fori_loop(0, NB // UN, up, 0)

        def down(q, carry):
            for n in [q * UN + k for k in range(UN)]:
                store(pl.ds(pl.multiple_of(n * DB, DB), DB), jnp.dot(act[0:rows, 0:FL], wd_s[n], preferred_element_type=F32))
            return carry
        lax.fori_loop(0, NB // UN, down, 0)

    def mlp_home(u):
        def store(c, val):
            pacc[:, c] = val
        with jax.named_scope('mlp'):
            mlp(lax.rem(u, 3), 0, 2 * T, store)

    def mlp_outer(u, b):
        def store(c, val):
            px[lax.rem(u, 2), pl.ds(pl.multiple_of(b * T, T), T), c] = val.astype(BF16)
        with jax.named_scope('mlp_o'):
            mlp(lax.rem(u, 3), pl.multiple_of(b * T, T), T, store)

    def forward(u):
        @pl.when((u >= 1) & (u <= N))
        def _():
            s2_copy(u - 1).wait_send()

        @pl.when(u < N)
        def _():
            with jax.named_scope('w_ag'):
                ag_wait(1 - hb, u)
            s2_copy(u).start()

    def combine(v):
        sl = lax.rem(v, 2)
        with jax.named_scope('w_s3'):
            s3_copy(v, 0).wait_recv()
            s3_copy(v, 1).wait_recv()

        @pl.when(v >= 1)
        def _():
            s4_copy(v - 1).wait_send()

        def comb(b, carry):
            rows = pl.ds(b * RB, RB)
            mine = pl.ds(pl.multiple_of(hb * T + b * RB, RB), RB)
            theirs = pl.ds(pl.multiple_of((1 - hb) * T + b * RB, RB), RB)
            oacc[rows, :] = pacc[mine, :] + px[sl, mine, :].astype(F32)
            sendb[rows, :] = (pacc[theirs, :] + px[sl, theirs, :].astype(F32)).astype(BF16)
            return carry
        lax.fori_loop(0, T // RB, comb, 0)
        s4_copy(v).start()

    def finish(u):
        @pl.when((u >= 2) & (u < N + 2))
        def _():
            v = u - 2
            with jax.named_scope('w_s4'):
                s4_copy(v).wait_recv()
            vw = v // NJ
            vj = lax.rem(v, NJ)

            @pl.when(v >= 1)
            def _():
                hin_copy(v).wait_send()

            def fin(b, carry):
                rows = pl.ds(b * RB, RB)
                d = (oacc[rows, :] + ps[lax.rem(v, 2), rows, :].astype(F32)).astype(BF16)
                h2b[rows, :] = (h1b[lax.rem(v, 3), rows, :].astype(F32) + d.astype(F32)).astype(BF16)
                return carry
            lax.fori_loop(0, T // RB, fin, 0)

            @pl.when((s < n_stages - 1) & (v >= HS))
            def _():
                with jax.named_scope('w_cred'):
                    pl.semaphore_wait(cred, 1)

            @pl.when(s < n_stages - 1)
            def _():
                hin_copy(v).start()

            @pl.when((s == n_stages - 1) & ((v < N - 1) | (hb == 0)))
            def _():
                park_copy(v).start()

            @pl.when((s == n_stages - 1) & (v == N - 1))
            def _():
                last_copy().start()

    def body(u, carry):
        @pl.when(is_home)
        def _():
            @pl.when(u < N)
            def _():
                attention(u)

            @pl.when((u >= 1) & (u <= N))
            def _():
                s1_outer(u - 1).wait_send()
                s1_peer(u - 1).wait_send()

            @pl.when(u < N)
            def _():
                s1_peer(u).start()
                s1_outer(u).start()

            @pl.when((u >= N) & (u < N + 2))
            def _():
                combine(u - 2)

            finish(u)

            @pl.when((u >= 1) & (u <= N))
            def _():
                mlp_home(u - 1)

            forward(u)

        @pl.when(is_outer & (u < N))
        def _():
            for k in (0, 1):
                b = inner - 1 if k == 0 else 2 - inner
                with jax.named_scope('w_ag_outer'):
                    ag_wait(b, u)

                @pl.when(u >= 2)
                def _():
                    s3_copy(u - 2, b).wait_send()
                mlp_outer(u, b)
                s3_copy(u, b).start()

        return carry

    def out_fwd(mb, p, sem):
        return rcopy(out_ref.at[mb], out_ref.at[mb], ofs.at[mb, p], sem, pp=p)

    lax.fori_loop(0, N + 2, body, 0)

    last_here = (s == n_stages - 1) & (z == NJ - 1)

    @pl.when(last_here)
    def _():
        for mb in (n_mb - 1, n_mb - 2):
            local(out_ref.at[mb], out_ref.at[mb], outr.at[mb]).wait()
            if mb == n_mb - 1:
                out_fwd(mb, 1, outr.at[mb]).start()
            out_fwd(mb, 2, outf).start()

    def od_copy(v):
        return rcopy(hin_hbm.at[v], out_ref.at[2 * (v // NJ) + hb], od.at[v], outr.at[2 * (v // NJ) + hb], tp=lax.rem(v, NJ))

    @pl.when(s == 1)
    def _():
        def spread(v, carry):
            vj = lax.rem(v, NJ)
            mine = 2 * (v // NJ) + hb

            here = is_home & ((v < N - 1) | (hb == 0))

            @pl.when(here)
            def _():
                local(hin_hbm.at[v], hin_hbm.at[v], op.at[v]).wait()

            @pl.when(here & (vj != z))
            def _():
                od_copy(v).start()

            @pl.when(is_home & (vj == z))
            def _():
                c = local(hin_hbm.at[v], hin.at[0], hv_sem)
                c.start()
                c.wait()
                c = local(hin.at[0], out_ref.at[mine], hv_sem)
                c.start()
                c.wait()

            @pl.when(vj == z)
            def _():
                for b in (0, 1):
                    mb = 2 * (v // NJ) + b

                    @pl.when(z - 1 != b)
                    def _(mb=mb):
                        local(out_ref.at[mb], out_ref.at[mb], outr.at[mb]).wait()
                    out_fwd(mb, 0, outf).start()

                    @pl.when(v < N - 1)
                    def _(mb=mb):
                        out_fwd(mb, 3, outf).start()
                        out_fwd(mb, 2, outf).start()
            return carry
        lax.fori_loop(0, N, spread, 0)

    @pl.when(is_home)
    def _():
        s4_copy(N - 1).wait_send()

        @pl.when((s < n_stages - 1) | (hb == 0))
        def _():
            hin_copy(N - 1).wait_send()

        @pl.when(s == n_stages - 1)
        def _():
            last_copy().wait_send()

    @pl.when(is_outer)
    def _():
        for b in (0, 1):
            s3_copy(N - 2, b).wait_send()
            s3_copy(N - 1, b).wait_send()

    @pl.when(s == 1)
    def _():
        for m in PM:
            y_send(0, m).wait_send()

        @pl.when(is_outer)
        def _():
            for m in PM:
                y_send(1, m).wait_send()

    @pl.when((s == 3) & is_home)
    def _():
        for m in PM:
            pp_send(m).wait_send()
            pf_send(m).wait_send()
            pxf_send(1, m).wait_send()
            for r, i in ((0, 0), (0, 1), (1, 0), (1, 1), (2, 0)):
                push(r, m, i).wait_send()

    @pl.when(is_home)
    def _():
        def sent(m):
            p_send(m).wait_send()
            f_send(m).wait_send()
            x_send(1, m).wait_send()
        for m in range(4):
            direct(m, functools.partial(sent, m))
            x_send(2, m).wait_send()

        @pl.when(s == 2)
        def _():
            for w in range(NW):
                for j in range(NJ):
                    @pl.when(z != j)
                    def _():
                        x_pass(w, j).wait_send()

        @pl.when(s == 1)
        def _():
            def spread_done(v, carry):
                @pl.when((lax.rem(v, NJ) != z) & ((v < N - 1) | (hb == 0)))
                def _():
                    od_copy(v).wait_send()
                return carry
            lax.fori_loop(0, N, spread_done, 0)

    for w in range(NW):
        x_each(w, lambda c: c.wait_send())

    @pl.when(s == 1)
    def _():
        for mb in range(n_mb):
            out_fwd(mb, 0, outf).wait_send()
            if mb < n_mb - 2:
                out_fwd(mb, 3, outf).wait_send()
                out_fwd(mb, 2, outf).wait_send()
            else:
                @pl.when(z < NJ - 1)
                def _(mb=mb):
                    out_fwd(mb, 3, outf).wait_send()
                    out_fwd(mb, 2, outf).wait_send()

    @pl.when(last_here)
    def _():
        for mb in (n_mb - 2, n_mb - 1):
            out_fwd(mb, 2, outf).wait_send()
        out_fwd(n_mb - 1, 1, outf).wait_send()
        early = out_ref.at[pl.ds(0, n_mb - 2)]
        local(early, early, outf).wait()

    @pl.when((s == n_stages - 1) & (z < NJ - 1))
    def _():
        local(out_ref, out_ref, outf).wait()

    @pl.when((s == 0) | (s == 2))
    def _():
        local(out_ref, out_ref, outf).wait()


def solution(mesh):
    n_stages = mesh.shape['pp']

    def stage_program(hidden_in, seg_ids, positions, attn_norm, w_query, w_key, w_value, w_out, mlp_norm, w_gate, w_up, w_down):
        n_mb, T, D = hidden_in.shape
        S = seg_ids.shape[1]
        QL = w_query.shape[2]
        FL = w_gate.shape[2]
        NJ = S // T
        N = (n_mb // 2) * NJ
        NB = max(1, FL // 512)
        invf = jnp.asarray(np.tile(rope_freqs(), 2)[None, :], F32)
        any_spec = pl.BlockSpec(memory_space=pl.ANY)
        vmem = pl.BlockSpec(memory_space=pltpu.VMEM)
        dma = pltpu.SemaphoreType.DMA
        scratch = [
            pltpu.VMEM((NB, D, FL // NB), BF16), pltpu.VMEM((NB, D, FL // NB), BF16), pltpu.VMEM((NB, FL, D // NB), BF16),
            pltpu.VMEM((3, D, QL), BF16), pltpu.VMEM((2, 3, D, QL), BF16),
            pltpu.VMEM((3, 2 * T, D), BF16),
            pltpu.VMEM((2, 2 * T, D), BF16),
            pltpu.VMEM((2, T, D), BF16),
            pltpu.VMEM((4, S, QL), BF16), pltpu.VMEM((4, S, QL), BF16),
            pltpu.VMEM((3, T, D), BF16),
            pltpu.VMEM((3, T, D), BF16),
            pltpu.VMEM((2 * T, D), F32),
            pltpu.VMEM((T, D), F32),
            pltpu.VMEM((T, D), BF16),
            pltpu.VMEM((T, D), BF16),
            pltpu.VMEM((2 * T, max(D, FL, 4 * QL)), BF16),
            pltpu.VMEM((2, T, QL), BF16),
            pltpu.VMEM((n_mb // 2, S, HEAD_DIM), F32),
            pltpu.VMEM((T, S), F32), pltpu.VMEM((QL // HEAD_DIM, T, S), F32), pltpu.VMEM((QL // HEAD_DIM, T, S), BF16),
            dma((3, 8)), dma((2, 4)), dma((8,)), dma((4,)), dma((2, 4)),
            dma((N,)), dma((n_mb // 2, 2)), dma((2, 3)), dma((2,)), dma, dma((2, 2)), dma((2, 2)), dma((2,)), dma, dma,
            dma((n_mb,)), dma, dma((n_mb, n_stages)),
            dma((3,)), dma((2, 3)), dma, dma((3, NB)), dma, dma, dma((N,)), dma((n_mb // 2, NJ)), dma((N,)), dma((N,)),
            dma((4,)), dma((4,)), dma((4,)), dma((4,)), dma((2,)), dma((2,)), dma((2,)), dma((2,)), dma((2, 2)), dma((2, 2)), dma((3, 2, 2)),
            pltpu.SemaphoreType.REGULAR, pltpu.SemaphoreType.REGULAR,
        ]
        return pl.pallas_call(
            functools.partial(kernel, n_stages),
            out_shape=[jax.ShapeDtypeStruct(hidden_in.shape, BF16), jax.ShapeDtypeStruct((3, 3, D, QL), BF16),
                       jax.ShapeDtypeStruct((4 * QL, D), BF16), jax.ShapeDtypeStruct((N, T, D), BF16),
                       jax.ShapeDtypeStruct((4, D, QL), BF16), jax.ShapeDtypeStruct((4 * QL, D), BF16)],
            in_specs=[any_spec, vmem, vmem, vmem, vmem, vmem] + [any_spec] * 7,
            out_specs=[any_spec] * 6,
            scratch_shapes=scratch,
            compiler_params=pltpu.CompilerParams(collective_id=0, has_side_effects=True, vmem_limit_bytes=67_043_328),
        )(hidden_in, seg_ids, positions, invf, attn_norm, mlp_norm, w_query, w_key, w_value, w_out, w_gate, w_up, w_down)[0]

    act_spec = P('dp', 'tp', None)
    row_spec = P('dp', None)
    gain_spec = P('pp', None)
    col_spec = P('pp', None, 'tp')
    rows_spec = P('pp', 'tp', None)
    return jax.shard_map(stage_program, mesh=mesh,
                         in_specs=(act_spec, row_spec, row_spec, gain_spec, col_spec, col_spec, col_spec, rows_spec, gain_spec, col_spec, col_spec, rows_spec),
                         out_specs=act_spec, check_vma=False)
```

```python
import functools
import math

import jax
import jax.numpy as jnp
import numpy as np
from jax import lax
from jax.experimental import pallas as pl
from jax.experimental.pallas import tpu as pltpu
from jax.sharding import PartitionSpec as P

HEAD_DIM = 128
NORM_EPS = 1e-5
ROPE_THETA = 500000.0
ROPE_FACTOR = 8.0
LOW_FREQ = 1.0
HIGH_FREQ = 4.0
ORIG_CTX = 8192.0
NEG = -1e30
MESH = pl.DeviceIdType.MESH
F32 = jnp.float32
BF16 = jnp.bfloat16


def rope_freqs():
    base_freq = 1.0 / (ROPE_THETA ** (np.arange(0, HEAD_DIM, 2) / HEAD_DIM))
    wavelen = 2.0 * np.pi / base_freq
    smooth = (ORIG_CTX / wavelen - LOW_FREQ) / (HIGH_FREQ - LOW_FREQ)
    blended = (1.0 - smooth) * base_freq / ROPE_FACTOR + smooth * base_freq
    scaled = np.where(wavelen > ORIG_CTX / LOW_FREQ, base_freq / ROPE_FACTOR, blended)
    return np.where(wavelen < ORIG_CTX / HIGH_FREQ, base_freq, scaled)


def kernel(n_stages, x_ref, seg_ref, pos_ref, invf_ref, ga_ref, gm_ref,
           wq_ref, wk_ref, wv_ref, wo_ref, wg_ref, wu_ref, wd_ref,
           out_ref,
           wqkv_hbm, wo_hbm, hin_hbm, pv_hbm, po_hbm,
           wg_s, wu_s, wd_s, wres, wst, gb, px, ps, kc, vc, hin, h1b, pacc, oacc, sendb, h2b, act, qb,
           table, mask, sbuf, pbuf,
           wr, wx, wsnd, wfwd, wxs, hin_sem, xs, ag, s1s, s2s, pxr, pxs, psr, s4s, s5s, outr, outf, ofs,
           wres_sem, wst_sem, wo_sem, mlp_sem, hv_sem, s6s, xp, xq, op, od,
           ysn, yrc, pos, por, pps, ppr, pfs, pfr, pxfs, pxfr, pds, gate, cred):
    n_mb, T, D = x_ref.shape
    QL = wq_ref.shape[2]
    FL = wg_ref.shape[2]
    NB = wg_s.shape[0]
    FB = FL // NB
    S = seg_ref.shape[1]
    NJ = S // T
    NH = QL // HEAD_DIM
    N = (n_mb // 2) * NJ
    DB = D // NB
    scale = HEAD_DIM ** -0.5
    RB = 16
    NR = 32
    HS = hin.shape[0]
    OB = wst.shape[3]
    NO = D // OB

    hx = lax.axis_index("dp")
    z = lax.axis_index("tp")
    s = lax.axis_index("pp")
    is_home = (z == 1) | (z == 2)
    is_outer = (z == 0) | (z == 3)
    hb = lax.rem(z + 1, 2) * 0 + (z - 1)
    peer = 3 - z
    outer = 3 * (z - 1)
    inner = 1 + z // 2
    odd = lax.rem(s, 2)

    def rcopy(src, dst, ssem, rsem, **dev):
        return pltpu.make_async_remote_copy(src_ref=src, dst_ref=dst, send_sem=ssem, recv_sem=rsem,
                                            device_id=dev, device_id_type=MESH)

    def local(src, dst, sem):
        return pltpu.make_async_copy(src, dst, sem)

    def column(ref, mb, j):
        row = ref[pl.ds(mb, 1), :]
        part = row[:, 0:T]
        for c in range(1, NJ):
            part = jnp.where(j == c, row[:, c * T:(c + 1) * T], part)
        return jnp.broadcast_to(part, (HEAD_DIM, T)).T

    barrier = pltpu.get_barrier_semaphore()
    for k in range(1, 4):
        pl.semaphore_signal(barrier, inc=1, device_id={"tp": lax.rem(z + k, 4)}, device_id_type=MESH)
        pl.semaphore_signal(barrier, inc=1, device_id={"pp": lax.rem(s + k, 4)}, device_id_type=MESH)
    pl.semaphore_signal(barrier, inc=1, device_id={"dp": 1 - hx}, device_id_type=MESH)
    pl.semaphore_wait(barrier, 7)

    wqkv_own = (wq_ref, wk_ref, wv_ref, wo_ref)

    def mlp_copies():
        cps = []
        for n in range(NB):
            cps.append(local(wg_ref.at[0, :, pl.ds(n * FB, FB)], wg_s.at[n], mlp_sem.at[0, n]))
            cps.append(local(wu_ref.at[0, :, pl.ds(n * FB, FB)], wu_s.at[n], mlp_sem.at[1, n]))
            cps.append(local(wd_ref.at[0, :, pl.ds(n * DB, DB)], wd_s.at[n], mlp_sem.at[2, n]))
        return cps

    NW = n_mb // 2

    def x_copy(w, home):
        u = w * NJ + z
        return rcopy(x_ref.at[2 * w + (home - 1)], hin_hbm.at[u], xs.at[w, home - 1], xp.at[u], tp=home)

    def x_each(w, act):
        for home in (1, 2):
            @pl.when((s == 2) & (z != home))
            def _():
                act(x_copy(w, home))

    def x_pass(w, j):
        u = w * NJ + j
        return rcopy(hin_hbm.at[u], hin_hbm.at[u], xq.at[w, j], hin_sem.at[u], pp=0)

    def x_relay(ws):
        @pl.when((s == 2) & is_home)
        def _():
            for w in ws:
                for j in range(NJ):
                    @pl.when(z != j)
                    def _():
                        local(hin_hbm.at[w * NJ + j], hin_hbm.at[w * NJ + j], xp.at[w * NJ + j]).wait()
                        x_pass(w, j).start()

    x_each(0, lambda c: c.start())
    x_relay([0])

    def half(ref, m, h):
        rows = (D if m < 3 else QL) // 2
        return ref.at[pl.ds(h * rows, rows), :]

    def wslot(r, m):
        return wqkv_hbm.at[r, m] if m < 3 else wo_hbm.at[pl.ds((r + 1) * QL, QL)]

    def own_w(m):
        return wqkv_own[m].at[0]

    def wo_own():
        return local(own_w(3), wo_hbm.at[pl.ds(0, QL)], wo_sem)

    def o_send(k):
        h = hx if k < 4 else 1 - hx
        return rcopy(half(own_w(k % 4), k % 4, h), half(wslot(0, k % 4), k % 4, h), wsnd.at[k], wr.at[0, k], tp=inner)

    def p_send(m):
        return rcopy(half(own_w(m), m, hx), half(wslot(1, m), m, hx), wsnd.at[m], wr.at[1, m], tp=peer)

    def f_send(m):
        return rcopy(half(wslot(0, m), m, hx), half(wslot(2, m), m, hx), wfwd.at[m], wr.at[2, m], tp=peer)

    def x_send(r, m):
        return rcopy(half(wslot(r, m), m, hx), half(wslot(r, m), m, hx), wxs.at[r - 1, m], wx.at[r - 1, m], dp=1 - hx)

    def w_ready(rs, ms):
        def pushed(m):
            if 0 in rs:
                o_send(m).wait_recv()
            if 1 in rs:
                p_send(m).wait_recv()
        for m in ms:
            if m in PM:
                pl.when(s == 1)(functools.partial(pushed, m))
            if 0 in rs:
                o_send(4 + m).wait_recv()
            for r in (1, 2):
                if r in rs:
                    x_send(r, m).wait_recv()

    PM = (2, 3)

    def pb(r, m):
        return pv_hbm.at[r] if m == 2 else po_hbm.at[pl.ds(r * QL, QL)]

    def hh(i):
        return hx if i == 0 else 1 - hx

    def y_send(i, m):
        return rcopy(half(own_w(m), m, hh(i)), half(pb(3, m), m, hh(i)), ysn.at[2 * i + m - 2], yrc.at[2 * i + m - 2], pp=3)

    def po_send(i, m):
        return rcopy(half(pb(3, m), m, hh(i)), half(pb(0, m), m, hh(i)), pos.at[2 * i + m - 2], por.at[2 * i + m - 2], tp=inner)

    def pp_send(m):
        return rcopy(half(pb(3, m), m, hx), half(pb(1, m), m, hx), pps.at[m - 2], ppr.at[m - 2], tp=peer)

    def pf_send(m):
        return rcopy(half(pb(0, m), m, hx), half(pb(2, m), m, hx), pfs.at[m - 2], pfr.at[m - 2], tp=peer)

    def pxf_send(r, m):
        return rcopy(half(pb(r, m), m, hx), half(pb(r, m), m, hx), pxfs.at[r - 1, m - 2], pxfr.at[r - 1, m - 2], dp=1 - hx)

    def push(r, m, i):
        rsem = wr.at[0, 4 * i + m] if r == 0 else (wr.at[r, m] if i == 0 else wx.at[r - 1, m])
        return rcopy(half(pb(r, m), m, hh(i)), half(wslot(r, m), m, hh(i)), pds.at[r, m - 2, i], rsem, pp=1)

    def direct(m, f):
        if m in PM:
            pl.when(s != 1)(f)
        else:
            f()

    @pl.when(s == 1)
    def _():
        for m in PM:
            y_send(0, m).start()

        @pl.when(is_outer)
        def _():
            for m in PM:
                y_send(1, m).start()

    @pl.when((s == 3) & is_outer)
    def _():
        for i in (0, 1):
            for m in PM:
                y_send(i, m).wait_recv()
                po_send(i, m).start()
        for i in (0, 1):
            for m in PM:
                po_send(i, m).wait_send()

    @pl.when((s == 3) & is_home)
    def _():
        for m in PM:
            y_send(0, m).wait_recv()
            pp_send(m).start()
        for kind, m, a in (("p", 2, 0), ("o", 2, 0), ("p", 3, 0), ("o", 3, 0), ("f", 2, 0), ("f", 3, 0), ("o", 2, 1), ("x", 2, 1),
                           ("o", 3, 1), ("x", 3, 1)):
            with jax.named_scope('wp_' + kind + str(m) + str(a)):
                if kind == "p":
                    pp_send(m).wait_recv()
                    pxf_send(1, m).start()
                    push(1, m, 0).start()
                elif kind == "o":
                    po_send(a, m).wait_recv()
                    if a == 0:
                        pf_send(m).start()
                    push(0, m, a).start()
                elif kind == "f":
                    pf_send(m).wait_recv()
                    push(2, m, 0).start()
                else:
                    pxf_send(a, m).wait_recv()
                    push(a, m, 1).start()

    @pl.when(s == 3)
    def _():
        pl.semaphore_signal(gate, inc=1, device_id={"pp": 2}, device_id_type=MESH)

    def release():
        @pl.when(odd == 0)
        def _():
            pl.semaphore_signal(gate, inc=1, device_id={"pp": s + 1}, device_id_type=MESH)

    @pl.when(s != 0)
    def _():
        for c in mlp_copies():
            c.start()
        with jax.named_scope('w_gate'):
            pl.semaphore_wait(gate, 1)

    if NW > 1:
        x_each(1, lambda c: c.start())

    @pl.when(is_outer)
    def _():
        for k in range(8):
            direct(k % 4, lambda k=k: o_send(k).start())

        @pl.when(s == 0)
        def _():
            for c in mlp_copies():
                c.start()
        for k in range(8):
            direct(k % 4, lambda k=k: o_send(k).wait_send())
            if k == 5:
                pl.when(s == 2)(release)
        pl.when(s == 0)(release)
        for w in range(2, NW):
            x_each(w, lambda c: c.start())

    @pl.when(is_home)
    def _():
        for m in range(4):
            direct(m, lambda m=m: p_send(m).start())
        wo_own().start()

        @pl.when(s == 0)
        def _():
            for c in mlp_copies():
                c.start()
        def zero_rows(b, carry):
            for i in range(4):
                kc[i, pl.ds(b * RB, RB), :] = jnp.zeros((RB, QL), BF16)
                vc[i, pl.ds(b * RB, RB), :] = jnp.zeros((RB, QL), BF16)
            return carry
        lax.fori_loop(0, S // RB, zero_rows, 0)

        def tables(w):
            lane = lax.broadcasted_iota(jnp.int32, (T, HEAD_DIM), 1)

            def table_rows(b, carry):
                rows = pl.ds(pl.multiple_of(b * T, T), T)
                ang = column(pos_ref, 2 * w + hb, b).astype(F32) * invf_ref[0:1, :]
                table[w, rows, :] = jnp.where(lane < HEAD_DIM // 2, jnp.cos(ang), jnp.sin(ang))
                return carry
            with jax.named_scope('table'):
                lax.fori_loop(0, NJ, table_rows, 0)

        steps = [("o", 0), ("p", 0), ("t", 0), ("y", 2), ("o", 1), ("p", 1), ("t", 1), ("y", 3), ("o", 2), ("p", 2), ("t", 2), ("o", 3), ("p", 3), ("t", 3),
                 ("f", 0), ("r", 0), ("f", 1), ("g", 2), ("f", 2), ("f", 3), ("g", 0)]

        def step(kind, m):
            if kind == "o":
                o_send(m).wait_recv()
                f_send(m).start()
            elif kind == "p":
                p_send(m).wait_recv()
                x_send(1, m).start()
            else:
                f_send(m).wait_recv()
                x_send(2, m).start()

        for kind, m in steps:
            with jax.named_scope('w_' + kind + str(m)):
                if kind in "op":
                    direct(m, lambda kind=kind, m=m: step(kind, m))
                elif kind == "f" and m in PM:
                    pl.when(s != 1)(functools.partial(step, kind, m))
                elif kind == "f":
                    step(kind, m)
                elif kind == "y":
                    pl.when(s == 1)(functools.partial(step, "f", m))
                elif kind == "g":
                    pl.when(s == (0 if m == 0 else 2))(release)
                elif kind == "r":
                    x_relay([1] if NW > 1 else [])
                elif m < n_mb // 2:
                    tables(m)
        for w in range(2, NW):
            x_each(w, lambda c: c.start())
        w_ready([0, 1], range(3))
        x_relay(range(2, NW))

    def gslot(g, u):
        return lax.rem(g - 1 + u, 2)

    def group_copies(g, u):
        if g == 0:
            return [local(own_w(m), wres.at[m], wres_sem.at[m]) for m in range(3)]
        p = gslot(g, u)
        if g < 4:
            return [local(wqkv_hbm.at[g - 1], wst.at[p], wst_sem.at[p, 0])]
        return [local(wo_hbm.at[:, pl.ds(((g - 4) * 3 + m) * OB, OB)], wst.at[p, m], wst_sem.at[p, m]) for m in range(3 if g == 4 else 1)]

    def group_start(g, u):
        for c in group_copies(g, u):
            c.start()

    def group_wait(g, u):
        for c in group_copies(g, u):
            c.wait()

    def h_fetch(u):
        mb = 2 * (u // NJ) + hb
        here = lax.rem(u, NJ) == z
        dst = hin.at[lax.rem(u, HS)]

        @pl.when((s == 0) & here)
        def _():
            local(x_ref.at[mb], dst, hv_sem).start()

        @pl.when((s == 0) & jnp.logical_not(here))
        def _():
            local(hin_hbm.at[u], hin_hbm.at[u], hin_sem.at[u]).wait()
            local(hin_hbm.at[u], dst, hv_sem).start()

    @pl.when(is_home)
    def _():
        group_start(0, 0)
        group_start(1, 0)
        group_start(2, 0)
        h_fetch(0)

    for c in mlp_copies():
        c.wait()

    def hin_copy(u):
        return rcopy(h2b, hin.at[lax.rem(u, HS)], s5s, hin_sem.at[u], pp=lax.rem(s + 1, n_stages))

    def s1_outer(u):
        blk = gb.at[lax.rem(u, 3), pl.ds(pl.multiple_of(hb * T, T), T), :]
        return rcopy(blk, blk, s1s.at[0], ag.at[hb, lax.rem(u, 3)], tp=outer)

    def s1_peer(u):
        blk = gb.at[lax.rem(u, 3), pl.ds(pl.multiple_of(hb * T, T), T), :]
        return rcopy(blk, blk, s1s.at[1], ag.at[hb, lax.rem(u, 3)], tp=peer)

    def s2_copy(u):
        blk = gb.at[lax.rem(u, 3), pl.ds(pl.multiple_of((1 - hb) * T, T), T), :]
        return rcopy(blk, blk, s2s, ag.at[1 - hb, lax.rem(u, 3)], tp=outer)

    def ag_wait(b, u):
        blk = gb.at[lax.rem(u, 3), pl.ds(pl.multiple_of(b * T, T), T), :]
        local(blk, blk, ag.at[b, lax.rem(u, 3)]).wait()

    def s3_copy(u, b):
        sl = lax.rem(u, 2)
        blk = px.at[sl, pl.ds(pl.multiple_of(b * T, T), T), :]
        return rcopy(blk, blk, pxs.at[sl, b], pxr.at[sl, b], tp=inner)

    def s4_copy(u):
        return rcopy(sendb, ps.at[lax.rem(u, 2)], s4s, psr.at[lax.rem(u, 2)], tp=peer)

    def park_copy(u):
        return rcopy(h2b, hin_hbm.at[u], s5s, op.at[u], pp=1)

    def last_copy():
        mb = n_mb - 2 + hb
        return rcopy(h2b, out_ref.at[mb], s6s, outr.at[mb], tp=NJ - 1)

    def norm_rows(src, gain, dst):
        hf = src.astype(F32)
        inv = lax.rsqrt(jnp.mean(hf * hf, axis=-1, keepdims=True) + NORM_EPS)
        return (hf * inv * gain.astype(F32)).astype(BF16)

    def attention(u):
      with jax.named_scope('attn'):
        attention_(u)

    def attention_(u):
        w = u // NJ
        j = lax.rem(u, NJ)
        mb = 2 * w + hb
        row0 = pl.multiple_of(j * T, T)
        hs = lax.rem(u, HS)

        with jax.named_scope('w_hin'):
            @pl.when(s == 0)
            def _():
                local(x_ref.at[mb], hin.at[hs], hv_sem).wait()

            @pl.when(s > 0)
            def _():
                hin_copy(u).wait_recv()

        def norm_a(b, carry):
            rows = pl.ds(b * NR, NR)
            act[pl.ds(pl.multiple_of(T + b * NR, NR), NR), 0:D] = norm_rows(hin[hs, rows, :], ga_ref[0:1, :], None)
            return carry
        lax.fori_loop(0, T // NR, norm_a, 0)

        segrow = seg_ref[pl.ds(mb, 1), :]
        segc = column(seg_ref, mb, j)
        ti = lax.broadcasted_iota(jnp.int32, (T, HEAD_DIM), 0) + row0
        for c in range(0, S, HEAD_DIM):
            segr = segrow[:, c:c + HEAD_DIM]
            ui = lax.broadcasted_iota(jnp.int32, (T, HEAD_DIM), 1) + c
            mask[:, c:c + HEAD_DIM] = jnp.where((segc == segr) & (ui <= ti), 1.0, 0.0)

        def rope(val):
            pk = table[w, pl.ds(row0, T), :]
            lane = lax.broadcasted_iota(jnp.int32, (T, HEAD_DIM), 1)
            swapped = pltpu.roll(pk, HEAD_DIM // 2, 1)
            cosw = jnp.where(lane < HEAD_DIM // 2, pk, swapped)
            sinw = jnp.where(lane < HEAD_DIM // 2, -swapped, pk)
            outs = []
            for h in range(NH):
                v = val[:, h * HEAD_DIM:(h + 1) * HEAD_DIM]
                outs.append((v * cosw + pltpu.roll(v, HEAD_DIM // 2, 1) * sinw).astype(BF16))
            return outs

        def hcols(h):
            return slice(h * HEAD_DIM, (h + 1) * HEAD_DIM)

        def proj(i):
            p = i % 2

            def w(m):
                return wres[m] if i == 0 else wst[gslot(i, u), m]
            for h, val in enumerate(rope(jnp.dot(act[T:2 * T, 0:D], w(0), preferred_element_type=F32))):
                qb[p, :, hcols(h)] = val
            for h, val in enumerate(rope(jnp.dot(act[T:2 * T, 0:D], w(1), preferred_element_type=F32))):
                kc[i, pl.ds(row0, T), hcols(h)] = val
            vc[i, pl.ds(row0, T), :] = jnp.dot(act[T:2 * T, 0:D], w(2), preferred_element_type=F32).astype(BF16)

        def heads(i):
            for h in range(NH):
                sc = lax.dot_general(qb[i % 2, :, hcols(h)], kc[i, :, hcols(h)], (((1,), (1,)), ((), ())),
                                     preferred_element_type=F32) * scale
                sbuf[h] = jnp.where(mask[...] > 0.5, sc, NEG)
            for h in range(NH):
                for r in range(0, T, 32):
                    sc = sbuf[h, r:r + 32, :]
                    e = jnp.exp(sc - jnp.max(sc, axis=-1, keepdims=True))
                    pbuf[h, r:r + 32, :] = (e * (1.0 / jnp.sum(e, axis=-1, keepdims=True))).astype(BF16)
            for h in range(NH):
                act[0:T, i * QL + h * HEAD_DIM:i * QL + (h + 1) * HEAD_DIM] = jnp.dot(
                    pbuf[h], vc[i, :, hcols(h)], preferred_element_type=F32).astype(BF16)

        with jax.named_scope('shards'):
            @pl.when(u == 0)
            def _():
                group_wait(0, u)
            proj(0)

            @pl.when(u >= 2)
            def _():
                combine(u - 2)
            for i in range(3):
                group_wait(i + 1, u)
                proj(i + 1)
                if i < 2:
                    @pl.when(u == 0)
                    def _():
                        if i == 0:
                            w_ready([2], range(3))
                        else:
                            w_ready([0, 1, 2], [3])
                            wo_own().wait()
                group_start(i + 3, u)
                heads(i)
                if i == 0:
                    @pl.when(u < N - 1)
                    def _():
                        h_fetch(u + 1)
            heads(3)

        with jax.named_scope('wo'):
            def wo_block(n, w):
                act[T:2 * T, n * OB:(n + 1) * OB] = jnp.dot(act[0:T, 0:4 * QL], w, preferred_element_type=F32).astype(BF16)

            group_wait(4, u)
            for n in range(3):
                wo_block(n, wst[gslot(4, u), n])

            group_wait(5, u)
            wo_block(3, wst[gslot(5, u), 0])

            @pl.when(u < N - 1)
            def _():
                group_start(1, u + 1)
                group_start(2, u + 1)

        def norm_b(b, carry):
            rows = pl.ds(b * NR, NR)
            h1 = (hin[hs, rows, :].astype(F32) + act[pl.ds(pl.multiple_of(T + b * NR, NR), NR), 0:D].astype(F32)).astype(BF16)
            h1b[lax.rem(u, 3), rows, :] = h1
            gb[lax.rem(u, 3), pl.ds(pl.multiple_of(hb * T + b * NR, NR), NR), :] = norm_rows(h1, gm_ref[0:1, :], None)
            return carry
        lax.fori_loop(0, T // NR, norm_b, 0)

        @pl.when((s > 0) & (u < N - HS))
        def _():
            pl.semaphore_signal(cred, inc=1, device_id={"pp": s - 1}, device_id_type=MESH)

    def mlp(sl, row0, rows, store):
        UN = 2 if NB % 2 == 0 else 1

        def up(q, carry):
            for n in [q * UN + k for k in range(UN)]:
                xin = gb[sl, pl.ds(row0, rows), :]
                g = jnp.dot(xin, wg_s[n], preferred_element_type=F32)
                u_ = jnp.dot(xin, wu_s[n], preferred_element_type=F32)
                act[0:rows, pl.ds(pl.multiple_of(n * FB, FB), FB)] = (jax.nn.silu(g) * u_).astype(BF16)
            return carry
        lax.fori_loop(0, NB // UN, up, 0)

        def down(q, carry):
            for n in [q * UN + k for k in range(UN)]:
                store(pl.ds(pl.multiple_of(n * DB, DB), DB), jnp.dot(act[0:rows, 0:FL], wd_s[n], preferred_element_type=F32))
            return carry
        lax.fori_loop(0, NB // UN, down, 0)

    def mlp_home(u):
        def store(c, val):
            pacc[:, c] = val
        with jax.named_scope('mlp'):
            mlp(lax.rem(u, 3), 0, 2 * T, store)

    def mlp_outer(u, b):
        def store(c, val):
            px[lax.rem(u, 2), pl.ds(pl.multiple_of(b * T, T), T), c] = val.astype(BF16)
        with jax.named_scope('mlp_o'):
            mlp(lax.rem(u, 3), pl.multiple_of(b * T, T), T, store)

    def forward(u):
        @pl.when((u >= 1) & (u <= N))
        def _():
            s2_copy(u - 1).wait_send()

        @pl.when(u < N)
        def _():
            with jax.named_scope('w_ag'):
                ag_wait(1 - hb, u)
            s2_copy(u).start()

    def combine(v):
        sl = lax.rem(v, 2)
        with jax.named_scope('w_s3'):
            s3_copy(v, 0).wait_recv()
            s3_copy(v, 1).wait_recv()

        @pl.when(v >= 1)
        def _():
            s4_copy(v - 1).wait_send()

        def comb(b, carry):
            rows = pl.ds(b * RB, RB)
            mine = pl.ds(pl.multiple_of(hb * T + b * RB, RB), RB)
            theirs = pl.ds(pl.multiple_of((1 - hb) * T + b * RB, RB), RB)
            oacc[rows, :] = pacc[mine, :] + px[sl, mine, :].astype(F32)
            sendb[rows, :] = (pacc[theirs, :] + px[sl, theirs, :].astype(F32)).astype(BF16)
            return carry
        lax.fori_loop(0, T // RB, comb, 0)
        s4_copy(v).start()

    def finish(u):
        @pl.when((u >= 2) & (u < N + 2))
        def _():
            v = u - 2
            with jax.named_scope('w_s4'):
                s4_copy(v).wait_recv()
            vw = v // NJ
            vj = lax.rem(v, NJ)

            @pl.when(v >= 1)
            def _():
                hin_copy(v).wait_send()

            def fin(b, carry):
                rows = pl.ds(b * RB, RB)
                d = (oacc[rows, :] + ps[lax.rem(v, 2), rows, :].astype(F32)).astype(BF16)
                h2b[rows, :] = (h1b[lax.rem(v, 3), rows, :].astype(F32) + d.astype(F32)).astype(BF16)
                return carry
            lax.fori_loop(0, T // RB, fin, 0)

            @pl.when((s < n_stages - 1) & (v >= HS))
            def _():
                with jax.named_scope('w_cred'):
                    pl.semaphore_wait(cred, 1)

            @pl.when(s < n_stages - 1)
            def _():
                hin_copy(v).start()

            @pl.when((s == n_stages - 1) & ((v < N - 1) | (hb == 0)))
            def _():
                park_copy(v).start()

            @pl.when((s == n_stages - 1) & (v == N - 1))
            def _():
                last_copy().start()

    def body(u, carry):
        @pl.when(is_home)
        def _():
            @pl.when(u < N)
            def _():
                attention(u)

            @pl.when((u >= 1) & (u <= N))
            def _():
                s1_outer(u - 1).wait_send()
                s1_peer(u - 1).wait_send()

            @pl.when(u < N)
            def _():
                s1_peer(u).start()
                s1_outer(u).start()

            @pl.when((u >= N) & (u < N + 2))
            def _():
                combine(u - 2)

            finish(u)

            @pl.when((u >= 1) & (u <= N))
            def _():
                mlp_home(u - 1)

            forward(u)

        @pl.when(is_outer & (u < N))
        def _():
            for k in (0, 1):
                b = inner - 1 if k == 0 else 2 - inner
                with jax.named_scope('w_ag_outer'):
                    ag_wait(b, u)

                @pl.when(u >= 2)
                def _():
                    s3_copy(u - 2, b).wait_send()
                mlp_outer(u, b)
                s3_copy(u, b).start()

        return carry

    def out_fwd(mb, p, sem):
        return rcopy(out_ref.at[mb], out_ref.at[mb], ofs.at[mb, p], sem, pp=p)

    lax.fori_loop(0, N + 2, body, 0)

    last_here = (s == n_stages - 1) & (z == NJ - 1)

    @pl.when(last_here)
    def _():
        for mb in (n_mb - 1, n_mb - 2):
            local(out_ref.at[mb], out_ref.at[mb], outr.at[mb]).wait()
            if mb == n_mb - 1:
                out_fwd(mb, 1, outr.at[mb]).start()
            out_fwd(mb, 2, outf).start()

    def od_copy(v):
        return rcopy(hin_hbm.at[v], out_ref.at[2 * (v // NJ) + hb], od.at[v], outr.at[2 * (v // NJ) + hb], tp=lax.rem(v, NJ))

    @pl.when(s == 1)
    def _():
        def spread(v, carry):
            vj = lax.rem(v, NJ)
            mine = 2 * (v // NJ) + hb

            here = is_home & ((v < N - 1) | (hb == 0))

            @pl.when(here)
            def _():
                local(hin_hbm.at[v], hin_hbm.at[v], op.at[v]).wait()

            @pl.when(here & (vj != z))
            def _():
                od_copy(v).start()

            @pl.when(is_home & (vj == z))
            def _():
                c = local(hin_hbm.at[v], hin.at[0], hv_sem)
                c.start()
                c.wait()
                c = local(hin.at[0], out_ref.at[mine], hv_sem)
                c.start()
                c.wait()

            @pl.when(vj == z)
            def _():
                for b in (0, 1):
                    mb = 2 * (v // NJ) + b

                    @pl.when(z - 1 != b)
                    def _(mb=mb):
                        local(out_ref.at[mb], out_ref.at[mb], outr.at[mb]).wait()
                    out_fwd(mb, 0, outf).start()

                    @pl.when(v < N - 1)
                    def _(mb=mb):
                        out_fwd(mb, 3, outf).start()
                        out_fwd(mb, 2, outf).start()
            return carry
        lax.fori_loop(0, N, spread, 0)

    @pl.when(is_home)
    def _():
        s4_copy(N - 1).wait_send()

        @pl.when((s < n_stages - 1) | (hb == 0))
        def _():
            hin_copy(N - 1).wait_send()

        @pl.when(s == n_stages - 1)
        def _():
            last_copy().wait_send()

    @pl.when(is_outer)
    def _():
        for b in (0, 1):
            s3_copy(N - 2, b).wait_send()
            s3_copy(N - 1, b).wait_send()

    @pl.when(s == 1)
    def _():
        for m in PM:
            y_send(0, m).wait_send()

        @pl.when(is_outer)
        def _():
            for m in PM:
                y_send(1, m).wait_send()

    @pl.when((s == 3) & is_home)
    def _():
        for m in PM:
            pp_send(m).wait_send()
            pf_send(m).wait_send()
            pxf_send(1, m).wait_send()
            for r, i in ((0, 0), (0, 1), (1, 0), (1, 1), (2, 0)):
                push(r, m, i).wait_send()

    @pl.when(is_home)
    def _():
        def sent(m):
            p_send(m).wait_send()
            f_send(m).wait_send()
            x_send(1, m).wait_send()
        for m in range(4):
            direct(m, functools.partial(sent, m))
            x_send(2, m).wait_send()

        @pl.when(s == 2)
        def _():
            for w in range(NW):
                for j in range(NJ):
                    @pl.when(z != j)
                    def _():
                        x_pass(w, j).wait_send()

        @pl.when(s == 1)
        def _():
            def spread_done(v, carry):
                @pl.when((lax.rem(v, NJ) != z) & ((v < N - 1) | (hb == 0)))
                def _():
                    od_copy(v).wait_send()
                return carry
            lax.fori_loop(0, N, spread_done, 0)

    for w in range(NW):
        x_each(w, lambda c: c.wait_send())

    @pl.when(s == 1)
    def _():
        for mb in range(n_mb):
            out_fwd(mb, 0, outf).wait_send()
            if mb < n_mb - 2:
                out_fwd(mb, 3, outf).wait_send()
                out_fwd(mb, 2, outf).wait_send()
            else:
                @pl.when(z < NJ - 1)
                def _(mb=mb):
                    out_fwd(mb, 3, outf).wait_send()
                    out_fwd(mb, 2, outf).wait_send()

    @pl.when(last_here)
    def _():
        for mb in (n_mb - 2, n_mb - 1):
            out_fwd(mb, 2, outf).wait_send()
        out_fwd(n_mb - 1, 1, outf).wait_send()
        early = out_ref.at[pl.ds(0, n_mb - 2)]
        local(early, early, outf).wait()

    @pl.when((s == n_stages - 1) & (z < NJ - 1))
    def _():
        local(out_ref, out_ref, outf).wait()

    @pl.when((s == 0) | (s == 2))
    def _():
        local(out_ref, out_ref, outf).wait()


def solution(mesh):
    n_stages = mesh.shape['pp']

    def stage_program(hidden_in, seg_ids, positions, attn_norm, w_query, w_key, w_value, w_out, mlp_norm, w_gate, w_up, w_down):
        n_mb, T, D = hidden_in.shape
        S = seg_ids.shape[1]
        QL = w_query.shape[2]
        FL = w_gate.shape[2]
        NJ = S // T
        N = (n_mb // 2) * NJ
        NB = max(1, FL // 512)
        invf = jnp.asarray(np.tile(rope_freqs(), 2)[None, :], F32)
        any_spec = pl.BlockSpec(memory_space=pl.ANY)
        vmem = pl.BlockSpec(memory_space=pltpu.VMEM)
        dma = pltpu.SemaphoreType.DMA
        scratch = [
            pltpu.VMEM((NB, D, FL // NB), BF16), pltpu.VMEM((NB, D, FL // NB), BF16), pltpu.VMEM((NB, FL, D // NB), BF16),
            pltpu.VMEM((3, D, QL), BF16), pltpu.VMEM((2, 3, D, QL), BF16),
            pltpu.VMEM((3, 2 * T, D), BF16),
            pltpu.VMEM((2, 2 * T, D), BF16),
            pltpu.VMEM((2, T, D), BF16),
            pltpu.VMEM((4, S, QL), BF16), pltpu.VMEM((4, S, QL), BF16),
            pltpu.VMEM((3, T, D), BF16),
            pltpu.VMEM((3, T, D), BF16),
            pltpu.VMEM((2 * T, D), F32),
            pltpu.VMEM((T, D), F32),
            pltpu.VMEM((T, D), BF16),
            pltpu.VMEM((T, D), BF16),
            pltpu.VMEM((2 * T, max(D, FL, 4 * QL)), BF16),
            pltpu.VMEM((2, T, QL), BF16),
            pltpu.VMEM((n_mb // 2, S, HEAD_DIM), F32),
            pltpu.VMEM((T, S), F32), pltpu.VMEM((QL // HEAD_DIM, T, S), F32), pltpu.VMEM((QL // HEAD_DIM, T, S), BF16),
            dma((3, 8)), dma((2, 4)), dma((8,)), dma((4,)), dma((2, 4)),
            dma((N,)), dma((n_mb // 2, 2)), dma((2, 3)), dma((2,)), dma, dma((2, 2)), dma((2, 2)), dma((2,)), dma, dma,
            dma((n_mb,)), dma, dma((n_mb, n_stages)),
            dma((3,)), dma((2, 3)), dma, dma((3, NB)), dma, dma, dma((N,)), dma((n_mb // 2, NJ)), dma((N,)), dma((N,)),
            dma((4,)), dma((4,)), dma((4,)), dma((4,)), dma((2,)), dma((2,)), dma((2,)), dma((2,)), dma((2, 2)), dma((2, 2)), dma((3, 2, 2)),
            pltpu.SemaphoreType.REGULAR, pltpu.SemaphoreType.REGULAR,
        ]
        return pl.pallas_call(
            functools.partial(kernel, n_stages),
            out_shape=[jax.ShapeDtypeStruct(hidden_in.shape, BF16), jax.ShapeDtypeStruct((3, 3, D, QL), BF16),
                       jax.ShapeDtypeStruct((4 * QL, D), BF16), jax.ShapeDtypeStruct((N, T, D), BF16),
                       jax.ShapeDtypeStruct((4, D, QL), BF16), jax.ShapeDtypeStruct((4 * QL, D), BF16)],
            in_specs=[any_spec, vmem, vmem, vmem, vmem, vmem] + [any_spec] * 7,
            out_specs=[any_spec] * 6,
            scratch_shapes=scratch,
            compiler_params=pltpu.CompilerParams(collective_id=0, has_side_effects=True, vmem_limit_bytes=67_043_328),
        )(hidden_in, seg_ids, positions, invf, attn_norm, mlp_norm, w_query, w_key, w_value, w_out, w_gate, w_up, w_down)[0]

    act_spec = P('dp', 'tp', None)
    row_spec = P('dp', None)
    gain_spec = P('pp', None)
    col_spec = P('pp', None, 'tp')
    rows_spec = P('pp', 'tp', None)
    return jax.shard_map(stage_program, mesh=mesh,
                         in_specs=(act_spec, row_spec, row_spec, gain_spec, col_spec, col_spec, col_spec, rows_spec, gain_spec, col_spec, col_spec, rows_spec),
                         out_specs=act_spec, check_vma=False)
```
